32 devices in a mesh: shard: 4 (over z), replica: 8 (over y, x, core).
Axes of the slice: x: 2, y: 2, z: 4, core: 2. Of those that a mesh axis runs over, the one named last changes fastest.
Arguments:
- block_in: bfloat16 [4096, 2048], P(('shard', 'replica')), may hold values from -6 to 6
- positions: int32 [4096], P(('shard', 'replica')), may hold values from 0 to 127, as said below
- out_grad: bfloat16 [4096, 2048], P(('shard', 'replica')), may hold values from -6 to 6
- w_qkv: bfloat16 [2048, 6144], P('shard'), may hold values from -0.125 to 0.125
- b_qkv: bfloat16 [6144], P('shard'), may hold values from -4.75 to 4.75
- w_out: bfloat16 [2048, 2048], P('shard'), may hold values from -0.25 to 0.25
- b_out: bfloat16 [2048], P('shard'), may hold values from -3 to 3
- w_up: bfloat16 [2048, 8192], P('shard'), may hold values from -0.125 to 0.125
- b_up: bfloat16 [8192], P('shard'), may hold values from -3 to 3
- w_down: bfloat16 [8192, 2048], P('shard'), may hold values from -0.0625 to 0.0625
- b_down: bfloat16 [2048], P('shard'), may hold values from -3 to 3
- first_gain: bfloat16 [2048], P('shard'), may hold values from 0.5 to 1.5
- first_shift: bfloat16 [2048], P('shard'), may hold values from -3 to 3
- second_gain: bfloat16 [2048], P('shard'), may hold values from 0.5 to 1.5
- second_shift: bfloat16 [2048], P('shard'), may hold values from -3 to 3
Outputs:
- block_out: bfloat16 [4096, 2048], P(('shard', 'replica'))
- in_grad: bfloat16 [4096, 2048], P(('shard', 'replica'))
- grad_w_qkv: float32 [2048, 6144], P('shard')
- grad_b_qkv: float32 [6144], P('shard')
- grad_w_out: float32 [2048, 2048], P('shard')
- grad_b_out: float32 [2048], P('shard')
- grad_w_up: float32 [2048, 8192], P('shard')
- grad_b_up: float32 [8192], P('shard')
- grad_w_down: float32 [8192, 2048], P('shard')
- grad_b_down: float32 [2048], P('shard')
- grad_first_gain: float32 [2048], P('shard')
- grad_first_shift: float32 [2048], P('shard')
- grad_second_gain: float32 [2048], P('shard')
- grad_second_shift: float32 [2048], P('shard')
The draws below stay inside these ranges and needn't reach their ends.
Inputs may be any that keep to these rules, and one draw needn't show every extreme that they name: `positions`: each device's 128 tokens hold whole sequences: a position is 0 at a sequence's start and at each device's first token and otherwise one more than the position before; some device holds one sequence of 128 tokens.
All inputs are finite; a program needn't handle non-finite values.
Results may differ from the reference program's by a relative error of at most 0.006.
The reference program's roundings to bfloat16 on the way count: a program that leaves them out, or rounds other values in their place, can miss the bound.
Values may be sent and summed in bfloat16 or wider, within the bound.
A program may use at most 384 MiB of HBM per device.

```python
import math
import jax
import jax.numpy as jnp
from jax import lax

D = 2048
FF = 8192
H = 8
HD = 256
ROT = 64
TOK_DEV = 128
TOKENS = 4096


def draw_positions(key, part):
    devices_all = TOKENS // TOK_DEV
    first_key, second_key, third_key = jax.random.split(jax.random.fold_in(key, 17), 3)
    levels = jax.random.randint(first_key, (devices_all, 1), 1, 8)
    raw_bits = jax.random.randint(second_key, (devices_all, TOK_DEV), 0, 1 << 30)
    cutting = jnp.right_shift(raw_bits, 30 - levels) == 0
    whole_one = jax.random.randint(third_key, (), 0, devices_all)
    device_rows = jnp.arange(devices_all, dtype=jnp.int32)[:, None]
    index = jnp.arange(TOK_DEV, dtype=jnp.int32)[None, :]
    cutting = cutting & (device_rows != whole_one) | (index == 0)
    starts = lax.cummax(jnp.where(cutting, index, 0), axis=1)
    return (index - starts).reshape(-1).astype(jnp.int32)


def draw_b_qkv(key, part):
    level_key, noise_key, sign_key, pick_key = jax.random.split(jax.random.fold_in(key, 29), 4)
    head_index = jnp.arange(H, dtype=jnp.int32)
    strong_head = jax.random.randint(pick_key, (), 0, H)
    noise = jnp.clip(0.5 * jax.random.normal(noise_key, (3 * D,), jnp.float32), -3.0, 3.0)
    levels = jax.random.uniform(level_key, (H,), jnp.float32, 0.0, 1.5)
    levels = jnp.where(head_index == strong_head, jnp.float32(4.75), levels)
    signs = jnp.where(jax.random.bernoulli(sign_key, 0.5, (H, HD)), jnp.float32(1.0), jnp.float32(-1.0))
    beyond = jnp.broadcast_to((jnp.arange(HD, dtype=jnp.int32) >= ROT)[None, :], (H, HD)).reshape(D)
    aligned = (levels[:, None] * signs).reshape(D)
    query_part = jnp.where(beyond, aligned, noise[:D])
    key_part = jnp.where(beyond, aligned, noise[D:2 * D])
    return jnp.concatenate([query_part, key_part, noise[2 * D:]]).astype(jnp.float32).astype(jnp.bfloat16)


def steps_of(stream_key, dims, cuts, least, high):
    def one(position, blocks):
        draws = jax.random.uniform(jax.random.fold_in(jax.random.fold_in(stream_key, 6), position), (blocks,), jnp.float32, least / len(cuts), high / len(cuts))
        return jnp.repeat(jnp.exp(draws), dims[position] // blocks).reshape((-1,) + (1,) * (len(dims) - position - 1))

    loudness = one(*cuts[0])
    for cut in cuts[1:]:
        loudness = loudness * one(*cut)
    return loudness


def centred(key, dims, scale, reach, cuts=(), held_as=jnp.bfloat16):
    loudness = steps_of(key, dims, cuts, -0.22, 0.18) if cuts else 1.0
    drawn = jax.random.normal(key, dims, jnp.float32) * scale * loudness
    return jnp.minimum(jnp.maximum(drawn, -reach), reach).astype(held_as)


def setup_inputs(seed: int = 0) -> dict:
    splits = jax.random.split(jax.random.key(seed), 16)
    block_in = centred(splits[0], (TOKENS, D), 1.0, 6.0, ((0, 32),))
    positions = draw_positions(jax.random.fold_in(splits[15], 71), 0)
    out_grad = centred(splits[2], (TOKENS, D), 1.0, 6.0, ((0, 32),))
    w_qkv = centred(splits[3], (D, 3 * D), D ** -0.5, 0.125, ((0, 4),))
    b_qkv = draw_b_qkv(jax.random.fold_in(splits[15], 71), 0)
    w_out = centred(splits[5], (D, D), (D // 4) ** -0.5, 0.25, ((0, 4),))
    b_out = centred(splits[6], (D,), 0.5, 3.0, ((0, 4),))
    w_up = centred(splits[7], (D, FF), D ** -0.5, 0.125, ((0, 4),))
    b_up = centred(splits[8], (FF,), 0.5, 3.0, ((0, 4),))
    w_down = centred(splits[9], (FF, D), FF ** -0.5, 0.0625, ((0, 4),))
    b_down = centred(splits[10], (D,), 0.5, 3.0, ((0, 4),))
    first_gain = jnp.clip(1.0 + 0.1 * jax.random.normal(splits[11], (D,), jnp.float32), 0.5, 1.5).astype(jnp.bfloat16)
    first_shift = centred(splits[12], (D,), 0.5, 3.0, ((0, 4),))
    second_gain = jnp.clip(1.0 + 0.1 * jax.random.normal(splits[13], (D,), jnp.float32), 0.5, 1.5).astype(jnp.bfloat16)
    second_shift = centred(splits[14], (D,), 0.5, 3.0, ((0, 4),))
    return dict(block_in=block_in, positions=positions, out_grad=out_grad, w_qkv=w_qkv, b_qkv=b_qkv, w_out=w_out, b_out=b_out, w_up=w_up, b_up=b_up, w_down=w_down, b_down=b_down, first_gain=first_gain, first_shift=first_shift, second_gain=second_gain, second_shift=second_shift)


epsilon = 1e-05

def norm_forward(values, gain, shift):
    centre = lax.optimization_barrier(jnp.mean(values, axis=-1, keepdims=True))
    offsets = values - centre
    spread = lax.optimization_barrier(jnp.mean(offsets * offsets, axis=-1, keepdims=True))
    inverse = lax.rsqrt(spread + epsilon)
    normed = offsets * inverse
    return (normed * gain.astype(jnp.float32) + shift.astype(jnp.float32), normed, inverse)

def norm_backward(upstream, normed, inverse, gain):
    scaled = upstream * gain.astype(jnp.float32)
    inward = inverse * (scaled - lax.optimization_barrier(jnp.mean(scaled, axis=-1, keepdims=True)) - normed * lax.optimization_barrier(jnp.mean(scaled * normed, axis=-1, keepdims=True)))
    return (inward, lax.optimization_barrier(jnp.sum(upstream * normed, axis=0)), lax.optimization_barrier(jnp.sum(upstream, axis=0)))

def rotary_tables(positions):
    half_rot = ROT // 2
    freqs = 10000.0 ** (-(jnp.arange(half_rot, dtype=jnp.float32) * (2.0 / ROT)))
    angles = positions.astype(jnp.float32)[:, None] * freqs[None, :]
    return (jnp.cos(angles)[:, None, :], jnp.sin(angles)[:, None, :])

def rotate(values, cosine, sine):
    half_rot = ROT // 2
    first = values[..., :half_rot]
    second = values[..., half_rot:ROT]
    return jnp.concatenate([first * cosine - second * sine, second * cosine + first * sine, values[..., ROT:]], axis=-1)

def gelu_value(values):
    return 0.5 * values * (1.0 + lax.erf(values * 0.7071067811865476))

def gelu_slope(values):
    return 0.5 * (1.0 + lax.erf(values * 0.7071067811865476)) + values * jnp.exp(-0.5 * values * values) * 0.3989422804014327

def contract_rows(left, right):
    return lax.dot_general(left, right, (((0,), (0,)), ((), ())), preferred_element_type=jnp.float32)

def times_transpose(left, right):
    return lax.dot_general(left, right, (((1,), (1,)), ((), ())), preferred_element_type=jnp.float32)

def causal_mask(positions):
    count = positions.shape[0]
    index = jnp.arange(count, dtype=jnp.int32)
    behind = index[:, None] - index[None, :]
    return (behind >= 0) & (behind <= positions[:, None])

def attend_forward(queries, keys, values, positions):
    allowed = causal_mask(positions)
    scale = HD ** (-0.5)

    def one_head(triple):
        head_query, head_key, head_value = triple
        scores = jnp.where(allowed, times_transpose(head_query, head_key) * scale, -1e+30)
        peak = lax.optimization_barrier(jnp.max(scores, axis=-1, keepdims=True))
        logsum = peak + jnp.log(lax.optimization_barrier(jnp.sum(jnp.exp(scores - peak), axis=-1, keepdims=True)))
        probs = jnp.exp(scores - logsum).astype(jnp.bfloat16)
        return (jnp.dot(probs, head_value, preferred_element_type=jnp.float32).astype(jnp.bfloat16), logsum[:, 0])
    outputs, logsums = lax.map(one_head, (queries.transpose(1, 0, 2), keys.transpose(1, 0, 2), values.transpose(1, 0, 2)))
    return (outputs.transpose(1, 0, 2).reshape(queries.shape[0], D), logsums)

def attend_backward(queries, keys, values, attended_grad, logsums, positions):
    allowed = causal_mask(positions)
    scale = HD ** (-0.5)
    upstream = attended_grad.reshape(queries.shape[0], H, HD)

    def one_head(items):
        head_query, head_key, head_value, head_up, logsum = items
        scores = jnp.where(allowed, times_transpose(head_query, head_key) * scale, -1e+30)
        probs = jnp.exp(scores - logsum[:, None])
        probs_low = probs.astype(jnp.bfloat16)
        dprobs = times_transpose(head_up, head_value)
        total = lax.optimization_barrier(jnp.sum(probs * dprobs, axis=-1, keepdims=True))
        dscores = (probs * (dprobs - total) * scale).astype(jnp.bfloat16)
        query_grad = jnp.dot(dscores, head_key, preferred_element_type=jnp.float32)
        key_grad = contract_rows(dscores, head_query)
        value_grad = contract_rows(probs_low, head_up)
        return (query_grad, key_grad, value_grad)
    query_grad, key_grad, value_grad = lax.map(one_head, (queries.transpose(1, 0, 2), keys.transpose(1, 0, 2), values.transpose(1, 0, 2), upstream.transpose(1, 0, 2), logsums))
    return (query_grad.transpose(1, 0, 2), key_grad.transpose(1, 0, 2), value_grad.transpose(1, 0, 2))

def layer_forward(block_in, positions, params, attend):
    w_qkv, b_qkv, w_out, b_out, w_up, b_up, w_down, b_down, first_gain, first_shift, second_gain, second_shift = params
    count = block_in.shape[0]
    wide_in = block_in.astype(jnp.float32)
    first_full, first_normed, first_inverse = norm_forward(wide_in, first_gain, first_shift)
    second_full, second_normed, second_inverse = norm_forward(wide_in, second_gain, second_shift)
    first_low = first_full.astype(jnp.bfloat16)
    second_low = second_full.astype(jnp.bfloat16)
    mixed = jnp.dot(first_low, w_qkv, preferred_element_type=jnp.float32) + b_qkv.astype(jnp.float32)
    cosine, sine = rotary_tables(positions)
    queries = rotate(mixed[:, :D].reshape(count, H, HD), cosine, sine).astype(jnp.bfloat16)
    keys = rotate(mixed[:, D:2 * D].reshape(count, H, HD), cosine, sine).astype(jnp.bfloat16)
    values = mixed[:, 2 * D:].reshape(count, H, HD).astype(jnp.bfloat16)
    attended, logsums = attend(queries, keys, values, positions)
    branch_attn = jnp.dot(attended, w_out, preferred_element_type=jnp.float32) + b_out.astype(jnp.float32)
    hidden_pre = jnp.dot(second_low, w_up, preferred_element_type=jnp.float32) + b_up.astype(jnp.float32)
    activated = gelu_value(hidden_pre).astype(jnp.bfloat16)
    branch_ffn = jnp.dot(activated, w_down, preferred_element_type=jnp.float32) + b_down.astype(jnp.float32)
    block_out = (wide_in + branch_attn + branch_ffn).astype(jnp.bfloat16)
    saved = (first_normed, first_inverse, second_normed, second_inverse, first_low, second_low, queries, keys, values, attended, logsums, hidden_pre, activated, cosine, sine, positions)
    return (block_out, saved)

def layer_backward(saved, out_grad, params, attend_back):
    w_qkv, b_qkv, w_out, b_out, w_up, b_up, w_down, b_down, first_gain, first_shift, second_gain, second_shift = params
    first_normed, first_inverse, second_normed, second_inverse, first_low, second_low, queries, keys, values, attended, logsums, hidden_pre, activated, cosine, sine, positions = saved
    count = out_grad.shape[0]
    upstream = out_grad.astype(jnp.float32)
    grad_b_out = lax.optimization_barrier(jnp.sum(upstream, axis=0))
    grad_b_down = lax.optimization_barrier(jnp.sum(upstream, axis=0))
    grad_w_down = contract_rows(activated, out_grad)
    grad_w_out = contract_rows(attended, out_grad)
    hidden_grad = times_transpose(out_grad, w_down) * gelu_slope(hidden_pre)
    grad_b_up = lax.optimization_barrier(jnp.sum(hidden_grad, axis=0))
    hidden_low = hidden_grad.astype(jnp.bfloat16)
    grad_w_up = contract_rows(second_low, hidden_low)
    second_grad = times_transpose(hidden_low, w_up)
    attended_grad = times_transpose(out_grad, w_out).astype(jnp.bfloat16)
    query_grad, key_grad, value_grad = attend_back(queries, keys, values, attended_grad, logsums, positions)
    query_grad = rotate(query_grad, cosine, -sine)
    key_grad = rotate(key_grad, cosine, -sine)
    mixed_grad = jnp.concatenate([query_grad.reshape(count, D), key_grad.reshape(count, D), value_grad.reshape(count, D)], axis=1)
    grad_b_qkv = lax.optimization_barrier(jnp.sum(mixed_grad, axis=0))
    mixed_low = mixed_grad.astype(jnp.bfloat16)
    grad_w_qkv = contract_rows(first_low, mixed_low)
    first_grad = times_transpose(mixed_low, w_qkv)
    first_term, grad_first_gain, grad_first_shift = norm_backward(first_grad, first_normed, first_inverse, first_gain)
    second_term, grad_second_gain, grad_second_shift = norm_backward(second_grad, second_normed, second_inverse, second_gain)
    in_grad = (upstream + first_term + second_term).astype(jnp.bfloat16)
    grads = (grad_w_qkv, grad_b_qkv, grad_w_out, grad_b_out, grad_w_up, grad_b_up, grad_w_down, grad_b_down, grad_first_gain, grad_first_shift, grad_second_gain, grad_second_shift)
    return (in_grad, grads)

def reference(block_in, positions, out_grad, w_qkv, b_qkv, w_out, b_out, w_up, b_up, w_down, b_down, first_gain, first_shift, second_gain, second_shift):
    params = (w_qkv, b_qkv, w_out, b_out, w_up, b_up, w_down, b_down, first_gain, first_shift, second_gain, second_shift)
    block_rows = math.gcd(TOKENS, 4096)
    block_count = TOKENS // block_rows

    def step(totals, item):
        piece_in, piece_pos, piece_grad = item
        output, saved = layer_forward(piece_in, piece_pos, params, attend_forward)
        piece_back, grads = layer_backward(saved, piece_grad, params, attend_backward)
        return (tuple((total + grad for total, grad in zip(totals, grads))), (output, piece_back))
    initial = tuple((jnp.zeros(param.shape, jnp.float32) for param in params))
    totals, (outputs, backs) = lax.scan(step, initial, (block_in.reshape(block_count, block_rows, D), positions.reshape(block_count, block_rows), out_grad.reshape(block_count, block_rows, D)))
    return (outputs.reshape(TOKENS, D), backs.reshape(TOKENS, D), totals[0], totals[1], totals[2], totals[3], totals[4], totals[5], totals[6], totals[7], totals[8], totals[9], totals[10], totals[11])
```

```python
import jax
import jax.numpy as jnp
from jax import lax
from jax.experimental import pallas as pl
from jax.sharding import PartitionSpec as P

H = 8
HD = 256
ROT = 64

epsilon = 1e-05


F32 = jnp.float32
BF16 = jnp.bfloat16


def rotary_tables(positions):
    half_rot = ROT // 2
    freqs = 10000.0 ** (-(jnp.arange(half_rot, dtype=F32) * (2.0 / ROT)))
    angles = positions[:, None] * freqs[None, :]
    return jnp.cos(angles), jnp.sin(angles)


def rotate(values, cosine, sine):
    half_rot = ROT // 2
    first = values[..., :half_rot]
    second = values[..., half_rot:ROT]
    return jnp.concatenate(
        [first * cosine - second * sine, second * cosine + first * sine, values[..., ROT:]], axis=-1
    )


def gelu_value(values):
    return 0.5 * values * (1.0 + lax.erf(values * 0.7071067811865476))


def gelu_slope(values):
    return (
        0.5 * (1.0 + lax.erf(values * 0.7071067811865476))
        + values * jnp.exp(-0.5 * values * values) * 0.3989422804014327
    )


def dot(left, right, left_dim, right_dim):
    return lax.dot_general(
        left, right, (((left_dim,), (right_dim,)), ((), ())), preferred_element_type=F32
    )


def unwritten(shape, dtype):
    return pl.pallas_call(
        lambda out_ref: None,
        out_shape=jax.ShapeDtypeStruct(shape, dtype),
        out_specs=pl.BlockSpec(memory_space=pl.ANY),
    )()


def bits_of(mask):
    return [1 << i for i in range(mask.bit_length()) if mask >> i & 1]


def solution(mesh):
    S = mesh.shape["shard"]
    R = mesh.shape["replica"]
    TP = [1] if R > 1 and H % (2 * S) == 0 else []
    DP = [bit for bit in bits_of(R - 1) if bit not in TP]
    NT, ND = 2 ** len(TP), 2 ** len(DP)
    ring = list(range(S))[:1] + list(range(1, S, 2)) + list(range(2, S, 2))[::-1]
    place = [ring.index(i) for i in range(S)]

    def to_ring(value, hops):
        return lax.ppermute(value, "shard", [(ring[i], ring[(i + hops) % S]) for i in range(S)])

    def flip(value, bit):
        return lax.ppermute(value, "replica", [(i, i ^ bit) for i in range(R)])

    def body(
        block_in, positions, out_grad, w_qkv, b_qkv, w_out, b_out, w_up, b_up, w_down, b_down,
        first_gain, first_shift, second_gain, second_shift,
    ):
        T, D = block_in.shape
        rows = w_qkv.shape[0]
        FS = w_down.shape[0]
        FD = FS // NT
        HN = H // S // NT
        AD = HN * HD
        G = NT * S
        s = lax.axis_index("shard")
        r = lax.axis_index("replica")
        mine = {bit: (r // bit) % 2 for bit in bits_of(R - 1)}
        t = sum((mine[bit] * 2**i for i, bit in enumerate(TP)), jnp.int32(0))
        p = jnp.array(place, jnp.int32)[s]
        ring_array = jnp.array(ring, jnp.int32)
        behind = [ring_array[(p - k) % S] for k in range(S)]
        ahead = [ring_array[(p + k) % S] for k in range(S)]

        small = jnp.concatenate(
            [b_qkv, b_out, b_down, first_gain, first_shift, second_gain, second_shift,
             positions.astype(BF16)]
        )
        small_rel = [small] + [to_ring(small, k) for k in range(1, S)]
        doubled = jnp.concatenate([jnp.stack(small_rel)] * 2, axis=0)
        order = (p - jnp.array(place, jnp.int32)) % S
        natural = jnp.stack(
            [lax.dynamic_index_in_dim(doubled, order[j], 0, keepdims=False) for j in range(S)]
        )
        sizes = [b_qkv.shape[0]] + [rows] * 6
        starts = [sum(sizes[:i]) for i in range(len(sizes))]
        whole = [natural[:, a : a + n].reshape(-1).astype(F32) for a, n in zip(starts, sizes)]
        full_b_qkv, full_b_out, full_b_down, gain_1, shift_1, gain_2, shift_2 = whole
        pos_own = jnp.concatenate([v[sum(sizes) :] for v in small_rel])
        pos_all = pos_own
        for bit in TP:
            pos_all = jnp.concatenate([pos_all, flip(pos_all, bit)])
        pos_all = pos_all.astype(F32)

        def gather_tokens(value):
            blocks = [value]
            for _ in range(1, S):
                blocks.append(to_ring(blocks[-1], 1))
            for bit in TP:
                blocks = blocks + [flip(b, bit) for b in blocks]
            return jnp.concatenate(blocks, axis=0)

        part = rows // ND
        d = sum((mine[bit] * 2**i for i, bit in enumerate(DP)), jnp.int32(0))

        def up_cols(w, shard):
            return lax.dynamic_slice_in_dim(w, shard * FS + t * FD, FD, 1)

        def qkv_cols(w, shard):
            w = w.reshape(w.shape[0], 3, w.shape[1] // 3)
            w = lax.dynamic_slice_in_dim(w, (shard * NT + t) * AD, AD, 2)
            return w.reshape(w.shape[0], 3 * AD)

        def spread(w, take, order):
            w_part = lax.dynamic_slice_in_dim(w, d * part, part, 0)
            got = [to_ring(take(w_part, ahead[k]), k) for k in range(1, S)]
            pieces = {0: jnp.stack(got)}
            for bit in order:
                pieces.update({m | bit: flip(v, bit) for m, v in list(pieces.items())})
            own = take(w, s)
            full = unwritten((S, ND, part, own.shape[1]), BF16)
            full = lax.dynamic_update_slice(
                full, own.reshape(1, ND, part, -1), (s, 0, 0, 0)
            )
            for m, piece in pieces.items():
                mask = sum(2**i for i, bit in enumerate(DP) if m & bit)
                for k in range(1, S):
                    full = lax.dynamic_update_slice(
                        full, piece[k - 1][None, None], (behind[k], d ^ mask, 0, 0)
                    )
            return full.reshape(S * rows, -1)

        grad_all = gather_tokens(out_grad)
        x_all = gather_tokens(block_in)
        up = spread(w_up, up_cols, DP)
        qkv = spread(w_qkv, qkv_cols, DP[::-1])
        down = lax.dynamic_slice_in_dim(w_down, t * FD, FD, 0)
        out = lax.dynamic_slice_in_dim(w_out, t * AD, AD, 0)
        bias_up = lax.dynamic_slice_in_dim(b_up, t * FD, FD, 0).astype(F32)
        bias_qkv = lax.dynamic_slice_in_dim(
            full_b_qkv.reshape(3, -1), (s * NT + t) * AD, AD, 1
        ).reshape(-1)

        hidden_up = dot(grad_all, down, 1, 1)
        attended_grad = dot(grad_all, out, 1, 1).astype(BF16)

        def normed_of(block):
            wide = block.astype(F32)
            offsets = wide - jnp.mean(wide, axis=-1, keepdims=True)
            inverse = lax.rsqrt(jnp.mean(offsets * offsets, axis=-1, keepdims=True) + epsilon)
            return offsets * inverse, inverse

        normed, _ = normed_of(x_all)
        first_low = (normed * gain_1 + shift_1).astype(BF16)
        second_low = (normed * gain_2 + shift_2).astype(BF16)

        hidden_pre = dot(second_low, up, 1, 0) + bias_up
        activated = gelu_value(hidden_pre).astype(BF16)
        hidden_grad = hidden_up * gelu_slope(hidden_pre)
        sum_b_up = jnp.sum(hidden_grad, axis=0)
        hidden_low = hidden_grad.astype(BF16)

        mixed = dot(first_low, qkv, 1, 0) + bias_qkv
        cosine, sine = rotary_tables(pos_all)
        cosine, sine = [v.reshape(G, T, 1, -1) for v in (cosine, sine)]

        def heads(v):
            return v.reshape(G, T, HN, HD)

        queries = rotate(heads(mixed[:, :AD]), cosine, sine).astype(BF16)
        keys = rotate(heads(mixed[:, AD : 2 * AD]), cosine, sine).astype(BF16)
        values = heads(mixed[:, 2 * AD :]).astype(BF16)
        index = jnp.arange(T, dtype=jnp.int32)
        away = index[:, None] - index[None, :]
        allowed = (away >= 0) & (
            away <= pos_all.astype(jnp.int32).reshape(G, T)[:, :, None]
        )
        allowed = allowed[:, None]
        scale = HD ** (-0.5)
        scores = jnp.einsum("gqhd,gkhd->ghqk", queries, keys, preferred_element_type=F32) * scale
        scores = jnp.where(allowed, scores, -1e30)
        peak = jnp.max(scores, axis=-1, keepdims=True)
        logsum = peak + jnp.log(jnp.sum(jnp.exp(scores - peak), axis=-1, keepdims=True))
        probs = jnp.exp(scores - logsum)
        probs_low = probs.astype(BF16)
        attended = jnp.einsum("ghqk,gkhd->gqhd", probs_low, values, preferred_element_type=F32)
        attended = attended.astype(BF16).reshape(G * T, AD)

        def sum_group(own, others):
            for i, bit in reversed(list(enumerate(TP))):
                pass
            return own, others

        lower = jnp.concatenate([attended, activated], axis=1)
        lower_w = jnp.concatenate([out, down], axis=0)

        def reduce_tokens(parts):
            held = {i: parts(i) for i in range(NT)}
            for i in reversed(range(len(TP))):
                for j in range(2**i):
                    held[j] = held[j] + flip(held[j + 2**i].astype(BF16), TP[i]).astype(F32)
            total = held[0].reshape(S, T, -1)
            got = [to_ring(total[k].astype(BF16), -k) for k in range(1, S)]
            return sum((g.astype(F32) for g in got), total[0])

        branch = reduce_tokens(
            lambda i: dot(lower[i * S * T : (i + 1) * S * T], lower_w, 1, 0)
        )
        block_out = (block_in.astype(F32) + branch + full_b_out + full_b_down).astype(BF16)

        upstream = attended_grad.reshape(G, T, HN, HD)
        dprobs = jnp.einsum("gqhd,gkhd->ghqk", upstream, values, preferred_element_type=F32)
        total = jnp.sum(probs * dprobs, axis=-1, keepdims=True)
        dscores = (probs * (dprobs - total) * scale).astype(BF16)
        query_grad = jnp.einsum("ghqk,gkhd->gqhd", dscores, keys, preferred_element_type=F32)
        key_grad = jnp.einsum("ghqk,gqhd->gkhd", dscores, queries, preferred_element_type=F32)
        value_grad = jnp.einsum("ghqk,gqhd->gkhd", probs_low, upstream, preferred_element_type=F32)
        query_grad = rotate(query_grad, cosine, -sine)
        key_grad = rotate(key_grad, cosine, -sine)
        mixed_grad = jnp.concatenate(
            [v.reshape(G * T, AD) for v in (query_grad, key_grad, value_grad)], axis=1
        )
        sum_b_qkv = jnp.sum(mixed_grad, axis=0)
        mixed_low = mixed_grad.astype(BF16)

        def split_sum(grad, lead):
            n, width = grad.shape[2:]
            halves = []
            for half, order in enumerate((DP, DP[::-1])):
                value = grad[:, :, half * n // 2 : (half + 1) * n // 2]
                value = value.reshape((lead,) + (2,) * len(DP) + (n // 2, width))
                axes = list(DP[::-1])
                for bit in order:
                    axis = 1 + axes.index(bit)
                    axes.remove(bit)
                    sent = lax.dynamic_index_in_dim(value, 1 - mine[bit], axis, keepdims=False)
                    kept = lax.dynamic_index_in_dim(value, mine[bit], axis, keepdims=False)
                    value = kept + flip(sent.astype(BF16), bit).astype(F32)
                halves.append(value)
            return halves

        def across(value):
            got = [lax.dynamic_index_in_dim(value, s, 0, keepdims=True)]
            got += [
                to_ring(lax.dynamic_index_in_dim(value, ahead[k], 0, keepdims=True), k)
                for k in range(1, S)
            ]
            full = jnp.concatenate(got, axis=0)
            return jnp.stack(
                [lax.dynamic_index_in_dim(full, order[j], 0, keepdims=False) for j in range(S)]
            )

        def share(halves, write, result):
            for half, (value, order) in enumerate(zip(halves, (DP, DP[::-1]))):
                value = lax.optimization_barrier(value)
                pieces = {0: value}
                for bit in list(order) + TP:
                    pieces.update({m | bit: flip(v, bit) for m, v in list(pieces.items())})
                for m, piece in pieces.items():
                    dmask = sum(2**i for i, bit in enumerate(DP) if m & bit)
                    tmask = sum(2**i for i, bit in enumerate(TP) if m & bit)
                    result = write(result, piece.astype(F32), d ^ dmask, t ^ tmask, half)
            return result

        grad_down = split_sum(
            dot(activated, grad_all, 0, 0).reshape(1, ND, FD // ND, D), 1
        )
        n = FD // ND // 2
        grad_w_down = share(
            [v.reshape(n, D).astype(BF16) for v in grad_down],
            lambda res, v, dd, tt, half: lax.dynamic_update_slice(
                res, v, (tt * FD + dd * 2 * n + half * n, 0)
            ),
            unwritten(w_down.shape, F32),
        )

        grad_up = split_sum(
            dot(second_low, hidden_low, 0, 0).reshape(S, ND, part, FD), S
        )
        m = part // 2
        grad_w_up = share(
            [across(v.astype(BF16)).swapaxes(0, 1) for v in grad_up],
            lambda res, v, dd, tt, half: lax.dynamic_update_slice(
                res, v[:, :, None], (dd * part + half * m, 0, tt, 0)
            ),
            unwritten((rows, S, NT, FD), F32),
        ).reshape(w_up.shape)

        grad_out = split_sum(dot(attended, grad_all, 0, 0).reshape(1, ND, AD // ND, D), 1)
        n2 = AD // ND // 2
        grad_w_out = share(
            [v.reshape(n2, D).astype(BF16) for v in grad_out],
            lambda res, v, dd, tt, half: lax.dynamic_update_slice(
                res, v, (tt * AD + dd * 2 * n2 + half * n2, 0)
            ),
            unwritten(w_out.shape, F32),
        )

        grad_qkv = split_sum(
            dot(first_low, mixed_low, 0, 0).reshape(S, ND, part, 3 * AD), S
        )
        grad_w_qkv = share(
            [
                across(v.astype(BF16)).reshape(S, m, 3, AD).transpose(1, 2, 0, 3)
                for v in grad_qkv
            ],
            lambda res, v, dd, tt, half: lax.dynamic_update_slice(
                res, v[:, :, :, None], (dd * part + half * m, 0, 0, tt, 0)
            ),
            unwritten((rows, 3, S, NT, AD), F32),
        ).reshape(w_qkv.shape)

        first_grad = dot(mixed_low, qkv, 1, 1)
        second_grad = dot(hidden_low, up, 1, 1)
        sum_gain_1 = jnp.sum(first_grad * normed, axis=0)
        sum_shift_1 = jnp.sum(first_grad, axis=0)
        sum_gain_2 = jnp.sum(second_grad * normed, axis=0)
        sum_shift_2 = jnp.sum(second_grad, axis=0)
        inner = first_grad * gain_1 + second_grad * gain_2
        scaled = reduce_tokens(lambda i: inner[i * S * T : (i + 1) * S * T])
        normed_own, inverse_own = normed_of(block_in)
        term = inverse_own * (
            scaled
            - jnp.mean(scaled, axis=-1, keepdims=True)
            - normed_own * jnp.mean(scaled * normed_own, axis=-1, keepdims=True)
        )
        wide_grad = out_grad.astype(F32)
        in_grad = (wide_grad + term).astype(BF16)

        def placed(length, value, offset):
            return lax.dynamic_update_slice(jnp.zeros((length,), F32), value, (offset,))

        width = w_out.shape[0] * S
        col = (s * NT + t) * AD
        sums = [placed(width, sum_b_qkv[i * AD : (i + 1) * AD], col) for i in range(3)]
        sums += [jnp.sum(wide_grad, axis=0), placed(FS * S, sum_b_up, s * FS + t * FD)]
        sums += [sum_gain_1, sum_shift_1, sum_gain_2, sum_shift_2]
        lengths = [v.shape[0] for v in sums]
        sums = jnp.concatenate(sums)
        for bit in bits_of(R - 1):
            sums = sums + flip(sums, bit)
        for bit in bits_of(S - 1):
            sums = sums + lax.ppermute(sums, "shard", [(i, i ^ bit) for i in range(S)])
        at = [sum(lengths[:i]) for i in range(len(lengths))]

        def owned(start, length):
            return lax.dynamic_slice_in_dim(sums, start + s * (length // S), length // S, 0)

        grad_b_qkv = owned(at[0], 3 * width)
        grad_b_out = owned(at[3], D)
        grad_b_up = owned(at[4], FS * S)
        smalls = [owned(at[5 + i], D) for i in range(4)]
        return (
            block_out, in_grad, grad_w_qkv, grad_b_qkv, grad_w_out, grad_b_out, grad_w_up, grad_b_up,
            grad_w_down, grad_b_out, *smalls,
        )

    rows2, row1, par2, par1 = P(("shard", "replica"), None), P(("shard", "replica")), P("shard", None), P("shard")
    return jax.shard_map(
        body,
        mesh=mesh,
        in_specs=(
            rows2, row1, rows2, par2, par1, par2, par1, par2, par1, par2, par1, par1, par1, par1, par1,
        ),
        out_specs=(
            rows2, rows2, par2, par1, par2, par1, par2, par1, par2, par1, par1, par1, par1, par1,
        ),
        check_vma=False,
    )
```

```python
import jax
import jax.numpy as jnp
from jax import lax
from jax.experimental import pallas as pl
from jax.experimental.pallas import tpu as pltpu
from jax.sharding import PartitionSpec as P

H = 8
HD = 256
ROT = 64

epsilon = 1e-05


F32 = jnp.float32
BF16 = jnp.bfloat16
MESH = pl.DeviceIdType.MESH


def rotary_tables(positions):
    half_rot = ROT // 2
    freqs = 10000.0 ** (-(jnp.arange(half_rot, dtype=F32) * (2.0 / ROT)))
    angles = positions[:, None] * freqs[None, :]
    return jnp.cos(angles), jnp.sin(angles)


def rotate(values, cosine, sine):
    half_rot = ROT // 2
    first = values[..., :half_rot]
    second = values[..., half_rot:ROT]
    return jnp.concatenate(
        [first * cosine - second * sine, second * cosine + first * sine, values[..., ROT:]], axis=-1
    )


def gelu_value(values):
    return 0.5 * values * (1.0 + lax.erf(values * 0.7071067811865476))


def gelu_slope(values):
    return (
        0.5 * (1.0 + lax.erf(values * 0.7071067811865476))
        + values * jnp.exp(-0.5 * values * values) * 0.3989422804014327
    )


def dot(left, right, left_dim, right_dim):
    return lax.dot_general(
        left, right, (((left_dim,), (right_dim,)), ((), ())), preferred_element_type=F32
    )


def unwritten(shape, dtype):
    return pl.pallas_call(
        lambda out_ref: None,
        out_shape=jax.ShapeDtypeStruct(shape, dtype),
        out_specs=pl.BlockSpec(memory_space=pl.ANY),
    )()


def bits_of(mask):
    return [1 << i for i in range(mask.bit_length()) if mask >> i & 1]

def fetch(block_in, out_grad, small, w_up, w_qkv, S, R, TP, DP, FD, AD):
    T, D = block_in.shape
    rows = w_up.shape[0]
    NT, ND = 2 ** len(TP), 2 ** len(DP)
    part = rows // ND
    third = w_qkv.shape[1] // 3
    tokens = (small, out_grad, block_in)
    widths = (FD, 3 * AD)

    def kernel(
        small_ref, grad_ref, in_ref, up_ref, qkv_ref, small_all, grad_all, in_all, up_all, qkv_all,
        up_own, qkv_own, line_send, line_recv, tp_send, tp_recv, z_send, z_recv, dp_send, dp_recv, local,
    ):
        s = lax.axis_index("shard")
        r = lax.axis_index("replica")
        t = sum(((r // bit) % 2 * 2**i for i, bit in enumerate(TP)), jnp.int32(0))
        d = sum(((r // bit) % 2 * 2**i for i, bit in enumerate(DP)), jnp.int32(0))

        def partner(bit):
            return {"replica": r + bit - 2 * bit * ((r // bit) % 2)}

        copies = []
        gathered = (small_all, grad_all, in_all)
        for i, (own, every) in enumerate(zip((small_ref, grad_ref, in_ref), gathered)):
            copies.append(pltpu.make_async_copy(own, every.at[t, s], local.at[i]))
        first = [
            pltpu.make_async_copy(up_ref.at[:, pl.ds(pl.multiple_of((s * NT + t) * FD, FD), FD)], up_own, local.at[3])
        ]
        for j in range(3):
            first.append(
                pltpu.make_async_copy(
                    qkv_ref.at[:, pl.ds(pl.multiple_of(j * third + (s * NT + t) * AD, AD), AD)],
                    qkv_own.at[:, j * AD : (j + 1) * AD],
                    local.at[4 + j],
                )
            )
        for copy in copies + first:
            copy.start()

        barrier = pltpu.get_barrier_semaphore()
        for k in range(1, S):
            pl.semaphore_signal(barrier, inc=1, device_id={"shard": lax.rem(s + k, S)}, device_id_type=MESH)
        for bit in TP + DP:
            pl.semaphore_signal(barrier, inc=1, device_id=partner(bit), device_id_type=MESH)
        pl.semaphore_wait(barrier, S - 1 + len(TP) + len(DP))

        def line(i, j, way, source):
            return pltpu.make_async_remote_copy(
                src_ref=source, dst_ref=gathered[i].at[t, j], send_sem=line_send.at[i, j, way],
                recv_sem=line_recv.at[i, j], device_id={"shard": s + 2 * way - 1}, device_id_type=MESH,
            )

        def across(i, j, b, m, source):
            slot = gathered[i].at[t ^ m, j]
            return pltpu.make_async_remote_copy(
                src_ref=slot if source is None else source, dst_ref=slot, send_sem=tp_send.at[i, j, m | 1 << b],
                recv_sem=tp_recv.at[i, j, m | 1 << b], device_id=partner(TP[b]), device_id_type=MESH,
            )

        def z_copies(w, k, sending):
            to = lax.rem(s + k, S)
            at = (s if sending else lax.rem(s + S - k, S)) * rows + d * part
            at = pl.multiple_of(at, part)
            out = []
            for j in range(1 if w == 0 else 3):
                if w == 0:
                    source = up_ref.at[pl.ds(pl.multiple_of(d * part, part), part), pl.ds(pl.multiple_of((to * NT + t) * FD, FD), FD)]
                    target = up_all.at[pl.ds(at, part), :]
                else:
                    source = qkv_ref.at[
                        pl.ds(pl.multiple_of(d * part, part), part), pl.ds(pl.multiple_of(j * third + (to * NT + t) * AD, AD), AD)
                    ]
                    target = qkv_all.at[pl.ds(at, part), j * AD : (j + 1) * AD]
                out.append(
                    pltpu.make_async_remote_copy(
                        src_ref=source, dst_ref=target, send_sem=z_send.at[k, w + j], recv_sem=z_recv.at[k, w + j],
                        device_id={"shard": to}, device_id_type=MESH,
                    )
                )
            return out

        def shared(w, k, half, m, b):
            way = DP if half == 0 else DP[::-1]
            mask = sum(2 ** DP.index(way[i]) for i in range(len(DP)) if m >> i & 1)
            at = lax.rem(s + S - k, S) * rows + (d ^ mask) * part + half * (part // 2)
            slot = (up_all, qkv_all)[w].at[pl.ds(pl.multiple_of(at, part // 2), part // 2), :]
            return pltpu.make_async_remote_copy(
                src_ref=slot, dst_ref=slot, send_sem=dp_send.at[w, k, half, m | 1 << b], recv_sem=dp_recv.at[w, k, half, m | 1 << b],
                device_id=partner(way[b]), device_id_type=MESH,
            )

        mine = (small_ref, grad_ref, in_ref)
        for i in range(3):
            @pl.when(s + 1 < S)
            def _():
                line(i, s, 1, mine[i]).start()

            @pl.when(s > 0)
            def _():
                line(i, s, 0, mine[i]).start()

            for b in range(len(TP)):
                across(i, s, b, 0, mine[i]).start()
        for k in range(1, S):
            for w in range(2):
                for copy in z_copies(w, k, True):
                    copy.start()

        def pass_on(i, j, m, top):
            for b in range(top + 1, len(TP)):
                across(i, j, b, m, None).start()

        def share_from(w, k, half, m, top):
            for b in range(top + 1, len(DP)):
                shared(w, k, half, m, b).start()

        for copy in first:
            copy.wait()
        at_own = pl.multiple_of(s * rows, rows)
        second = [
            pltpu.make_async_copy(up_own, up_all.at[pl.ds(at_own, rows), :], local.at[3]),
            pltpu.make_async_copy(qkv_own, qkv_all.at[pl.ds(at_own, rows), :], local.at[4]),
        ]
        for copy in second:
            copy.start()

        for k in range(1, S):
            for i in range(3):
                @pl.when(s - k >= 0)
                def _():
                    line(i, s - k, 1, gathered[i].at[t, s - k]).wait_recv()

                    @pl.when(s + 1 < S)
                    def _():
                        line(i, s - k, 1, gathered[i].at[t, s - k]).start()

                    pass_on(i, s - k, 0, -1)

                @pl.when(s + k < S)
                def _():
                    line(i, s + k, 0, gathered[i].at[t, s + k]).wait_recv()

                    @pl.when(s > 0)
                    def _():
                        line(i, s + k, 0, gathered[i].at[t, s + k]).start()

                    pass_on(i, s + k, 0, -1)

            for w in range(2):
                for copy in z_copies(w, k, False):
                    copy.wait_recv()
                for half in range(2):
                    share_from(w, k, half, 0, -1)

        for m in range(1, ND):
            top = m.bit_length() - 1
            for k in range(1, S):
                for w in range(2):
                    for half in range(2):
                        came = m ^ (1 << top)
                        shared(w, k, half, came, top).wait_recv()
                        share_from(w, k, half, m, top)
        for m in range(1, NT):
            top = m.bit_length() - 1
            for i in range(3):
                for j in range(S):
                    across(i, j, top, m ^ (1 << top), None).wait_recv()
                    pass_on(i, j, m, top)

        for i in range(3):
            for j in range(S):
                @pl.when((s + 1 < S) & (j <= s))
                def _():
                    line(i, j, 1, gathered[i].at[t, j]).wait_send()

                @pl.when((s > 0) & (j >= s))
                def _():
                    line(i, j, 0, gathered[i].at[t, j]).wait_send()

                for m in range(NT):
                    for b in range(m.bit_length(), len(TP)):
                        across(i, j, b, m, None).wait_send()
        for k in range(1, S):
            for w in range(2):
                for copy in z_copies(w, k, True):
                    copy.wait_send()
                for half in range(2):
                    for m in range(ND):
                        for b in range(m.bit_length(), len(DP)):
                            shared(w, k, half, m, b).wait_send()
        for copy in copies + second:
            copy.wait()

    any_spec = pl.BlockSpec(memory_space=pl.ANY)
    shapes = [jax.ShapeDtypeStruct((NT, S) + v.shape, BF16) for v in tokens]
    shapes += [jax.ShapeDtypeStruct((S * rows, width), BF16) for width in widths]
    small_all, grad_all, in_all, up, qkv = pl.pallas_call(
        kernel,
        out_shape=shapes,
        in_specs=[any_spec] * 5,
        out_specs=[any_spec] * 5,
        scratch_shapes=[
            pltpu.VMEM((rows, FD), BF16),
            pltpu.VMEM((rows, 3 * AD), BF16),
            pltpu.SemaphoreType.DMA((3, S, 2)),
            pltpu.SemaphoreType.DMA((3, S)),
            pltpu.SemaphoreType.DMA((3, S, NT)),
            pltpu.SemaphoreType.DMA((3, S, NT)),
            pltpu.SemaphoreType.DMA((S, 4)),
            pltpu.SemaphoreType.DMA((S, 4)),
            pltpu.SemaphoreType.DMA((2, S, 2, ND)),
            pltpu.SemaphoreType.DMA((2, S, 2, ND)),
            pltpu.SemaphoreType.DMA((7,)),
        ],
        compiler_params=pltpu.CompilerParams(collective_id=0, has_side_effects=True),
        name="fetch",
    )(*tokens, w_up, w_qkv)
    return in_all, grad_all, small_all, up, qkv


def solution(mesh):
    S = mesh.shape["shard"]
    R = mesh.shape["replica"]
    TP = [1] if R > 1 and H % (2 * S) == 0 else []
    DP = [bit for bit in bits_of(R - 1) if bit not in TP]
    NT, ND = 2 ** len(TP), 2 ** len(DP)
    ring = list(range(S))[:1] + list(range(1, S, 2)) + list(range(2, S, 2))[::-1]
    place = [ring.index(i) for i in range(S)]

    def to_ring(value, hops):
        return lax.ppermute(value, "shard", [(ring[i], ring[(i + hops) % S]) for i in range(S)])

    def flip(value, bit):
        return lax.ppermute(value, "replica", [(i, i ^ bit) for i in range(R)])

    def body(
        block_in, positions, out_grad, w_qkv, b_qkv, w_out, b_out, w_up, b_up, w_down, b_down,
        first_gain, first_shift, second_gain, second_shift,
    ):
        T, D = block_in.shape
        rows = w_qkv.shape[0]
        FS = w_down.shape[0]
        FD = FS // NT
        HN = H // S // NT
        AD = HN * HD
        G = NT * S
        s = lax.axis_index("shard")
        r = lax.axis_index("replica")
        mine = {bit: (r // bit) % 2 for bit in bits_of(R - 1)}
        t = sum((mine[bit] * 2**i for i, bit in enumerate(TP)), jnp.int32(0))
        p = jnp.array(place, jnp.int32)[s]
        ring_array = jnp.array(ring, jnp.int32)
        behind = [ring_array[(p - k) % S] for k in range(S)]
        ahead = [ring_array[(p + k) % S] for k in range(S)]
        order = (p - jnp.array(place, jnp.int32)) % S

        small = jnp.concatenate(
            [b_qkv, b_out, b_down, first_gain, first_shift, second_gain, second_shift,
             positions.astype(BF16)]
        )
        small = small.reshape(-1, 128)
        x_all, grad_all, small_all, up, qkv = fetch(
            block_in, out_grad, small, w_up, w_qkv, S, R, TP, DP, FD, AD
        )
        small_all = small_all.reshape(NT, S, -1)
        natural = small_all[0]
        sizes = [b_qkv.shape[0]] + [rows] * 6
        starts = [sum(sizes[:i]) for i in range(len(sizes))]
        whole = [natural[:, a : a + n].reshape(-1).astype(F32) for a, n in zip(starts, sizes)]
        full_b_qkv, full_b_out, full_b_down, gain_1, shift_1, gain_2, shift_2 = whole
        pos_all = small_all[:, :, sum(sizes) :].reshape(-1).astype(F32)
        x_all = x_all.reshape(G * T, D)
        grad_all = grad_all.reshape(G * T, D)
        down = lax.dynamic_slice_in_dim(w_down, t * FD, FD, 0)
        out = lax.dynamic_slice_in_dim(w_out, t * AD, AD, 0)
        bias_up = lax.dynamic_slice_in_dim(b_up, t * FD, FD, 0).astype(F32)
        bias_qkv = lax.dynamic_slice_in_dim(
            full_b_qkv.reshape(3, -1), (s * NT + t) * AD, AD, 1
        ).reshape(-1)
        part = rows // ND
        d = sum((mine[bit] * 2**i for i, bit in enumerate(DP)), jnp.int32(0))

        hidden_up = dot(grad_all, down, 1, 1)
        attended_grad = dot(grad_all, out, 1, 1).astype(BF16)

        def normed_of(block):
            wide = block.astype(F32)
            offsets = wide - jnp.mean(wide, axis=-1, keepdims=True)
            inverse = lax.rsqrt(jnp.mean(offsets * offsets, axis=-1, keepdims=True) + epsilon)
            return offsets * inverse, inverse

        normed, _ = normed_of(x_all)
        first_low = (normed * gain_1 + shift_1).astype(BF16)
        second_low = (normed * gain_2 + shift_2).astype(BF16)

        hidden_pre = dot(second_low, up, 1, 0) + bias_up
        activated = gelu_value(hidden_pre).astype(BF16)
        hidden_grad = hidden_up * gelu_slope(hidden_pre)
        sum_b_up = jnp.sum(hidden_grad, axis=0)
        hidden_low = hidden_grad.astype(BF16)

        mixed = dot(first_low, qkv, 1, 0) + bias_qkv
        cosine, sine = rotary_tables(pos_all)
        cosine, sine = [v.reshape(G, T, 1, -1) for v in (cosine, sine)]

        def heads(v):
            return v.reshape(G, T, HN, HD)

        queries = rotate(heads(mixed[:, :AD]), cosine, sine).astype(BF16)
        keys = rotate(heads(mixed[:, AD : 2 * AD]), cosine, sine).astype(BF16)
        values = heads(mixed[:, 2 * AD :]).astype(BF16)
        index = jnp.arange(T, dtype=jnp.int32)
        away = index[:, None] - index[None, :]
        allowed = (away >= 0) & (
            away <= pos_all.astype(jnp.int32).reshape(G, T)[:, :, None]
        )
        allowed = allowed[:, None]
        scale = HD ** (-0.5)
        scores = jnp.einsum("gqhd,gkhd->ghqk", queries, keys, preferred_element_type=F32) * scale
        scores = jnp.where(allowed, scores, -1e30)
        peak = jnp.max(scores, axis=-1, keepdims=True)
        logsum = peak + jnp.log(jnp.sum(jnp.exp(scores - peak), axis=-1, keepdims=True))
        probs = jnp.exp(scores - logsum)
        probs_low = probs.astype(BF16)
        attended = jnp.einsum("ghqk,gkhd->gqhd", probs_low, values, preferred_element_type=F32)
        attended = attended.astype(BF16).reshape(G * T, AD)

        lower = jnp.concatenate([attended, activated], axis=1)
        lower_w = jnp.concatenate([out, down], axis=0)

        def reduce_tokens(part_of):
            held = {m: part_of(t ^ m) for m in range(NT)}
            for i in reversed(range(len(TP))):
                for j in range(2**i):
                    held[j] = held[j] + flip(held[j + 2**i].astype(BF16), TP[i]).astype(F32)
            total = held[0].reshape(S, T, -1)

            def block(j):
                return lax.dynamic_index_in_dim(total, j, 0, keepdims=False)

            got = [to_ring(block(ahead[k]).astype(BF16), k) for k in range(1, S)]
            return sum((g.astype(F32) for g in got), block(s))

        def rows_of(value, i):
            return lax.dynamic_slice_in_dim(value, i * S * T, S * T, 0)

        branch = reduce_tokens(
            lambda i: dot(rows_of(lower, i), lower_w, 1, 0)
        )
        block_out = (block_in.astype(F32) + branch + full_b_out + full_b_down).astype(BF16)

        upstream = attended_grad.reshape(G, T, HN, HD)
        dprobs = jnp.einsum("gqhd,gkhd->ghqk", upstream, values, preferred_element_type=F32)
        total = jnp.sum(probs * dprobs, axis=-1, keepdims=True)
        dscores = (probs * (dprobs - total) * scale).astype(BF16)
        query_grad = jnp.einsum("ghqk,gkhd->gqhd", dscores, keys, preferred_element_type=F32)
        key_grad = jnp.einsum("ghqk,gqhd->gkhd", dscores, queries, preferred_element_type=F32)
        value_grad = jnp.einsum("ghqk,gqhd->gkhd", probs_low, upstream, preferred_element_type=F32)
        query_grad = rotate(query_grad, cosine, -sine)
        key_grad = rotate(key_grad, cosine, -sine)
        mixed_grad = jnp.concatenate(
            [v.reshape(G * T, AD) for v in (query_grad, key_grad, value_grad)], axis=1
        )
        sum_b_qkv = jnp.sum(mixed_grad, axis=0)
        mixed_low = mixed_grad.astype(BF16)

        def split_rows(grad):
            halves = []
            lead, rest = grad.shape[0], grad.shape[2:]
            for half, way in enumerate((DP, DP[::-1])):
                value = lax.index_in_dim(grad, half, grad.ndim - 3, keepdims=False)
                value = value.reshape((lead,) + (2,) * len(DP) + value.shape[2:])
                axes = list(DP[::-1])
                for bit in way:
                    axis = 1 + axes.index(bit)
                    axes.remove(bit)
                    sent = lax.dynamic_index_in_dim(value, 1 - mine[bit], axis, keepdims=False)
                    kept = lax.dynamic_index_in_dim(value, mine[bit], axis, keepdims=False)
                    value = kept + flip(sent.astype(BF16), bit).astype(F32)
                halves.append(value.astype(BF16))
            return halves

        def across(halves):
            value = jnp.concatenate(halves, axis=2)
            held = {0: lax.dynamic_index_in_dim(value, t, 1, keepdims=False)}
            for m in range(1, NT):
                there = lax.dynamic_index_in_dim(value, t ^ m, 1, keepdims=False)
                mask = sum(bit for i, bit in enumerate(TP) if m >> i & 1)
                held[m] = flip(there, mask)
            every = jnp.stack([held[m] for m in range(NT)], axis=1)
            got = [lax.dynamic_index_in_dim(every, s, 0, keepdims=True)]
            got += [
                to_ring(lax.dynamic_index_in_dim(every, ahead[k], 0, keepdims=True), k)
                for k in range(1, S)
            ]
            full = jnp.concatenate(got, axis=0)
            return jnp.stack(
                [
                    lax.dynamic_slice(
                        full, (order[j], t ^ u) + (0,) * (full.ndim - 2), (1, 1) + full.shape[2:]
                    ).reshape(full.shape[2:])
                    for j in range(S)
                    for u in range(NT)
                ],
                axis=1,
            )

        def share(halves, write, result):
            for half, (value, order) in enumerate(zip(halves, (DP, DP[::-1]))):
                value = lax.optimization_barrier(value)
                pieces = {0: value}
                for bit in list(order) + TP:
                    pieces.update({m | bit: flip(v, bit) for m, v in list(pieces.items())})
                for m, piece in pieces.items():
                    dmask = sum(2**i for i, bit in enumerate(DP) if m & bit)
                    tmask = sum(2**i for i, bit in enumerate(TP) if m & bit)
                    result = write(result, piece.astype(F32), d ^ dmask, t ^ tmask, half)
            return result

        def own_rows(left, result):
            count = left.shape[1]
            n = count // ND // 2
            halves = split_rows(dot(left, grad_all, 0, 0).reshape(1, ND, 2, n, D))
            return share(
                [v.reshape(n, D) for v in halves],
                lambda res, v, dd, tt, half: lax.dynamic_update_slice(
                    res, v, (tt * count + dd * 2 * n + half * n, 0)
                ),
                unwritten(result, F32),
            )

        grad_w_down = own_rows(activated, w_down.shape)

        m = part // NT // 2

        def half_rows(value):
            value = value.reshape(2 * m, -1)
            return [value[:m], value[m:]]

        def place_rows(res, v, dd, tt, half):
            return lax.dynamic_update_slice(res, v, ((dd * NT + tt) * 2 * m + half * m, 0))

        def by_rows(value):
            return value.reshape(S, ND, NT, 2, m, -1)

        grad_up = split_rows(by_rows(dot(second_low, hidden_low, 0, 0)))
        grad_w_up = share(
            half_rows(across(grad_up)), place_rows, unwritten(w_up.shape, F32)
        )

        grad_w_out = own_rows(attended, w_out.shape)

        grad_qkv = split_rows(by_rows(dot(first_low, mixed_low, 0, 0)))
        grad_w_qkv = share(
            half_rows(
                across([v.reshape(v.shape[:3] + (3, AD)) for v in grad_qkv]).transpose(0, 2, 1, 3)
            ),
            place_rows,
            unwritten(w_qkv.shape, F32),
        )

        first_grad = dot(mixed_low, qkv, 1, 1)
        second_grad = dot(hidden_low, up, 1, 1)
        sum_gain_1 = jnp.sum(first_grad * normed, axis=0)
        sum_shift_1 = jnp.sum(first_grad, axis=0)
        sum_gain_2 = jnp.sum(second_grad * normed, axis=0)
        sum_shift_2 = jnp.sum(second_grad, axis=0)
        inner = first_grad * gain_1 + second_grad * gain_2
        scaled = reduce_tokens(lambda i: rows_of(inner, i))
        normed_own, inverse_own = normed_of(block_in)
        term = inverse_own * (
            scaled
            - jnp.mean(scaled, axis=-1, keepdims=True)
            - normed_own * jnp.mean(scaled * normed_own, axis=-1, keepdims=True)
        )
        wide_grad = out_grad.astype(F32)
        in_grad = (wide_grad + term).astype(BF16)

        def placed(length, value, offset):
            return lax.dynamic_update_slice(jnp.zeros((length,), F32), value, (offset,))

        width = w_out.shape[0] * S
        col = (s * NT + t) * AD
        sums = [placed(width, sum_b_qkv[i * AD : (i + 1) * AD], col) for i in range(3)]
        sums += [jnp.sum(wide_grad, axis=0), placed(FS * S, sum_b_up, s * FS + t * FD)]
        sums += [sum_gain_1, sum_shift_1, sum_gain_2, sum_shift_2]
        lengths = [v.shape[0] for v in sums]
        sums = jnp.concatenate(sums)
        for bit in bits_of(R - 1):
            sums = sums + flip(sums, bit)
        for bit in bits_of(S - 1):
            sums = sums + lax.ppermute(sums, "shard", [(i, i ^ bit) for i in range(S)])
        at = [sum(lengths[:i]) for i in range(len(lengths))]

        def owned(start, length):
            return lax.dynamic_slice_in_dim(sums, start + s * (length // S), length // S, 0)

        grad_b_qkv = owned(at[0], 3 * width)
        grad_b_out = owned(at[3], D)
        grad_b_up = owned(at[4], FS * S)
        smalls = [owned(at[5 + i], D) for i in range(4)]
        return (
            block_out, in_grad, grad_w_qkv, grad_b_qkv, grad_w_out, grad_b_out, grad_w_up, grad_b_up,
            grad_w_down, grad_b_out, *smalls,
        )

    rows2, row1, par2, par1 = P(("shard", "replica"), None), P(("shard", "replica")), P("shard", None), P("shard")
    return jax.shard_map(
        body,
        mesh=mesh,
        in_specs=(
            rows2, row1, rows2, par2, par1, par2, par1, par2, par1, par2, par1, par1, par1, par1, par1,
        ),
        out_specs=(
            rows2, rows2, par2, par1, par2, par1, par2, par1, par2, par1, par1, par1, par1, par1,
        ),
        check_vma=False,
    )
```

```python
import jax
import jax.numpy as jnp
from jax import lax
from jax.experimental import pallas as pl
from jax.experimental.pallas import tpu as pltpu
from jax.sharding import PartitionSpec as P

H = 8
HD = 256
ROT = 64

epsilon = 1e-05


F32 = jnp.float32
BF16 = jnp.bfloat16
MESH = pl.DeviceIdType.MESH


def rotary_tables(positions):
    half_rot = ROT // 2
    freqs = 10000.0 ** (-(jnp.arange(half_rot, dtype=F32) * (2.0 / ROT)))
    angles = positions[:, None] * freqs[None, :]
    return jnp.cos(angles), jnp.sin(angles)


def dot(left, right, left_dim, right_dim):
    return lax.dot_general(
        left, right, (((left_dim,), (right_dim,)), ((), ())), preferred_element_type=F32
    )


def unwritten(shape, dtype):
    return pl.pallas_call(
        lambda out_ref: None,
        out_shape=jax.ShapeDtypeStruct(shape, dtype),
        out_specs=pl.BlockSpec(memory_space=pl.ANY),
    )()


def bits_of(mask):
    return [1 << i for i in range(mask.bit_length()) if mask >> i & 1]

def fetch(block_in, out_grad, small, w_up, w_qkv, S, R, TP, DP, FD, AD):
    T, D = block_in.shape
    rows = w_up.shape[0]
    NT, ND = 2 ** len(TP), 2 ** len(DP)
    part = rows // ND
    third = w_qkv.shape[1] // 3
    tokens = (small, out_grad, block_in)
    widths = (FD, 3 * AD)

    def kernel(
        small_ref, grad_ref, in_ref, up_ref, qkv_ref, small_all, grad_all, in_all, up_all, qkv_all,
        in_own, grad_own, up_own, qkv_own, small_send, small_recv, line_send, line_recv, tp_send, tp_recv, z_send, z_recv, dp_send, dp_recv, local,
    ):
        s = lax.axis_index("shard")
        r = lax.axis_index("replica")
        t = sum(((r // bit) % 2 * 2**i for i, bit in enumerate(TP)), jnp.int32(0))
        d = sum(((r // bit) % 2 * 2**i for i, bit in enumerate(DP)), jnp.int32(0))

        def partner(bit):
            return {"replica": r + bit - 2 * bit * ((r // bit) % 2)}

        copies = [pltpu.make_async_copy(small_ref, small_all.at[t, s], local.at[0])]
        gathered = (grad_all, in_all)
        first = [
            pltpu.make_async_copy(in_ref, in_own, local.at[1]),
            pltpu.make_async_copy(grad_ref, grad_own, local.at[2]),
            pltpu.make_async_copy(
                up_ref.at[:, pl.ds(pl.multiple_of((s * NT + t) * FD, FD), FD)], up_own, local.at[3]
            ),
        ]
        for j in range(3):
            first.append(
                pltpu.make_async_copy(
                    qkv_ref.at[:, pl.ds(pl.multiple_of(j * third + (s * NT + t) * AD, AD), AD)],
                    qkv_own.at[:, j * AD : (j + 1) * AD],
                    local.at[4 + j],
                )
            )
        for copy in copies + first:
            copy.start()

        def other(k, m):
            mask = sum(bit for i, bit in enumerate(TP) if m >> i & 1)
            flipped = sum((bit * (1 - 2 * ((r // bit) % 2)) for bit in bits_of(mask)), r)
            return {"shard": lax.rem(s + k, S), "replica": flipped}

        group = [(k, m) for k in range(S) for m in range(NT) if k or m]
        plane = range(1, ND)

        def mate(m):
            mask = sum(bit for i, bit in enumerate(DP) if m >> i & 1)
            return {"replica": sum((bit * (1 - 2 * ((r // bit) % 2)) for bit in bits_of(mask)), r)}

        barrier = pltpu.get_barrier_semaphore()
        for k, m in group:
            pl.semaphore_signal(barrier, inc=1, device_id=other(k, m), device_id_type=MESH)
        for m in plane:
            pl.semaphore_signal(barrier, inc=1, device_id=mate(m), device_id_type=MESH)
        pl.semaphore_wait(barrier, len(group) + len(plane))

        def small_copy(k, m):
            return pltpu.make_async_remote_copy(
                src_ref=small_ref, dst_ref=small_all.at[t, s], send_sem=small_send.at[k, m],
                recv_sem=small_recv.at[k, m], device_id=other(k, m), device_id_type=MESH,
            )

        def line(i, j, way, source):
            return pltpu.make_async_remote_copy(
                src_ref=source, dst_ref=gathered[i].at[t, j], send_sem=line_send.at[i, j, way],
                recv_sem=line_recv.at[i, j], device_id={"shard": s + 2 * way - 1}, device_id_type=MESH,
            )

        def across(i, j, b, m, source):
            slot = gathered[i].at[t ^ m, j]
            return pltpu.make_async_remote_copy(
                src_ref=slot if source is None else source, dst_ref=slot, send_sem=tp_send.at[i, j, m | 1 << b],
                recv_sem=tp_recv.at[i, j, m | 1 << b], device_id=partner(TP[b]), device_id_type=MESH,
            )

        def z_copies(w, k, sending):
            to = lax.rem(s + k, S)
            at = (s if sending else lax.rem(s + S - k, S)) * rows + d * part
            at = pl.multiple_of(at, part)
            out = []
            for j in range(1 if w == 0 else 3):
                if w == 0:
                    source = up_ref.at[pl.ds(pl.multiple_of(d * part, part), part), pl.ds(pl.multiple_of((to * NT + t) * FD, FD), FD)]
                    target = up_all.at[pl.ds(at, part), :]
                else:
                    source = qkv_ref.at[
                        pl.ds(pl.multiple_of(d * part, part), part), pl.ds(pl.multiple_of(j * third + (to * NT + t) * AD, AD), AD)
                    ]
                    target = qkv_all.at[pl.ds(at, part), j * AD : (j + 1) * AD]
                out.append(
                    pltpu.make_async_remote_copy(
                        src_ref=source, dst_ref=target, send_sem=z_send.at[k, w + j], recv_sem=z_recv.at[k, w + j],
                        device_id={"shard": to}, device_id_type=MESH,
                    )
                )
            return out

        def shared(w, k, m):
            at = pl.multiple_of(lax.rem(s + S - k, S) * rows + d * part, part)
            slot = (up_all, qkv_all)[w].at[pl.ds(at, part), :]
            return pltpu.make_async_remote_copy(
                src_ref=slot, dst_ref=slot, send_sem=dp_send.at[w, k, m], recv_sem=dp_recv.at[w, k, m],
                device_id=mate(m), device_id_type=MESH,
            )

        mine = (grad_ref, in_ref)
        for k, m in group:
            small_copy(k, m).start()
        for i in range(2):

            @pl.when(s + 1 < S)
            def _():
                line(i, s, 1, mine[i]).start()

            @pl.when(s > 0)
            def _():
                line(i, s, 0, mine[i]).start()

        for k in range(1, S):
            for w in range(2):
                for copy in z_copies(w, k, True):
                    copy.start()
        for i in range(2):
            for b in range(len(TP)):
                across(i, s, b, 0, mine[i]).start()

        def pass_on(i, j, m, top):
            for b in range(top + 1, len(TP)):
                across(i, j, b, m, None).start()

        def from_line(i, k):
            @pl.when(s - k >= 0)
            def _():
                line(i, s - k, 1, gathered[i].at[t, s - k]).wait_recv()

                @pl.when(s + 1 < S)
                def _():
                    line(i, s - k, 1, gathered[i].at[t, s - k]).start()

                pass_on(i, s - k, 0, -1)

            @pl.when(s + k < S)
            def _():
                line(i, s + k, 0, gathered[i].at[t, s + k]).wait_recv()

                @pl.when(s > 0)
                def _():
                    line(i, s + k, 0, gathered[i].at[t, s + k]).start()

                pass_on(i, s + k, 0, -1)

        for copy in first:
            copy.wait()
        at_own = pl.multiple_of(s * rows, rows)
        second = [
            pltpu.make_async_copy(in_own, in_all.at[t, s], local.at[1]),
            pltpu.make_async_copy(grad_own, grad_all.at[t, s], local.at[2]),
            pltpu.make_async_copy(up_own, up_all.at[pl.ds(at_own, rows), :], local.at[3]),
            pltpu.make_async_copy(qkv_own, qkv_all.at[pl.ds(at_own, rows), :], local.at[4]),
        ]
        for copy in second:
            copy.start()

        for k in range(1, S):
            for i in range(2):
                from_line(i, k)
            if k == 1:
                for back in range(1, S):
                    for w in range(2):
                        for copy in z_copies(w, back, False):
                            copy.wait_recv()
                        for m in plane:
                            shared(w, back, m).start()

        for m in range(1, NT):
            top = m.bit_length() - 1
            for i in range(2):
                for j in range(S):
                    across(i, j, top, m ^ (1 << top), None).wait_recv()
                    pass_on(i, j, m, top)
        for k, m in group:
            small_copy(k, m).wait_recv()
        for k in range(1, S):
            for w in range(2):
                for m in plane:
                    shared(w, k, m).wait_recv()

        for i in range(2):
            for j in range(S):

                @pl.when((s + 1 < S) & (j <= s))
                def _():
                    line(i, j, 1, gathered[i].at[t, j]).wait_send()

                @pl.when((s > 0) & (j >= s))
                def _():
                    line(i, j, 0, gathered[i].at[t, j]).wait_send()

                for m in range(NT):
                    for b in range(m.bit_length(), len(TP)):
                        across(i, j, b, m, None).wait_send()
        for k, m in group:
            small_copy(k, m).wait_send()
        for k in range(1, S):
            for w in range(2):
                for copy in z_copies(w, k, True):
                    copy.wait_send()
                for m in plane:
                    shared(w, k, m).wait_send()
        for copy in copies + second:
            copy.wait()

    any_spec = pl.BlockSpec(memory_space=pl.ANY)
    shapes = [jax.ShapeDtypeStruct((NT, S) + v.shape, BF16) for v in tokens]
    shapes += [jax.ShapeDtypeStruct((S * rows, width), BF16) for width in widths]
    small_all, grad_all, in_all, up, qkv = pl.pallas_call(
        kernel,
        out_shape=shapes,
        in_specs=[any_spec] * 5,
        out_specs=[any_spec] * 5,
        scratch_shapes=[
            pltpu.VMEM((T, D), BF16),
            pltpu.VMEM((T, D), BF16),
            pltpu.VMEM((rows, FD), BF16),
            pltpu.VMEM((rows, 3 * AD), BF16),
            pltpu.SemaphoreType.DMA((S, NT)),
            pltpu.SemaphoreType.DMA((S, NT)),
            pltpu.SemaphoreType.DMA((2, S, 2)),
            pltpu.SemaphoreType.DMA((2, S)),
            pltpu.SemaphoreType.DMA((2, S, NT)),
            pltpu.SemaphoreType.DMA((2, S, NT)),
            pltpu.SemaphoreType.DMA((S, 4)),
            pltpu.SemaphoreType.DMA((S, 4)),
            pltpu.SemaphoreType.DMA((2, S, ND)),
            pltpu.SemaphoreType.DMA((2, S, ND)),
            pltpu.SemaphoreType.DMA((7,)),
        ],
        compiler_params=pltpu.CompilerParams(collective_id=0, has_side_effects=True),
        name="fetch",
    )(*tokens, w_up, w_qkv)
    return in_all, grad_all, small_all, up, qkv

def layer(in_all, grad_all, tables, norms, bias_qkv, up, qkv, b_up, w_down, w_out, t, T, tile):
    N, D = in_all.shape
    FD = up.shape[1]
    AD = qkv.shape[1] // 3
    heads = AD // HD
    scale = HD ** (-0.5)

    def kernel(
        t_ref, in_ref, grad_ref, tables_ref, norms_ref, bias_qkv_ref, up_ref, qkv_ref, b_up_ref, down_ref, out_ref,
        first_ref, second_ref, attended_ref, activated_ref, mixed_ref, hidden_ref, branch_ref, inner_ref,
        sum_qkv_ref, sum_up_ref, sum_norm_ref,
    ):
        @pl.when(pl.program_id(0) == 0)
        def _():
            sum_qkv_ref[...] = jnp.zeros_like(sum_qkv_ref)
            sum_up_ref[...] = jnp.zeros_like(sum_up_ref)
            sum_norm_ref[...] = jnp.zeros_like(sum_norm_ref)

        gain_1, shift_1, gain_2, shift_2 = [norms_ref[i : i + 1, :] for i in range(4)]
        wide = in_ref[...].astype(F32)
        offsets = wide - jnp.mean(wide, axis=-1, keepdims=True)
        inverse = lax.rsqrt(jnp.mean(offsets * offsets, axis=-1, keepdims=True) + epsilon)
        normed = offsets * inverse
        first = (normed * gain_1 + shift_1).astype(BF16)
        second = (normed * gain_2 + shift_2).astype(BF16)
        first_ref[...] = first
        second_ref[...] = second
        grad = grad_ref[...]

        mixed = dot(first, qkv_ref[...], 1, 0) + bias_qkv_ref[...]
        attended_grad = dot(grad, out_ref[...], 1, 1).astype(BF16)
        straight, ahead, back, position = [tables_ref[i] for i in range(4)]

        def turn(value, sign):
            low = value[:, :128]
            low = low * straight + sign * (pltpu.roll(low, 96, 1) * ahead + pltpu.roll(low, 32, 1) * back)
            return jnp.concatenate([low, value[:, 128:]], axis=1)

        row = lax.broadcasted_iota(jnp.int32, (T, T), 0)
        col = lax.broadcasted_iota(jnp.int32, (T, T), 1)
        away = (row - col).astype(F32)
        attended, query_grads, key_grads, value_grads = [], [], [], []
        for h in range(heads):
            at = slice(h * HD, (h + 1) * HD)
            queries = turn(mixed[:, at], 1.0).astype(BF16)
            keys = turn(mixed[:, AD + h * HD : AD + (h + 1) * HD], 1.0).astype(BF16)
            values = mixed[:, 2 * AD + h * HD : 2 * AD + (h + 1) * HD].astype(BF16)
            parts = [[], [], [], []]
            for b in range(tile // T):
                rows = slice(b * T, (b + 1) * T)
                q, k, v, u = queries[rows], keys[rows], values[rows], attended_grad[rows, at]
                allowed = (away >= 0) & (away <= position[rows, :1])
                scores = jnp.where(allowed, dot(q, k, 1, 1) * scale, -1e30)
                peak = jnp.max(scores, axis=-1, keepdims=True)
                logsum = peak + jnp.log(jnp.sum(jnp.exp(scores - peak), axis=-1, keepdims=True))
                probs = jnp.exp(scores - logsum)
                low = probs.astype(BF16)
                parts[0].append(dot(low, v, 1, 0).astype(BF16))
                dprobs = dot(u, v, 1, 1)
                total = jnp.sum(probs * dprobs, axis=-1, keepdims=True)
                dscores = (probs * (dprobs - total) * scale).astype(BF16)
                parts[1].append(dot(dscores, k, 1, 0))
                parts[2].append(dot(dscores, q, 0, 0))
                parts[3].append(dot(low, u, 0, 0))
            joined = [jnp.concatenate(v, axis=0) for v in parts]
            attended.append(joined[0])
            query_grads.append(turn(joined[1], -1.0))
            key_grads.append(turn(joined[2], -1.0))
            value_grads.append(joined[3])
        attended = jnp.concatenate(attended, axis=1)
        attended_ref[...] = attended
        mixed_grad = jnp.concatenate(query_grads + key_grads + value_grads, axis=1)
        sum_qkv_ref[...] += jnp.sum(mixed_grad, axis=0, keepdims=True)
        mixed_low = mixed_grad.astype(BF16)
        mixed_ref[...] = mixed_low

        pre = dot(second, up_ref[...], 1, 0) + b_up_ref[...].astype(F32)
        bell = 0.5 * (1.0 + lax.erf(pre * 0.7071067811865476))
        activated = (pre * bell).astype(BF16)
        activated_ref[...] = activated
        slope = bell + pre * jnp.exp(-0.5 * pre * pre) * 0.3989422804014327
        hidden_grad = dot(grad, down_ref[...], 1, 1) * slope
        sum_up_ref[...] += jnp.sum(hidden_grad, axis=0, keepdims=True)
        hidden_low = hidden_grad.astype(BF16)
        hidden_ref[...] = hidden_low

        branch = dot(attended, out_ref[...], 1, 0) + dot(activated, down_ref[...], 1, 0)
        branch_ref[...] = branch.astype(BF16)

        first_grad = dot(mixed_low, qkv_ref[...], 1, 1)
        second_grad = dot(hidden_low, up_ref[...], 1, 1)
        sum_norm_ref[0:1, :] += jnp.sum(first_grad * normed, axis=0, keepdims=True)
        sum_norm_ref[1:2, :] += jnp.sum(first_grad, axis=0, keepdims=True)
        sum_norm_ref[2:3, :] += jnp.sum(second_grad * normed, axis=0, keepdims=True)
        sum_norm_ref[3:4, :] += jnp.sum(second_grad, axis=0, keepdims=True)
        inner_ref[...] = (first_grad * gain_1 + second_grad * gain_2).astype(BF16)

    def rows(width):
        return pl.BlockSpec((tile, width), lambda i, t_ref: (i, 0))

    def whole(shape, index=lambda i, t_ref: (0, 0)):
        return pl.BlockSpec(shape, index, pipeline_mode=pl.Buffered(1))

    widths = [D, D, AD, FD, 3 * AD, FD, D, D]
    flops = 2 * N * D * (2 * 3 * AD + 2 * FD + 2 * FD + 2 * AD)
    return pl.pallas_call(
        kernel,
        out_shape=[jax.ShapeDtypeStruct((N, w), BF16) for w in widths]
        + [jax.ShapeDtypeStruct(v, F32) for v in ((1, 3 * AD), (1, FD), (4, D))],
        grid_spec=pltpu.PrefetchScalarGridSpec(
            num_scalar_prefetch=1,
            grid=(N // tile,),
            in_specs=[
                rows(D),
                rows(D),
                pl.BlockSpec((4, tile, 128), lambda i, t_ref: (0, i, 0)),
                whole((4, D)),
                whole((1, 3 * AD)),
                whole((D, FD)),
                whole((D, 3 * AD)),
                whole((1, FD), lambda i, t_ref: (0, t_ref[0])),
                whole((FD, D), lambda i, t_ref: (t_ref[0], 0)),
                whole((AD, D), lambda i, t_ref: (t_ref[0], 0)),
            ],
            out_specs=[rows(w) for w in widths] + [whole((1, 3 * AD)), whole((1, FD)), whole((4, D))],
        ),
        compiler_params=pltpu.CompilerParams(
            dimension_semantics=("arbitrary",), vmem_limit_bytes=63 * 2**20
        ),
        cost_estimate=pl.CostEstimate(flops=flops, bytes_accessed=50 * 2**20, transcendentals=N * FD * 2),
        name="layer",
    )(t.reshape(1), in_all, grad_all, tables, norms, bias_qkv, up, qkv, b_up.reshape(1, -1), w_down, w_out)


def solution(mesh):
    S = mesh.shape["shard"]
    R = mesh.shape["replica"]
    TP = [1] if R > 1 and H % (2 * S) == 0 else []
    DP = [bit for bit in bits_of(R - 1) if bit not in TP]
    NT, ND = 2 ** len(TP), 2 ** len(DP)
    ring = list(range(S))[:1] + list(range(1, S, 2)) + list(range(2, S, 2))[::-1]
    place = [ring.index(i) for i in range(S)]

    def to_ring(value, hops):
        return lax.ppermute(value, "shard", [(ring[i], ring[(i + hops) % S]) for i in range(S)])

    def flip(value, bit):
        return lax.ppermute(value, "replica", [(i, i ^ bit) for i in range(R)])

    def body(
        block_in, positions, out_grad, w_qkv, b_qkv, w_out, b_out, w_up, b_up, w_down, b_down,
        first_gain, first_shift, second_gain, second_shift,
    ):
        T, D = block_in.shape
        rows = w_qkv.shape[0]
        FS = w_down.shape[0]
        FD = FS // NT
        HN = H // S // NT
        AD = HN * HD
        G = NT * S
        s = lax.axis_index("shard")
        r = lax.axis_index("replica")
        mine = {bit: (r // bit) % 2 for bit in bits_of(R - 1)}
        t = sum((mine[bit] * 2**i for i, bit in enumerate(TP)), jnp.int32(0))
        p = jnp.array(place, jnp.int32)[s]
        ring_array = jnp.array(ring, jnp.int32)
        behind = [ring_array[(p - k) % S] for k in range(S)]
        ahead = [ring_array[(p + k) % S] for k in range(S)]
        order = (p - jnp.array(place, jnp.int32)) % S

        small = jnp.concatenate(
            [b_qkv, b_out, b_down, first_gain, first_shift, second_gain, second_shift,
             positions.astype(BF16)]
        )
        small = small.reshape(-1, 128)
        x_all, grad_all, small_all, up, qkv = fetch(
            block_in, out_grad, small, w_up, w_qkv, S, R, TP, DP, FD, AD
        )
        small_all = small_all.reshape(NT, S, -1)
        natural = small_all[0]
        sizes = [b_qkv.shape[0]] + [rows] * 6
        starts = [sum(sizes[:i]) for i in range(len(sizes))]
        whole = [natural[:, a : a + n].reshape(-1).astype(F32) for a, n in zip(starts, sizes)]
        full_b_qkv, full_b_out, full_b_down, gain_1, shift_1, gain_2, shift_2 = whole
        pos_all = small_all[:, :, sum(sizes) :].reshape(-1).astype(F32)
        x_all = x_all.reshape(G * T, D)
        grad_all = grad_all.reshape(G * T, D)
        bias_qkv = lax.dynamic_slice_in_dim(
            full_b_qkv.reshape(3, -1), (s * NT + t) * AD, AD, 1
        ).reshape(-1)
        part = rows // ND
        d = sum((mine[bit] * 2**i for i, bit in enumerate(DP)), jnp.int32(0))

        def normed_of(block):
            wide = block.astype(F32)
            offsets = wide - jnp.mean(wide, axis=-1, keepdims=True)
            inverse = lax.rsqrt(jnp.mean(offsets * offsets, axis=-1, keepdims=True) + epsilon)
            return offsets * inverse, inverse

        half = ROT // 2
        cosine, sine = rotary_tables(pos_all)
        pad = jnp.zeros((G * T, 128 - ROT), F32)
        none = jnp.zeros((G * T, half), F32)
        tables = jnp.stack(
            [
                jnp.concatenate([cosine, cosine, pad + 1.0], axis=1),
                jnp.concatenate([-sine, none, pad], axis=1),
                jnp.concatenate([none, sine, pad], axis=1),
                jnp.broadcast_to(pos_all[:, None], (G * T, 128)),
            ]
        )
        norms = jnp.stack([gain_1, shift_1, gain_2, shift_2])
        (
            first_low, second_low, attended, activated, mixed_low, hidden_low, branch_part, inner_part,
            sum_b_qkv, sum_b_up, sum_norms,
        ) = layer(
            x_all, grad_all, tables, norms, bias_qkv.reshape(1, -1), up, qkv, b_up, w_down, w_out, t, T, 2 * T
        )
        sum_b_qkv, sum_b_up = sum_b_qkv.reshape(-1), sum_b_up.reshape(-1)

        def reduce_tokens(parts):
            parts = parts.reshape(NT, S, T, -1)

            def of(m):
                return lax.dynamic_index_in_dim(parts, t ^ m, 0, keepdims=False)

            held = {m: of(m) for m in range(NT)}
            for i in reversed(range(len(TP))):
                for j in range(2**i):
                    held[j] = held[j].astype(F32) + flip(held[j + 2**i].astype(BF16), TP[i]).astype(F32)
            total = held[0]

            def block(j):
                return lax.dynamic_index_in_dim(total, j, 0, keepdims=False)

            got = [to_ring(block(ahead[k]).astype(BF16), k) for k in range(1, S)]
            return sum((g.astype(F32) for g in got), block(s).astype(F32))

        branch = reduce_tokens(branch_part)
        block_out = (block_in.astype(F32) + branch + full_b_out + full_b_down).astype(BF16)

        def split_rows(grad):
            halves = []
            lead, rest = grad.shape[0], grad.shape[2:]
            for half, way in enumerate((DP, DP[::-1])):
                value = lax.index_in_dim(grad, half, grad.ndim - 3, keepdims=False)
                value = value.reshape((lead,) + (2,) * len(DP) + value.shape[2:])
                axes = list(DP[::-1])
                for bit in way:
                    axis = 1 + axes.index(bit)
                    axes.remove(bit)
                    sent = lax.dynamic_index_in_dim(value, 1 - mine[bit], axis, keepdims=False)
                    kept = lax.dynamic_index_in_dim(value, mine[bit], axis, keepdims=False)
                    value = kept + flip(sent.astype(BF16), bit).astype(F32)
                halves.append(value.astype(BF16))
            return halves

        def across(halves):
            value = jnp.concatenate(halves, axis=2)
            held = {0: lax.dynamic_index_in_dim(value, t, 1, keepdims=False)}
            for m in range(1, NT):
                there = lax.dynamic_index_in_dim(value, t ^ m, 1, keepdims=False)
                mask = sum(bit for i, bit in enumerate(TP) if m >> i & 1)
                held[m] = flip(there, mask)
            every = jnp.stack([held[m] for m in range(NT)], axis=1)
            got = [lax.dynamic_index_in_dim(every, s, 0, keepdims=True)]
            got += [
                to_ring(lax.dynamic_index_in_dim(every, ahead[k], 0, keepdims=True), k)
                for k in range(1, S)
            ]
            full = jnp.concatenate(got, axis=0)
            return jnp.stack(
                [
                    lax.dynamic_slice(
                        full, (order[j], t ^ u) + (0,) * (full.ndim - 2), (1, 1) + full.shape[2:]
                    ).reshape(full.shape[2:])
                    for j in range(S)
                    for u in range(NT)
                ],
                axis=1,
            )

        def share(halves, write, result):
            for half, (value, order) in enumerate(zip(halves, (DP, DP[::-1]))):
                value = lax.optimization_barrier(value)
                pieces = {0: value}
                for bit in list(order) + TP:
                    pieces.update({m | bit: flip(v, bit) for m, v in list(pieces.items())})
                for m, piece in pieces.items():
                    dmask = sum(2**i for i, bit in enumerate(DP) if m & bit)
                    tmask = sum(2**i for i, bit in enumerate(TP) if m & bit)
                    result = write(result, piece.astype(F32), d ^ dmask, t ^ tmask, half)
            return result

        def own_rows(left, result):
            count = left.shape[1]
            n = count // ND // 2
            halves = split_rows(dot(left, grad_all, 0, 0).reshape(1, ND, 2, n, D))
            return share(
                [v.reshape(n, D) for v in halves],
                lambda res, v, dd, tt, half: lax.dynamic_update_slice(
                    res, v, (tt * count + dd * 2 * n + half * n, 0)
                ),
                unwritten(result, F32),
            )

        grad_w_down = own_rows(activated, w_down.shape)

        m = part // NT // 2

        def half_rows(value):
            value = value.reshape(2 * m, -1)
            return [value[:m], value[m:]]

        def place_rows(res, v, dd, tt, half):
            return lax.dynamic_update_slice(res, v, ((dd * NT + tt) * 2 * m + half * m, 0))

        def by_rows(value):
            return value.reshape(S, ND, NT, 2, m, -1)

        grad_up = split_rows(by_rows(dot(second_low, hidden_low, 0, 0)))
        grad_w_up = share(
            half_rows(across(grad_up)), place_rows, unwritten(w_up.shape, F32)
        )

        grad_w_out = own_rows(attended, w_out.shape)

        grad_qkv = split_rows(by_rows(dot(first_low, mixed_low, 0, 0)))
        grad_w_qkv = share(
            half_rows(
                across([v.reshape(v.shape[:3] + (3, AD)) for v in grad_qkv]).transpose(0, 2, 1, 3)
            ),
            place_rows,
            unwritten(w_qkv.shape, F32),
        )

        scaled = reduce_tokens(inner_part)
        normed_own, inverse_own = normed_of(block_in)
        term = inverse_own * (
            scaled
            - jnp.mean(scaled, axis=-1, keepdims=True)
            - normed_own * jnp.mean(scaled * normed_own, axis=-1, keepdims=True)
        )
        wide_grad = out_grad.astype(F32)
        in_grad = (wide_grad + term).astype(BF16)

        def placed(length, value, offset):
            return lax.dynamic_update_slice(jnp.zeros((length,), F32), value, (offset,))

        width = w_out.shape[0] * S
        col = (s * NT + t) * AD
        sums = [placed(width, sum_b_qkv[i * AD : (i + 1) * AD], col) for i in range(3)]
        sums += [jnp.sum(wide_grad, axis=0), placed(FS * S, sum_b_up, s * FS + t * FD)]
        sums += [sum_norms[i] for i in range(4)]
        lengths = [v.shape[0] for v in sums]
        sums = jnp.concatenate(sums)
        for bit in bits_of(R - 1):
            sums = sums + flip(sums, bit)
        for bit in bits_of(S - 1):
            sums = sums + lax.ppermute(sums, "shard", [(i, i ^ bit) for i in range(S)])
        at = [sum(lengths[:i]) for i in range(len(lengths))]

        def owned(start, length):
            return lax.dynamic_slice_in_dim(sums, start + s * (length // S), length // S, 0)

        grad_b_qkv = owned(at[0], 3 * width)
        grad_b_out = owned(at[3], D)
        grad_b_up = owned(at[4], FS * S)
        smalls = [owned(at[5 + i], D) for i in range(4)]
        return (
            block_out, in_grad, grad_w_qkv, grad_b_qkv, grad_w_out, grad_b_out, grad_w_up, grad_b_up,
            grad_w_down, grad_b_out, *smalls,
        )

    rows2, row1, par2, par1 = P(("shard", "replica"), None), P(("shard", "replica")), P("shard", None), P("shard")
    return jax.shard_map(
        body,
        mesh=mesh,
        in_specs=(
            rows2, row1, rows2, par2, par1, par2, par1, par2, par1, par2, par1, par1, par1, par1, par1,
        ),
        out_specs=(
            rows2, rows2, par2, par1, par2, par1, par2, par1, par2, par1, par1, par1, par1, par1,
        ),
        check_vma=False,
    )
```

```python
import jax
import jax.numpy as jnp
from jax import lax
from jax.experimental import pallas as pl
from jax.experimental.pallas import tpu as pltpu
from jax.sharding import PartitionSpec as P

H = 8
HD = 256
ROT = 64

epsilon = 1e-05


F32 = jnp.float32
BF16 = jnp.bfloat16
MESH = pl.DeviceIdType.MESH


def rotary_tables(positions):
    half_rot = ROT // 2
    freqs = 10000.0 ** (-(jnp.arange(half_rot, dtype=F32) * (2.0 / ROT)))
    angles = positions[:, None] * freqs[None, :]
    return jnp.cos(angles), jnp.sin(angles)


def dot(left, right, left_dim, right_dim):
    return lax.dot_general(
        left, right, (((left_dim,), (right_dim,)), ((), ())), preferred_element_type=F32
    )


def unwritten(shape, dtype):
    return pl.pallas_call(
        lambda out_ref: None,
        out_shape=jax.ShapeDtypeStruct(shape, dtype),
        out_specs=pl.BlockSpec(memory_space=pl.ANY),
    )()


def bits_of(mask):
    return [1 << i for i in range(mask.bit_length()) if mask >> i & 1]

def fetch(block_in, out_grad, small, w_up, w_qkv, S, R, TP, DP, FD, AD):
    T, D = block_in.shape
    rows = w_up.shape[0]
    NT, ND = 2 ** len(TP), 2 ** len(DP)
    part = rows // ND
    third = w_qkv.shape[1] // 3
    tokens = (small, out_grad, block_in)
    widths = (FD, 3 * AD)

    def kernel(
        small_ref, grad_ref, in_ref, up_ref, qkv_ref, small_all, grad_all, in_all, up_all, qkv_all,
        in_own, grad_own, up_own, qkv_own, small_send, small_recv, line_send, line_recv, tp_send, tp_recv, z_send, z_recv, dp_send, dp_recv, local,
    ):
        s = lax.axis_index("shard")
        r = lax.axis_index("replica")
        t = sum(((r // bit) % 2 * 2**i for i, bit in enumerate(TP)), jnp.int32(0))
        d = sum(((r // bit) % 2 * 2**i for i, bit in enumerate(DP)), jnp.int32(0))

        def partner(bit):
            return {"replica": r + bit - 2 * bit * ((r // bit) % 2)}

        copies = [pltpu.make_async_copy(small_ref, small_all.at[t, s], local.at[0])]
        gathered = (grad_all, in_all)
        first = [
            pltpu.make_async_copy(in_ref, in_own, local.at[1]),
            pltpu.make_async_copy(grad_ref, grad_own, local.at[2]),
            pltpu.make_async_copy(
                up_ref.at[:, pl.ds(pl.multiple_of((s * NT + t) * FD, FD), FD)], up_own, local.at[3]
            ),
        ]
        for j in range(3):
            first.append(
                pltpu.make_async_copy(
                    qkv_ref.at[:, pl.ds(pl.multiple_of(j * third + (s * NT + t) * AD, AD), AD)],
                    qkv_own.at[:, j * AD : (j + 1) * AD],
                    local.at[4 + j],
                )
            )
        for copy in copies + first:
            copy.start()

        def other(k, m):
            mask = sum(bit for i, bit in enumerate(TP) if m >> i & 1)
            flipped = sum((bit * (1 - 2 * ((r // bit) % 2)) for bit in bits_of(mask)), r)
            return {"shard": lax.rem(s + k, S), "replica": flipped}

        group = [(k, m) for k in range(S) for m in range(NT) if k or m]
        plane = range(1, ND)

        def mate(m):
            mask = sum(bit for i, bit in enumerate(DP) if m >> i & 1)
            return {"replica": sum((bit * (1 - 2 * ((r // bit) % 2)) for bit in bits_of(mask)), r)}

        barrier = pltpu.get_barrier_semaphore()
        for k, m in group:
            pl.semaphore_signal(barrier, inc=1, device_id=other(k, m), device_id_type=MESH)
        for m in plane:
            pl.semaphore_signal(barrier, inc=1, device_id=mate(m), device_id_type=MESH)
        pl.semaphore_wait(barrier, len(group) + len(plane))

        def small_copy(k, m):
            return pltpu.make_async_remote_copy(
                src_ref=small_ref, dst_ref=small_all.at[t, s], send_sem=small_send.at[k, m],
                recv_sem=small_recv.at[k, m], device_id=other(k, m), device_id_type=MESH,
            )

        def line(i, j, way, source):
            return pltpu.make_async_remote_copy(
                src_ref=source, dst_ref=gathered[i].at[t, j], send_sem=line_send.at[i, j, way],
                recv_sem=line_recv.at[i, j], device_id={"shard": s + 2 * way - 1}, device_id_type=MESH,
            )

        def across(i, j, b, m, source):
            slot = gathered[i].at[t ^ m, j]
            return pltpu.make_async_remote_copy(
                src_ref=slot if source is None else source, dst_ref=slot, send_sem=tp_send.at[i, j, m | 1 << b],
                recv_sem=tp_recv.at[i, j, m | 1 << b], device_id=partner(TP[b]), device_id_type=MESH,
            )

        def z_copies(w, k, sending):
            to = lax.rem(s + k, S)
            at = (s if sending else lax.rem(s + S - k, S)) * rows + d * part
            at = pl.multiple_of(at, part)
            out = []
            for j in range(1 if w == 0 else 3):
                if w == 0:
                    source = up_ref.at[pl.ds(pl.multiple_of(d * part, part), part), pl.ds(pl.multiple_of((to * NT + t) * FD, FD), FD)]
                    target = up_all.at[pl.ds(at, part), :]
                else:
                    source = qkv_ref.at[
                        pl.ds(pl.multiple_of(d * part, part), part), pl.ds(pl.multiple_of(j * third + (to * NT + t) * AD, AD), AD)
                    ]
                    target = qkv_all.at[pl.ds(at, part), j * AD : (j + 1) * AD]
                out.append(
                    pltpu.make_async_remote_copy(
                        src_ref=source, dst_ref=target, send_sem=z_send.at[k, w + j], recv_sem=z_recv.at[k, w + j],
                        device_id={"shard": to}, device_id_type=MESH,
                    )
                )
            return out

        def shared(w, k, m):
            at = pl.multiple_of(lax.rem(s + S - k, S) * rows + d * part, part)
            slot = (up_all, qkv_all)[w].at[pl.ds(at, part), :]
            return pltpu.make_async_remote_copy(
                src_ref=slot, dst_ref=slot, send_sem=dp_send.at[w, k, m], recv_sem=dp_recv.at[w, k, m],
                device_id=mate(m), device_id_type=MESH,
            )

        mine = (grad_ref, in_ref)
        for k, m in group:
            small_copy(k, m).start()
        for i in range(2):

            @pl.when(s + 1 < S)
            def _():
                line(i, s, 1, mine[i]).start()

            @pl.when(s > 0)
            def _():
                line(i, s, 0, mine[i]).start()

        for k in range(1, S):
            for w in range(2):
                for copy in z_copies(w, k, True):
                    copy.start()
        for i in range(2):
            for b in range(len(TP)):
                across(i, s, b, 0, mine[i]).start()

        def pass_on(i, j, m, top):
            for b in range(top + 1, len(TP)):
                across(i, j, b, m, None).start()

        def from_line(i, k):
            @pl.when(s - k >= 0)
            def _():
                line(i, s - k, 1, gathered[i].at[t, s - k]).wait_recv()

                @pl.when(s + 1 < S)
                def _():
                    line(i, s - k, 1, gathered[i].at[t, s - k]).start()

                pass_on(i, s - k, 0, -1)

            @pl.when(s + k < S)
            def _():
                line(i, s + k, 0, gathered[i].at[t, s + k]).wait_recv()

                @pl.when(s > 0)
                def _():
                    line(i, s + k, 0, gathered[i].at[t, s + k]).start()

                pass_on(i, s + k, 0, -1)

        for copy in first:
            copy.wait()
        at_own = pl.multiple_of(s * rows, rows)
        second = [
            pltpu.make_async_copy(in_own, in_all.at[t, s], local.at[1]),
            pltpu.make_async_copy(grad_own, grad_all.at[t, s], local.at[2]),
            pltpu.make_async_copy(up_own, up_all.at[pl.ds(at_own, rows), :], local.at[3]),
            pltpu.make_async_copy(qkv_own, qkv_all.at[pl.ds(at_own, rows), :], local.at[4]),
        ]
        for copy in second:
            copy.start()

        for k in range(1, S):
            for i in range(2):
                from_line(i, k)
            if k == 1:
                for back in range(1, S):
                    for w in range(2):
                        for copy in z_copies(w, back, False):
                            copy.wait_recv()
                        for m in plane:
                            shared(w, back, m).start()

        for m in range(1, NT):
            top = m.bit_length() - 1
            for i in range(2):
                for j in range(S):
                    across(i, j, top, m ^ (1 << top), None).wait_recv()
                    pass_on(i, j, m, top)
        for k, m in group:
            small_copy(k, m).wait_recv()
        for k in range(1, S):
            for w in range(2):
                for m in plane:
                    shared(w, k, m).wait_recv()

        for i in range(2):
            for j in range(S):

                @pl.when((s + 1 < S) & (j <= s))
                def _():
                    line(i, j, 1, gathered[i].at[t, j]).wait_send()

                @pl.when((s > 0) & (j >= s))
                def _():
                    line(i, j, 0, gathered[i].at[t, j]).wait_send()

                for m in range(NT):
                    for b in range(m.bit_length(), len(TP)):
                        across(i, j, b, m, None).wait_send()
        for k, m in group:
            small_copy(k, m).wait_send()
        for k in range(1, S):
            for w in range(2):
                for copy in z_copies(w, k, True):
                    copy.wait_send()
                for m in plane:
                    shared(w, k, m).wait_send()
        for copy in copies + second:
            copy.wait()

    any_spec = pl.BlockSpec(memory_space=pl.ANY)
    shapes = [jax.ShapeDtypeStruct((NT, S) + v.shape, BF16) for v in tokens]
    shapes += [jax.ShapeDtypeStruct((S * rows, width), BF16) for width in widths]
    small_all, grad_all, in_all, up, qkv = pl.pallas_call(
        kernel,
        out_shape=shapes,
        in_specs=[any_spec] * 5,
        out_specs=[any_spec] * 5,
        scratch_shapes=[
            pltpu.VMEM((T, D), BF16),
            pltpu.VMEM((T, D), BF16),
            pltpu.VMEM((rows, FD), BF16),
            pltpu.VMEM((rows, 3 * AD), BF16),
            pltpu.SemaphoreType.DMA((S, NT)),
            pltpu.SemaphoreType.DMA((S, NT)),
            pltpu.SemaphoreType.DMA((2, S, 2)),
            pltpu.SemaphoreType.DMA((2, S)),
            pltpu.SemaphoreType.DMA((2, S, NT)),
            pltpu.SemaphoreType.DMA((2, S, NT)),
            pltpu.SemaphoreType.DMA((S, 4)),
            pltpu.SemaphoreType.DMA((S, 4)),
            pltpu.SemaphoreType.DMA((2, S, ND)),
            pltpu.SemaphoreType.DMA((2, S, ND)),
            pltpu.SemaphoreType.DMA((7,)),
        ],
        compiler_params=pltpu.CompilerParams(collective_id=0, has_side_effects=True),
        name="fetch",
    )(*tokens, w_up, w_qkv)
    return in_all, grad_all, small_all, up, qkv

def layer(in_all, grad_all, tables, norms, bias_qkv, up, qkv, b_up, w_down, w_out, t, T, tile):
    N, D = in_all.shape
    FD = up.shape[1]
    AD = qkv.shape[1] // 3
    heads = AD // HD
    scale = HD ** (-0.5)

    def kernel(
        t_ref, in_ref, grad_ref, tables_ref, norms_ref, bias_qkv_ref, up_ref, qkv_ref, b_up_ref, down_ref, out_ref,
        first_ref, second_ref, attended_ref, activated_ref, mixed_ref, hidden_ref, branch_ref, inner_ref,
        sum_qkv_ref, sum_up_ref, sum_norm_ref,
    ):
        @pl.when(pl.program_id(0) == 0)
        def _():
            sum_qkv_ref[...] = jnp.zeros_like(sum_qkv_ref)
            sum_up_ref[...] = jnp.zeros_like(sum_up_ref)
            sum_norm_ref[...] = jnp.zeros_like(sum_norm_ref)

        gain_1, shift_1, gain_2, shift_2 = [norms_ref[i : i + 1, :] for i in range(4)]
        wide = in_ref[...].astype(F32)
        offsets = wide - jnp.mean(wide, axis=-1, keepdims=True)
        inverse = lax.rsqrt(jnp.mean(offsets * offsets, axis=-1, keepdims=True) + epsilon)
        normed = offsets * inverse
        first = (normed * gain_1 + shift_1).astype(BF16)
        second = (normed * gain_2 + shift_2).astype(BF16)
        first_ref[...] = first
        second_ref[...] = second
        grad = grad_ref[...]

        mixed = dot(first, qkv_ref[...], 1, 0) + bias_qkv_ref[...]
        attended_grad = dot(grad, out_ref[...], 1, 1).astype(BF16)
        straight, ahead, back, position = [tables_ref[i] for i in range(4)]

        def turn(value, sign):
            low = value[:, :128]
            low = low * straight + sign * (pltpu.roll(low, 96, 1) * ahead + pltpu.roll(low, 32, 1) * back)
            return jnp.concatenate([low, value[:, 128:]], axis=1)

        row = lax.broadcasted_iota(jnp.int32, (T, T), 0)
        col = lax.broadcasted_iota(jnp.int32, (T, T), 1)
        away = (row - col).astype(F32)
        attended, query_grads, key_grads, value_grads = [], [], [], []
        for h in range(heads):
            at = slice(h * HD, (h + 1) * HD)
            queries = turn(mixed[:, at], 1.0).astype(BF16)
            keys = turn(mixed[:, AD + h * HD : AD + (h + 1) * HD], 1.0).astype(BF16)
            values = mixed[:, 2 * AD + h * HD : 2 * AD + (h + 1) * HD].astype(BF16)
            parts = [[], [], [], []]
            for b in range(tile // T):
                rows = slice(b * T, (b + 1) * T)
                q, k, v, u = queries[rows], keys[rows], values[rows], attended_grad[rows, at]
                allowed = (away >= 0) & (away <= position[rows, :1])
                scores = jnp.where(allowed, dot(q, k, 1, 1) * scale, -1e30)
                peak = jnp.max(scores, axis=-1, keepdims=True)
                logsum = peak + jnp.log(jnp.sum(jnp.exp(scores - peak), axis=-1, keepdims=True))
                probs = jnp.exp(scores - logsum)
                low = probs.astype(BF16)
                parts[0].append(dot(low, v, 1, 0).astype(BF16))
                dprobs = dot(u, v, 1, 1)
                total = jnp.sum(probs * dprobs, axis=-1, keepdims=True)
                dscores = (probs * (dprobs - total) * scale).astype(BF16)
                parts[1].append(dot(dscores, k, 1, 0))
                parts[2].append(dot(dscores, q, 0, 0))
                parts[3].append(dot(low, u, 0, 0))
            joined = [jnp.concatenate(v, axis=0) for v in parts]
            attended.append(joined[0])
            query_grads.append(turn(joined[1], -1.0))
            key_grads.append(turn(joined[2], -1.0))
            value_grads.append(joined[3])
        attended = jnp.concatenate(attended, axis=1)
        attended_ref[...] = attended
        mixed_grad = jnp.concatenate(query_grads + key_grads + value_grads, axis=1)
        sum_qkv_ref[...] += jnp.sum(mixed_grad, axis=0, keepdims=True)
        mixed_low = mixed_grad.astype(BF16)
        mixed_ref[...] = mixed_low

        pre = dot(second, up_ref[...], 1, 0) + b_up_ref[...].astype(F32)
        bell = 0.5 * (1.0 + lax.erf(pre * 0.7071067811865476))
        activated = (pre * bell).astype(BF16)
        activated_ref[...] = activated
        slope = bell + pre * jnp.exp(-0.5 * pre * pre) * 0.3989422804014327
        hidden_grad = dot(grad, down_ref[...], 1, 1) * slope
        sum_up_ref[...] += jnp.sum(hidden_grad, axis=0, keepdims=True)
        hidden_low = hidden_grad.astype(BF16)
        hidden_ref[...] = hidden_low

        branch = dot(attended, out_ref[...], 1, 0) + dot(activated, down_ref[...], 1, 0)
        branch_ref[...] = branch.astype(BF16)

        first_grad = dot(mixed_low, qkv_ref[...], 1, 1)
        second_grad = dot(hidden_low, up_ref[...], 1, 1)
        sum_norm_ref[0:1, :] += jnp.sum(first_grad * normed, axis=0, keepdims=True)
        sum_norm_ref[1:2, :] += jnp.sum(first_grad, axis=0, keepdims=True)
        sum_norm_ref[2:3, :] += jnp.sum(second_grad * normed, axis=0, keepdims=True)
        sum_norm_ref[3:4, :] += jnp.sum(second_grad, axis=0, keepdims=True)
        inner_ref[...] = (first_grad * gain_1 + second_grad * gain_2).astype(BF16)

    def rows(width):
        return pl.BlockSpec((tile, width), lambda i, t_ref: (i, 0))

    def whole(shape, index=lambda i, t_ref: (0, 0)):
        return pl.BlockSpec(shape, index, pipeline_mode=pl.Buffered(1))

    widths = [D, D, AD, FD, 3 * AD, FD, D, D]
    flops = 2 * N * D * (2 * 3 * AD + 2 * FD + 2 * FD + 2 * AD)
    return pl.pallas_call(
        kernel,
        out_shape=[jax.ShapeDtypeStruct((N, w), BF16) for w in widths]
        + [jax.ShapeDtypeStruct(v, F32) for v in ((1, 3 * AD), (1, FD), (4, D))],
        grid_spec=pltpu.PrefetchScalarGridSpec(
            num_scalar_prefetch=1,
            grid=(N // tile,),
            in_specs=[
                rows(D),
                rows(D),
                pl.BlockSpec((4, tile, 128), lambda i, t_ref: (0, i, 0)),
                whole((4, D)),
                whole((1, 3 * AD)),
                whole((D, FD)),
                whole((D, 3 * AD)),
                whole((1, FD), lambda i, t_ref: (0, t_ref[0])),
                whole((FD, D), lambda i, t_ref: (t_ref[0], 0)),
                whole((AD, D), lambda i, t_ref: (t_ref[0], 0)),
            ],
            out_specs=[rows(w) for w in widths] + [whole((1, 3 * AD)), whole((1, FD)), whole((4, D))],
        ),
        compiler_params=pltpu.CompilerParams(
            dimension_semantics=("arbitrary",), vmem_limit_bytes=63 * 2**20
        ),
        cost_estimate=pl.CostEstimate(flops=flops, bytes_accessed=50 * 2**20, transcendentals=N * FD * 2),
        name="layer",
    )(t.reshape(1), in_all, grad_all, tables, norms, bias_qkv, up, qkv, b_up.reshape(1, -1), w_down, w_out)

def grads(first, second, attended, activated, mixed, hidden, grad, S, R, TP, DP):
    N, D = grad.shape
    FD, AD = activated.shape[1], attended.shape[1]
    NT, ND, steps = 2 ** len(TP), 2 ** len(DP), len(DP)
    rows = D // S
    names = ("up", "qkv", "down", "out")
    lefts = (second, first, activated, attended)
    rights = (hidden, mixed, grad, grad)
    which_right = (0, 1, 2, 2)
    pieces = []
    for left, right, lead, mid in zip(lefts, rights, (S, S, 1, 1), (NT, NT, 1, 1)):
        pieces.append((lead, mid, left.shape[1] // (lead * ND * mid * 2), right.shape[1]))
    ways = []
    for way in (DP, DP[::-1]):
        ways.append([(bit, 1 << DP.index(bit)) for bit in way])

    def masks(bits):
        out = [0]
        for _, bit in bits:
            out += [v | bit for v in out]
        return sorted(out)

    slots = []
    for way in ways:
        table = {}
        for j in range(steps):
            for u in masks(way[j + 1 :]):
                table[j, u] = len(table)
        slots.append(table)

    def kernel(
        second_hbm, first_hbm, activated_hbm, attended_hbm, hidden_hbm, mixed_hbm, grad_hbm,
        own_up, own_qkv, own_down, own_out,
        second_v, first_v, activated_v, attended_v, hidden_v, mixed_v, grad_v,
        part_up, part_qkv, part_down, part_out, came_up, came_qkv, came_down, came_out, all_up, all_qkv,
        load, dp_send, dp_recv, z_send, z_recv,
    ):
        s = lax.axis_index("shard")
        r = lax.axis_index("replica")
        t = sum(((r // bit) % 2 * 2**i for i, bit in enumerate(TP)), jnp.int32(0))
        d = sum(((r // bit) % 2 * 2**i for i, bit in enumerate(DP)), jnp.int32(0))

        def flipped(value, mask):
            return sum((bit * (1 - 2 * ((value // bit) % 2)) for bit in bits_of(mask)), value)

        def other(k, m):
            mask = sum(bit for i, bit in enumerate(TP) if m >> i & 1)
            return {"shard": lax.rem(s + k, S), "replica": flipped(r, mask)}

        loads = []
        order = ((hidden_hbm, hidden_v), (second_hbm, second_v), (mixed_hbm, mixed_v), (first_hbm, first_v),
                 (grad_hbm, grad_v), (activated_hbm, activated_v), (attended_hbm, attended_v))
        for i, (source, target) in enumerate(order):
            loads.append(pltpu.make_async_copy(source, target, load.at[i]))
            loads[-1].start()

        group = [(k, m) for k in range(S) for m in range(NT) if k or m]
        barrier = pltpu.get_barrier_semaphore()
        for k, m in group:
            pl.semaphore_signal(barrier, inc=1, device_id=other(k, m), device_id_type=MESH)
        for bit in DP:
            pl.semaphore_signal(barrier, inc=1, device_id={"replica": flipped(r, bit)}, device_id_type=MESH)
        pl.semaphore_wait(barrier, len(group) + steps)

        left_refs = (second_v, first_v, activated_v, attended_v)
        right_refs = (hidden_v, mixed_v, grad_v, grad_v)
        part = (part_up, part_qkv, part_down, part_out)
        came = (came_up, came_qkv, came_down, came_out)
        own = (own_up, own_qkv, own_down, own_out)

        def product(i):
            lead, mid, n, _ = pieces[i]
            if lead > 1:
                width = ND * mid * 2 * n

                def body(l, carry):
                    cols = pl.ds(pl.multiple_of(l * width, width), width)
                    value = dot(left_refs[i][:, cols], right_refs[i][...], 0, 0).astype(BF16)
                    for q in range(ND):
                        for c in range(mid):
                            for h in range(2):
                                at = ((q * mid + c) * 2 + h) * n
                                part[i][h, q, l, c] = value[at : at + n]
                    return carry

                lax.fori_loop(0, lead, body, 0)
            else:
                total = ND * 2 * n
                chunk = min(total, 512)
                per = chunk // (2 * n)

                def body(l, carry):
                    cols = pl.ds(pl.multiple_of(l * chunk, chunk), chunk)
                    value = dot(left_refs[i][:, cols], right_refs[i][...], 0, 0).astype(BF16)
                    for q in range(per):
                        for h in range(2):
                            at = (q * 2 + h) * n
                            part[i][h, l * per + q, 0, 0] = value[at : at + n]
                    return carry

                lax.fori_loop(0, total // chunk, body, 0)

        def halving(i, h, j, u):
            bit, dbit = ways[h][j]
            slot = slots[h][j, u]
            return pltpu.make_async_remote_copy(
                src_ref=part[i].at[h, flipped(d, dbit | u)], dst_ref=came[i].at[h, slot],
                send_sem=dp_send.at[i, h, slot], recv_sem=dp_recv.at[i, h, slot],
                device_id={"replica": flipped(r, bit)}, device_id_type=MESH,
            )

        def summed(i, h, mask, count, write):
            lead, mid, _, _ = pieces[i]
            at = flipped(d, mask)
            for j in range(count):
                halving(i, h, j, mask).wait_recv()

            def body(l, carry):
                for c in range(mid):
                    value = part[i][h, at, l, c].astype(F32)
                    for j in range(count):
                        value = value + came[i][h, slots[h][j, mask], l, c].astype(F32)
                    write(l, c, value.astype(BF16))
                return carry

            lax.fori_loop(0, lead, body, 0)

        def step(i, j):
            for h in range(2):
                for u in masks(ways[h][j + 1 :]):
                    mask = ways[h][j][1] | u
                    at = flipped(d, mask)
                    if j:

                        def write(l, c, value, h=h, at=at):
                            part[i][h, at, l, c] = value

                        summed(i, h, mask, j, write)
                    halving(i, h, j, u).start()

        everyone = (all_up, all_qkv)

        def to_shard(i, h, k, m):
            there = lax.rem(s + k, S)
            return pltpu.make_async_remote_copy(
                src_ref=part[i].at[h, d, there, flipped(t, m)], dst_ref=everyone[i].at[s, t, h],
                send_sem=z_send.at[i, h, k, m], recv_sem=z_recv.at[i, h, k, m],
                device_id=other(k, m), device_id_type=MESH,
            )

        def last(i):
            for h in range(2):
                if i < 2:

                    def write(l, c, value, h=h):
                        part[i][h, d, l, c] = value

                else:

                    def write(l, c, value, h=h):
                        own[i][h] = value

                summed(i, h, 0, steps, write)
            if i < 2:
                for k, m in group:
                    for h in range(2):
                        to_shard(i, h, k, m).start()
                for h in range(2):
                    everyone[i][s, t, h] = part[i][h, d, s, t]

        def collect(i):
            width = pieces[i][3]
            runs = 1 if i == 0 else 3
            n = width // runs
            for k, m in group:
                for h in range(2):
                    to_shard(i, h, k, m).wait_recv()
            for h in range(2):
                for j in range(S):
                    for u in range(NT):
                        block = everyone[i][j, u, h]
                        for v in range(runs):
                            at = (v * S * NT + j * NT + u) * n
                            own[i][h, :, at : at + n] = block[:, v * n : (v + 1) * n]

        loads[0].wait()
        loads[1].wait()
        product(0)
        step(0, 0)
        loads[2].wait()
        loads[3].wait()
        product(1)
        step(1, 0)
        for j in range(1, steps):
            step(0, j)
        loads[4].wait()
        loads[5].wait()
        product(2)
        step(2, 0)
        for j in range(1, steps):
            step(1, j)
        loads[6].wait()
        product(3)
        step(3, 0)
        last(0)
        for j in range(1, steps):
            step(2, j)
        last(1)
        for j in range(1, steps):
            step(3, j)
        collect(0)
        last(2)
        last(3)
        collect(1)

        for i in range(4):
            for h in range(2):
                for j, u in slots[h]:
                    halving(i, h, j, u).wait_send()
        for i in range(2):
            for h in range(2):
                for k, m in group:
                    to_shard(i, h, k, m).wait_send()

    def scratch(value):
        return pltpu.VMEM(value.shape, BF16)

    any_spec = pl.BlockSpec(memory_space=pl.ANY)
    operands = (second, first, activated, attended, hidden, mixed, grad)
    outs = []
    for i, (lead, mid, n, width) in enumerate(pieces):
        outs.append(jax.ShapeDtypeStruct((2, n, width * S * NT if lead > 1 else width), BF16))
    sent = sum(2 * (ND - 1) * a * b * n * w * 2 for a, b, n, w in pieces)
    return pl.pallas_call(
        kernel,
        out_shape=outs,
        in_specs=[any_spec] * 7,
        out_specs=[pl.BlockSpec(memory_space=pltpu.VMEM)] * 4,
        scratch_shapes=[scratch(v) for v in operands]
        + [pltpu.VMEM((2, ND) + piece, BF16) for piece in pieces]
        + [pltpu.VMEM((2, ND - 1) + piece, BF16) for piece in pieces]
        + [pltpu.VMEM((S, NT, 2) + piece[2:], BF16) for piece in pieces[:2]]
        + [
            pltpu.SemaphoreType.DMA((7,)),
            pltpu.SemaphoreType.DMA((4, 2, ND - 1)),
            pltpu.SemaphoreType.DMA((4, 2, ND - 1)),
            pltpu.SemaphoreType.DMA((2, 2, S, NT)),
            pltpu.SemaphoreType.DMA((2, 2, S, NT)),
        ],
        compiler_params=pltpu.CompilerParams(
            collective_id=1, has_side_effects=True, vmem_limit_bytes=63 * 2**20
        ),
        cost_estimate=pl.CostEstimate(
            flops=2 * N * sum(v.shape[1] * w.shape[1] for v, w in zip(lefts, rights)),
            bytes_accessed=sent * 8, transcendentals=0,
        ),
        name="grads",
    )(*operands)


def solution(mesh):
    S = mesh.shape["shard"]
    R = mesh.shape["replica"]
    TP = [1] if R > 1 and H % (2 * S) == 0 else []
    DP = [bit for bit in bits_of(R - 1) if bit not in TP]
    NT, ND = 2 ** len(TP), 2 ** len(DP)
    ring = list(range(S))[:1] + list(range(1, S, 2)) + list(range(2, S, 2))[::-1]
    place = [ring.index(i) for i in range(S)]

    def to_ring(value, hops):
        return lax.ppermute(value, "shard", [(ring[i], ring[(i + hops) % S]) for i in range(S)])

    def flip(value, bit):
        return lax.ppermute(value, "replica", [(i, i ^ bit) for i in range(R)])

    def body(
        block_in, positions, out_grad, w_qkv, b_qkv, w_out, b_out, w_up, b_up, w_down, b_down,
        first_gain, first_shift, second_gain, second_shift,
    ):
        T, D = block_in.shape
        rows = w_qkv.shape[0]
        FS = w_down.shape[0]
        FD = FS // NT
        HN = H // S // NT
        AD = HN * HD
        G = NT * S
        s = lax.axis_index("shard")
        r = lax.axis_index("replica")
        mine = {bit: (r // bit) % 2 for bit in bits_of(R - 1)}
        t = sum((mine[bit] * 2**i for i, bit in enumerate(TP)), jnp.int32(0))
        p = jnp.array(place, jnp.int32)[s]
        ring_array = jnp.array(ring, jnp.int32)
        behind = [ring_array[(p - k) % S] for k in range(S)]
        ahead = [ring_array[(p + k) % S] for k in range(S)]
        order = (p - jnp.array(place, jnp.int32)) % S

        small = jnp.concatenate(
            [b_qkv, b_out, b_down, first_gain, first_shift, second_gain, second_shift,
             positions.astype(BF16)]
        )
        small = small.reshape(-1, 128)
        x_all, grad_all, small_all, up, qkv = fetch(
            block_in, out_grad, small, w_up, w_qkv, S, R, TP, DP, FD, AD
        )
        small_all = small_all.reshape(NT, S, -1)
        natural = small_all[0]
        sizes = [b_qkv.shape[0]] + [rows] * 6
        starts = [sum(sizes[:i]) for i in range(len(sizes))]
        whole = [natural[:, a : a + n].reshape(-1).astype(F32) for a, n in zip(starts, sizes)]
        full_b_qkv, full_b_out, full_b_down, gain_1, shift_1, gain_2, shift_2 = whole
        pos_all = small_all[:, :, sum(sizes) :].reshape(-1).astype(F32)
        x_all = x_all.reshape(G * T, D)
        grad_all = grad_all.reshape(G * T, D)
        bias_qkv = lax.dynamic_slice_in_dim(
            full_b_qkv.reshape(3, -1), (s * NT + t) * AD, AD, 1
        ).reshape(-1)
        part = rows // ND
        d = sum((mine[bit] * 2**i for i, bit in enumerate(DP)), jnp.int32(0))

        def normed_of(block):
            wide = block.astype(F32)
            offsets = wide - jnp.mean(wide, axis=-1, keepdims=True)
            inverse = lax.rsqrt(jnp.mean(offsets * offsets, axis=-1, keepdims=True) + epsilon)
            return offsets * inverse, inverse

        half = ROT // 2
        cosine, sine = rotary_tables(pos_all)
        pad = jnp.zeros((G * T, 128 - ROT), F32)
        none = jnp.zeros((G * T, half), F32)
        tables = jnp.stack(
            [
                jnp.concatenate([cosine, cosine, pad + 1.0], axis=1),
                jnp.concatenate([-sine, none, pad], axis=1),
                jnp.concatenate([none, sine, pad], axis=1),
                jnp.broadcast_to(pos_all[:, None], (G * T, 128)),
            ]
        )
        norms = jnp.stack([gain_1, shift_1, gain_2, shift_2])
        (
            first_low, second_low, attended, activated, mixed_low, hidden_low, branch_part, inner_part,
            sum_b_qkv, sum_b_up, sum_norms,
        ) = layer(
            x_all, grad_all, tables, norms, bias_qkv.reshape(1, -1), up, qkv, b_up, w_down, w_out, t, T, 2 * T
        )
        sum_b_qkv, sum_b_up = sum_b_qkv.reshape(-1), sum_b_up.reshape(-1)

        def reduce_tokens(parts):
            parts = parts.reshape(NT, S, T, -1)

            def of(m):
                return lax.dynamic_index_in_dim(parts, t ^ m, 0, keepdims=False)

            held = {m: of(m) for m in range(NT)}
            for i in reversed(range(len(TP))):
                for j in range(2**i):
                    held[j] = held[j].astype(F32) + flip(held[j + 2**i].astype(BF16), TP[i]).astype(F32)
            total = held[0]

            def block(j):
                return lax.dynamic_index_in_dim(total, j, 0, keepdims=False)

            got = [to_ring(block(ahead[k]).astype(BF16), k) for k in range(1, S)]
            return sum((g.astype(F32) for g in got), block(s).astype(F32))

        branch = reduce_tokens(branch_part)
        block_out = (block_in.astype(F32) + branch + full_b_out + full_b_down).astype(BF16)

        def share(halves, write, result):
            for half, (value, order) in enumerate(zip(halves, (DP, DP[::-1]))):
                value = lax.optimization_barrier(value)
                pieces = {0: value}
                for bit in list(order) + TP:
                    pieces.update({m | bit: flip(v, bit) for m, v in list(pieces.items())})
                for m, piece in pieces.items():
                    dmask = sum(2**i for i, bit in enumerate(DP) if m & bit)
                    tmask = sum(2**i for i, bit in enumerate(TP) if m & bit)
                    result = write(result, piece.astype(F32), d ^ dmask, t ^ tmask, half)
            return result

        def placed_rows(halves, group_rows, shape):
            n = halves.shape[1]

            def write(res, v, dd, tt, half):
                if group_rows is None:
                    at = (dd * NT + tt) * 2 * n
                else:
                    at = tt * group_rows + dd * 2 * n
                return lax.dynamic_update_slice(res, v, (at + half * n, 0))

            return share([halves[0], halves[1]], write, unwritten(shape, F32))

        own_up, own_qkv, own_down, own_out = grads(
            first_low, second_low, attended, activated, mixed_low, hidden_low, grad_all, S, R, TP, DP
        )
        grad_w_down = placed_rows(own_down, FD, w_down.shape)
        grad_w_up = placed_rows(own_up, None, w_up.shape)
        grad_w_qkv = placed_rows(own_qkv, None, w_qkv.shape)
        grad_w_out = placed_rows(own_out, AD, w_out.shape)

        scaled = reduce_tokens(inner_part)
        normed_own, inverse_own = normed_of(block_in)
        term = inverse_own * (
            scaled
            - jnp.mean(scaled, axis=-1, keepdims=True)
            - normed_own * jnp.mean(scaled * normed_own, axis=-1, keepdims=True)
        )
        wide_grad = out_grad.astype(F32)
        in_grad = (wide_grad + term).astype(BF16)

        def placed(length, value, offset):
            return lax.dynamic_update_slice(jnp.zeros((length,), F32), value, (offset,))

        width = w_out.shape[0] * S
        col = (s * NT + t) * AD
        sums = [placed(width, sum_b_qkv[i * AD : (i + 1) * AD], col) for i in range(3)]
        sums += [jnp.sum(wide_grad, axis=0), placed(FS * S, sum_b_up, s * FS + t * FD)]
        sums += [sum_norms[i] for i in range(4)]
        lengths = [v.shape[0] for v in sums]
        sums = jnp.concatenate(sums)
        for bit in bits_of(R - 1):
            sums = sums + flip(sums, bit)
        for bit in bits_of(S - 1):
            sums = sums + lax.ppermute(sums, "shard", [(i, i ^ bit) for i in range(S)])
        at = [sum(lengths[:i]) for i in range(len(lengths))]

        def owned(start, length):
            return lax.dynamic_slice_in_dim(sums, start + s * (length // S), length // S, 0)

        grad_b_qkv = owned(at[0], 3 * width)
        grad_b_out = owned(at[3], D)
        grad_b_up = owned(at[4], FS * S)
        smalls = [owned(at[5 + i], D) for i in range(4)]
        return (
            block_out, in_grad, grad_w_qkv, grad_b_qkv, grad_w_out, grad_b_out, grad_w_up, grad_b_up,
            grad_w_down, grad_b_out, *smalls,
        )

    rows2, row1, par2, par1 = P(("shard", "replica"), None), P(("shard", "replica")), P("shard", None), P("shard")
    return jax.shard_map(
        body,
        mesh=mesh,
        in_specs=(
            rows2, row1, rows2, par2, par1, par2, par1, par2, par1, par2, par1, par1, par1, par1, par1,
        ),
        out_specs=(
            rows2, rows2, par2, par1, par2, par1, par2, par1, par2, par1, par1, par1, par1, par1,
        ),
        check_vma=False,
    )
```

```python
import jax
import jax.numpy as jnp
from jax import lax
from jax.experimental import pallas as pl
from jax.experimental.pallas import tpu as pltpu
from jax.sharding import PartitionSpec as P

H = 8
HD = 256
ROT = 64

epsilon = 1e-05


F32 = jnp.float32
BF16 = jnp.bfloat16
MESH = pl.DeviceIdType.MESH


def rotary_freqs():
    freqs = 10000.0 ** (-(jnp.arange(ROT // 2, dtype=F32) * (2.0 / ROT)))
    return jnp.concatenate([freqs, freqs, jnp.zeros((128 - ROT,), F32)]).reshape(1, 128)


def dot(left, right, left_dim, right_dim):
    return lax.dot_general(
        left, right, (((left_dim,), (right_dim,)), ((), ())), preferred_element_type=F32
    )


def unwritten(shape, dtype):
    return pl.pallas_call(
        lambda out_ref: None,
        out_shape=jax.ShapeDtypeStruct(shape, dtype),
        out_specs=pl.BlockSpec(memory_space=pl.ANY),
    )()


def bits_of(mask):
    return [1 << i for i in range(mask.bit_length()) if mask >> i & 1]

def fetch(block_in, out_grad, small, w_up, w_qkv, S, R, TP, DP, FD, AD):
    T, D = block_in.shape
    rows = w_up.shape[0]
    NT, ND = 2 ** len(TP), 2 ** len(DP)
    part = rows // ND
    third = w_qkv.shape[1] // 3
    tokens = (small, out_grad, block_in)
    widths = (FD, 3 * AD)

    def kernel(
        small_ref, grad_ref, in_ref, up_ref, qkv_ref, small_all, grad_all, in_all, up_all, qkv_all,
        in_own, grad_own, up_own, qkv_own, small_send, small_recv, line_send, line_recv, tp_send, tp_recv, z_send, z_recv, dp_send, dp_recv, local,
    ):
        s = lax.axis_index("shard")
        r = lax.axis_index("replica")
        t = sum(((r // bit) % 2 * 2**i for i, bit in enumerate(TP)), jnp.int32(0))
        d = sum(((r // bit) % 2 * 2**i for i, bit in enumerate(DP)), jnp.int32(0))

        def partner(bit):
            return {"replica": r + bit - 2 * bit * ((r // bit) % 2)}

        copies = [pltpu.make_async_copy(small_ref, small_all.at[t, s], local.at[0])]
        gathered = (grad_all, in_all)
        first = [
            pltpu.make_async_copy(in_ref, in_own, local.at[1]),
            pltpu.make_async_copy(grad_ref, grad_own, local.at[2]),
            pltpu.make_async_copy(
                up_ref.at[:, pl.ds(pl.multiple_of((s * NT + t) * FD, FD), FD)], up_own, local.at[3]
            ),
        ]
        for j in range(3):
            first.append(
                pltpu.make_async_copy(
                    qkv_ref.at[:, pl.ds(pl.multiple_of(j * third + (s * NT + t) * AD, AD), AD)],
                    qkv_own.at[:, j * AD : (j + 1) * AD],
                    local.at[4 + j],
                )
            )
        for copy in copies + first:
            copy.start()

        def other(k, m):
            mask = sum(bit for i, bit in enumerate(TP) if m >> i & 1)
            flipped = sum((bit * (1 - 2 * ((r // bit) % 2)) for bit in bits_of(mask)), r)
            return {"shard": lax.rem(s + k, S), "replica": flipped}

        group = [(k, m) for k in range(S) for m in range(NT) if k or m]
        plane = range(1, ND)

        def mate(m):
            mask = sum(bit for i, bit in enumerate(DP) if m >> i & 1)
            return {"replica": sum((bit * (1 - 2 * ((r // bit) % 2)) for bit in bits_of(mask)), r)}

        barrier = pltpu.get_barrier_semaphore()
        for k, m in group:
            pl.semaphore_signal(barrier, inc=1, device_id=other(k, m), device_id_type=MESH)
        for m in plane:
            pl.semaphore_signal(barrier, inc=1, device_id=mate(m), device_id_type=MESH)
        pl.semaphore_wait(barrier, len(group) + len(plane))

        def small_copy(k, m):
            return pltpu.make_async_remote_copy(
                src_ref=small_ref, dst_ref=small_all.at[t, s], send_sem=small_send.at[k, m],
                recv_sem=small_recv.at[k, m], device_id=other(k, m), device_id_type=MESH,
            )

        def line(i, j, way, source):
            return pltpu.make_async_remote_copy(
                src_ref=source, dst_ref=gathered[i].at[t, j], send_sem=line_send.at[i, j, way],
                recv_sem=line_recv.at[i, j], device_id={"shard": s + 2 * way - 1}, device_id_type=MESH,
            )

        def across(i, j, b, m, source):
            slot = gathered[i].at[t ^ m, j]
            return pltpu.make_async_remote_copy(
                src_ref=slot if source is None else source, dst_ref=slot, send_sem=tp_send.at[i, j, m | 1 << b],
                recv_sem=tp_recv.at[i, j, m | 1 << b], device_id=partner(TP[b]), device_id_type=MESH,
            )

        def z_copies(w, k, sending):
            to = lax.rem(s + k, S)
            at = (s if sending else lax.rem(s + S - k, S)) * rows + d * part
            at = pl.multiple_of(at, part)
            out = []
            for j in range(1 if w == 0 else 3):
                if w == 0:
                    source = up_ref.at[pl.ds(pl.multiple_of(d * part, part), part), pl.ds(pl.multiple_of((to * NT + t) * FD, FD), FD)]
                    target = up_all.at[pl.ds(at, part), :]
                else:
                    source = qkv_ref.at[
                        pl.ds(pl.multiple_of(d * part, part), part), pl.ds(pl.multiple_of(j * third + (to * NT + t) * AD, AD), AD)
                    ]
                    target = qkv_all.at[pl.ds(at, part), j * AD : (j + 1) * AD]
                out.append(
                    pltpu.make_async_remote_copy(
                        src_ref=source, dst_ref=target, send_sem=z_send.at[k, w + j], recv_sem=z_recv.at[k, w + j],
                        device_id={"shard": to}, device_id_type=MESH,
                    )
                )
            return out

        def shared(w, k, m):
            at = pl.multiple_of(lax.rem(s + S - k, S) * rows + d * part, part)
            slot = (up_all, qkv_all)[w].at[pl.ds(at, part), :]
            return pltpu.make_async_remote_copy(
                src_ref=slot, dst_ref=slot, send_sem=dp_send.at[w, k, m], recv_sem=dp_recv.at[w, k, m],
                device_id=mate(m), device_id_type=MESH,
            )

        mine = (grad_ref, in_ref)
        for k, m in group:
            small_copy(k, m).start()
        for i in range(2):

            @pl.when(s + 1 < S)
            def _():
                line(i, s, 1, mine[i]).start()

            @pl.when(s > 0)
            def _():
                line(i, s, 0, mine[i]).start()

        for k in range(1, S):
            for w in range(2):
                for copy in z_copies(w, k, True):
                    copy.start()
        for i in range(2):
            for b in range(len(TP)):
                across(i, s, b, 0, mine[i]).start()

        def pass_on(i, j, m, top):
            for b in range(top + 1, len(TP)):
                across(i, j, b, m, None).start()

        def from_line(i, k):
            @pl.when(s - k >= 0)
            def _():
                line(i, s - k, 1, gathered[i].at[t, s - k]).wait_recv()

                @pl.when(s + 1 < S)
                def _():
                    line(i, s - k, 1, gathered[i].at[t, s - k]).start()

                pass_on(i, s - k, 0, -1)

            @pl.when(s + k < S)
            def _():
                line(i, s + k, 0, gathered[i].at[t, s + k]).wait_recv()

                @pl.when(s > 0)
                def _():
                    line(i, s + k, 0, gathered[i].at[t, s + k]).start()

                pass_on(i, s + k, 0, -1)

        for copy in first:
            copy.wait()
        at_own = pl.multiple_of(s * rows, rows)
        second = [
            pltpu.make_async_copy(in_own, in_all.at[t, s], local.at[1]),
            pltpu.make_async_copy(grad_own, grad_all.at[t, s], local.at[2]),
            pltpu.make_async_copy(up_own, up_all.at[pl.ds(at_own, rows), :], local.at[3]),
            pltpu.make_async_copy(qkv_own, qkv_all.at[pl.ds(at_own, rows), :], local.at[4]),
        ]
        for copy in second:
            copy.start()

        for k in range(1, S):
            for i in range(2):
                from_line(i, k)
            if k == 1:
                for back in range(1, S):
                    for w in range(2):
                        for copy in z_copies(w, back, False):
                            copy.wait_recv()
                        for m in plane:
                            shared(w, back, m).start()

        for m in range(1, NT):
            top = m.bit_length() - 1
            for i in range(2):
                for j in range(S):
                    across(i, j, top, m ^ (1 << top), None).wait_recv()
                    pass_on(i, j, m, top)
        for k, m in group:
            small_copy(k, m).wait_recv()
        for k in range(1, S):
            for w in range(2):
                for m in plane:
                    shared(w, k, m).wait_recv()

        for i in range(2):
            for j in range(S):

                @pl.when((s + 1 < S) & (j <= s))
                def _():
                    line(i, j, 1, gathered[i].at[t, j]).wait_send()

                @pl.when((s > 0) & (j >= s))
                def _():
                    line(i, j, 0, gathered[i].at[t, j]).wait_send()

                for m in range(NT):
                    for b in range(m.bit_length(), len(TP)):
                        across(i, j, b, m, None).wait_send()
        for k, m in group:
            small_copy(k, m).wait_send()
        for k in range(1, S):
            for w in range(2):
                for copy in z_copies(w, k, True):
                    copy.wait_send()
                for m in plane:
                    shared(w, k, m).wait_send()
        for copy in copies + second:
            copy.wait()

    any_spec = pl.BlockSpec(memory_space=pl.ANY)
    shapes = [jax.ShapeDtypeStruct((NT, S) + v.shape, BF16) for v in tokens]
    shapes += [jax.ShapeDtypeStruct((S * rows, width), BF16) for width in widths]
    small_all, grad_all, in_all, up, qkv = pl.pallas_call(
        kernel,
        out_shape=shapes,
        in_specs=[any_spec] * 5,
        out_specs=[any_spec] * 5,
        scratch_shapes=[
            pltpu.VMEM((T, D), BF16),
            pltpu.VMEM((T, D), BF16),
            pltpu.VMEM((rows, FD), BF16),
            pltpu.VMEM((rows, 3 * AD), BF16),
            pltpu.SemaphoreType.DMA((S, NT)),
            pltpu.SemaphoreType.DMA((S, NT)),
            pltpu.SemaphoreType.DMA((2, S, 2)),
            pltpu.SemaphoreType.DMA((2, S)),
            pltpu.SemaphoreType.DMA((2, S, NT)),
            pltpu.SemaphoreType.DMA((2, S, NT)),
            pltpu.SemaphoreType.DMA((S, 4)),
            pltpu.SemaphoreType.DMA((S, 4)),
            pltpu.SemaphoreType.DMA((2, S, ND)),
            pltpu.SemaphoreType.DMA((2, S, ND)),
            pltpu.SemaphoreType.DMA((7,)),
        ],
        compiler_params=pltpu.CompilerParams(collective_id=0, has_side_effects=True),
        name="fetch",
    )(*tokens, w_up, w_qkv)
    return in_all, grad_all, small_all, up, qkv

def layer(in_all, grad_all, small_all, freqs, up, qkv, b_up, w_down, w_out, where, S, NT, T, tile):
    N, D = in_all.shape
    FD = up.shape[1]
    AD = qkv.shape[1] // 3
    FS = w_down.shape[0]
    heads = AD // HD
    scale = HD ** (-0.5)
    width = S * NT * AD
    per = 3 * width // S // 128
    rest = D // S // 128
    base_out = 3 * width // 128
    base_up = base_out + D // 128
    base_norm = base_up + FS * S // 128
    count = base_norm + 4 * D // 128

    def kernel(
        where_ref, in_ref, grad_ref, small_ref, freqs_ref, up_ref, qkv_ref, b_up_ref, down_ref, out_ref,
        first_ref, second_ref, attended_ref, activated_ref, mixed_ref, hidden_ref, branch_ref, inner_ref, sums_ref,
        wide_small, norms_ref, bias_ref, sum_qkv_ref, sum_up_ref, sum_norm_ref, sum_grad_ref,
    ):
        step = pl.program_id(0)
        place = where_ref[0] * NT + where_ref[1]

        @pl.when(step == 0)
        def _():
            for ref in (sum_qkv_ref, sum_up_ref, sum_norm_ref, sum_grad_ref):
                ref[...] = jnp.zeros_like(ref)
            wide_small[...] = small_ref[0].astype(F32)
            for v in range(4):
                for j in range(S):
                    for i in range(rest):
                        at = (j * rest + i) * 128
                        line = per + (2 + v) * rest + i
                        norms_ref[v : v + 1, at : at + 128] = wide_small[j, line : line + 1, :]
            for v in range(3):
                for i in range(AD // 128):
                    flat = v * (width // 128) + place * (AD // 128) + i
                    at = v * AD + i * 128
                    bias_ref[0:1, at : at + 128] = wide_small[flat // per, pl.ds(flat % per, 1), :]

        gain_1, shift_1, gain_2, shift_2 = [norms_ref[i : i + 1, :] for i in range(4)]
        wide = in_ref[...].astype(F32)
        offsets = wide - jnp.mean(wide, axis=-1, keepdims=True)
        inverse = lax.rsqrt(jnp.mean(offsets * offsets, axis=-1, keepdims=True) + epsilon)
        normed = offsets * inverse
        first = (normed * gain_1 + shift_1).astype(BF16)
        second = (normed * gain_2 + shift_2).astype(BF16)
        first_ref[...] = first
        second_ref[...] = second
        grad = grad_ref[...]
        sum_grad_ref[...] += jnp.sum(grad.astype(F32), axis=0, keepdims=True)

        mixed = dot(first, qkv_ref[...], 1, 0) + bias_ref[...]
        attended_grad = dot(grad, out_ref[...], 1, 1).astype(BF16)
        row = lax.broadcasted_iota(jnp.int32, (T, T), 0)
        col = lax.broadcasted_iota(jnp.int32, (T, T), 1)
        away = (row - col).astype(F32)
        lane = lax.broadcasted_iota(jnp.int32, (T, 128), 1)
        positions, tables = [], []
        for b in range(tile // T):
            block = step * (tile // T) + b
            flat = small_ref[block // S, block % S, -1:, :].astype(F32)
            position = jnp.sum(jnp.where(row == col, flat, 0.0), axis=1, keepdims=True)
            angle = position * freqs_ref[...]
            sine = jnp.sin(angle)
            positions.append(position)
            tables.append(
                (
                    jnp.cos(angle),
                    jnp.where(lane < ROT // 2, -sine, 0.0),
                    jnp.where((lane >= ROT // 2) & (lane < ROT), sine, 0.0),
                )
            )

        def turn(value, table, sign):
            straight, ahead, back = table
            low = value[:, :128]
            low = low * straight + sign * (
                pltpu.roll(low, 128 - ROT // 2, 1) * ahead + pltpu.roll(low, ROT // 2, 1) * back
            )
            return jnp.concatenate([low, value[:, 128:]], axis=1)

        attended_parts, mixed_parts = [], []
        for b in range(tile // T):
            rows = slice(b * T, (b + 1) * T)
            allowed = (away >= 0) & (away <= positions[b])
            outs, q_grads, k_grads, v_grads = [], [], [], []
            for h in range(heads):
                at = slice(h * HD, (h + 1) * HD)
                u = attended_grad[rows, at]
                q = turn(mixed[rows, at], tables[b], 1.0).astype(BF16)
                k = turn(mixed[rows, AD + h * HD : AD + (h + 1) * HD], tables[b], 1.0).astype(BF16)
                v = mixed[rows, 2 * AD + h * HD : 2 * AD + (h + 1) * HD].astype(BF16)
                scores = jnp.where(allowed, dot(q, k, 1, 1) * scale, -1e30)
                peak = jnp.max(scores, axis=-1, keepdims=True)
                logsum = peak + jnp.log(jnp.sum(jnp.exp(scores - peak), axis=-1, keepdims=True))
                probs = jnp.exp(scores - logsum)
                low = probs.astype(BF16)
                outs.append(dot(low, v, 1, 0).astype(BF16))
                dprobs = dot(u, v, 1, 1)
                total = jnp.sum(probs * dprobs, axis=-1, keepdims=True)
                dscores = (probs * (dprobs - total) * scale).astype(BF16)
                q_grads.append(turn(dot(dscores, k, 1, 0), tables[b], -1.0))
                k_grads.append(turn(dot(dscores, q, 0, 0), tables[b], -1.0))
                v_grads.append(dot(low, u, 0, 0))
            attended_parts.append(jnp.concatenate(outs, axis=1))
            mixed_parts.append(jnp.concatenate(q_grads + k_grads + v_grads, axis=1))
        attended = jnp.concatenate(attended_parts, axis=0)
        attended_ref[...] = attended
        mixed_grad = jnp.concatenate(mixed_parts, axis=0)
        sum_qkv_ref[...] += jnp.sum(mixed_grad, axis=0, keepdims=True)
        mixed_low = mixed_grad.astype(BF16)
        mixed_ref[...] = mixed_low

        pre = dot(second, up_ref[...], 1, 0) + b_up_ref[...].astype(F32)
        bell = 0.5 * (1.0 + lax.erf(pre * 0.7071067811865476))
        activated = (pre * bell).astype(BF16)
        activated_ref[...] = activated
        slope = bell + pre * jnp.exp(-0.5 * pre * pre) * 0.3989422804014327
        hidden_grad = dot(grad, down_ref[...], 1, 1) * slope
        sum_up_ref[...] += jnp.sum(hidden_grad, axis=0, keepdims=True)
        hidden_low = hidden_grad.astype(BF16)
        hidden_ref[...] = hidden_low

        branch = dot(attended, out_ref[...], 1, 0) + dot(activated, down_ref[...], 1, 0)
        branch_ref[...] = branch.astype(BF16)

        first_grad = dot(mixed_low, qkv_ref[...], 1, 1)
        second_grad = dot(hidden_low, up_ref[...], 1, 1)
        sum_norm_ref[0:1, :] += jnp.sum(first_grad * normed, axis=0, keepdims=True)
        sum_norm_ref[1:2, :] += jnp.sum(first_grad, axis=0, keepdims=True)
        sum_norm_ref[2:3, :] += jnp.sum(second_grad * normed, axis=0, keepdims=True)
        sum_norm_ref[3:4, :] += jnp.sum(second_grad, axis=0, keepdims=True)
        inner_ref[...] = (first_grad * gain_1 + second_grad * gain_2).astype(BF16)

        @pl.when(step == pl.num_programs(0) - 1)
        def _():
            sums_ref[...] = jnp.zeros_like(sums_ref)
            n = AD // 128
            for v in range(3):
                for i in range(n):
                    at = v * AD + i * 128
                    sums_ref[pl.ds(v * (width // 128) + place * n + i, 1), :] = sum_qkv_ref[:, at : at + 128]
            for i in range(FD // 128):
                sums_ref[pl.ds(base_up + place * (FD // 128) + i, 1), :] = sum_up_ref[:, i * 128 : (i + 1) * 128]
            for i in range(D // 128):
                at = slice(i * 128, (i + 1) * 128)
                sums_ref[base_out + i : base_out + i + 1, :] = sum_grad_ref[:, at] * (1.0 / (S * NT))
                for v in range(4):
                    line = base_norm + v * (D // 128) + i
                    sums_ref[line : line + 1, :] = sum_norm_ref[v : v + 1, at]

    def rows(width):
        return pl.BlockSpec((tile, width), lambda i, where: (i, 0))

    def whole(shape, index=None):
        zeros = (0,) * len(shape)
        return pl.BlockSpec(shape, index or (lambda i, where: zeros), pipeline_mode=pl.Buffered(1))

    widths = [D, D, AD, FD, 3 * AD, FD, D, D]
    flops = 2 * N * D * (2 * 3 * AD + 2 * FD + 2 * FD + 2 * AD)
    return pl.pallas_call(
        kernel,
        out_shape=[jax.ShapeDtypeStruct((N, w), BF16) for w in widths] + [jax.ShapeDtypeStruct((count, 128), F32)],
        grid_spec=pltpu.PrefetchScalarGridSpec(
            num_scalar_prefetch=1,
            grid=(N // tile,),
            in_specs=[
                rows(D),
                rows(D),
                whole(small_all.shape),
                whole((1, 128)),
                whole((D, FD)),
                whole((D, 3 * AD)),
                whole((1, FD), lambda i, where: (0, where[1])),
                whole((FD, D), lambda i, where: (where[1], 0)),
                whole((AD, D), lambda i, where: (where[1], 0)),
            ],
            out_specs=[rows(w) for w in widths] + [whole((count, 128))],
            scratch_shapes=[
                pltpu.VMEM(small_all.shape[1:], F32),
                pltpu.VMEM((4, D), F32),
                pltpu.VMEM((1, 3 * AD), F32),
                pltpu.VMEM((1, 3 * AD), F32),
                pltpu.VMEM((1, FD), F32),
                pltpu.VMEM((4, D), F32),
                pltpu.VMEM((1, D), F32),
            ],
        ),
        compiler_params=pltpu.CompilerParams(
            dimension_semantics=("arbitrary",), vmem_limit_bytes=63 * 2**20
        ),
        cost_estimate=pl.CostEstimate(flops=flops, bytes_accessed=50 * 2**20, transcendentals=N * FD * 2),
        name="layer",
    )(where, in_all, grad_all, small_all, freqs, up, qkv, b_up.reshape(1, -1), w_down, w_out)


def grads(first, second, attended, activated, mixed, hidden, grad, branch, inner, sums, S, R, T, TP, DP):
    N, D = grad.shape
    FD, AD = activated.shape[1], attended.shape[1]
    NT, ND, steps = 2 ** len(TP), 2 ** len(DP), len(DP)
    rows = D // S
    names = ("up", "qkv", "down", "out")
    lefts = (second, first, activated, attended)
    rights = (hidden, mixed, grad, grad)
    which_right = (0, 1, 2, 2)
    pieces = []
    for left, right, lead, mid in zip(lefts, rights, (S, S, 1, 1), (NT, NT, 1, 1)):
        pieces.append((lead, mid, left.shape[1] // (lead * ND * mid * 2), right.shape[1]))
    ways = []
    for way in (DP, DP[::-1]):
        ways.append([(bit, 1 << DP.index(bit)) for bit in way])

    def masks(bits):
        out = [0]
        for _, bit in bits:
            out += [v | bit for v in out]
        return sorted(out)

    slots = []
    for way in ways:
        table = {}
        for j in range(steps):
            for u in masks(way[j + 1 :]):
                table[j, u] = len(table)
        slots.append(table)

    def kernel(
        second_hbm, first_hbm, activated_hbm, attended_hbm, hidden_hbm, mixed_hbm, grad_hbm, branch_hbm, inner_hbm, sums_hbm,
        whole_up, whole_down, whole_out, own_qkv, branch_out, inner_out, sums_out,
        own_up, own_down, own_out, near, near_came, far_came, held, held_came,
        second_v, first_v, activated_v, attended_v, hidden_v, mixed_v, grad_v,
        part_up, part_qkv, part_down, part_out, came_up, came_qkv, came_down, came_out, all_up, all_qkv,
        load, dp_send, dp_recv, z_send, z_recv, near_send, near_recv, far_send, far_recv, held_send, held_recv,
        plane_send, plane_recv,
    ):
        s = lax.axis_index("shard")
        r = lax.axis_index("replica")
        t = sum(((r // bit) % 2 * 2**i for i, bit in enumerate(TP)), jnp.int32(0))
        d = sum(((r // bit) % 2 * 2**i for i, bit in enumerate(DP)), jnp.int32(0))

        def flipped(value, mask):
            return sum((bit * (1 - 2 * ((value // bit) % 2)) for bit in bits_of(mask)), value)

        def other(k, m):
            mask = sum(bit for i, bit in enumerate(TP) if m >> i & 1)
            return {"shard": lax.rem(s + k, S), "replica": flipped(r, mask)}

        loads = []
        order = ((hidden_hbm, hidden_v), (second_hbm, second_v), (mixed_hbm, mixed_v), (first_hbm, first_v),
                 (grad_hbm, grad_v), (activated_hbm, activated_v), (attended_hbm, attended_v))
        parts_hbm = (branch_hbm, inner_hbm)
        for i, (source, target) in enumerate(order):
            loads.append(pltpu.make_async_copy(source, target, load.at[i]))
        token_loads = [
            pltpu.make_async_copy(parts_hbm[i].at[t], near.at[i], load.at[7 + i]) for i in range(2)
        ]
        held_load = pltpu.make_async_copy(sums_hbm, held.at[0], load.at[9])
        for copy in (*loads[:2], held_load, *token_loads, *loads[2:]):
            copy.start()

        group = [(k, m) for k in range(S) for m in range(NT) if k or m]
        barrier = pltpu.get_barrier_semaphore()
        for k, m in group:
            pl.semaphore_signal(barrier, inc=1, device_id=other(k, m), device_id_type=MESH)
        for bit in DP:
            pl.semaphore_signal(barrier, inc=1, device_id={"replica": flipped(r, bit)}, device_id_type=MESH)
        pl.semaphore_wait(barrier, len(group) + steps)

        left_refs = (second_v, first_v, activated_v, attended_v)
        right_refs = (hidden_v, mixed_v, grad_v, grad_v)
        part = (part_up, part_qkv, part_down, part_out)
        came = (came_up, came_qkv, came_down, came_out)
        own = (own_up, own_qkv, own_down, own_out)

        def product(i):
            lead, mid, n, _ = pieces[i]
            if lead > 1:
                width = ND * mid * 2 * n

                def body(l, carry):
                    cols = pl.ds(pl.multiple_of(l * width, width), width)
                    value = dot(left_refs[i][:, cols], right_refs[i][...], 0, 0).astype(BF16)
                    for q in range(ND):
                        for c in range(mid):
                            for h in range(2):
                                at = ((q * mid + c) * 2 + h) * n
                                part[i][h, q, l, c] = value[at : at + n]
                    return carry

                lax.fori_loop(0, lead, body, 0)
            else:
                total = ND * 2 * n
                chunk = min(total, 512)
                per = chunk // (2 * n)

                def body(l, carry):
                    cols = pl.ds(pl.multiple_of(l * chunk, chunk), chunk)
                    value = dot(left_refs[i][:, cols], right_refs[i][...], 0, 0).astype(BF16)
                    for q in range(per):
                        for h in range(2):
                            at = (q * 2 + h) * n
                            part[i][h, l * per + q, 0, 0] = value[at : at + n]
                    return carry

                lax.fori_loop(0, total // chunk, body, 0)

        def halving(i, h, j, u):
            bit, dbit = ways[h][j]
            slot = slots[h][j, u]
            return pltpu.make_async_remote_copy(
                src_ref=part[i].at[h, flipped(d, dbit | u)], dst_ref=came[i].at[h, slot],
                send_sem=dp_send.at[i, h, slot], recv_sem=dp_recv.at[i, h, slot],
                device_id={"replica": flipped(r, bit)}, device_id_type=MESH,
            )

        def summed(i, h, mask, count, write):
            lead, mid, _, _ = pieces[i]
            at = flipped(d, mask)
            for j in range(count):
                halving(i, h, j, mask).wait_recv()

            def body(l, carry):
                for c in range(mid):
                    value = part[i][h, at, l, c].astype(F32)
                    for j in range(count):
                        value = value + came[i][h, slots[h][j, mask], l, c].astype(F32)
                    write(l, c, value.astype(BF16))
                return carry

            lax.fori_loop(0, lead, body, 0)

        def step(i, j):
            for h in range(2):
                for u in masks(ways[h][j + 1 :]):
                    mask = ways[h][j][1] | u
                    at = flipped(d, mask)
                    if j:

                        def write(l, c, value, h=h, at=at):
                            part[i][h, at, l, c] = value

                        summed(i, h, mask, j, write)
                    halving(i, h, j, u).start()

        everyone = (all_up, all_qkv)

        def to_shard(i, h, k, m):
            there = lax.rem(s + k, S)
            return pltpu.make_async_remote_copy(
                src_ref=part[i].at[h, d, there, flipped(t, m)], dst_ref=everyone[i].at[s, t, h],
                send_sem=z_send.at[i, h, k, m], recv_sem=z_recv.at[i, h, k, m],
                device_id=other(k, m), device_id_type=MESH,
            )

        def last(i):
            for h in range(2):
                if i < 2:

                    def write(l, c, value, h=h):
                        part[i][h, d, l, c] = value

                else:

                    def write(l, c, value, h=h):
                        own[i][h] = value

                summed(i, h, 0, steps, write)
            if i < 2:
                for k, m in group:
                    for h in range(2):
                        to_shard(i, h, k, m).start()
                for h in range(2):
                    everyone[i][s, t, h] = part[i][h, d, s, t]

        def collect(i):
            width = pieces[i][3]
            runs = 1 if i == 0 else 3
            n = width // runs
            for k, m in group:
                for h in range(2):
                    to_shard(i, h, k, m).wait_recv()
            for h in range(2):
                for j in range(S):
                    for u in range(NT):
                        block = everyone[i][j, u, h]
                        for v in range(runs):
                            at = (v * S * NT + j * NT + u) * n
                            own[i][h, :, at : at + n] = block[:, v * n : (v + 1) * n]

        def near_copy(i, m):
            return pltpu.make_async_remote_copy(
                src_ref=parts_hbm[i].at[flipped(t, m)], dst_ref=near_came.at[i, m - 1],
                send_sem=near_send.at[i, m], recv_sem=near_recv.at[i, m], device_id=other(0, m), device_id_type=MESH,
            )

        def far_copy(i, k):
            return pltpu.make_async_remote_copy(
                src_ref=near.at[i, lax.rem(s + k, S)], dst_ref=far_came.at[i, k - 1],
                send_sem=far_send.at[i, k], recv_sem=far_recv.at[i, k], device_id=other(k, 0), device_id_type=MESH,
            )

        def near_sum(i, j):
            value = near[i, j].astype(F32)
            for m in range(1, NT):
                value = value + near_came[i, m - 1, j].astype(F32)
            return value

        def tokens_near(i):
            token_loads[i].wait()
            for m in range(1, NT):
                near_copy(i, m).wait_recv()

            def body(k, carry):
                j = lax.rem(s + k, S)
                near[i, j] = near_sum(i, j).astype(BF16)
                return carry

            lax.fori_loop(1, S, body, 0)
            for k in range(1, S):
                far_copy(i, k).start()

        token_outs = (branch_out, inner_out)

        def tokens_far(i):
            value = near_sum(i, s)
            for k in range(1, S):
                far_copy(i, k).wait_recv()
                value = value + far_came[i, k - 1].astype(F32)
            token_outs[i][...] = value

        bits = [(0, bit) for bit in bits_of(R - 1)] + [(1, bit) for bit in bits_of(S - 1)]

        def double(i):
            axis, bit = bits[i]
            to = {"replica": flipped(r, bit)} if axis == 0 else {"shard": flipped(s, bit)}
            return pltpu.make_async_remote_copy(
                src_ref=held.at[i], dst_ref=held_came.at[i], send_sem=held_send.at[i], recv_sem=held_recv.at[i],
                device_id=to, device_id_type=MESH,
            )

        def doubled(i):
            double(i).wait_recv()
            value = held[i] + held_came[i]
            if i + 1 < len(bits):
                held[i + 1] = value
                double(i + 1).start()
            else:
                sums_out[...] = value

        wholes = {0: whole_up, 2: whole_down, 3: whole_out}
        order_of = {0: 0, 2: 1, 3: 2}

        def slot_of(i, h, dd, tt):
            n = pieces[i][2]
            if i == 0:
                at = (dd * NT + tt) * 2 * n + h * n
            else:
                at = tt * (ND * 2 * n) + dd * 2 * n + h * n
            return wholes[i].at[pl.ds(pl.multiple_of(at, n), n), :]

        def gather(i, h, m, b):
            dmask = sum(ways[h][v][1] for v in range(steps) if m >> v & 1)
            tmask = m >> steps
            slot = slot_of(i, h, flipped(d, dmask), flipped(t, tmask))
            bit = ways[h][b][0] if b < steps else TP[b - steps]
            return pltpu.make_async_remote_copy(
                src_ref=own[i].at[h] if m == 0 else slot, dst_ref=slot,
                send_sem=plane_send.at[order_of[i], h, m | 1 << b], recv_sem=plane_recv.at[order_of[i], h, m | 1 << b],
                device_id={"replica": flipped(r, bit)}, device_id_type=MESH,
            )

        positions = steps + len(TP)

        def keep_own(i, h):
            return pltpu.make_async_copy(own[i].at[h], slot_of(i, h, d, t), load.at[10 + order_of[i] * 2 + h])

        def share_own(i):
            for h in range(2):
                for b in range(positions):
                    gather(i, h, 0, b).start()
                keep_own(i, h).start()

        def share_on(i, m):
            top = m.bit_length() - 1
            for h in range(2):
                gather(i, h, m ^ 1 << top, top).wait_recv()
                for b in range(top + 1, positions):
                    gather(i, h, m, b).start()

        for i in range(2):
            for m in range(1, NT):
                near_copy(i, m).start()
        held_load.wait()
        double(0).start()
        loads[0].wait()
        loads[1].wait()
        product(0)
        step(0, 0)
        tokens_near(0)
        doubled(0)
        loads[2].wait()
        loads[3].wait()
        product(1)
        step(1, 0)
        tokens_near(1)
        for j in range(1, steps):
            step(0, j)
        doubled(1)
        loads[4].wait()
        loads[5].wait()
        product(2)
        step(2, 0)
        for j in range(1, steps):
            step(1, j)
        loads[6].wait()
        product(3)
        step(3, 0)
        last(0)
        for i in range(2, len(bits)):
            doubled(i)
        for j in range(1, steps):
            step(2, j)
        last(1)
        for j in range(1, steps):
            step(3, j)
        last(2)
        share_own(2)
        last(3)
        share_own(3)
        collect(0)
        share_own(0)
        for m in range(1, 1 << steps):
            for i in (2, 3, 0):
                share_on(i, m)
        for i in range(2):
            tokens_far(i)
        collect(1)
        for m in range(1 << steps, 1 << positions):
            for i in (2, 3, 0):
                share_on(i, m)

        for i in (2, 3, 0):
            for h in range(2):
                keep_own(i, h).wait()
                for m in range(1 << positions):
                    for b in range(m.bit_length(), positions):
                        gather(i, h, m, b).wait_send()
        for i in range(2):
            for m in range(1, NT):
                near_copy(i, m).wait_send()
            for k in range(1, S):
                far_copy(i, k).wait_send()
        for i in range(len(bits)):
            double(i).wait_send()
        for i in range(4):
            for h in range(2):
                for j, u in slots[h]:
                    halving(i, h, j, u).wait_send()
        for i in range(2):
            for h in range(2):
                for k, m in group:
                    to_shard(i, h, k, m).wait_send()

    def scratch(value):
        return pltpu.VMEM(value.shape, BF16)

    any_spec = pl.BlockSpec(memory_space=pl.ANY)
    vmem_spec = pl.BlockSpec(memory_space=pltpu.VMEM)
    operands = (second, first, activated, attended, hidden, mixed, grad)
    owns = [(2, n, width * S * NT if lead > 1 else width) for lead, _, n, width in pieces]
    wholes = [(2 * n * ND * NT, width) for _, n, width in owns]
    outs = [jax.ShapeDtypeStruct(wholes[i], BF16) for i in (0, 2, 3)]
    outs += [jax.ShapeDtypeStruct(owns[1], BF16)] + [jax.ShapeDtypeStruct((T, D), F32)] * 2
    outs += [jax.ShapeDtypeStruct(sums.shape, F32)]
    sent = sum(2 * (ND - 1) * a * b * n * w * 2 for a, b, n, w in pieces)
    count = len(bits_of(R - 1)) + len(bits_of(S - 1))
    return pl.pallas_call(
        kernel,
        out_shape=outs,
        in_specs=[any_spec] * 10,
        out_specs=[any_spec] * 3 + [vmem_spec] * 4,
        scratch_shapes=[pltpu.VMEM(owns[i], BF16) for i in (0, 2, 3)]
        + [
            pltpu.VMEM((2, S, T, D), BF16),
            pltpu.VMEM((2, max(1, NT - 1), S, T, D), BF16),
            pltpu.VMEM((2, S - 1, T, D), BF16),
            pltpu.VMEM((count,) + sums.shape, F32),
            pltpu.VMEM((count,) + sums.shape, F32),
        ]
        + [scratch(v) for v in operands]
        + [pltpu.VMEM((2, ND) + piece, BF16) for piece in pieces]
        + [pltpu.VMEM((2, ND - 1) + piece, BF16) for piece in pieces]
        + [pltpu.VMEM((S, NT, 2) + piece[2:], BF16) for piece in pieces[:2]]
        + [
            pltpu.SemaphoreType.DMA((16,)),
            pltpu.SemaphoreType.DMA((4, 2, ND - 1)),
            pltpu.SemaphoreType.DMA((4, 2, ND - 1)),
            pltpu.SemaphoreType.DMA((2, 2, S, NT)),
            pltpu.SemaphoreType.DMA((2, 2, S, NT)),
            pltpu.SemaphoreType.DMA((2, NT)),
            pltpu.SemaphoreType.DMA((2, NT)),
            pltpu.SemaphoreType.DMA((2, S)),
            pltpu.SemaphoreType.DMA((2, S)),
            pltpu.SemaphoreType.DMA((count,)),
            pltpu.SemaphoreType.DMA((count,)),
            pltpu.SemaphoreType.DMA((3, 2, ND * NT)),
            pltpu.SemaphoreType.DMA((3, 2, ND * NT)),
        ],
        compiler_params=pltpu.CompilerParams(
            collective_id=1, has_side_effects=True, vmem_limit_bytes=67043328
        ),
        cost_estimate=pl.CostEstimate(
            flops=2 * N * sum(v.shape[1] * w.shape[1] for v, w in zip(lefts, rights)),
            bytes_accessed=sent * 8, transcendentals=0,
        ),
        name="grads",
    )(*operands, branch.reshape(NT, S, T, D), inner.reshape(NT, S, T, D), sums)


def solution(mesh):
    S = mesh.shape["shard"]
    R = mesh.shape["replica"]
    TP = [1] if R > 1 and H % (2 * S) == 0 else []
    DP = [bit for bit in bits_of(R - 1) if bit not in TP]
    NT, ND = 2 ** len(TP), 2 ** len(DP)
    def flip(value, bit):
        return lax.ppermute(value, "replica", [(i, i ^ bit) for i in range(R)])

    def body(
        block_in, positions, out_grad, w_qkv, b_qkv, w_out, b_out, w_up, b_up, w_down, b_down,
        first_gain, first_shift, second_gain, second_shift,
    ):
        T, D = block_in.shape
        rows = w_qkv.shape[0]
        FS = w_down.shape[0]
        FD = FS // NT
        HN = H // S // NT
        AD = HN * HD
        G = NT * S
        s = lax.axis_index("shard")
        r = lax.axis_index("replica")
        mine = {bit: (r // bit) % 2 for bit in bits_of(R - 1)}
        t = sum((mine[bit] * 2**i for i, bit in enumerate(TP)), jnp.int32(0))

        small = jnp.concatenate(
            [b_qkv, b_out, b_down, first_gain, first_shift, second_gain, second_shift,
             positions.astype(BF16)]
        )
        small = small.reshape(-1, 128)
        x_all, grad_all, small_all, up, qkv = fetch(
            block_in, out_grad, small, w_up, w_qkv, S, R, TP, DP, FD, AD
        )
        sizes = [b_qkv.shape[0]] + [rows] * 2
        flat = small_all[0].reshape(S, -1)
        biases = flat[:, sizes[0] : sum(sizes)].reshape(S, 2, rows).astype(F32)
        full_b_out, full_b_down = biases[:, 0].reshape(-1), biases[:, 1].reshape(-1)
        x_all = x_all.reshape(G * T, D)
        grad_all = grad_all.reshape(G * T, D)
        d = sum((mine[bit] * 2**i for i, bit in enumerate(DP)), jnp.int32(0))

        def normed_of(block):
            wide = block.astype(F32)
            offsets = wide - jnp.mean(wide, axis=-1, keepdims=True)
            inverse = lax.rsqrt(jnp.mean(offsets * offsets, axis=-1, keepdims=True) + epsilon)
            return offsets * inverse, inverse

        (
            first_low, second_low, attended, activated, mixed_low, hidden_low, branch_part, inner_part, sums,
        ) = layer(
            x_all, grad_all, small_all, rotary_freqs(), up, qkv, b_up, w_down, w_out,
            jnp.stack([s, t]), S, NT, T, 2 * T,
        )

        def share(halves, write, result):
            for half, (value, order) in enumerate(zip(halves, (DP, DP[::-1]))):
                value = lax.optimization_barrier(value)
                pieces = {0: value}
                for bit in list(order) + TP:
                    pieces.update({m | bit: flip(v, bit) for m, v in list(pieces.items())})
                for m, piece in pieces.items():
                    dmask = sum(2**i for i, bit in enumerate(DP) if m & bit)
                    tmask = sum(2**i for i, bit in enumerate(TP) if m & bit)
                    result = write(result, piece.astype(F32), d ^ dmask, t ^ tmask, half)
            return result

        def placed_rows(halves, group_rows, shape):
            n = halves.shape[1]

            def write(res, v, dd, tt, half):
                if group_rows is None:
                    at = (dd * NT + tt) * 2 * n
                else:
                    at = tt * group_rows + dd * 2 * n
                return lax.dynamic_update_slice(res, v, (at + half * n, 0))

            return share([halves[0], halves[1]], write, unwritten(shape, F32))

        whole_up, whole_down, whole_out, own_qkv, branch, scaled, sums = grads(
            first_low, second_low, attended, activated, mixed_low, hidden_low, grad_all, branch_part, inner_part,
            sums, S, R, T, TP, DP,
        )
        grad_w_qkv = placed_rows(own_qkv, None, w_qkv.shape)
        grad_w_up = whole_up.astype(F32)
        grad_w_down = whole_down.astype(F32)
        grad_w_out = whole_out.astype(F32)

        block_out = (block_in.astype(F32) + branch + full_b_out + full_b_down).astype(BF16)
        normed_own, inverse_own = normed_of(block_in)
        term = inverse_own * (
            scaled
            - jnp.mean(scaled, axis=-1, keepdims=True)
            - normed_own * jnp.mean(scaled * normed_own, axis=-1, keepdims=True)
        )
        in_grad = (out_grad.astype(F32) + term).astype(BF16)

        sums = sums.reshape(-1)
        width = w_out.shape[0] * S
        lengths = [width] * 3 + [D, FS * S] + [D] * 4
        at = [sum(lengths[:i]) for i in range(len(lengths))]

        def owned(start, length):
            return lax.dynamic_slice_in_dim(sums, start + s * (length // S), length // S, 0)

        grad_b_qkv = owned(at[0], 3 * width)
        grad_b_out = owned(at[3], D)
        grad_b_up = owned(at[4], FS * S)
        smalls = [owned(at[5 + i], D) for i in range(4)]
        return (
            block_out, in_grad, grad_w_qkv, grad_b_qkv, grad_w_out, grad_b_out, grad_w_up, grad_b_up,
            grad_w_down, grad_b_out, *smalls,
        )

    rows2, row1, par2, par1 = P(("shard", "replica"), None), P(("shard", "replica")), P("shard", None), P("shard")
    return jax.shard_map(
        body,
        mesh=mesh,
        in_specs=(
            rows2, row1, rows2, par2, par1, par2, par1, par2, par1, par2, par1, par1, par1, par1, par1,
        ),
        out_specs=(
            rows2, rows2, par2, par1, par2, par1, par2, par1, par2, par1, par1, par1, par1, par1,
        ),
        check_vma=False,
    )
```

```python
import jax
import jax.numpy as jnp
from jax import lax
from jax.experimental import pallas as pl
from jax.experimental.pallas import tpu as pltpu
from jax.sharding import PartitionSpec as P

H = 8
HD = 256
ROT = 64

epsilon = 1e-05


F32 = jnp.float32
BF16 = jnp.bfloat16
MESH = pl.DeviceIdType.MESH


def rotary_freqs():
    freqs = 10000.0 ** (-(jnp.arange(ROT // 2, dtype=F32) * (2.0 / ROT)))
    return jnp.concatenate([freqs, freqs, jnp.zeros((128 - ROT,), F32)]).reshape(1, 128)


def dot(left, right, left_dim, right_dim):
    return lax.dot_general(
        left, right, (((left_dim,), (right_dim,)), ((), ())), preferred_element_type=F32
    )


def widen(value):
    rows, width = value.shape
    n = min(rows, max(8, 2**20 // width))

    def kernel(in_ref, out_ref):
        out_ref[...] = in_ref[...].astype(F32)

    spec = pl.BlockSpec((n, width), lambda i: (i, 0))
    return pl.pallas_call(
        kernel,
        grid=(rows // n,),
        in_specs=[spec],
        out_specs=spec,
        out_shape=jax.ShapeDtypeStruct(value.shape, F32),
        cost_estimate=pl.CostEstimate(flops=0, bytes_accessed=6 * rows * width, transcendentals=0),
        name="widen",
    )(value)


def unwritten(shape, dtype):
    return pl.pallas_call(
        lambda out_ref: None,
        out_shape=jax.ShapeDtypeStruct(shape, dtype),
        out_specs=pl.BlockSpec(memory_space=pl.ANY),
    )()


def bits_of(mask):
    return [1 << i for i in range(mask.bit_length()) if mask >> i & 1]

def fetch(block_in, out_grad, small, w_up, w_qkv, S, R, TP, DP, FD, AD):
    T, D = block_in.shape
    rows = w_up.shape[0]
    NT, ND = 2 ** len(TP), 2 ** len(DP)
    part = rows // ND
    third = w_qkv.shape[1] // 3
    tokens = (small, out_grad, block_in)
    widths = (FD, 3 * AD)

    def kernel(
        small_ref, grad_ref, in_ref, up_ref, qkv_ref, small_all, grad_all, in_all, up_all, qkv_all,
        in_own, grad_own, up_own, qkv_own, small_send, small_recv, line_send, line_recv, tp_send, tp_recv, z_send, z_recv, dp_send, dp_recv, local,
    ):
        s = lax.axis_index("shard")
        r = lax.axis_index("replica")
        t = sum(((r // bit) % 2 * 2**i for i, bit in enumerate(TP)), jnp.int32(0))
        d = sum(((r // bit) % 2 * 2**i for i, bit in enumerate(DP)), jnp.int32(0))

        def partner(bit):
            return {"replica": r + bit - 2 * bit * ((r // bit) % 2)}

        copies = [pltpu.make_async_copy(small_ref, small_all.at[t, s], local.at[0])]
        gathered = (grad_all, in_all)
        first = [
            pltpu.make_async_copy(in_ref, in_own, local.at[1]),
            pltpu.make_async_copy(grad_ref, grad_own, local.at[2]),
            pltpu.make_async_copy(
                up_ref.at[:, pl.ds(pl.multiple_of((s * NT + t) * FD, FD), FD)], up_own, local.at[3]
            ),
        ]
        for j in range(3):
            first.append(
                pltpu.make_async_copy(
                    qkv_ref.at[:, pl.ds(pl.multiple_of(j * third + (s * NT + t) * AD, AD), AD)],
                    qkv_own.at[:, j * AD : (j + 1) * AD],
                    local.at[4 + j],
                )
            )
        for copy in copies + first:
            copy.start()

        def other(k, m):
            mask = sum(bit for i, bit in enumerate(TP) if m >> i & 1)
            flipped = sum((bit * (1 - 2 * ((r // bit) % 2)) for bit in bits_of(mask)), r)
            return {"shard": lax.rem(s + k, S), "replica": flipped}

        group = [(k, m) for k in range(S) for m in range(NT) if k or m]
        plane = range(1, ND)

        def mate(m):
            mask = sum(bit for i, bit in enumerate(DP) if m >> i & 1)
            return {"replica": sum((bit * (1 - 2 * ((r // bit) % 2)) for bit in bits_of(mask)), r)}

        barrier = pltpu.get_barrier_semaphore()
        for k, m in group:
            pl.semaphore_signal(barrier, inc=1, device_id=other(k, m), device_id_type=MESH)
        for m in plane:
            pl.semaphore_signal(barrier, inc=1, device_id=mate(m), device_id_type=MESH)
        pl.semaphore_wait(barrier, len(group) + len(plane))

        def small_copy(k, m):
            return pltpu.make_async_remote_copy(
                src_ref=small_ref, dst_ref=small_all.at[t, s], send_sem=small_send.at[k, m],
                recv_sem=small_recv.at[k, m], device_id=other(k, m), device_id_type=MESH,
            )

        def line(i, j, way, source):
            return pltpu.make_async_remote_copy(
                src_ref=source, dst_ref=gathered[i].at[t, j], send_sem=line_send.at[i, j, way],
                recv_sem=line_recv.at[i, j], device_id={"shard": s + 2 * way - 1}, device_id_type=MESH,
            )

        def across(i, j, b, m, source):
            slot = gathered[i].at[t ^ m, j]
            return pltpu.make_async_remote_copy(
                src_ref=slot if source is None else source, dst_ref=slot, send_sem=tp_send.at[i, j, m | 1 << b],
                recv_sem=tp_recv.at[i, j, m | 1 << b], device_id=partner(TP[b]), device_id_type=MESH,
            )

        def z_copies(w, k, sending):
            to = lax.rem(s + k, S)
            at = (s if sending else lax.rem(s + S - k, S)) * rows + d * part
            at = pl.multiple_of(at, part)
            out = []
            for j in range(1 if w == 0 else 3):
                if w == 0:
                    source = up_ref.at[pl.ds(pl.multiple_of(d * part, part), part), pl.ds(pl.multiple_of((to * NT + t) * FD, FD), FD)]
                    target = up_all.at[pl.ds(at, part), :]
                else:
                    source = qkv_ref.at[
                        pl.ds(pl.multiple_of(d * part, part), part), pl.ds(pl.multiple_of(j * third + (to * NT + t) * AD, AD), AD)
                    ]
                    target = qkv_all.at[pl.ds(at, part), j * AD : (j + 1) * AD]
                out.append(
                    pltpu.make_async_remote_copy(
                        src_ref=source, dst_ref=target, send_sem=z_send.at[k, w + j], recv_sem=z_recv.at[k, w + j],
                        device_id={"shard": to}, device_id_type=MESH,
                    )
                )
            return out

        def shared(w, k, m):
            at = pl.multiple_of(lax.rem(s + S - k, S) * rows + d * part, part)
            slot = (up_all, qkv_all)[w].at[pl.ds(at, part), :]
            return pltpu.make_async_remote_copy(
                src_ref=slot, dst_ref=slot, send_sem=dp_send.at[w, k, m], recv_sem=dp_recv.at[w, k, m],
                device_id=mate(m), device_id_type=MESH,
            )

        mine = (grad_ref, in_ref)
        for k, m in group:
            small_copy(k, m).start()
        for i in range(2):

            @pl.when(s + 1 < S)
            def _():
                line(i, s, 1, mine[i]).start()

            @pl.when(s > 0)
            def _():
                line(i, s, 0, mine[i]).start()

        for k in range(1, S):
            for w in range(2):
                for copy in z_copies(w, k, True):
                    copy.start()
        for i in range(2):
            for b in range(len(TP)):
                across(i, s, b, 0, mine[i]).start()

        def pass_on(i, j, m, top):
            for b in range(top + 1, len(TP)):
                across(i, j, b, m, None).start()

        def from_line(i, k):
            @pl.when(s - k >= 0)
            def _():
                line(i, s - k, 1, gathered[i].at[t, s - k]).wait_recv()

                @pl.when(s + 1 < S)
                def _():
                    line(i, s - k, 1, gathered[i].at[t, s - k]).start()

                pass_on(i, s - k, 0, -1)

            @pl.when(s + k < S)
            def _():
                line(i, s + k, 0, gathered[i].at[t, s + k]).wait_recv()

                @pl.when(s > 0)
                def _():
                    line(i, s + k, 0, gathered[i].at[t, s + k]).start()

                pass_on(i, s + k, 0, -1)

        for copy in first:
            copy.wait()
        at_own = pl.multiple_of(s * rows, rows)
        second = [
            pltpu.make_async_copy(in_own, in_all.at[t, s], local.at[1]),
            pltpu.make_async_copy(grad_own, grad_all.at[t, s], local.at[2]),
            pltpu.make_async_copy(up_own, up_all.at[pl.ds(at_own, rows), :], local.at[3]),
            pltpu.make_async_copy(qkv_own, qkv_all.at[pl.ds(at_own, rows), :], local.at[4]),
        ]
        for copy in second:
            copy.start()

        for k in range(1, S):
            for i in range(2):
                from_line(i, k)
            if k == 1:
                for back in range(1, S):
                    for w in range(2):
                        for copy in z_copies(w, back, False):
                            copy.wait_recv()
                        for m in plane:
                            shared(w, back, m).start()

        for m in range(1, NT):
            top = m.bit_length() - 1
            for i in range(2):
                for j in range(S):
                    across(i, j, top, m ^ (1 << top), None).wait_recv()
                    pass_on(i, j, m, top)
        for k, m in group:
            small_copy(k, m).wait_recv()
        for k in range(1, S):
            for w in range(2):
                for m in plane:
                    shared(w, k, m).wait_recv()

        for i in range(2):
            for j in range(S):

                @pl.when((s + 1 < S) & (j <= s))
                def _():
                    line(i, j, 1, gathered[i].at[t, j]).wait_send()

                @pl.when((s > 0) & (j >= s))
                def _():
                    line(i, j, 0, gathered[i].at[t, j]).wait_send()

                for m in range(NT):
                    for b in range(m.bit_length(), len(TP)):
                        across(i, j, b, m, None).wait_send()
        for k, m in group:
            small_copy(k, m).wait_send()
        for k in range(1, S):
            for w in range(2):
                for copy in z_copies(w, k, True):
                    copy.wait_send()
                for m in plane:
                    shared(w, k, m).wait_send()
        for copy in copies + second:
            copy.wait()

    any_spec = pl.BlockSpec(memory_space=pl.ANY)
    shapes = [jax.ShapeDtypeStruct((NT, S) + v.shape, BF16) for v in tokens]
    shapes += [jax.ShapeDtypeStruct((S * rows, width), BF16) for width in widths]
    small_all, grad_all, in_all, up, qkv = pl.pallas_call(
        kernel,
        out_shape=shapes,
        in_specs=[any_spec] * 5,
        out_specs=[any_spec] * 5,
        scratch_shapes=[
            pltpu.VMEM((T, D), BF16),
            pltpu.VMEM((T, D), BF16),
            pltpu.VMEM((rows, FD), BF16),
            pltpu.VMEM((rows, 3 * AD), BF16),
            pltpu.SemaphoreType.DMA((S, NT)),
            pltpu.SemaphoreType.DMA((S, NT)),
            pltpu.SemaphoreType.DMA((2, S, 2)),
            pltpu.SemaphoreType.DMA((2, S)),
            pltpu.SemaphoreType.DMA((2, S, NT)),
            pltpu.SemaphoreType.DMA((2, S, NT)),
            pltpu.SemaphoreType.DMA((S, 4)),
            pltpu.SemaphoreType.DMA((S, 4)),
            pltpu.SemaphoreType.DMA((2, S, ND)),
            pltpu.SemaphoreType.DMA((2, S, ND)),
            pltpu.SemaphoreType.DMA((7,)),
        ],
        compiler_params=pltpu.CompilerParams(collective_id=0, has_side_effects=True),
        name="fetch",
    )(*tokens, w_up, w_qkv)
    return in_all, grad_all, small_all, up, qkv

def layer(in_all, grad_all, small_all, freqs, up, qkv, w_down, w_out, where, S, NT, T, tile):
    N, D = in_all.shape
    FD = up.shape[1]
    AD = qkv.shape[1] // 3
    FS = w_down.shape[0]
    heads = AD // HD
    scale = HD ** (-0.5)
    width = S * NT * AD
    per = 3 * width // S // 128
    rest = D // S // 128
    base_out = 3 * width // 128
    base_up = base_out + D // 128
    base_norm = base_up + FS * S // 128
    count = base_norm + 4 * D // 128

    def kernel(
        where_ref, in_ref, grad_ref, small_ref, freqs_ref, up_ref, qkv_ref, down_ref, out_ref,
        first_ref, second_ref, attended_ref, activated_ref, mixed_ref, hidden_ref, branch_ref, inner_ref, sums_ref,
        wide_small, norms_ref, bias_ref, bias_up_ref, sum_qkv_ref, sum_up_ref, sum_norm_ref, sum_grad_ref,
    ):
        step = pl.program_id(0)
        place = where_ref[0] * NT + where_ref[1]

        @pl.when(step == 0)
        def _():
            for ref in (sum_qkv_ref, sum_up_ref, sum_norm_ref, sum_grad_ref):
                ref[...] = jnp.zeros_like(ref)
            wide_small[...] = small_ref[0].astype(F32)
            for v in range(4):
                for j in range(S):
                    for i in range(rest):
                        at = (j * rest + i) * 128
                        line = per + (2 + v) * rest + i
                        norms_ref[v : v + 1, at : at + 128] = wide_small[j, line : line + 1, :]
            for v in range(3):
                for i in range(AD // 128):
                    flat = v * (width // 128) + place * (AD // 128) + i
                    at = v * AD + i * 128
                    bias_ref[0:1, at : at + 128] = wide_small[flat // per, pl.ds(flat % per, 1), :]
            for i in range(FD // 128):
                line = per + 6 * rest + where_ref[1] * (FD // 128) + i
                bias_up_ref[0:1, i * 128 : (i + 1) * 128] = wide_small[where_ref[0], pl.ds(line, 1), :]

        gain_1, shift_1, gain_2, shift_2 = [norms_ref[i : i + 1, :] for i in range(4)]
        wide = in_ref[...].astype(F32)
        offsets = wide - jnp.mean(wide, axis=-1, keepdims=True)
        inverse = lax.rsqrt(jnp.mean(offsets * offsets, axis=-1, keepdims=True) + epsilon)
        normed = offsets * inverse
        first = (normed * gain_1 + shift_1).astype(BF16)
        second = (normed * gain_2 + shift_2).astype(BF16)
        first_ref[...] = first
        second_ref[...] = second
        grad = grad_ref[...]
        sum_grad_ref[...] += jnp.sum(grad.astype(F32), axis=0, keepdims=True)

        mixed = dot(first, qkv_ref[...], 1, 0) + bias_ref[...]
        attended_grad = dot(grad, out_ref[...], 1, 1).astype(BF16)
        row = lax.broadcasted_iota(jnp.int32, (T, T), 0)
        col = lax.broadcasted_iota(jnp.int32, (T, T), 1)
        away = (row - col).astype(F32)
        lane = lax.broadcasted_iota(jnp.int32, (T, 128), 1)
        positions, tables = [], []
        for b in range(tile // T):
            block = step * (tile // T) + b
            flat = small_ref[block // S, block % S, -1:, :].astype(F32)
            position = jnp.sum(jnp.where(row == col, flat, 0.0), axis=1, keepdims=True)
            angle = position * freqs_ref[...]
            sine = jnp.sin(angle)
            positions.append(position)
            tables.append(
                (
                    jnp.cos(angle),
                    jnp.where(lane < ROT // 2, -sine, 0.0),
                    jnp.where((lane >= ROT // 2) & (lane < ROT), sine, 0.0),
                )
            )

        def turn(value, table, sign):
            straight, ahead, back = table
            low = value[:, :128]
            low = low * straight + sign * (
                pltpu.roll(low, 128 - ROT // 2, 1) * ahead + pltpu.roll(low, ROT // 2, 1) * back
            )
            return jnp.concatenate([low, value[:, 128:]], axis=1)

        attended_parts, mixed_parts = [], []
        for b in range(tile // T):
            rows = slice(b * T, (b + 1) * T)
            allowed = (away >= 0) & (away <= positions[b])
            outs, q_grads, k_grads, v_grads = [], [], [], []
            for h in range(heads):
                at = slice(h * HD, (h + 1) * HD)
                u = attended_grad[rows, at]
                q = turn(mixed[rows, at], tables[b], 1.0).astype(BF16)
                k = turn(mixed[rows, AD + h * HD : AD + (h + 1) * HD], tables[b], 1.0).astype(BF16)
                v = mixed[rows, 2 * AD + h * HD : 2 * AD + (h + 1) * HD].astype(BF16)
                scores = jnp.where(allowed, dot(q, k, 1, 1) * scale, -1e30)
                peak = jnp.max(scores, axis=-1, keepdims=True)
                logsum = peak + jnp.log(jnp.sum(jnp.exp(scores - peak), axis=-1, keepdims=True))
                probs = jnp.exp(scores - logsum)
                low = probs.astype(BF16)
                outs.append(dot(low, v, 1, 0).astype(BF16))
                dprobs = dot(u, v, 1, 1)
                total = jnp.sum(probs * dprobs, axis=-1, keepdims=True)
                dscores = (probs * (dprobs - total) * scale).astype(BF16)
                q_grads.append(turn(dot(dscores, k, 1, 0), tables[b], -1.0))
                k_grads.append(turn(dot(dscores, q, 0, 0), tables[b], -1.0))
                v_grads.append(dot(low, u, 0, 0))
            attended_parts.append(jnp.concatenate(outs, axis=1))
            mixed_parts.append(jnp.concatenate(q_grads + k_grads + v_grads, axis=1))
        attended = jnp.concatenate(attended_parts, axis=0)
        attended_ref[...] = attended
        mixed_grad = jnp.concatenate(mixed_parts, axis=0)
        sum_qkv_ref[...] += jnp.sum(mixed_grad, axis=0, keepdims=True)
        mixed_low = mixed_grad.astype(BF16)
        mixed_ref[...] = mixed_low

        pre = dot(second, up_ref[...], 1, 0) + bias_up_ref[...]
        bell = 0.5 * (1.0 + lax.erf(pre * 0.7071067811865476))
        activated = (pre * bell).astype(BF16)
        activated_ref[...] = activated
        slope = bell + pre * jnp.exp(-0.5 * pre * pre) * 0.3989422804014327
        hidden_grad = dot(grad, down_ref[...], 1, 1) * slope
        sum_up_ref[...] += jnp.sum(hidden_grad, axis=0, keepdims=True)
        hidden_low = hidden_grad.astype(BF16)
        hidden_ref[...] = hidden_low

        branch = dot(attended, out_ref[...], 1, 0) + dot(activated, down_ref[...], 1, 0)
        branch_ref[...] = branch.astype(BF16)

        first_grad = dot(mixed_low, qkv_ref[...], 1, 1)
        second_grad = dot(hidden_low, up_ref[...], 1, 1)
        sum_norm_ref[0:1, :] += jnp.sum(first_grad * normed, axis=0, keepdims=True)
        sum_norm_ref[1:2, :] += jnp.sum(first_grad, axis=0, keepdims=True)
        sum_norm_ref[2:3, :] += jnp.sum(second_grad * normed, axis=0, keepdims=True)
        sum_norm_ref[3:4, :] += jnp.sum(second_grad, axis=0, keepdims=True)
        inner_ref[...] = (first_grad * gain_1 + second_grad * gain_2).astype(BF16)

        @pl.when(step == pl.num_programs(0) - 1)
        def _():
            sums_ref[...] = jnp.zeros_like(sums_ref)
            n = AD // 128
            for v in range(3):
                for i in range(n):
                    at = v * AD + i * 128
                    sums_ref[pl.ds(v * (width // 128) + place * n + i, 1), :] = sum_qkv_ref[:, at : at + 128]
            for i in range(FD // 128):
                sums_ref[pl.ds(base_up + place * (FD // 128) + i, 1), :] = sum_up_ref[:, i * 128 : (i + 1) * 128]
            for i in range(D // 128):
                at = slice(i * 128, (i + 1) * 128)
                sums_ref[base_out + i : base_out + i + 1, :] = sum_grad_ref[:, at] * (1.0 / (S * NT))
                for v in range(4):
                    line = base_norm + v * (D // 128) + i
                    sums_ref[line : line + 1, :] = sum_norm_ref[v : v + 1, at]

    def rows(width):
        return pl.BlockSpec((tile, width), lambda i, where: (i, 0))

    def whole(shape, index=None):
        zeros = (0,) * len(shape)
        return pl.BlockSpec(shape, index or (lambda i, where: zeros), pipeline_mode=pl.Buffered(1))

    widths = [D, D, AD, FD, 3 * AD, FD, D, D]
    flops = 2 * N * D * (2 * 3 * AD + 2 * FD + 2 * FD + 2 * AD)
    return pl.pallas_call(
        kernel,
        out_shape=[jax.ShapeDtypeStruct((N, w), BF16) for w in widths] + [jax.ShapeDtypeStruct((count, 128), F32)],
        grid_spec=pltpu.PrefetchScalarGridSpec(
            num_scalar_prefetch=1,
            grid=(N // tile,),
            in_specs=[
                rows(D),
                rows(D),
                whole(small_all.shape),
                whole((1, 128)),
                whole((D, FD)),
                whole((D, 3 * AD)),
                whole((FD, D), lambda i, where: (where[1], 0)),
                whole((AD, D), lambda i, where: (where[1], 0)),
            ],
            out_specs=[rows(w) for w in widths] + [whole((count, 128))],
            scratch_shapes=[
                pltpu.VMEM(small_all.shape[1:], F32),
                pltpu.VMEM((4, D), F32),
                pltpu.VMEM((1, 3 * AD), F32),
                pltpu.VMEM((1, FD), F32),
                pltpu.VMEM((1, 3 * AD), F32),
                pltpu.VMEM((1, FD), F32),
                pltpu.VMEM((4, D), F32),
                pltpu.VMEM((1, D), F32),
            ],
        ),
        compiler_params=pltpu.CompilerParams(
            dimension_semantics=("arbitrary",), vmem_limit_bytes=63 * 2**20
        ),
        cost_estimate=pl.CostEstimate(flops=flops, bytes_accessed=50 * 2**20, transcendentals=N * FD * 2),
        name="layer",
    )(where, in_all, grad_all, small_all, freqs, up, qkv, w_down, w_out)


def grads(first, second, attended, activated, mixed, hidden, grad, branch, inner, sums, S, R, T, TP, DP):
    N, D = grad.shape
    FD, AD = activated.shape[1], attended.shape[1]
    NT, ND, steps = 2 ** len(TP), 2 ** len(DP), len(DP)
    rows = D // S
    names = ("up", "qkv", "down", "out")
    lefts = (second, first, activated, attended)
    rights = (hidden, mixed, grad, grad)
    which_right = (0, 1, 2, 2)
    pieces = []
    for left, right, lead, mid in zip(lefts, rights, (S, S, 1, 1), (NT, NT, 1, 1)):
        pieces.append((lead, mid, left.shape[1] // (lead * ND * mid * 2), right.shape[1]))
    ways = []
    for way in (DP, DP[::-1]):
        ways.append([(bit, 1 << DP.index(bit)) for bit in way])

    def masks(bits):
        out = [0]
        for _, bit in bits:
            out += [v | bit for v in out]
        return sorted(out)

    slots = []
    for way in ways:
        table = {}
        for j in range(steps):
            for u in masks(way[j + 1 :]):
                table[j, u] = len(table)
        slots.append(table)

    def kernel(
        second_hbm, first_hbm, activated_hbm, attended_hbm, hidden_hbm, mixed_hbm, grad_hbm, branch_hbm, inner_hbm, sums_hbm,
        whole_up, whole_down, whole_out, own_qkv, branch_out, inner_out, sums_out,
        own_up, own_down, own_out, near, near_came, far_came, held, held_came,
        second_v, first_v, activated_v, attended_v, hidden_v, mixed_v, grad_v,
        part_up, part_qkv, part_down, part_out, came_up, came_qkv, came_down, came_out, all_up, all_qkv,
        load, dp_send, dp_recv, z_send, z_recv, near_send, near_recv, far_send, far_recv, held_send, held_recv,
        plane_send, plane_recv,
    ):
        s = lax.axis_index("shard")
        r = lax.axis_index("replica")
        t = sum(((r // bit) % 2 * 2**i for i, bit in enumerate(TP)), jnp.int32(0))
        d = sum(((r // bit) % 2 * 2**i for i, bit in enumerate(DP)), jnp.int32(0))

        def flipped(value, mask):
            return sum((bit * (1 - 2 * ((value // bit) % 2)) for bit in bits_of(mask)), value)

        def other(k, m):
            mask = sum(bit for i, bit in enumerate(TP) if m >> i & 1)
            return {"shard": lax.rem(s + k, S), "replica": flipped(r, mask)}

        loads = []
        order = ((hidden_hbm, hidden_v), (second_hbm, second_v), (mixed_hbm, mixed_v), (first_hbm, first_v),
                 (grad_hbm, grad_v), (activated_hbm, activated_v), (attended_hbm, attended_v))
        parts_hbm = (branch_hbm, inner_hbm)
        for i, (source, target) in enumerate(order):
            loads.append(pltpu.make_async_copy(source, target, load.at[i]))
        token_loads = [
            pltpu.make_async_copy(parts_hbm[i].at[t], near.at[i], load.at[7 + i]) for i in range(2)
        ]
        held_load = pltpu.make_async_copy(sums_hbm, held.at[0], load.at[9])
        for copy in (*loads[:2], held_load, *token_loads, *loads[2:]):
            copy.start()

        group = [(k, m) for k in range(S) for m in range(NT) if k or m]
        barrier = pltpu.get_barrier_semaphore()
        for k, m in group:
            pl.semaphore_signal(barrier, inc=1, device_id=other(k, m), device_id_type=MESH)
        for bit in DP:
            pl.semaphore_signal(barrier, inc=1, device_id={"replica": flipped(r, bit)}, device_id_type=MESH)
        pl.semaphore_wait(barrier, len(group) + steps)

        left_refs = (second_v, first_v, activated_v, attended_v)
        right_refs = (hidden_v, mixed_v, grad_v, grad_v)
        part = (part_up, part_qkv, part_down, part_out)
        came = (came_up, came_qkv, came_down, came_out)
        own = (own_up, own_qkv, own_down, own_out)

        def product(i):
            lead, mid, n, _ = pieces[i]
            if lead > 1:
                width = ND * mid * 2 * n

                def body(l, carry):
                    cols = pl.ds(pl.multiple_of(l * width, width), width)
                    value = dot(left_refs[i][:, cols], right_refs[i][...], 0, 0).astype(BF16)
                    for q in range(ND):
                        for c in range(mid):
                            for h in range(2):
                                at = ((q * mid + c) * 2 + h) * n
                                part[i][h, q, l, c] = value[at : at + n]
                    return carry

                lax.fori_loop(0, lead, body, 0)
            else:
                total = ND * 2 * n
                chunk = min(total, 512)
                per = chunk // (2 * n)

                def body(l, carry):
                    cols = pl.ds(pl.multiple_of(l * chunk, chunk), chunk)
                    value = dot(left_refs[i][:, cols], right_refs[i][...], 0, 0).astype(BF16)
                    for q in range(per):
                        for h in range(2):
                            at = (q * 2 + h) * n
                            part[i][h, l * per + q, 0, 0] = value[at : at + n]
                    return carry

                lax.fori_loop(0, total // chunk, body, 0)

        def halving(i, h, j, u):
            bit, dbit = ways[h][j]
            slot = slots[h][j, u]
            return pltpu.make_async_remote_copy(
                src_ref=part[i].at[h, flipped(d, dbit | u)], dst_ref=came[i].at[h, slot],
                send_sem=dp_send.at[i, h, slot], recv_sem=dp_recv.at[i, h, slot],
                device_id={"replica": flipped(r, bit)}, device_id_type=MESH,
            )

        def summed(i, h, mask, count, write):
            lead, mid, _, _ = pieces[i]
            at = flipped(d, mask)
            for j in range(count):
                halving(i, h, j, mask).wait_recv()

            def body(l, carry):
                for c in range(mid):
                    value = part[i][h, at, l, c].astype(F32)
                    for j in range(count):
                        value = value + came[i][h, slots[h][j, mask], l, c].astype(F32)
                    write(l, c, value.astype(BF16))
                return carry

            lax.fori_loop(0, lead, body, 0)

        def step(i, j):
            for h in range(2):
                for u in masks(ways[h][j + 1 :]):
                    mask = ways[h][j][1] | u
                    at = flipped(d, mask)
                    if j:

                        def write(l, c, value, h=h, at=at):
                            part[i][h, at, l, c] = value

                        summed(i, h, mask, j, write)
                    halving(i, h, j, u).start()

        everyone = (all_up, all_qkv)

        def to_shard(i, h, k, m):
            there = lax.rem(s + k, S)
            return pltpu.make_async_remote_copy(
                src_ref=part[i].at[h, d, there, flipped(t, m)], dst_ref=everyone[i].at[s, t, h],
                send_sem=z_send.at[i, h, k, m], recv_sem=z_recv.at[i, h, k, m],
                device_id=other(k, m), device_id_type=MESH,
            )

        def last(i):
            for h in range(2):
                if i < 2:

                    def write(l, c, value, h=h):
                        part[i][h, d, l, c] = value

                else:

                    def write(l, c, value, h=h):
                        own[i][h] = value

                summed(i, h, 0, steps, write)
            if i < 2:
                for k, m in group:
                    for h in range(2):
                        to_shard(i, h, k, m).start()
                for h in range(2):
                    everyone[i][s, t, h] = part[i][h, d, s, t]

        def collect(i):
            width = pieces[i][3]
            runs = 1 if i == 0 else 3
            n = width // runs
            for k, m in group:
                for h in range(2):
                    to_shard(i, h, k, m).wait_recv()
            for h in range(2):
                for j in range(S):
                    for u in range(NT):
                        block = everyone[i][j, u, h]
                        for v in range(runs):
                            at = (v * S * NT + j * NT + u) * n
                            own[i][h, :, at : at + n] = block[:, v * n : (v + 1) * n]

        def near_copy(i, m):
            return pltpu.make_async_remote_copy(
                src_ref=parts_hbm[i].at[flipped(t, m)], dst_ref=near_came.at[i, m - 1],
                send_sem=near_send.at[i, m], recv_sem=near_recv.at[i, m], device_id=other(0, m), device_id_type=MESH,
            )

        def far_copy(i, k):
            return pltpu.make_async_remote_copy(
                src_ref=near.at[i, lax.rem(s + k, S)], dst_ref=far_came.at[i, k - 1],
                send_sem=far_send.at[i, k], recv_sem=far_recv.at[i, k], device_id=other(k, 0), device_id_type=MESH,
            )

        def near_sum(i, j):
            value = near[i, j].astype(F32)
            for m in range(1, NT):
                value = value + near_came[i, m - 1, j].astype(F32)
            return value

        def tokens_near(i):
            token_loads[i].wait()
            for m in range(1, NT):
                near_copy(i, m).wait_recv()

            def body(k, carry):
                j = lax.rem(s + k, S)
                near[i, j] = near_sum(i, j).astype(BF16)
                return carry

            lax.fori_loop(1, S, body, 0)
            for k in range(1, S):
                far_copy(i, k).start()

        token_outs = (branch_out, inner_out)

        def tokens_far(i):
            value = near_sum(i, s)
            for k in range(1, S):
                far_copy(i, k).wait_recv()
                value = value + far_came[i, k - 1].astype(F32)
            token_outs[i][...] = value

        bits = [(0, bit) for bit in bits_of(R - 1)] + [(1, bit) for bit in bits_of(S - 1)]

        def double(i):
            axis, bit = bits[i]
            to = {"replica": flipped(r, bit)} if axis == 0 else {"shard": flipped(s, bit)}
            return pltpu.make_async_remote_copy(
                src_ref=held.at[i], dst_ref=held_came.at[i], send_sem=held_send.at[i], recv_sem=held_recv.at[i],
                device_id=to, device_id_type=MESH,
            )

        def doubled(i):
            double(i).wait_recv()
            value = held[i] + held_came[i]
            if i + 1 < len(bits):
                held[i + 1] = value
                double(i + 1).start()
            else:
                sums_out[...] = value

        wholes = {0: whole_up, 2: whole_down, 3: whole_out}
        order_of = {0: 0, 2: 1, 3: 2}

        def slot_of(i, h, dd, tt):
            n = pieces[i][2]
            if i == 0:
                at = (dd * NT + tt) * 2 * n + h * n
            else:
                at = tt * (ND * 2 * n) + dd * 2 * n + h * n
            return wholes[i].at[pl.ds(pl.multiple_of(at, n), n), :]

        def gather(i, h, m, b):
            dmask = sum(ways[h][v][1] for v in range(steps) if m >> v & 1)
            tmask = m >> steps
            slot = slot_of(i, h, flipped(d, dmask), flipped(t, tmask))
            bit = ways[h][b][0] if b < steps else TP[b - steps]
            return pltpu.make_async_remote_copy(
                src_ref=own[i].at[h] if m == 0 else slot, dst_ref=slot,
                send_sem=plane_send.at[order_of[i], h, m | 1 << b], recv_sem=plane_recv.at[order_of[i], h, m | 1 << b],
                device_id={"replica": flipped(r, bit)}, device_id_type=MESH,
            )

        positions = steps + len(TP)

        def keep_own(i, h):
            return pltpu.make_async_copy(own[i].at[h], slot_of(i, h, d, t), load.at[10 + order_of[i] * 2 + h])

        def share_own(i):
            for h in range(2):
                for b in range(positions):
                    gather(i, h, 0, b).start()
                keep_own(i, h).start()

        def share_on(i, m):
            top = m.bit_length() - 1
            for h in range(2):
                gather(i, h, m ^ 1 << top, top).wait_recv()
                for b in range(top + 1, positions):
                    gather(i, h, m, b).start()

        for i in range(2):
            for m in range(1, NT):
                near_copy(i, m).start()
        held_load.wait()
        double(0).start()
        loads[0].wait()
        loads[1].wait()
        product(0)
        step(0, 0)
        tokens_near(0)
        doubled(0)
        loads[2].wait()
        loads[3].wait()
        product(1)
        step(1, 0)
        for j in range(1, steps):
            step(0, j)
        doubled(1)
        loads[4].wait()
        loads[5].wait()
        product(2)
        step(2, 0)
        for j in range(1, steps):
            step(1, j)
        loads[6].wait()
        product(3)
        step(3, 0)
        last(0)
        for i in range(2, len(bits)):
            doubled(i)
        for j in range(1, steps):
            step(2, j)
        last(1)
        for j in range(1, steps):
            step(3, j)
        tokens_near(1)
        collect(0)
        share_own(0)
        last(2)
        share_own(2)
        last(3)
        share_own(3)
        for m in range(1, 1 << steps):
            for i in (0, 2, 3):
                share_on(i, m)
        collect(1)
        for i in range(2):
            tokens_far(i)
        for m in range(1 << steps, 1 << positions):
            for i in (0, 2, 3):
                share_on(i, m)

        for i in (2, 3, 0):
            for h in range(2):
                keep_own(i, h).wait()
                for m in range(1 << positions):
                    for b in range(m.bit_length(), positions):
                        gather(i, h, m, b).wait_send()
        for i in range(2):
            for m in range(1, NT):
                near_copy(i, m).wait_send()
            for k in range(1, S):
                far_copy(i, k).wait_send()
        for i in range(len(bits)):
            double(i).wait_send()
        for i in range(4):
            for h in range(2):
                for j, u in slots[h]:
                    halving(i, h, j, u).wait_send()
        for i in range(2):
            for h in range(2):
                for k, m in group:
                    to_shard(i, h, k, m).wait_send()

    def scratch(value):
        return pltpu.VMEM(value.shape, BF16)

    any_spec = pl.BlockSpec(memory_space=pl.ANY)
    vmem_spec = pl.BlockSpec(memory_space=pltpu.VMEM)
    operands = (second, first, activated, attended, hidden, mixed, grad)
    owns = [(2, n, width * S * NT if lead > 1 else width) for lead, _, n, width in pieces]
    wholes = [(2 * n * ND * NT, width) for _, n, width in owns]
    outs = [jax.ShapeDtypeStruct(wholes[i], BF16) for i in (0, 2, 3)]
    outs += [jax.ShapeDtypeStruct(owns[1], BF16)] + [jax.ShapeDtypeStruct((T, D), F32)] * 2
    outs += [jax.ShapeDtypeStruct(sums.shape, F32)]
    sent = sum(2 * (ND - 1) * a * b * n * w * 2 for a, b, n, w in pieces)
    count = len(bits_of(R - 1)) + len(bits_of(S - 1))
    return pl.pallas_call(
        kernel,
        out_shape=outs,
        in_specs=[any_spec] * 10,
        out_specs=[any_spec] * 3 + [vmem_spec] * 4,
        scratch_shapes=[pltpu.VMEM(owns[i], BF16) for i in (0, 2, 3)]
        + [
            pltpu.VMEM((2, S, T, D), BF16),
            pltpu.VMEM((2, max(1, NT - 1), S, T, D), BF16),
            pltpu.VMEM((2, S - 1, T, D), BF16),
            pltpu.VMEM((count,) + sums.shape, F32),
            pltpu.VMEM((count,) + sums.shape, F32),
        ]
        + [scratch(v) for v in operands]
        + [pltpu.VMEM((2, ND) + piece, BF16) for piece in pieces]
        + [pltpu.VMEM((2, ND - 1) + piece, BF16) for piece in pieces]
        + [pltpu.VMEM((S, NT, 2) + piece[2:], BF16) for piece in pieces[:2]]
        + [
            pltpu.SemaphoreType.DMA((16,)),
            pltpu.SemaphoreType.DMA((4, 2, ND - 1)),
            pltpu.SemaphoreType.DMA((4, 2, ND - 1)),
            pltpu.SemaphoreType.DMA((2, 2, S, NT)),
            pltpu.SemaphoreType.DMA((2, 2, S, NT)),
            pltpu.SemaphoreType.DMA((2, NT)),
            pltpu.SemaphoreType.DMA((2, NT)),
            pltpu.SemaphoreType.DMA((2, S)),
            pltpu.SemaphoreType.DMA((2, S)),
            pltpu.SemaphoreType.DMA((count,)),
            pltpu.SemaphoreType.DMA((count,)),
            pltpu.SemaphoreType.DMA((3, 2, ND * NT)),
            pltpu.SemaphoreType.DMA((3, 2, ND * NT)),
        ],
        compiler_params=pltpu.CompilerParams(
            collective_id=1, has_side_effects=True, vmem_limit_bytes=67043328
        ),
        cost_estimate=pl.CostEstimate(
            flops=2 * N * sum(v.shape[1] * w.shape[1] for v, w in zip(lefts, rights)),
            bytes_accessed=sent * 8, transcendentals=0,
        ),
        name="grads",
    )(*operands, branch.reshape(NT, S, T, D), inner.reshape(NT, S, T, D), sums)


def solution(mesh):
    S = mesh.shape["shard"]
    R = mesh.shape["replica"]
    TP = [1] if R > 1 and H % (2 * S) == 0 else []
    DP = [bit for bit in bits_of(R - 1) if bit not in TP]
    NT, ND = 2 ** len(TP), 2 ** len(DP)
    def flip(value, bit):
        return lax.ppermute(value, "replica", [(i, i ^ bit) for i in range(R)])

    def body(
        block_in, positions, out_grad, w_qkv, b_qkv, w_out, b_out, w_up, b_up, w_down, b_down,
        first_gain, first_shift, second_gain, second_shift,
    ):
        T, D = block_in.shape
        rows = w_qkv.shape[0]
        FS = w_down.shape[0]
        FD = FS // NT
        HN = H // S // NT
        AD = HN * HD
        G = NT * S
        s = lax.axis_index("shard")
        r = lax.axis_index("replica")
        mine = {bit: (r // bit) % 2 for bit in bits_of(R - 1)}
        t = sum((mine[bit] * 2**i for i, bit in enumerate(TP)), jnp.int32(0))

        vectors = [
            b_qkv, b_out, b_down, first_gain, first_shift, second_gain, second_shift, b_up, positions.astype(BF16)
        ]
        ends = [sum(v.shape[0] for v in vectors[: i + 1]) for i in range(len(vectors))]
        small = sum(lax.pad(v, jnp.zeros((), BF16), [(end - v.shape[0], ends[-1] - end, 0)]) for v, end in zip(vectors, ends))
        small = small.reshape(-1, 128)
        x_all, grad_all, small_all, up, qkv = fetch(
            block_in, out_grad, small, w_up, w_qkv, S, R, TP, DP, FD, AD
        )
        sizes = [b_qkv.shape[0]] + [rows] * 2
        flat = small_all[0].reshape(S, -1)
        biases = flat[:, sizes[0] : sum(sizes)].reshape(S, 2, rows).astype(F32)
        full_b_out, full_b_down = biases[:, 0].reshape(-1), biases[:, 1].reshape(-1)
        x_all = x_all.reshape(G * T, D)
        grad_all = grad_all.reshape(G * T, D)
        d = sum((mine[bit] * 2**i for i, bit in enumerate(DP)), jnp.int32(0))

        def normed_of(block):
            wide = block.astype(F32)
            offsets = wide - jnp.mean(wide, axis=-1, keepdims=True)
            inverse = lax.rsqrt(jnp.mean(offsets * offsets, axis=-1, keepdims=True) + epsilon)
            return offsets * inverse, inverse

        (
            first_low, second_low, attended, activated, mixed_low, hidden_low, branch_part, inner_part, sums,
        ) = layer(
            x_all, grad_all, small_all, rotary_freqs(), up, qkv, w_down, w_out,
            jnp.stack([s, t]), S, NT, T, 2 * T,
        )

        whole_up, whole_down, whole_out, own_qkv, branch, scaled, sums = grads(
            first_low, second_low, attended, activated, mixed_low, hidden_low, grad_all, branch_part, inner_part,
            sums, S, R, T, TP, DP,
        )
        ways = [DP + TP, DP[::-1] + TP]
        got = [{0: own_qkv[half]} for half in range(2)]
        for half in range(2):
            got[half][ways[half][0]] = flip(got[half][0], ways[half][0])
        grad_w_down = widen(whole_down)
        whole_up, whole_out, got = lax.optimization_barrier((whole_up, whole_out, got))
        for half in range(2):
            for i, bit in enumerate(ways[half][1:]):
                for m, value in list(got[half].items()):
                    got[half][m | bit] = flip(value, bit)
        grad_w_up = widen(whole_up)
        grad_w_out = widen(whole_out)
        n = own_qkv.shape[1]
        grad_w_qkv = unwritten(w_qkv.shape, F32)
        for half in range(2):
            for m, value in got[half].items():
                dmask = sum(2**i for i, bit in enumerate(DP) if m & bit)
                tmask = sum(2**i for i, bit in enumerate(TP) if m & bit)
                at = ((d ^ dmask) * NT + (t ^ tmask)) * 2 * n + half * n
                grad_w_qkv = lax.dynamic_update_slice(grad_w_qkv, value.astype(F32), (at, 0))

        block_out = (block_in.astype(F32) + branch + full_b_out + full_b_down).astype(BF16)
        normed_own, inverse_own = normed_of(block_in)
        term = inverse_own * (
            scaled
            - jnp.mean(scaled, axis=-1, keepdims=True)
            - normed_own * jnp.mean(scaled * normed_own, axis=-1, keepdims=True)
        )
        in_grad = (out_grad.astype(F32) + term).astype(BF16)

        sums = sums.reshape(-1)
        width = w_out.shape[0] * S
        lengths = [width] * 3 + [D, FS * S] + [D] * 4
        at = [sum(lengths[:i]) for i in range(len(lengths))]

        def owned(start, length):
            return lax.dynamic_slice_in_dim(sums, start + s * (length // S), length // S, 0)

        grad_b_qkv = owned(at[0], 3 * width)
        grad_b_out = owned(at[3], D)
        grad_b_up = owned(at[4], FS * S)
        smalls = [owned(at[5 + i], D) for i in range(4)]
        return (
            block_out, in_grad, grad_w_qkv, grad_b_qkv, grad_w_out, grad_b_out, grad_w_up, grad_b_up,
            grad_w_down, grad_b_out, *smalls,
        )

    rows2, row1, par2, par1 = P(("shard", "replica"), None), P(("shard", "replica")), P("shard", None), P("shard")
    return jax.shard_map(
        body,
        mesh=mesh,
        in_specs=(
            rows2, row1, rows2, par2, par1, par2, par1, par2, par1, par2, par1, par1, par1, par1, par1,
        ),
        out_specs=(
            rows2, rows2, par2, par1, par2, par1, par2, par1, par2, par1, par1, par1, par1, par1,
        ),
        check_vma=False,
    )
```

```python
import jax
import jax.numpy as jnp
from jax import lax
from jax.experimental import pallas as pl
from jax.experimental.pallas import tpu as pltpu
from jax.sharding import PartitionSpec as P

H = 8
HD = 256
ROT = 64

epsilon = 1e-05


F32 = jnp.float32
BF16 = jnp.bfloat16
MESH = pl.DeviceIdType.MESH


def rotary_freqs():
    freqs = 10000.0 ** (-(jnp.arange(ROT // 2, dtype=F32) * (2.0 / ROT)))
    return jnp.concatenate([freqs, freqs, jnp.zeros((128 - ROT,), F32)]).reshape(1, 128)


def dot(left, right, left_dim, right_dim):
    return lax.dot_general(
        left, right, (((left_dim,), (right_dim,)), ((), ())), preferred_element_type=F32
    )


def widen(value):
    rows, width = value.shape
    n = min(rows, max(8, 2**20 // width))

    def kernel(in_ref, out_ref):
        out_ref[...] = in_ref[...].astype(F32)

    spec = pl.BlockSpec((n, width), lambda i: (i, 0))
    return pl.pallas_call(
        kernel,
        grid=(rows // n,),
        in_specs=[spec],
        out_specs=spec,
        out_shape=jax.ShapeDtypeStruct(value.shape, F32),
        cost_estimate=pl.CostEstimate(flops=0, bytes_accessed=6 * rows * width, transcendentals=0),
        name="widen",
    )(value)


def unwritten(shape, dtype):
    return pl.pallas_call(
        lambda out_ref: None,
        out_shape=jax.ShapeDtypeStruct(shape, dtype),
        out_specs=pl.BlockSpec(memory_space=pl.ANY),
    )()


def bits_of(mask):
    return [1 << i for i in range(mask.bit_length()) if mask >> i & 1]

def layer(block_in, out_grad, small, freqs, w_up, w_qkv, w_down, w_out, S, R, TP, DP):
    T, D = block_in.shape
    rows, FS = w_up.shape[0], w_down.shape[0]
    NT, ND = 2 ** len(TP), 2 ** len(DP)
    FD, AD = FS // NT, w_out.shape[0] // NT
    heads = AD // HD
    scale = HD ** (-0.5)
    part = rows // ND
    third = w_qkv.shape[1] // 3
    tile = NT * T
    per = third * 3 // S // 128
    rest = D // S // 128
    base_out = 3 * third // 128
    base_up = base_out + D // 128
    base_norm = base_up + FS * S // 128
    count = base_norm + 4 * D // 128
    widths = [D, D, AD, FD, 3 * AD, FD, D, D]

    def kernel(
        small_ref, grad_ref, in_ref, up_ref, qkv_ref, down_ref, out_ref, freqs_ref,
        first_hbm, second_hbm, attended_hbm, activated_hbm, mixed_hbm, hidden_hbm, branch_hbm, inner_hbm, grad_hbm,
        small_all, sums_ref,
        first_v, second_v, attended_v, activated_v, mixed_v, hidden_v, branch_v, inner_v,
        grad_all, in_all, up_all, qkv_all, down_all, out_all,
        wide_small, norms_ref, bias_ref, bias_up_ref, sum_qkv_ref, sum_up_ref, sum_norm_ref, sum_grad_ref,
        small_send, small_recv, line_send, line_recv, tp_send, tp_recv, z_send, z_recv, dp_send, dp_recv, local, leave,
    ):
        s = lax.axis_index("shard")
        r = lax.axis_index("replica")
        t = sum(((r // bit) % 2 * 2**i for i, bit in enumerate(TP)), jnp.int32(0))
        d = sum(((r // bit) % 2 * 2**i for i, bit in enumerate(DP)), jnp.int32(0))
        place = s * NT + t

        def flipped(value, mask):
            return sum((bit * (1 - 2 * ((value // bit) % 2)) for bit in bits_of(mask)), value)

        def other(k, m):
            mask = sum(bit for i, bit in enumerate(TP) if m >> i & 1)
            return {"shard": lax.rem(s + k, S), "replica": flipped(r, mask)}

        def mate(m):
            return {"replica": flipped(r, sum(bit for i, bit in enumerate(DP) if m >> i & 1))}

        group = [(k, m) for k in range(S) for m in range(NT) if k or m]
        plane = range(1, ND)
        gathered = (grad_all, in_all)
        mine = (grad_ref, in_ref)

        def columns(ref, at, n):
            return ref.at[:, pl.ds(pl.multiple_of(at, n), n)]

        here = pl.ds(pl.multiple_of(s * rows, rows), rows)
        copies = [
            pltpu.make_async_copy(small_ref, small_all.at[t, s], local.at[0]),
            pltpu.make_async_copy(grad_ref, grad_all.at[t, s], local.at[1]),
            pltpu.make_async_copy(in_ref, in_all.at[t, s], local.at[2]),
            pltpu.make_async_copy(columns(up_ref, place * FD, FD), up_all.at[here, :], local.at[3]),
            pltpu.make_async_copy(down_ref.at[pl.ds(pl.multiple_of(t * FD, FD), FD), :], down_all, local.at[4]),
            pltpu.make_async_copy(out_ref.at[pl.ds(pl.multiple_of(t * AD, AD), AD), :], out_all, local.at[5]),
        ]
        for j in range(3):
            source = columns(qkv_ref, j * third + place * AD, AD)
            copies.append(
                pltpu.make_async_copy(source, qkv_all.at[here, j * AD : (j + 1) * AD], local.at[6 + j])
            )
        for copy in copies:
            copy.start()

        barrier = pltpu.get_barrier_semaphore()
        for k, m in group:
            pl.semaphore_signal(barrier, inc=1, device_id=other(k, m), device_id_type=MESH)
        for m in plane:
            pl.semaphore_signal(barrier, inc=1, device_id=mate(m), device_id_type=MESH)
        pl.semaphore_wait(barrier, len(group) + len(plane))

        def small_copy(k, m):
            return pltpu.make_async_remote_copy(
                src_ref=small_ref, dst_ref=small_all.at[t, s], send_sem=small_send.at[k, m],
                recv_sem=small_recv.at[k, m], device_id=other(k, m), device_id_type=MESH,
            )

        def line(i, j, way, source):
            return pltpu.make_async_remote_copy(
                src_ref=source, dst_ref=gathered[i].at[t, j], send_sem=line_send.at[i, j, way],
                recv_sem=line_recv.at[i, j], device_id={"shard": s + 2 * way - 1}, device_id_type=MESH,
            )

        def across(i, j, m, source):
            slot = gathered[i].at[t, j]
            return pltpu.make_async_remote_copy(
                src_ref=slot if source is None else source, dst_ref=slot, send_sem=tp_send.at[i, j, m],
                recv_sem=tp_recv.at[i, j, m], device_id=other(0, m), device_id_type=MESH,
            )

        def z_copies(w, k, sending):
            to = lax.rem(s + k, S)
            at = (s if sending else lax.rem(s + S - k, S)) * rows + d * part
            at = pl.ds(pl.multiple_of(at, part), part)
            source_rows = pl.ds(pl.multiple_of(d * part, part), part)
            out = []
            for j in range(1 if w == 0 else 3):
                if w == 0:
                    source = up_ref.at[source_rows, pl.ds(pl.multiple_of((to * NT + t) * FD, FD), FD)]
                    target = up_all.at[at, :]
                else:
                    col = pl.multiple_of(j * third + (to * NT + t) * AD, AD)
                    source = qkv_ref.at[source_rows, pl.ds(col, AD)]
                    target = qkv_all.at[at, j * AD : (j + 1) * AD]
                out.append(
                    pltpu.make_async_remote_copy(
                        src_ref=source, dst_ref=target, send_sem=z_send.at[k, w + j], recv_sem=z_recv.at[k, w + j],
                        device_id={"shard": to}, device_id_type=MESH,
                    )
                )
            return out

        def shared(w, k, m):
            at = pl.multiple_of(lax.rem(s + S - k, S) * rows + d * part, part)
            slot = (up_all, qkv_all)[w].at[pl.ds(at, part), :]
            return pltpu.make_async_remote_copy(
                src_ref=slot, dst_ref=slot, send_sem=dp_send.at[w, k, m], recv_sem=dp_recv.at[w, k, m],
                device_id=mate(m), device_id_type=MESH,
            )

        for k, m in group:
            small_copy(k, m).start()
        for w in range(2):
            for k in range(1, S):
                for copy in z_copies(w, k, True):
                    copy.start()
        for i in range(2):

            @pl.when(s + 1 < S)
            def _():
                line(i, s, 1, mine[i]).start()

            @pl.when(s > 0)
            def _():
                line(i, s, 0, mine[i]).start()

            for m in range(1, NT):
                across(i, s, m, mine[i]).start()

        for ref in (sum_qkv_ref, sum_up_ref, sum_norm_ref, sum_grad_ref):
            ref[...] = jnp.zeros_like(ref)
        for w in range(2):
            for k in range(1, S):
                for copy in z_copies(w, k, False):
                    copy.wait_recv()
                for m in plane:
                    shared(w, k, m).start()
        for k, m in group:
            small_copy(k, m).wait_recv()
        for copy in copies:
            copy.wait()

        wide_small[...] = small_all[0].astype(F32)
        for v in range(4):
            for j in range(S):
                for i in range(rest):
                    at = (j * rest + i) * 128
                    row = per + (2 + v) * rest + i
                    norms_ref[v : v + 1, at : at + 128] = wide_small[j, row : row + 1, :]
        for v in range(3):
            for i in range(AD // 128):
                flat = v * (third // 128) + place * (AD // 128) + i
                at = v * AD + i * 128
                bias_ref[0:1, at : at + 128] = wide_small[flat // per, pl.ds(flat % per, 1), :]
        for i in range(FD // 128):
            row = per + 6 * rest + t * (FD // 128) + i
            bias_up_ref[0:1, i * 128 : (i + 1) * 128] = wide_small[s, pl.ds(row, 1), :]

        def from_line(i, j, way):
            line(i, j, way, gathered[i].at[t, j]).wait_recv()

            @pl.when((s + 1 < S) if way else (s > 0))
            def _():
                line(i, j, way, gathered[i].at[t, j]).start()

            for m in range(1, NT):
                across(i, j, m, None).start()

        def advance(k):
            for i in range(2):

                @pl.when(s - k >= 0)
                def _():
                    from_line(i, s - k, 1)

                @pl.when(s + k < S)
                def _():
                    from_line(i, s + k, 0)

        least = jnp.where(s < S - 1 - s, s, S - 1 - s)

        def block_at(i):
            both = jnp.where(i % 2 == 1, s - (i + 1) // 2, s + i // 2)
            one = jnp.where(s < S - 1 - s, i, S - 1 - i)
            return jnp.where(i <= 2 * least, both, one)

        row = lax.broadcasted_iota(jnp.int32, (T, T), 0)
        col = lax.broadcasted_iota(jnp.int32, (T, T), 1)
        away = (row - col).astype(F32)
        lane = lax.broadcasted_iota(jnp.int32, (T, 128), 1)

        def turn(value, table, sign):
            straight, ahead, back = table
            low = value[:, :128]
            low = low * straight + sign * (
                pltpu.roll(low, 128 - ROT // 2, 1) * ahead + pltpu.roll(low, ROT // 2, 1) * back
            )
            return jnp.concatenate([low, value[:, 128:]], axis=1)

        leaving = (
            (first_v, first_hbm), (second_v, second_hbm), (attended_v, attended_hbm), (activated_v, activated_hbm),
            (mixed_v, mixed_hbm), (hidden_v, hidden_hbm), (branch_v, branch_hbm), (inner_v, inner_hbm),
            (grad_all, grad_hbm),
        )

        def depart(v, u, j):
            source, target = leaving[v]
            return pltpu.make_async_copy(source.at[u, j], target.at[u, j], leave.at[v, u, j])

        def compute(i, carry):
            j = block_at(i)

            @pl.when(i == 0)
            def _():
                advance(1)
                for k in range(1, S):
                    for m in plane:
                        shared(0, k, m).wait_recv()

            @pl.when(i >= 2)
            def _():
                advance(i)

            for m in range(1, NT):
                for v in range(2):
                    across(v, j, m, None).wait_recv()

            def join(ref):
                return jnp.concatenate([ref[u, j] for u in range(NT)], axis=0)

            def put(v, value):
                for u in range(NT):
                    leaving[v][0][u, j] = value[u * T : (u + 1) * T]

            gain_1, shift_1, gain_2, shift_2 = [norms_ref[v : v + 1, :] for v in range(4)]
            wide = join(in_all).astype(F32)
            offsets = wide - jnp.mean(wide, axis=-1, keepdims=True)
            inverse = lax.rsqrt(jnp.mean(offsets * offsets, axis=-1, keepdims=True) + epsilon)
            normed = offsets * inverse
            first = (normed * gain_1 + shift_1).astype(BF16)
            second = (normed * gain_2 + shift_2).astype(BF16)
            put(0, first)
            put(1, second)
            grad = join(grad_all)
            sum_grad_ref[...] += jnp.sum(grad.astype(F32), axis=0, keepdims=True)

            pre = dot(second, up_all[...], 1, 0) + bias_up_ref[...]
            bell = 0.5 * (1.0 + lax.erf(pre * 0.7071067811865476))
            activated = (pre * bell).astype(BF16)
            put(3, activated)
            slope = bell + pre * jnp.exp(-0.5 * pre * pre) * 0.3989422804014327
            hidden_grad = dot(grad, down_all[...], 1, 1) * slope
            sum_up_ref[...] += jnp.sum(hidden_grad, axis=0, keepdims=True)
            hidden_low = hidden_grad.astype(BF16)
            put(5, hidden_low)

            @pl.when(i == 0)
            def _():
                for k in range(1, S):
                    for m in plane:
                        shared(1, k, m).wait_recv()

            mixed = dot(first, qkv_all[...], 1, 0) + bias_ref[...]
            attended_grad = dot(grad, out_all[...], 1, 1).astype(BF16)
            attended_parts, mixed_parts = [], []
            for u in range(NT):
                flat = small_all[u, j, -1:, :].astype(F32)
                position = jnp.sum(jnp.where(row == col, flat, 0.0), axis=1, keepdims=True)
                angle = position * freqs_ref[...]
                sine = jnp.sin(angle)
                table = (
                    jnp.cos(angle),
                    jnp.where(lane < ROT // 2, -sine, 0.0),
                    jnp.where((lane >= ROT // 2) & (lane < ROT), sine, 0.0),
                )
                allowed = (away >= 0) & (away <= position)
                at_rows = slice(u * T, (u + 1) * T)
                outs, q_grads, k_grads, v_grads = [], [], [], []
                for h in range(heads):
                    at = slice(h * HD, (h + 1) * HD)
                    ag = attended_grad[at_rows, at]
                    q = turn(mixed[at_rows, at], table, 1.0).astype(BF16)
                    k = turn(mixed[at_rows, AD + h * HD : AD + (h + 1) * HD], table, 1.0).astype(BF16)
                    v = mixed[at_rows, 2 * AD + h * HD : 2 * AD + (h + 1) * HD].astype(BF16)
                    scores = jnp.where(allowed, dot(q, k, 1, 1) * scale, -1e30)
                    peak = jnp.max(scores, axis=-1, keepdims=True)
                    logsum = peak + jnp.log(jnp.sum(jnp.exp(scores - peak), axis=-1, keepdims=True))
                    probs = jnp.exp(scores - logsum)
                    low = probs.astype(BF16)
                    outs.append(dot(low, v, 1, 0).astype(BF16))
                    dprobs = dot(ag, v, 1, 1)
                    total = jnp.sum(probs * dprobs, axis=-1, keepdims=True)
                    dscores = (probs * (dprobs - total) * scale).astype(BF16)
                    q_grads.append(turn(dot(dscores, k, 1, 0), table, -1.0))
                    k_grads.append(turn(dot(dscores, q, 0, 0), table, -1.0))
                    v_grads.append(dot(low, ag, 0, 0))
                attended_parts.append(jnp.concatenate(outs, axis=1))
                mixed_parts.append(jnp.concatenate(q_grads + k_grads + v_grads, axis=1))
            attended = jnp.concatenate(attended_parts, axis=0)
            put(2, attended)
            mixed_grad = jnp.concatenate(mixed_parts, axis=0)
            sum_qkv_ref[...] += jnp.sum(mixed_grad, axis=0, keepdims=True)
            mixed_low = mixed_grad.astype(BF16)
            put(4, mixed_low)

            branch = dot(attended, out_all[...], 1, 0) + dot(activated, down_all[...], 1, 0)
            put(6, branch.astype(BF16))
            first_grad = dot(mixed_low, qkv_all[...], 1, 1)
            second_grad = dot(hidden_low, up_all[...], 1, 1)
            sum_norm_ref[0:1, :] += jnp.sum(first_grad * normed, axis=0, keepdims=True)
            sum_norm_ref[1:2, :] += jnp.sum(first_grad, axis=0, keepdims=True)
            sum_norm_ref[2:3, :] += jnp.sum(second_grad * normed, axis=0, keepdims=True)
            sum_norm_ref[3:4, :] += jnp.sum(second_grad, axis=0, keepdims=True)
            put(7, (first_grad * gain_1 + second_grad * gain_2).astype(BF16))
            for v in range(len(leaving)):
                for u in range(NT):
                    depart(v, u, j).start()
            return carry

        lax.fori_loop(0, S, compute, 0)

        sums_ref[...] = jnp.zeros_like(sums_ref)
        n = AD // 128
        for v in range(3):
            for i in range(n):
                at = v * AD + i * 128
                sums_ref[pl.ds(v * (third // 128) + place * n + i, 1), :] = sum_qkv_ref[:, at : at + 128]
        for i in range(FD // 128):
            sums_ref[pl.ds(base_up + place * (FD // 128) + i, 1), :] = sum_up_ref[:, i * 128 : (i + 1) * 128]
        for i in range(D // 128):
            at = slice(i * 128, (i + 1) * 128)
            sums_ref[base_out + i : base_out + i + 1, :] = sum_grad_ref[:, at] * (1.0 / (S * NT))
            for v in range(4):
                at_row = base_norm + v * (D // 128) + i
                sums_ref[at_row : at_row + 1, :] = sum_norm_ref[v : v + 1, at]

        for i in range(2):
            for j in range(S):

                @pl.when((s + 1 < S) & (j <= s))
                def _():
                    line(i, j, 1, gathered[i].at[t, j]).wait_send()

                @pl.when((s > 0) & (j >= s))
                def _():
                    line(i, j, 0, gathered[i].at[t, j]).wait_send()

                for m in range(1, NT):
                    across(i, j, m, None).wait_send()
        for k, m in group:
            small_copy(k, m).wait_send()
        for w in range(2):
            for k in range(1, S):
                for copy in z_copies(w, k, True):
                    copy.wait_send()
                for m in plane:
                    shared(w, k, m).wait_send()
        for v in range(len(leaving)):
            for u in range(NT):
                for j in range(S):
                    depart(v, u, j).wait()

    any_spec = pl.BlockSpec(memory_space=pl.ANY)
    vmem_spec = pl.BlockSpec(memory_space=pltpu.VMEM)
    outs = [jax.ShapeDtypeStruct((NT, S, T, w), BF16) for w in widths + [D]]
    outs += [jax.ShapeDtypeStruct((NT, S) + small.shape, BF16), jax.ShapeDtypeStruct((count, 128), F32)]
    flops = 2 * S * tile * D * (2 * 3 * AD + 2 * FD + 2 * FD + 2 * AD)
    return pl.pallas_call(
        kernel,
        out_shape=outs,
        in_specs=[any_spec] * 7 + [vmem_spec],
        out_specs=[any_spec] * 9 + [vmem_spec] * 2,
        scratch_shapes=[pltpu.VMEM((NT, S, T, w), BF16) for w in widths]
        + [
            pltpu.VMEM((NT, S, T, D), BF16),
            pltpu.VMEM((NT, S, T, D), BF16),
            pltpu.VMEM((D, FD), BF16),
            pltpu.VMEM((D, 3 * AD), BF16),
            pltpu.VMEM((FD, D), BF16),
            pltpu.VMEM((AD, D), BF16),
            pltpu.VMEM((S,) + small.shape, F32),
            pltpu.VMEM((4, D), F32),
            pltpu.VMEM((1, 3 * AD), F32),
            pltpu.VMEM((1, FD), F32),
            pltpu.VMEM((1, 3 * AD), F32),
            pltpu.VMEM((1, FD), F32),
            pltpu.VMEM((4, D), F32),
            pltpu.VMEM((1, D), F32),
            pltpu.SemaphoreType.DMA((S, NT)),
            pltpu.SemaphoreType.DMA((S, NT)),
            pltpu.SemaphoreType.DMA((2, S, 2)),
            pltpu.SemaphoreType.DMA((2, S)),
            pltpu.SemaphoreType.DMA((2, S, NT)),
            pltpu.SemaphoreType.DMA((2, S, NT)),
            pltpu.SemaphoreType.DMA((S, 4)),
            pltpu.SemaphoreType.DMA((S, 4)),
            pltpu.SemaphoreType.DMA((2, S, ND)),
            pltpu.SemaphoreType.DMA((2, S, ND)),
            pltpu.SemaphoreType.DMA((9,)),
            pltpu.SemaphoreType.DMA((9, NT, S)),
        ],
        compiler_params=pltpu.CompilerParams(
            collective_id=0, has_side_effects=True, vmem_limit_bytes=67043328
        ),
        cost_estimate=pl.CostEstimate(flops=flops, bytes_accessed=80 * 2**20, transcendentals=S * tile * FD * 2),
        name="layer",
    )(small, out_grad, block_in, w_up, w_qkv, w_down, w_out, freqs)


def grads(first, second, attended, activated, mixed, hidden, grad, branch, inner, sums, S, R, T, TP, DP):
    N, D = grad.shape
    FD, AD = activated.shape[1], attended.shape[1]
    NT, ND, steps = 2 ** len(TP), 2 ** len(DP), len(DP)
    rows = D // S
    names = ("up", "qkv", "down", "out")
    lefts = (second, first, activated, attended)
    rights = (hidden, mixed, grad, grad)
    which_right = (0, 1, 2, 2)
    pieces = []
    for left, right, lead, mid in zip(lefts, rights, (S, S, 1, 1), (NT, NT, 1, 1)):
        pieces.append((lead, mid, left.shape[1] // (lead * ND * mid * 2), right.shape[1]))
    ways = []
    for way in (DP, DP[::-1]):
        ways.append([(bit, 1 << DP.index(bit)) for bit in way])

    def masks(bits):
        out = [0]
        for _, bit in bits:
            out += [v | bit for v in out]
        return sorted(out)

    slots = []
    for way in ways:
        table = {}
        for j in range(steps):
            for u in masks(way[j + 1 :]):
                table[j, u] = len(table)
        slots.append(table)

    def kernel(
        second_hbm, first_hbm, activated_hbm, attended_hbm, hidden_hbm, mixed_hbm, grad_hbm, branch_hbm, inner_hbm, sums_hbm,
        whole_up, whole_down, whole_out, own_qkv, branch_out, inner_out, sums_out,
        own_up, own_down, own_out, near, near_came, far_came, held, held_came,
        second_v, first_v, activated_v, attended_v, hidden_v, mixed_v, grad_v,
        part_up, part_qkv, part_down, part_out, came_up, came_qkv, came_down, came_out, all_up, all_qkv,
        load, dp_send, dp_recv, z_send, z_recv, near_send, near_recv, far_send, far_recv, held_send, held_recv,
        plane_send, plane_recv,
    ):
        s = lax.axis_index("shard")
        r = lax.axis_index("replica")
        t = sum(((r // bit) % 2 * 2**i for i, bit in enumerate(TP)), jnp.int32(0))
        d = sum(((r // bit) % 2 * 2**i for i, bit in enumerate(DP)), jnp.int32(0))

        def flipped(value, mask):
            return sum((bit * (1 - 2 * ((value // bit) % 2)) for bit in bits_of(mask)), value)

        def other(k, m):
            mask = sum(bit for i, bit in enumerate(TP) if m >> i & 1)
            return {"shard": lax.rem(s + k, S), "replica": flipped(r, mask)}

        loads = []
        order = ((hidden_hbm, hidden_v), (second_hbm, second_v), (mixed_hbm, mixed_v), (first_hbm, first_v),
                 (grad_hbm, grad_v), (activated_hbm, activated_v), (attended_hbm, attended_v))
        parts_hbm = (branch_hbm, inner_hbm)
        for i, (source, target) in enumerate(order):
            loads.append(pltpu.make_async_copy(source, target, load.at[i]))
        token_loads = [
            pltpu.make_async_copy(parts_hbm[i].at[t], near.at[i], load.at[7 + i]) for i in range(2)
        ]
        held_load = pltpu.make_async_copy(sums_hbm, held.at[0], load.at[9])
        for copy in (*loads[:2], held_load, *token_loads, *loads[2:]):
            copy.start()

        group = [(k, m) for k in range(S) for m in range(NT) if k or m]
        barrier = pltpu.get_barrier_semaphore()
        for k, m in group:
            pl.semaphore_signal(barrier, inc=1, device_id=other(k, m), device_id_type=MESH)
        for bit in DP:
            pl.semaphore_signal(barrier, inc=1, device_id={"replica": flipped(r, bit)}, device_id_type=MESH)
        pl.semaphore_wait(barrier, len(group) + steps)

        left_refs = (second_v, first_v, activated_v, attended_v)
        right_refs = (hidden_v, mixed_v, grad_v, grad_v)
        part = (part_up, part_qkv, part_down, part_out)
        came = (came_up, came_qkv, came_down, came_out)
        own = (own_up, own_qkv, own_down, own_out)

        def product(i):
            lead, mid, n, _ = pieces[i]
            if lead > 1:
                width = ND * mid * 2 * n

                def body(l, carry):
                    cols = pl.ds(pl.multiple_of(l * width, width), width)
                    value = dot(left_refs[i][:, cols], right_refs[i][...], 0, 0).astype(BF16)
                    for q in range(ND):
                        for c in range(mid):
                            for h in range(2):
                                at = ((q * mid + c) * 2 + h) * n
                                part[i][h, q, l, c] = value[at : at + n]
                    return carry

                lax.fori_loop(0, lead, body, 0)
            else:
                total = ND * 2 * n
                chunk = min(total, 512)
                per = chunk // (2 * n)

                def body(l, carry):
                    cols = pl.ds(pl.multiple_of(l * chunk, chunk), chunk)
                    value = dot(left_refs[i][:, cols], right_refs[i][...], 0, 0).astype(BF16)
                    for q in range(per):
                        for h in range(2):
                            at = (q * 2 + h) * n
                            part[i][h, l * per + q, 0, 0] = value[at : at + n]
                    return carry

                lax.fori_loop(0, total // chunk, body, 0)

        def halving(i, h, j, u):
            bit, dbit = ways[h][j]
            slot = slots[h][j, u]
            return pltpu.make_async_remote_copy(
                src_ref=part[i].at[h, flipped(d, dbit | u)], dst_ref=came[i].at[h, slot],
                send_sem=dp_send.at[i, h, slot], recv_sem=dp_recv.at[i, h, slot],
                device_id={"replica": flipped(r, bit)}, device_id_type=MESH,
            )

        def summed(i, h, mask, count, write):
            lead, mid, _, _ = pieces[i]
            at = flipped(d, mask)
            for j in range(count):
                halving(i, h, j, mask).wait_recv()

            def body(l, carry):
                for c in range(mid):
                    value = part[i][h, at, l, c].astype(F32)
                    for j in range(count):
                        value = value + came[i][h, slots[h][j, mask], l, c].astype(F32)
                    write(l, c, value.astype(BF16))
                return carry

            lax.fori_loop(0, lead, body, 0)

        def step(i, j):
            for h in range(2):
                for u in masks(ways[h][j + 1 :]):
                    mask = ways[h][j][1] | u
                    at = flipped(d, mask)
                    if j:

                        def write(l, c, value, h=h, at=at):
                            part[i][h, at, l, c] = value

                        summed(i, h, mask, j, write)
                    halving(i, h, j, u).start()

        everyone = (all_up, all_qkv)

        def to_shard(i, h, k, m):
            there = lax.rem(s + k, S)
            return pltpu.make_async_remote_copy(
                src_ref=part[i].at[h, d, there, flipped(t, m)], dst_ref=everyone[i].at[s, t, h],
                send_sem=z_send.at[i, h, k, m], recv_sem=z_recv.at[i, h, k, m],
                device_id=other(k, m), device_id_type=MESH,
            )

        def last(i):
            for h in range(2):
                if i < 2:

                    def write(l, c, value, h=h):
                        part[i][h, d, l, c] = value

                else:

                    def write(l, c, value, h=h):
                        own[i][h] = value

                summed(i, h, 0, steps, write)
            if i < 2:
                for k, m in group:
                    for h in range(2):
                        to_shard(i, h, k, m).start()
                for h in range(2):
                    everyone[i][s, t, h] = part[i][h, d, s, t]

        def collect(i):
            width = pieces[i][3]
            runs = 1 if i == 0 else 3
            n = width // runs
            for k, m in group:
                for h in range(2):
                    to_shard(i, h, k, m).wait_recv()
            for h in range(2):
                for j in range(S):
                    for u in range(NT):
                        block = everyone[i][j, u, h]
                        for v in range(runs):
                            at = (v * S * NT + j * NT + u) * n
                            own[i][h, :, at : at + n] = block[:, v * n : (v + 1) * n]

        def near_copy(i, m):
            return pltpu.make_async_remote_copy(
                src_ref=parts_hbm[i].at[flipped(t, m)], dst_ref=near_came.at[i, m - 1],
                send_sem=near_send.at[i, m], recv_sem=near_recv.at[i, m], device_id=other(0, m), device_id_type=MESH,
            )

        def far_copy(i, k):
            return pltpu.make_async_remote_copy(
                src_ref=near.at[i, lax.rem(s + k, S)], dst_ref=far_came.at[i, k - 1],
                send_sem=far_send.at[i, k], recv_sem=far_recv.at[i, k], device_id=other(k, 0), device_id_type=MESH,
            )

        def near_sum(i, j):
            value = near[i, j].astype(F32)
            for m in range(1, NT):
                value = value + near_came[i, m - 1, j].astype(F32)
            return value

        def tokens_near(i):
            token_loads[i].wait()
            for m in range(1, NT):
                near_copy(i, m).wait_recv()

            def body(k, carry):
                j = lax.rem(s + k, S)
                near[i, j] = near_sum(i, j).astype(BF16)
                return carry

            lax.fori_loop(1, S, body, 0)
            for k in range(1, S):
                far_copy(i, k).start()

        token_outs = (branch_out, inner_out)

        def tokens_far(i):
            value = near_sum(i, s)
            for k in range(1, S):
                far_copy(i, k).wait_recv()
                value = value + far_came[i, k - 1].astype(F32)
            token_outs[i][...] = value

        bits = [(0, bit) for bit in bits_of(R - 1)] + [(1, bit) for bit in bits_of(S - 1)]

        def double(i):
            axis, bit = bits[i]
            to = {"replica": flipped(r, bit)} if axis == 0 else {"shard": flipped(s, bit)}
            return pltpu.make_async_remote_copy(
                src_ref=held.at[i], dst_ref=held_came.at[i], send_sem=held_send.at[i], recv_sem=held_recv.at[i],
                device_id=to, device_id_type=MESH,
            )

        def doubled(i):
            double(i).wait_recv()
            value = held[i] + held_came[i]
            if i + 1 < len(bits):
                held[i + 1] = value
                double(i + 1).start()
            else:
                sums_out[...] = value

        wholes = {0: whole_up, 2: whole_down, 3: whole_out}
        order_of = {0: 0, 2: 1, 3: 2}

        def slot_of(i, h, dd, tt):
            n = pieces[i][2]
            if i == 0:
                at = (dd * NT + tt) * 2 * n + h * n
            else:
                at = tt * (ND * 2 * n) + dd * 2 * n + h * n
            return wholes[i].at[pl.ds(pl.multiple_of(at, n), n), :]

        def gather(i, h, m, b):
            dmask = sum(ways[h][v][1] for v in range(steps) if m >> v & 1)
            tmask = m >> steps
            slot = slot_of(i, h, flipped(d, dmask), flipped(t, tmask))
            bit = ways[h][b][0] if b < steps else TP[b - steps]
            return pltpu.make_async_remote_copy(
                src_ref=own[i].at[h] if m == 0 else slot, dst_ref=slot,
                send_sem=plane_send.at[order_of[i], h, m | 1 << b], recv_sem=plane_recv.at[order_of[i], h, m | 1 << b],
                device_id={"replica": flipped(r, bit)}, device_id_type=MESH,
            )

        positions = steps + len(TP)

        def keep_own(i, h):
            return pltpu.make_async_copy(own[i].at[h], slot_of(i, h, d, t), load.at[10 + order_of[i] * 2 + h])

        def share_own(i):
            for h in range(2):
                for b in range(positions):
                    gather(i, h, 0, b).start()
                keep_own(i, h).start()

        def share_on(i, m):
            top = m.bit_length() - 1
            for h in range(2):
                gather(i, h, m ^ 1 << top, top).wait_recv()
                for b in range(top + 1, positions):
                    gather(i, h, m, b).start()

        for i in range(2):
            for m in range(1, NT):
                near_copy(i, m).start()
        held_load.wait()
        double(0).start()
        loads[0].wait()
        loads[1].wait()
        product(0)
        step(0, 0)
        tokens_near(0)
        doubled(0)
        loads[2].wait()
        loads[3].wait()
        product(1)
        step(1, 0)
        for j in range(1, steps):
            step(0, j)
        doubled(1)
        loads[4].wait()
        loads[5].wait()
        product(2)
        step(2, 0)
        for j in range(1, steps):
            step(1, j)
        loads[6].wait()
        product(3)
        step(3, 0)
        last(0)
        for i in range(2, len(bits)):
            doubled(i)
        for j in range(1, steps):
            step(2, j)
        last(1)
        for j in range(1, steps):
            step(3, j)
        tokens_near(1)
        collect(0)
        share_own(0)
        last(2)
        share_own(2)
        last(3)
        share_own(3)
        for m in range(1, 1 << steps):
            for i in (0, 2, 3):
                share_on(i, m)
        collect(1)
        for i in range(2):
            tokens_far(i)
        for m in range(1 << steps, 1 << positions):
            for i in (0, 2, 3):
                share_on(i, m)

        for i in (2, 3, 0):
            for h in range(2):
                keep_own(i, h).wait()
                for m in range(1 << positions):
                    for b in range(m.bit_length(), positions):
                        gather(i, h, m, b).wait_send()
        for i in range(2):
            for m in range(1, NT):
                near_copy(i, m).wait_send()
            for k in range(1, S):
                far_copy(i, k).wait_send()
        for i in range(len(bits)):
            double(i).wait_send()
        for i in range(4):
            for h in range(2):
                for j, u in slots[h]:
                    halving(i, h, j, u).wait_send()
        for i in range(2):
            for h in range(2):
                for k, m in group:
                    to_shard(i, h, k, m).wait_send()

    def scratch(value):
        return pltpu.VMEM(value.shape, BF16)

    any_spec = pl.BlockSpec(memory_space=pl.ANY)
    vmem_spec = pl.BlockSpec(memory_space=pltpu.VMEM)
    operands = (second, first, activated, attended, hidden, mixed, grad)
    owns = [(2, n, width * S * NT if lead > 1 else width) for lead, _, n, width in pieces]
    wholes = [(2 * n * ND * NT, width) for _, n, width in owns]
    outs = [jax.ShapeDtypeStruct(wholes[i], BF16) for i in (0, 2, 3)]
    outs += [jax.ShapeDtypeStruct(owns[1], BF16)] + [jax.ShapeDtypeStruct((T, D), F32)] * 2
    outs += [jax.ShapeDtypeStruct(sums.shape, F32)]
    sent = sum(2 * (ND - 1) * a * b * n * w * 2 for a, b, n, w in pieces)
    count = len(bits_of(R - 1)) + len(bits_of(S - 1))
    return pl.pallas_call(
        kernel,
        out_shape=outs,
        in_specs=[any_spec] * 10,
        out_specs=[any_spec] * 3 + [vmem_spec] * 4,
        scratch_shapes=[pltpu.VMEM(owns[i], BF16) for i in (0, 2, 3)]
        + [
            pltpu.VMEM((2, S, T, D), BF16),
            pltpu.VMEM((2, max(1, NT - 1), S, T, D), BF16),
            pltpu.VMEM((2, S - 1, T, D), BF16),
            pltpu.VMEM((count,) + sums.shape, F32),
            pltpu.VMEM((count,) + sums.shape, F32),
        ]
        + [scratch(v) for v in operands]
        + [pltpu.VMEM((2, ND) + piece, BF16) for piece in pieces]
        + [pltpu.VMEM((2, ND - 1) + piece, BF16) for piece in pieces]
        + [pltpu.VMEM((S, NT, 2) + piece[2:], BF16) for piece in pieces[:2]]
        + [
            pltpu.SemaphoreType.DMA((16,)),
            pltpu.SemaphoreType.DMA((4, 2, ND - 1)),
            pltpu.SemaphoreType.DMA((4, 2, ND - 1)),
            pltpu.SemaphoreType.DMA((2, 2, S, NT)),
            pltpu.SemaphoreType.DMA((2, 2, S, NT)),
            pltpu.SemaphoreType.DMA((2, NT)),
            pltpu.SemaphoreType.DMA((2, NT)),
            pltpu.SemaphoreType.DMA((2, S)),
            pltpu.SemaphoreType.DMA((2, S)),
            pltpu.SemaphoreType.DMA((count,)),
            pltpu.SemaphoreType.DMA((count,)),
            pltpu.SemaphoreType.DMA((3, 2, ND * NT)),
            pltpu.SemaphoreType.DMA((3, 2, ND * NT)),
        ],
        compiler_params=pltpu.CompilerParams(
            collective_id=1, has_side_effects=True, vmem_limit_bytes=67043328
        ),
        cost_estimate=pl.CostEstimate(
            flops=2 * N * sum(v.shape[1] * w.shape[1] for v, w in zip(lefts, rights)),
            bytes_accessed=sent * 8, transcendentals=0,
        ),
        name="grads",
    )(*operands, branch, inner, sums)


def solution(mesh):
    S = mesh.shape["shard"]
    R = mesh.shape["replica"]
    TP = [1] if R > 1 and H % (2 * S) == 0 else []
    DP = [bit for bit in bits_of(R - 1) if bit not in TP]
    NT, ND = 2 ** len(TP), 2 ** len(DP)
    def flip(value, bit):
        return lax.ppermute(value, "replica", [(i, i ^ bit) for i in range(R)])

    def body(
        block_in, positions, out_grad, w_qkv, b_qkv, w_out, b_out, w_up, b_up, w_down, b_down,
        first_gain, first_shift, second_gain, second_shift,
    ):
        T, D = block_in.shape
        rows = w_qkv.shape[0]
        FS = w_down.shape[0]
        FD = FS // NT
        HN = H // S // NT
        AD = HN * HD
        G = NT * S
        s = lax.axis_index("shard")
        r = lax.axis_index("replica")
        mine = {bit: (r // bit) % 2 for bit in bits_of(R - 1)}
        t = sum((mine[bit] * 2**i for i, bit in enumerate(TP)), jnp.int32(0))

        vectors = [
            b_qkv, b_out, b_down, first_gain, first_shift, second_gain, second_shift, b_up, positions.astype(BF16)
        ]
        ends = [sum(v.shape[0] for v in vectors[: i + 1]) for i in range(len(vectors))]
        small = sum(lax.pad(v, jnp.zeros((), BF16), [(end - v.shape[0], ends[-1] - end, 0)]) for v, end in zip(vectors, ends))
        small = small.reshape(-1, 128)
        (
            first_low, second_low, attended, activated, mixed_low, hidden_low, branch_part, inner_part, grad_all,
            small_all, sums,
        ) = layer(
            block_in, out_grad, small, rotary_freqs(), w_up, w_qkv, w_down, w_out, S, R, TP, DP
        )
        first_low, second_low, attended, activated, mixed_low, hidden_low, grad_all = [
            v.reshape(NT * S * T, -1)
            for v in (first_low, second_low, attended, activated, mixed_low, hidden_low, grad_all)
        ]
        sizes = [b_qkv.shape[0]] + [rows] * 2
        flat = small_all[0].reshape(S, -1)
        biases = flat[:, sizes[0] : sum(sizes)].reshape(S, 2, rows).astype(F32)
        full_b_out, full_b_down = biases[:, 0].reshape(-1), biases[:, 1].reshape(-1)
        d = sum((mine[bit] * 2**i for i, bit in enumerate(DP)), jnp.int32(0))

        def normed_of(block):
            wide = block.astype(F32)
            offsets = wide - jnp.mean(wide, axis=-1, keepdims=True)
            inverse = lax.rsqrt(jnp.mean(offsets * offsets, axis=-1, keepdims=True) + epsilon)
            return offsets * inverse, inverse

        whole_up, whole_down, whole_out, own_qkv, branch, scaled, sums = grads(
            first_low, second_low, attended, activated, mixed_low, hidden_low, grad_all, branch_part, inner_part,
            sums, S, R, T, TP, DP,
        )
        ways = [DP + TP, DP[::-1] + TP]
        got = [{0: own_qkv[half]} for half in range(2)]
        for half in range(2):
            got[half][ways[half][0]] = flip(got[half][0], ways[half][0])
        grad_w_down = widen(whole_down)
        whole_up, whole_out, got = lax.optimization_barrier((whole_up, whole_out, got))
        for half in range(2):
            for i, bit in enumerate(ways[half][1:]):
                for m, value in list(got[half].items()):
                    got[half][m | bit] = flip(value, bit)
        grad_w_up = widen(whole_up)
        grad_w_out = widen(whole_out)
        n = own_qkv.shape[1]
        grad_w_qkv = unwritten(w_qkv.shape, F32)
        for half in range(2):
            for m, value in got[half].items():
                dmask = sum(2**i for i, bit in enumerate(DP) if m & bit)
                tmask = sum(2**i for i, bit in enumerate(TP) if m & bit)
                at = ((d ^ dmask) * NT + (t ^ tmask)) * 2 * n + half * n
                grad_w_qkv = lax.dynamic_update_slice(grad_w_qkv, value.astype(F32), (at, 0))

        block_out = (block_in.astype(F32) + branch + full_b_out + full_b_down).astype(BF16)
        normed_own, inverse_own = normed_of(block_in)
        term = inverse_own * (
            scaled
            - jnp.mean(scaled, axis=-1, keepdims=True)
            - normed_own * jnp.mean(scaled * normed_own, axis=-1, keepdims=True)
        )
        in_grad = (out_grad.astype(F32) + term).astype(BF16)

        sums = sums.reshape(-1)
        width = w_out.shape[0] * S
        lengths = [width] * 3 + [D, FS * S] + [D] * 4
        at = [sum(lengths[:i]) for i in range(len(lengths))]

        def owned(start, length):
            return lax.dynamic_slice_in_dim(sums, start + s * (length // S), length // S, 0)

        grad_b_qkv = owned(at[0], 3 * width)
        grad_b_out = owned(at[3], D)
        grad_b_up = owned(at[4], FS * S)
        smalls = [owned(at[5 + i], D) for i in range(4)]
        return (
            block_out, in_grad, grad_w_qkv, grad_b_qkv, grad_w_out, grad_b_out, grad_w_up, grad_b_up,
            grad_w_down, grad_b_out, *smalls,
        )

    rows2, row1, par2, par1 = P(("shard", "replica"), None), P(("shard", "replica")), P("shard", None), P("shard")
    return jax.shard_map(
        body,
        mesh=mesh,
        in_specs=(
            rows2, row1, rows2, par2, par1, par2, par1, par2, par1, par2, par1, par1, par1, par1, par1,
        ),
        out_specs=(
            rows2, rows2, par2, par1, par2, par1, par2, par1, par2, par1, par1, par1, par1, par1,
        ),
        check_vma=False,
    )
```

```python
import jax
import jax.numpy as jnp
import numpy as np
from jax import lax
from jax.experimental import pallas as pl
from jax.experimental.pallas import tpu as pltpu
from jax.sharding import PartitionSpec as P

H = 8
HD = 256
ROT = 64

epsilon = 1e-05


F32 = jnp.float32
BF16 = jnp.bfloat16
MESH = pl.DeviceIdType.MESH


def rotary_freqs():
    freqs = 10000.0 ** (-(np.arange(ROT // 2) * (2.0 / ROT)))
    return np.concatenate([freqs, freqs, np.zeros(128 - ROT)]).astype(np.float32).reshape(1, 128)


def dot(left, right, left_dim, right_dim):
    return lax.dot_general(
        left, right, (((left_dim,), (right_dim,)), ((), ())), preferred_element_type=F32
    )


def widen(value):
    rows, width = value.shape
    n = min(rows, max(8, 2**20 // width))

    def kernel(in_ref, out_ref):
        out_ref[...] = in_ref[...].astype(F32)

    spec = pl.BlockSpec((n, width), lambda i: (i, 0))
    return pl.pallas_call(
        kernel,
        grid=(rows // n,),
        in_specs=[spec],
        out_specs=spec,
        out_shape=jax.ShapeDtypeStruct(value.shape, F32),
        cost_estimate=pl.CostEstimate(flops=0, bytes_accessed=6 * rows * width, transcendentals=0),
        name="widen",
    )(value)


def place(pieces, rows, result):
    n, width = pieces[0].shape
    count = len(pieces)

    def kernel(rows_ref, *refs):
        sources, target = refs[:count], refs[count + 1]
        low, wide, come, go = refs[count + 2 :]
        for i in range(count):
            pltpu.make_async_copy(sources[i], low.at[i], come.at[i]).start()
        copies = []
        for i in range(count):
            pltpu.make_async_copy(sources[i], low.at[i], come.at[i]).wait()
            wide[i] = low[i].astype(F32)
            at = pl.multiple_of(rows_ref[i], n)
            copies.append(pltpu.make_async_copy(wide.at[i], target.at[pl.ds(at, n), :], go.at[i]))
            copies[-1].start()
        for copy in copies:
            copy.wait()

    any_spec = pl.BlockSpec(memory_space=pl.ANY)
    return pl.pallas_call(
        kernel,
        in_specs=[pl.BlockSpec(memory_space=pltpu.SMEM)] + [any_spec] * (count + 1),
        out_specs=any_spec,
        out_shape=jax.ShapeDtypeStruct(result.shape, F32),
        scratch_shapes=[
            pltpu.VMEM((count, n, width), BF16),
            pltpu.VMEM((count, n, width), F32),
            pltpu.SemaphoreType.DMA((count,)),
            pltpu.SemaphoreType.DMA((count,)),
        ],
        input_output_aliases={count + 1: 0},
        cost_estimate=pl.CostEstimate(flops=0, bytes_accessed=6 * count * n * width, transcendentals=0),
        name="place",
    )(rows, *pieces, result)


def unwritten(shape, dtype):
    return pl.pallas_call(
        lambda out_ref: None,
        out_shape=jax.ShapeDtypeStruct(shape, dtype),
        out_specs=pl.BlockSpec(memory_space=pl.ANY),
    )()


def bits_of(mask):
    return [1 << i for i in range(mask.bit_length()) if mask >> i & 1]


def layer(block_in, out_grad, small, freqs, w_up, w_qkv, w_down, w_out, S, TP, DP):
    T, D = block_in.shape
    rows, FS = w_up.shape[0], w_down.shape[0]
    NT, ND = 2 ** len(TP), 2 ** len(DP)
    FD, AD = FS // NT, w_out.shape[0] // NT
    heads = AD // HD
    scale = HD ** (-0.5)
    part = rows // ND
    third = w_qkv.shape[1] // 3
    tile = NT * T
    per = third * 3 // S // 128
    rest = D // S // 128
    base_out = 3 * third // 128
    base_up = base_out + D // 128
    base_norm = base_up + FS * S // 128
    count = base_norm + 4 * D // 128
    widths = [D, D, AD, FD, 3 * AD, FD, D, D]

    def kernel(
        small_ref, grad_ref, in_ref, up_ref, qkv_ref, down_ref, out_ref, freqs_ref,
        first_hbm, second_hbm, attended_hbm, activated_hbm, mixed_hbm, hidden_hbm, branch_hbm, inner_hbm, grad_hbm,
        small_all, sums_ref, bias_sum_ref,
        first_v, second_v, attended_v, activated_v, mixed_v, hidden_v, branch_v, inner_v,
        grad_all, in_all, up_all, qkv_all, down_all, out_all,
        wide_small, norms_ref, bias_ref, bias_up_ref, sum_qkv_ref, sum_up_ref, sum_norm_ref, sum_grad_ref,
        small_send, small_recv, line_send, line_recv, tp_send, tp_recv, z_send, z_recv, dp_send, dp_recv, local, leave,
    ):
        s = lax.axis_index("shard")
        r = lax.axis_index("replica")
        t = sum(((r // bit) % 2 * 2**i for i, bit in enumerate(TP)), jnp.int32(0))
        d = sum(((r // bit) % 2 * 2**i for i, bit in enumerate(DP)), jnp.int32(0))
        place = s * NT + t

        def flipped(value, mask):
            return sum((bit * (1 - 2 * ((value // bit) % 2)) for bit in bits_of(mask)), value)

        def other(k, m):
            mask = sum(bit for i, bit in enumerate(TP) if m >> i & 1)
            return {"shard": lax.rem(s + k, S), "replica": flipped(r, mask)}

        def mate(m):
            return {"replica": flipped(r, sum(bit for i, bit in enumerate(DP) if m >> i & 1))}

        group = [(k, m) for k in range(S) for m in range(NT) if k or m]
        plane = range(1, ND)
        gathered = (grad_all, in_all)
        mine = (grad_ref, in_ref)

        def columns(ref, at, n):
            return ref.at[:, pl.ds(pl.multiple_of(at, n), n)]

        here = pl.ds(pl.multiple_of(s * rows, rows), rows)
        copies = [
            pltpu.make_async_copy(small_ref, small_all.at[t, s], local.at[0]),
            pltpu.make_async_copy(grad_ref, grad_all.at[t, s], local.at[1]),
            pltpu.make_async_copy(in_ref, in_all.at[t, s], local.at[2]),
            pltpu.make_async_copy(columns(up_ref, place * FD, FD), up_all.at[here, :], local.at[3]),
            pltpu.make_async_copy(down_ref.at[pl.ds(pl.multiple_of(t * FD, FD), FD), :], down_all, local.at[4]),
            pltpu.make_async_copy(out_ref.at[pl.ds(pl.multiple_of(t * AD, AD), AD), :], out_all, local.at[5]),
        ]
        for j in range(3):
            source = columns(qkv_ref, j * third + place * AD, AD)
            copies.append(
                pltpu.make_async_copy(source, qkv_all.at[here, j * AD : (j + 1) * AD], local.at[6 + j])
            )
        for copy in copies:
            copy.start()

        barrier = pltpu.get_barrier_semaphore()
        for k, m in group:
            pl.semaphore_signal(barrier, inc=1, device_id=other(k, m), device_id_type=MESH)
        for m in plane:
            pl.semaphore_signal(barrier, inc=1, device_id=mate(m), device_id_type=MESH)
        pl.semaphore_wait(barrier, len(group) + len(plane))

        def small_copy(k, m):
            return pltpu.make_async_remote_copy(
                src_ref=small_ref, dst_ref=small_all.at[t, s], send_sem=small_send.at[k, m],
                recv_sem=small_recv.at[k, m], device_id=other(k, m), device_id_type=MESH,
            )

        def line(i, j, way, source):
            return pltpu.make_async_remote_copy(
                src_ref=source, dst_ref=gathered[i].at[t, j], send_sem=line_send.at[i, j, way],
                recv_sem=line_recv.at[i, j], device_id={"shard": s + 2 * way - 1}, device_id_type=MESH,
            )

        def across(i, j, m, source):
            slot = gathered[i].at[t, j]
            return pltpu.make_async_remote_copy(
                src_ref=slot if source is None else source, dst_ref=slot, send_sem=tp_send.at[i, j, m],
                recv_sem=tp_recv.at[i, j, m], device_id=other(0, m), device_id_type=MESH,
            )

        def z_copies(w, k, sending):
            to = lax.rem(s + k, S)
            at = (s if sending else lax.rem(s + S - k, S)) * rows + d * part
            at = pl.ds(pl.multiple_of(at, part), part)
            source_rows = pl.ds(pl.multiple_of(d * part, part), part)
            out = []
            for j in range(1 if w == 0 else 3):
                if w == 0:
                    source = up_ref.at[source_rows, pl.ds(pl.multiple_of((to * NT + t) * FD, FD), FD)]
                    target = up_all.at[at, :]
                else:
                    col = pl.multiple_of(j * third + (to * NT + t) * AD, AD)
                    source = qkv_ref.at[source_rows, pl.ds(col, AD)]
                    target = qkv_all.at[at, j * AD : (j + 1) * AD]
                out.append(
                    pltpu.make_async_remote_copy(
                        src_ref=source, dst_ref=target, send_sem=z_send.at[k, w + j], recv_sem=z_recv.at[k, w + j],
                        device_id={"shard": to}, device_id_type=MESH,
                    )
                )
            return out

        def shared(w, k, m):
            at = pl.multiple_of(lax.rem(s + S - k, S) * rows + d * part, part)
            slot = (up_all, qkv_all)[w].at[pl.ds(at, part), :]
            return pltpu.make_async_remote_copy(
                src_ref=slot, dst_ref=slot, send_sem=dp_send.at[w, k, m], recv_sem=dp_recv.at[w, k, m],
                device_id=mate(m), device_id_type=MESH,
            )

        for k, m in group:
            small_copy(k, m).start()
        for w in range(2):
            for k in range(1, S):
                for copy in z_copies(w, k, True):
                    copy.start()
        for i in range(2):

            @pl.when(s + 1 < S)
            def _():
                line(i, s, 1, mine[i]).start()

            @pl.when(s > 0)
            def _():
                line(i, s, 0, mine[i]).start()

            for m in range(1, NT):
                across(i, s, m, mine[i]).start()

        for ref in (sum_qkv_ref, sum_up_ref, sum_norm_ref, sum_grad_ref):
            ref[...] = jnp.zeros_like(ref)
        for w in range(2):
            for k in range(1, S):
                for copy in z_copies(w, k, False):
                    copy.wait_recv()
                for m in plane:
                    shared(w, k, m).start()
        for k, m in group:
            small_copy(k, m).wait_recv()
        for copy in copies:
            copy.wait()

        wide_small[...] = small_all[0].astype(F32)
        for v in range(4):
            for j in range(S):
                for i in range(rest):
                    at = (j * rest + i) * 128
                    row = per + (2 + v) * rest + i
                    norms_ref[v : v + 1, at : at + 128] = wide_small[j, row : row + 1, :]
        for j in range(S):
            for i in range(rest):
                at = (j * rest + i) * 128
                row = per + i
                bias_sum_ref[0:1, at : at + 128] = (
                    wide_small[j, row : row + 1, :] + wide_small[j, row + rest : row + rest + 1, :]
                )
        for v in range(3):
            for i in range(AD // 128):
                flat = v * (third // 128) + place * (AD // 128) + i
                at = v * AD + i * 128
                bias_ref[0:1, at : at + 128] = wide_small[flat // per, pl.ds(flat % per, 1), :]
        for i in range(FD // 128):
            row = per + 6 * rest + t * (FD // 128) + i
            bias_up_ref[0:1, i * 128 : (i + 1) * 128] = wide_small[s, pl.ds(row, 1), :]

        def from_line(i, j, way):
            line(i, j, way, gathered[i].at[t, j]).wait_recv()

            @pl.when((s + 1 < S) if way else (s > 0))
            def _():
                line(i, j, way, gathered[i].at[t, j]).start()

            for m in range(1, NT):
                across(i, j, m, None).start()

        def advance(k):
            for i in range(2):

                @pl.when(s - k >= 0)
                def _():
                    from_line(i, s - k, 1)

                @pl.when(s + k < S)
                def _():
                    from_line(i, s + k, 0)

        least = jnp.where(s < S - 1 - s, s, S - 1 - s)

        def block_at(i):
            both = jnp.where(i % 2 == 1, s - (i + 1) // 2, s + i // 2)
            one = jnp.where(s < S - 1 - s, i, S - 1 - i)
            return jnp.where(i <= 2 * least, both, one)

        row = lax.broadcasted_iota(jnp.int32, (T, T), 0)
        col = lax.broadcasted_iota(jnp.int32, (T, T), 1)
        away = (row - col).astype(F32)
        lane = lax.broadcasted_iota(jnp.int32, (T, 128), 1)

        def turn(value, table, sign):
            straight, ahead, back = table
            low = value[:, :128]
            low = low * straight + sign * (
                pltpu.roll(low, 128 - ROT // 2, 1) * ahead + pltpu.roll(low, ROT // 2, 1) * back
            )
            return jnp.concatenate([low, value[:, 128:]], axis=1)

        leaving = (
            (first_v, first_hbm), (second_v, second_hbm), (attended_v, attended_hbm), (activated_v, activated_hbm),
            (mixed_v, mixed_hbm), (hidden_v, hidden_hbm), (branch_v, branch_hbm), (inner_v, inner_hbm),
            (grad_all, grad_hbm),
        )

        def depart(v, u, j):
            source, target = leaving[v]
            return pltpu.make_async_copy(source.at[u, j], target.at[u, j], leave.at[v, u, j])

        def compute(i, carry):
            j = block_at(i)

            @pl.when(i == 0)
            def _():
                advance(1)
                for k in range(1, S):
                    for m in plane:
                        shared(0, k, m).wait_recv()

            @pl.when(i >= 2)
            def _():
                advance(i)

            for m in range(1, NT):
                for v in range(2):
                    across(v, j, m, None).wait_recv()

            def join(ref):
                return jnp.concatenate([ref[u, j] for u in range(NT)], axis=0)

            def put(v, value):
                for u in range(NT):
                    leaving[v][0][u, j] = value[u * T : (u + 1) * T]

            gain_1, shift_1, gain_2, shift_2 = [norms_ref[v : v + 1, :] for v in range(4)]
            wide = join(in_all).astype(F32)
            offsets = wide - jnp.mean(wide, axis=-1, keepdims=True)
            inverse = lax.rsqrt(jnp.mean(offsets * offsets, axis=-1, keepdims=True) + epsilon)
            normed = offsets * inverse
            first = (normed * gain_1 + shift_1).astype(BF16)
            second = (normed * gain_2 + shift_2).astype(BF16)
            put(0, first)
            put(1, second)
            grad = join(grad_all)
            sum_grad_ref[...] += jnp.sum(grad.astype(F32), axis=0, keepdims=True)

            pre = dot(second, up_all[...], 1, 0) + bias_up_ref[...]
            bell = 0.5 * (1.0 + lax.erf(pre * 0.7071067811865476))
            activated = (pre * bell).astype(BF16)
            put(3, activated)
            slope = bell + pre * jnp.exp(-0.5 * pre * pre) * 0.3989422804014327
            hidden_grad = dot(grad, down_all[...], 1, 1) * slope
            sum_up_ref[...] += jnp.sum(hidden_grad, axis=0, keepdims=True)
            hidden_low = hidden_grad.astype(BF16)
            put(5, hidden_low)

            @pl.when(i == 0)
            def _():
                for k in range(1, S):
                    for m in plane:
                        shared(1, k, m).wait_recv()

            mixed = dot(first, qkv_all[...], 1, 0) + bias_ref[...]
            attended_grad = dot(grad, out_all[...], 1, 1).astype(BF16)
            attended_parts, mixed_parts = [], []
            for u in range(NT):
                flat = small_all[u, j, -1:, :].astype(F32)
                position = jnp.sum(jnp.where(row == col, flat, 0.0), axis=1, keepdims=True)
                angle = position * freqs_ref[...]
                sine = jnp.sin(angle)
                table = (
                    jnp.cos(angle),
                    jnp.where(lane < ROT // 2, -sine, 0.0),
                    jnp.where((lane >= ROT // 2) & (lane < ROT), sine, 0.0),
                )
                allowed = (away >= 0) & (away <= position)
                at_rows = slice(u * T, (u + 1) * T)
                outs, q_grads, k_grads, v_grads = [], [], [], []
                for h in range(heads):
                    at = slice(h * HD, (h + 1) * HD)
                    ag = attended_grad[at_rows, at]
                    q = turn(mixed[at_rows, at], table, 1.0).astype(BF16)
                    k = turn(mixed[at_rows, AD + h * HD : AD + (h + 1) * HD], table, 1.0).astype(BF16)
                    v = mixed[at_rows, 2 * AD + h * HD : 2 * AD + (h + 1) * HD].astype(BF16)
                    scores = jnp.where(allowed, dot(q, k, 1, 1) * scale, -1e30)
                    peak = jnp.max(scores, axis=-1, keepdims=True)
                    logsum = peak + jnp.log(jnp.sum(jnp.exp(scores - peak), axis=-1, keepdims=True))
                    probs = jnp.exp(scores - logsum)
                    low = probs.astype(BF16)
                    outs.append(dot(low, v, 1, 0).astype(BF16))
                    dprobs = dot(ag, v, 1, 1)
                    total = jnp.sum(probs * dprobs, axis=-1, keepdims=True)
                    dscores = (probs * (dprobs - total) * scale).astype(BF16)
                    q_grads.append(turn(dot(dscores, k, 1, 0), table, -1.0))
                    k_grads.append(turn(dot(dscores, q, 0, 0), table, -1.0))
                    v_grads.append(dot(low, ag, 0, 0))
                attended_parts.append(jnp.concatenate(outs, axis=1))
                mixed_parts.append(jnp.concatenate(q_grads + k_grads + v_grads, axis=1))
            attended = jnp.concatenate(attended_parts, axis=0)
            put(2, attended)
            mixed_grad = jnp.concatenate(mixed_parts, axis=0)
            sum_qkv_ref[...] += jnp.sum(mixed_grad, axis=0, keepdims=True)
            mixed_low = mixed_grad.astype(BF16)
            put(4, mixed_low)

            branch = dot(attended, out_all[...], 1, 0) + dot(activated, down_all[...], 1, 0)
            put(6, branch.astype(BF16))
            first_grad = dot(mixed_low, qkv_all[...], 1, 1)
            second_grad = dot(hidden_low, up_all[...], 1, 1)
            sum_norm_ref[0:1, :] += jnp.sum(first_grad * normed, axis=0, keepdims=True)
            sum_norm_ref[1:2, :] += jnp.sum(first_grad, axis=0, keepdims=True)
            sum_norm_ref[2:3, :] += jnp.sum(second_grad * normed, axis=0, keepdims=True)
            sum_norm_ref[3:4, :] += jnp.sum(second_grad, axis=0, keepdims=True)
            put(7, (first_grad * gain_1 + second_grad * gain_2).astype(BF16))
            for v in range(len(leaving)):
                for u in range(NT):
                    depart(v, u, j).start()
            return carry

        lax.fori_loop(0, S, compute, 0)

        sums_ref[...] = jnp.zeros_like(sums_ref)
        n = AD // 128
        for v in range(3):
            for i in range(n):
                at = v * AD + i * 128
                sums_ref[pl.ds(v * (third // 128) + place * n + i, 1), :] = sum_qkv_ref[:, at : at + 128]
        for i in range(FD // 128):
            sums_ref[pl.ds(base_up + place * (FD // 128) + i, 1), :] = sum_up_ref[:, i * 128 : (i + 1) * 128]
        for i in range(D // 128):
            at = slice(i * 128, (i + 1) * 128)
            sums_ref[base_out + i : base_out + i + 1, :] = sum_grad_ref[:, at] * (1.0 / (S * NT))
            for v in range(4):
                at_row = base_norm + v * (D // 128) + i
                sums_ref[at_row : at_row + 1, :] = sum_norm_ref[v : v + 1, at]

        for i in range(2):
            for j in range(S):

                @pl.when((s + 1 < S) & (j <= s))
                def _():
                    line(i, j, 1, gathered[i].at[t, j]).wait_send()

                @pl.when((s > 0) & (j >= s))
                def _():
                    line(i, j, 0, gathered[i].at[t, j]).wait_send()

                for m in range(1, NT):
                    across(i, j, m, None).wait_send()
        for k, m in group:
            small_copy(k, m).wait_send()
        for w in range(2):
            for k in range(1, S):
                for copy in z_copies(w, k, True):
                    copy.wait_send()
                for m in plane:
                    shared(w, k, m).wait_send()
        for v in range(len(leaving)):
            for u in range(NT):
                for j in range(S):
                    depart(v, u, j).wait()

    any_spec = pl.BlockSpec(memory_space=pl.ANY)
    vmem_spec = pl.BlockSpec(memory_space=pltpu.VMEM)
    outs = [jax.ShapeDtypeStruct((NT, S, T, w), BF16) for w in widths + [D]]
    outs += [jax.ShapeDtypeStruct((NT, S) + small.shape, BF16), jax.ShapeDtypeStruct((count, 128), F32)]
    outs += [jax.ShapeDtypeStruct((1, D), F32)]
    flops = 2 * S * tile * D * (2 * 3 * AD + 2 * FD + 2 * FD + 2 * AD)
    return pl.pallas_call(
        kernel,
        out_shape=outs,
        in_specs=[any_spec] * 7 + [vmem_spec],
        out_specs=[any_spec] * 9 + [vmem_spec] * 3,
        scratch_shapes=[pltpu.VMEM((NT, S, T, w), BF16) for w in widths]
        + [
            pltpu.VMEM((NT, S, T, D), BF16),
            pltpu.VMEM((NT, S, T, D), BF16),
            pltpu.VMEM((D, FD), BF16),
            pltpu.VMEM((D, 3 * AD), BF16),
            pltpu.VMEM((FD, D), BF16),
            pltpu.VMEM((AD, D), BF16),
            pltpu.VMEM((S,) + small.shape, F32),
            pltpu.VMEM((4, D), F32),
            pltpu.VMEM((1, 3 * AD), F32),
            pltpu.VMEM((1, FD), F32),
            pltpu.VMEM((1, 3 * AD), F32),
            pltpu.VMEM((1, FD), F32),
            pltpu.VMEM((4, D), F32),
            pltpu.VMEM((1, D), F32),
            pltpu.SemaphoreType.DMA((S, NT)),
            pltpu.SemaphoreType.DMA((S, NT)),
            pltpu.SemaphoreType.DMA((2, S, 2)),
            pltpu.SemaphoreType.DMA((2, S)),
            pltpu.SemaphoreType.DMA((2, S, NT)),
            pltpu.SemaphoreType.DMA((2, S, NT)),
            pltpu.SemaphoreType.DMA((S, 4)),
            pltpu.SemaphoreType.DMA((S, 4)),
            pltpu.SemaphoreType.DMA((2, S, ND)),
            pltpu.SemaphoreType.DMA((2, S, ND)),
            pltpu.SemaphoreType.DMA((9,)),
            pltpu.SemaphoreType.DMA((9, NT, S)),
        ],
        compiler_params=pltpu.CompilerParams(
            collective_id=0, has_side_effects=True, vmem_limit_bytes=67043328
        ),
        cost_estimate=pl.CostEstimate(flops=flops, bytes_accessed=80 * 2**20, transcendentals=S * tile * FD * 2),
        name="layer",
    )(small, out_grad, block_in, w_up, w_qkv, w_down, w_out, freqs)


def grads(
    first, second, attended, activated, mixed, hidden, grad, branch, inner, sums, block_in, out_grad, bias, S, R, TP, DP
):
    N, D = grad.shape
    T = block_in.shape[0]
    NT, ND, steps = 2 ** len(TP), 2 ** len(DP), len(DP)
    lefts = (second, first, activated, attended)
    rights = (hidden, mixed, grad, grad)
    pieces = []
    for left, right, lead, mid in zip(lefts, rights, (S, S, 1, 1), (NT, NT, 1, 1)):
        pieces.append((lead, mid, left.shape[1] // (lead * ND * mid * 2), right.shape[1]))
    ways = []
    for way in (DP, DP[::-1]):
        ways.append([(bit, 1 << DP.index(bit)) for bit in way])

    def masks(bits):
        out = [0]
        for _, bit in bits:
            out += [v | bit for v in out]
        return sorted(out)

    slots = []
    for way in ways:
        table = {}
        for j in range(steps):
            for u in masks(way[j + 1 :]):
                table[j, u] = len(table)
        slots.append(table)

    def kernel(
        second_hbm, first_hbm, activated_hbm, attended_hbm, hidden_hbm, mixed_hbm, grad_hbm, branch_hbm, inner_hbm, sums_hbm,
        block_hbm, out_hbm, bias_ref,
        whole_up, whole_down, whole_out, own_qkv_0, own_qkv_1, block_out, in_grad, sums_out,
        own_up, own_down, own_out, block_v, out_v, near, near_came, far_came, held, held_came,
        second_v, first_v, activated_v, attended_v, hidden_v, mixed_v, grad_v,
        part_up, part_qkv, part_down, part_out, came_up, came_qkv, came_down, came_out, all_up, all_qkv,
        load, dp_send, dp_recv, z_send, z_recv, near_send, near_recv, far_send, far_recv, held_send, held_recv,
        plane_send, plane_recv,
    ):
        s = lax.axis_index("shard")
        r = lax.axis_index("replica")
        t = sum(((r // bit) % 2 * 2**i for i, bit in enumerate(TP)), jnp.int32(0))
        d = sum(((r // bit) % 2 * 2**i for i, bit in enumerate(DP)), jnp.int32(0))

        def flipped(value, mask):
            return sum((bit * (1 - 2 * ((value // bit) % 2)) for bit in bits_of(mask)), value)

        def other(k, m):
            mask = sum(bit for i, bit in enumerate(TP) if m >> i & 1)
            return {"shard": lax.rem(s + k, S), "replica": flipped(r, mask)}

        loads = []
        order = ((hidden_hbm, hidden_v), (second_hbm, second_v), (mixed_hbm, mixed_v), (first_hbm, first_v),
                 (grad_hbm, grad_v), (activated_hbm, activated_v), (attended_hbm, attended_v))
        parts_hbm = (branch_hbm, inner_hbm)
        for i, (source, target) in enumerate(order):
            loads.append(pltpu.make_async_copy(source, target, load.at[i]))
        token_loads = [
            pltpu.make_async_copy(
                parts_hbm[i].at[t] if NT > 1 else parts_hbm[i].at[t, pl.ds(s, 1)], near.at[i], load.at[7 + i]
            )
            for i in range(2)
        ]
        held_load = pltpu.make_async_copy(sums_hbm, held.at[0], load.at[9])
        own_loads = [
            pltpu.make_async_copy(block_hbm, block_v, load.at[16]),
            pltpu.make_async_copy(out_hbm, out_v, load.at[17]),
        ]
        for copy in (loads[6], loads[4], *loads[:2], held_load, *token_loads, *loads[2:4], loads[5], *own_loads):
            copy.start()

        group = [(k, m) for k in range(S) for m in range(NT) if k or m]
        barrier = pltpu.get_barrier_semaphore()
        for k, m in group:
            pl.semaphore_signal(barrier, inc=1, device_id=other(k, m), device_id_type=MESH)
        for bit in DP:
            pl.semaphore_signal(barrier, inc=1, device_id={"replica": flipped(r, bit)}, device_id_type=MESH)
        pl.semaphore_wait(barrier, len(group) + steps)

        left_refs = (second_v, first_v, activated_v, attended_v)
        right_refs = (hidden_v, mixed_v, grad_v, grad_v)
        part = (part_up, part_qkv, part_down, part_out)
        came = (came_up, came_qkv, came_down, came_out)
        own = (own_up, (own_qkv_0, own_qkv_1), own_down, own_out)

        def product(i):
            lead, mid, n, _ = pieces[i]
            if lead > 1:
                width = ND * mid * 2 * n

                def body(l, carry):
                    cols = pl.ds(pl.multiple_of(l * width, width), width)
                    value = dot(left_refs[i][:, cols], right_refs[i][...], 0, 0).astype(BF16)
                    for q in range(ND):
                        for c in range(mid):
                            for h in range(2):
                                at = ((q * mid + c) * 2 + h) * n
                                part[i][h, q, l, c] = value[at : at + n]
                    return carry

                lax.fori_loop(0, lead, body, 0)
            else:
                total = ND * 2 * n
                chunk = min(total, 512)
                per = chunk // (2 * n)

                def body(l, carry):
                    cols = pl.ds(pl.multiple_of(l * chunk, chunk), chunk)
                    value = dot(left_refs[i][:, cols], right_refs[i][...], 0, 0).astype(BF16)
                    for q in range(per):
                        for h in range(2):
                            at = (q * 2 + h) * n
                            part[i][h, l * per + q, 0, 0] = value[at : at + n]
                    return carry

                lax.fori_loop(0, total // chunk, body, 0)

        def halving(i, h, j, u):
            bit, dbit = ways[h][j]
            slot = slots[h][j, u]
            return pltpu.make_async_remote_copy(
                src_ref=part[i].at[h, flipped(d, dbit | u)], dst_ref=came[i].at[h, slot],
                send_sem=dp_send.at[i, h, slot], recv_sem=dp_recv.at[i, h, slot],
                device_id={"replica": flipped(r, bit)}, device_id_type=MESH,
            )

        def summed(i, h, mask, count, write):
            lead, mid, _, _ = pieces[i]
            at = flipped(d, mask)
            for j in range(count):
                halving(i, h, j, mask).wait_recv()

            def body(l, carry):
                for c in range(mid):
                    value = part[i][h, at, l, c].astype(F32)
                    for j in range(count):
                        value = value + came[i][h, slots[h][j, mask], l, c].astype(F32)
                    write(l, c, value.astype(BF16))
                return carry

            lax.fori_loop(0, lead, body, 0)

        def step(i, j):
            for h in range(2):
                for u in masks(ways[h][j + 1 :]):
                    mask = ways[h][j][1] | u
                    at = flipped(d, mask)
                    if j:

                        def write(l, c, value, h=h, at=at):
                            part[i][h, at, l, c] = value

                        summed(i, h, mask, j, write)
                    halving(i, h, j, u).start()

        everyone = (all_up, all_qkv)

        def to_shard(i, h, k, m):
            there = lax.rem(s + k, S)
            return pltpu.make_async_remote_copy(
                src_ref=part[i].at[h, d, there, flipped(t, m)], dst_ref=everyone[i].at[s, t, h],
                send_sem=z_send.at[i, h, k, m], recv_sem=z_recv.at[i, h, k, m],
                device_id=other(k, m), device_id_type=MESH,
            )

        def last(i):
            for h in range(2):
                if i < 2:

                    def write(l, c, value, h=h):
                        part[i][h, d, l, c] = value

                else:

                    def write(l, c, value, h=h):
                        own[i][h] = value

                summed(i, h, 0, steps, write)
            if i < 2:
                for k, m in group:
                    for h in range(2):
                        to_shard(i, h, k, m).start()
                for h in range(2):
                    everyone[i][s, t, h] = part[i][h, d, s, t]

        def collect(i):
            width = pieces[i][3]
            runs = 1 if i == 0 else 3
            n = width // runs
            for k, m in group:
                for h in range(2):
                    to_shard(i, h, k, m).wait_recv()
            for h in range(2):
                for j in range(S):
                    for u in range(NT):
                        block = everyone[i][j, u, h]
                        for v in range(runs):
                            at = (v * S * NT + j * NT + u) * n
                            target = own[i][h] if i == 1 else own[i].at[h]
                            target[:, at : at + n] = block[:, v * n : (v + 1) * n]

        def near_copy(i, m):
            return pltpu.make_async_remote_copy(
                src_ref=parts_hbm[i].at[flipped(t, m)], dst_ref=near_came.at[i, m - 1],
                send_sem=near_send.at[i, m], recv_sem=near_recv.at[i, m], device_id=other(0, m), device_id_type=MESH,
            )

        def far_copy(i, k):
            there = lax.rem(s + k, S)
            return pltpu.make_async_remote_copy(
                src_ref=near.at[i, there] if NT > 1 else parts_hbm[i].at[t, there], dst_ref=far_came.at[i, k - 1],
                send_sem=far_send.at[i, k], recv_sem=far_recv.at[i, k], device_id=other(k, 0), device_id_type=MESH,
            )

        def near_sum(i, j):
            value = near[i, j if NT > 1 else 0].astype(F32)
            for m in range(1, NT):
                value = value + near_came[i, m - 1, j].astype(F32)
            return value

        def tokens_near(i):
            token_loads[i].wait()
            for m in range(1, NT):
                near_copy(i, m).wait_recv()

            def body(k, carry):
                j = lax.rem(s + k, S)
                near[i, j] = near_sum(i, j).astype(BF16)
                return carry

            if NT > 1:
                lax.fori_loop(1, S, body, 0)
            for k in range(1, S):
                far_copy(i, k).start()

        def tokens_far(i):
            value = near_sum(i, s)
            for k in range(1, S):
                far_copy(i, k).wait_recv()
                value = value + far_came[i, k - 1].astype(F32)
            return value

        def finish():
            for copy in own_loads:
                copy.wait()
            wide = block_v[...].astype(F32)
            block_out[...] = (wide + tokens_far(0) + bias_ref[...]).astype(BF16)
            offsets = wide - jnp.mean(wide, axis=-1, keepdims=True)
            inverse = lax.rsqrt(jnp.mean(offsets * offsets, axis=-1, keepdims=True) + epsilon)
            normed = offsets * inverse
            scaled = tokens_far(1)
            term = inverse * (
                scaled
                - jnp.mean(scaled, axis=-1, keepdims=True)
                - normed * jnp.mean(scaled * normed, axis=-1, keepdims=True)
            )
            in_grad[...] = (out_v[...].astype(F32) + term).astype(BF16)

        bits = [(0, bit) for bit in bits_of(R - 1)] + [(1, bit) for bit in bits_of(S - 1)]

        def double(i):
            axis, bit = bits[i]
            to = {"replica": flipped(r, bit)} if axis == 0 else {"shard": flipped(s, bit)}
            return pltpu.make_async_remote_copy(
                src_ref=held.at[i], dst_ref=held_came.at[i], send_sem=held_send.at[i], recv_sem=held_recv.at[i],
                device_id=to, device_id_type=MESH,
            )

        def doubled(i):
            double(i).wait_recv()
            value = held[i] + held_came[i]
            if i + 1 < len(bits):
                held[i + 1] = value
                double(i + 1).start()
            else:
                sums_out[...] = value

        wholes = {0: whole_up, 2: whole_down, 3: whole_out}
        order_of = {0: 0, 2: 1, 3: 2}

        def slot_of(i, h, dd, tt):
            n = pieces[i][2]
            if i == 0:
                at = (dd * NT + tt) * 2 * n + h * n
            else:
                at = tt * (ND * 2 * n) + dd * 2 * n + h * n
            return wholes[i].at[pl.ds(pl.multiple_of(at, n), n), :]

        def gather(i, h, m, b):
            dmask = sum(ways[h][v][1] for v in range(steps) if m >> v & 1)
            tmask = m >> steps
            slot = slot_of(i, h, flipped(d, dmask), flipped(t, tmask))
            bit = ways[h][b][0] if b < steps else TP[b - steps]
            return pltpu.make_async_remote_copy(
                src_ref=own[i].at[h] if m == 0 else slot, dst_ref=slot,
                send_sem=plane_send.at[order_of[i], h, m | 1 << b], recv_sem=plane_recv.at[order_of[i], h, m | 1 << b],
                device_id={"replica": flipped(r, bit)}, device_id_type=MESH,
            )

        positions = steps + len(TP)

        def keep_own(i, h):
            return pltpu.make_async_copy(own[i].at[h], slot_of(i, h, d, t), load.at[10 + order_of[i] * 2 + h])

        def share_own(i):
            for h in range(2):
                for b in range(positions):
                    gather(i, h, 0, b).start()
                keep_own(i, h).start()

        def share_on(i, m):
            top = m.bit_length() - 1
            for h in range(2):
                gather(i, h, m ^ 1 << top, top).wait_recv()
                for b in range(top + 1, positions):
                    gather(i, h, m, b).start()

        for i in range(2):
            for m in range(1, NT):
                near_copy(i, m).start()
        held_load.wait()
        double(0).start()
        loads[4].wait()
        loads[6].wait()
        product(3)
        step(3, 0)
        loads[0].wait()
        loads[1].wait()
        product(0)
        step(0, 0)
        tokens_near(0)
        doubled(0)
        loads[2].wait()
        loads[3].wait()
        product(1)
        step(1, 0)
        for j in range(1, steps):
            step(0, j)
        doubled(1)
        loads[5].wait()
        product(2)
        step(2, 0)
        for j in range(1, steps):
            step(1, j)
        last(0)
        for i in range(2, len(bits)):
            doubled(i)
        for j in range(1, steps):
            step(2, j)
        last(1)
        for j in range(1, steps):
            step(3, j)
        tokens_near(1)
        collect(0)
        share_own(0)
        last(2)
        share_own(2)
        last(3)
        share_own(3)
        for m in range(1, 1 << steps):
            for i in (0, 2, 3):
                share_on(i, m)
            if m == 1:
                collect(1)
                finish()
        for m in range(1 << steps, 1 << positions):
            for i in (0, 2, 3):
                share_on(i, m)

        for i in (2, 3, 0):
            for h in range(2):
                keep_own(i, h).wait()
                for m in range(1 << positions):
                    for b in range(m.bit_length(), positions):
                        gather(i, h, m, b).wait_send()
        for i in range(2):
            for m in range(1, NT):
                near_copy(i, m).wait_send()
            for k in range(1, S):
                far_copy(i, k).wait_send()
        for i in range(len(bits)):
            double(i).wait_send()
        for i in range(4):
            for h in range(2):
                for j, u in slots[h]:
                    halving(i, h, j, u).wait_send()
        for i in range(2):
            for h in range(2):
                for k, m in group:
                    to_shard(i, h, k, m).wait_send()

    def scratch(value):
        return pltpu.VMEM(value.shape, BF16)

    any_spec = pl.BlockSpec(memory_space=pl.ANY)
    vmem_spec = pl.BlockSpec(memory_space=pltpu.VMEM)
    operands = (second, first, activated, attended, hidden, mixed, grad)
    owns = [(2, n, width * S * NT if lead > 1 else width) for lead, _, n, width in pieces]
    wholes = [(2 * n * ND * NT, width) for _, n, width in owns]
    outs = [jax.ShapeDtypeStruct(wholes[i], BF16) for i in (0, 2, 3)]
    outs += [jax.ShapeDtypeStruct(owns[1][1:], BF16)] * 2 + [jax.ShapeDtypeStruct((T, D), BF16)] * 2
    outs += [jax.ShapeDtypeStruct(sums.shape, F32)]
    sent = sum(2 * (ND - 1) * a * b * n * w * 2 for a, b, n, w in pieces)
    count = len(bits_of(R - 1)) + len(bits_of(S - 1))
    return pl.pallas_call(
        kernel,
        out_shape=outs,
        in_specs=[any_spec] * 12 + [vmem_spec],
        out_specs=[any_spec] * 3 + [vmem_spec] * 5,
        scratch_shapes=[pltpu.VMEM(owns[i], BF16) for i in (0, 2, 3)]
        + [
            pltpu.VMEM((T, D), BF16),
            pltpu.VMEM((T, D), BF16),
            pltpu.VMEM((2, S if NT > 1 else 1, T, D), BF16),
            pltpu.VMEM((2, NT - 1, S, T, D) if NT > 1 else (1, 1, 1, 16, 128), BF16),
            pltpu.VMEM((2, S - 1, T, D), BF16),
            pltpu.VMEM((count,) + sums.shape, F32),
            pltpu.VMEM((count,) + sums.shape, F32),
        ]
        + [scratch(v) for v in operands]
        + [pltpu.VMEM((2, ND) + piece, BF16) for piece in pieces]
        + [pltpu.VMEM((2, ND - 1) + piece, BF16) for piece in pieces]
        + [pltpu.VMEM((S, NT, 2) + piece[2:], BF16) for piece in pieces[:2]]
        + [
            pltpu.SemaphoreType.DMA((18,)),
            pltpu.SemaphoreType.DMA((4, 2, ND - 1)),
            pltpu.SemaphoreType.DMA((4, 2, ND - 1)),
            pltpu.SemaphoreType.DMA((2, 2, S, NT)),
            pltpu.SemaphoreType.DMA((2, 2, S, NT)),
            pltpu.SemaphoreType.DMA((2, NT)),
            pltpu.SemaphoreType.DMA((2, NT)),
            pltpu.SemaphoreType.DMA((2, S)),
            pltpu.SemaphoreType.DMA((2, S)),
            pltpu.SemaphoreType.DMA((count,)),
            pltpu.SemaphoreType.DMA((count,)),
            pltpu.SemaphoreType.DMA((3, 2, ND * NT)),
            pltpu.SemaphoreType.DMA((3, 2, ND * NT)),
        ],
        compiler_params=pltpu.CompilerParams(
            collective_id=1, has_side_effects=True, vmem_limit_bytes=67043328
        ),
        cost_estimate=pl.CostEstimate(
            flops=2 * N * sum(v.shape[1] * w.shape[1] for v, w in zip(lefts, rights)),
            bytes_accessed=sent * 8, transcendentals=0,
        ),
        name="grads",
    )(*operands, branch, inner, sums, block_in, out_grad, bias)


def solution(mesh):
    S = mesh.shape["shard"]
    R = mesh.shape["replica"]
    TP = [1] if R > 1 and H % (2 * S) == 0 else []
    DP = [bit for bit in bits_of(R - 1) if bit not in TP]
    NT = 2 ** len(TP)

    def flip(value, bit):
        return lax.ppermute(value, "replica", [(i, i ^ bit) for i in range(R)])

    def body(
        block_in, positions, out_grad, w_qkv, b_qkv, w_out, b_out, w_up, b_up, w_down, b_down,
        first_gain, first_shift, second_gain, second_shift,
    ):
        T, D = block_in.shape
        FS = w_down.shape[0]
        s = lax.axis_index("shard")
        r = lax.axis_index("replica")
        mine = {bit: (r // bit) % 2 for bit in bits_of(R - 1)}
        t = sum((mine[bit] * 2**i for i, bit in enumerate(TP)), jnp.int32(0))

        vectors = [
            b_qkv, b_out, b_down, first_gain, first_shift, second_gain, second_shift, b_up, positions.astype(BF16)
        ]
        ends = [sum(v.shape[0] for v in vectors[: i + 1]) for i in range(len(vectors))]
        small = sum(lax.pad(v, jnp.zeros((), BF16), [(end - v.shape[0], ends[-1] - end, 0)]) for v, end in zip(vectors, ends))
        small = small.reshape(-1, 128)
        (
            first_low, second_low, attended, activated, mixed_low, hidden_low, branch_part, inner_part, grad_all,
            _, sums, bias,
        ) = layer(block_in, out_grad, small, rotary_freqs(), w_up, w_qkv, w_down, w_out, S, TP, DP)
        first_low, second_low, attended, activated, mixed_low, hidden_low, grad_all = [
            v.reshape(NT * S * T, -1)
            for v in (first_low, second_low, attended, activated, mixed_low, hidden_low, grad_all)
        ]
        d = sum((mine[bit] * 2**i for i, bit in enumerate(DP)), jnp.int32(0))

        whole_up, whole_down, whole_out, *own_qkv, block_out, in_grad, sums = grads(
            first_low, second_low, attended, activated, mixed_low, hidden_low, grad_all, branch_part, inner_part,
            sums, block_in, out_grad, bias, S, R, TP, DP,
        )

        ways = [DP + TP, DP[::-1] + TP]
        n = own_qkv[0].shape[0]

        def over(bit, value):
            return flip(value, bit)

        def placed(result, pieces):
            at = []
            for half, m, _ in pieces:
                dmask = sum(2**i for i, bit in enumerate(DP) if m & bit)
                tmask = sum(2**i for i, bit in enumerate(TP) if m & bit)
                at.append(((d ^ dmask) * NT + (t ^ tmask)) * 2 * n + half * n)
            return place([value for _, _, value in pieces], jnp.stack(at), result)

        def with_partners(pieces):
            for bit in TP:
                pieces = pieces + [(half, m | bit, flip(value, bit)) for half, m, value in pieces]
            return pieces

        got = [{0: own_qkv[half]} for half in range(2)]
        for i in range(len(DP)):
            for half in range(2):
                bit = ways[half][i]
                got[half].update({m | bit: over(bit, v) for m, v in list(got[half].items())})
        late = [ways[half][len(DP) - 1] for half in range(2)]
        early = [(half, m, v) for half in range(2) for m, v in got[half].items() if not m & late[half]]
        final = [(half, m, v) for half in range(2) for m, v in got[half].items() if m & late[half]]
        grad_w_down = widen(whole_down)
        grad_w_up = widen(whole_up)
        grad_w_out = widen(whole_out)
        grad_w_qkv = placed(unwritten(w_qkv.shape, F32), with_partners(early))
        grad_w_qkv = placed(grad_w_qkv, with_partners(final))

        sums = sums.reshape(-1)
        width = w_out.shape[0] * S
        lengths = [width] * 3 + [D, FS * S] + [D] * 4
        at = [sum(lengths[:i]) for i in range(len(lengths))]

        def owned(start, length):
            return lax.dynamic_slice_in_dim(sums, start + s * (length // S), length // S, 0)

        grad_b_qkv = owned(at[0], 3 * width)
        grad_b_out = owned(at[3], D)
        grad_b_up = owned(at[4], FS * S)
        smalls = [owned(at[5 + i], D) for i in range(4)]
        return (
            block_out, in_grad, grad_w_qkv, grad_b_qkv, grad_w_out, grad_b_out, grad_w_up, grad_b_up,
            grad_w_down, grad_b_out, *smalls,
        )

    rows2, row1, par2, par1 = P(("shard", "replica"), None), P(("shard", "replica")), P("shard", None), P("shard")
    return jax.shard_map(
        body,
        mesh=mesh,
        in_specs=(
            rows2, row1, rows2, par2, par1, par2, par1, par2, par1, par2, par1, par1, par1, par1, par1,
        ),
        out_specs=(
            rows2, rows2, par2, par1, par2, par1, par2, par1, par2, par1, par1, par1, par1, par1,
        ),
        check_vma=False,
    )
```

```python
import jax
import jax.numpy as jnp
import numpy as np
from jax import lax
from jax.experimental import pallas as pl
from jax.experimental.pallas import tpu as pltpu
from jax.sharding import PartitionSpec as P

H = 8
HD = 256
ROT = 64

epsilon = 1e-05


F32 = jnp.float32
BF16 = jnp.bfloat16
MESH = pl.DeviceIdType.MESH


def rotary_freqs():
    freqs = 10000.0 ** (-(np.arange(ROT // 2) * (2.0 / ROT)))
    return np.concatenate([freqs, freqs, np.zeros(128 - ROT)]).astype(np.float32).reshape(1, 128)


def all_masks(bits):
    out = [0]
    for bit in bits:
        out += [v | bit for v in out]
    return sorted(out, key=lambda v: (v.bit_count(), v))


def dot(left, right, left_dim, right_dim):
    return lax.dot_general(
        left, right, (((left_dim,), (right_dim,)), ((), ())), preferred_element_type=F32
    )


def widen(value):
    rows, width = value.shape
    n = min(rows, max(8, 2**20 // width))

    def kernel(in_ref, out_ref):
        out_ref[...] = in_ref[...].astype(F32)

    spec = pl.BlockSpec((n, width), lambda i: (i, 0))
    return pl.pallas_call(
        kernel,
        grid=(rows // n,),
        in_specs=[spec],
        out_specs=spec,
        out_shape=jax.ShapeDtypeStruct(value.shape, F32),
        cost_estimate=pl.CostEstimate(flops=0, bytes_accessed=6 * rows * width, transcendentals=0),
        name="widen",
    )(value)


def place(pieces, rows, result):
    n, width = pieces[0].shape
    count = len(pieces)

    def kernel(rows_ref, *refs):
        sources, target = refs[:count], refs[count + 1]
        low, wide, come, go = refs[count + 2 :]
        for i in range(count):
            pltpu.make_async_copy(sources[i], low.at[i], come.at[i]).start()
        copies = []
        for i in range(count):
            pltpu.make_async_copy(sources[i], low.at[i], come.at[i]).wait()
            wide[i] = low[i].astype(F32)
            at = pl.multiple_of(rows_ref[i], n)
            copies.append(pltpu.make_async_copy(wide.at[i], target.at[pl.ds(at, n), :], go.at[i]))
            copies[-1].start()
        for copy in copies:
            copy.wait()

    any_spec = pl.BlockSpec(memory_space=pl.ANY)
    return pl.pallas_call(
        kernel,
        in_specs=[pl.BlockSpec(memory_space=pltpu.SMEM)] + [any_spec] * (count + 1),
        out_specs=any_spec,
        out_shape=jax.ShapeDtypeStruct(result.shape, F32),
        scratch_shapes=[
            pltpu.VMEM((count, n, width), BF16),
            pltpu.VMEM((count, n, width), F32),
            pltpu.SemaphoreType.DMA((count,)),
            pltpu.SemaphoreType.DMA((count,)),
        ],
        input_output_aliases={count + 1: 0},
        cost_estimate=pl.CostEstimate(flops=0, bytes_accessed=6 * count * n * width, transcendentals=0),
        name="place",
    )(rows, *pieces, result)


def input_grad(block_in, out_grad, own, others):
    def kernel(block_ref, out_ref, own_ref, *refs):
        wide = block_ref[...].astype(F32)
        offsets = wide - jnp.mean(wide, axis=-1, keepdims=True)
        inverse = lax.rsqrt(jnp.mean(offsets * offsets, axis=-1, keepdims=True) + epsilon)
        normed = offsets * inverse
        scaled = own_ref[...]
        for ref in refs[:-1]:
            scaled = scaled + ref[...].astype(F32)
        term = inverse * (
            scaled
            - jnp.mean(scaled, axis=-1, keepdims=True)
            - normed * jnp.mean(scaled * normed, axis=-1, keepdims=True)
        )
        refs[-1][...] = (out_ref[...].astype(F32) + term).astype(BF16)

    return pl.pallas_call(
        kernel,
        out_shape=jax.ShapeDtypeStruct(block_in.shape, BF16),
        cost_estimate=pl.CostEstimate(flops=0, bytes_accessed=8 * 2**20, transcendentals=0),
        name="input_grad",
    )(block_in, out_grad, own, *others)


def unwritten(shape, dtype):
    return pl.pallas_call(
        lambda out_ref: None,
        out_shape=jax.ShapeDtypeStruct(shape, dtype),
        out_specs=pl.BlockSpec(memory_space=pl.ANY),
    )()


def bits_of(mask):
    return [1 << i for i in range(mask.bit_length()) if mask >> i & 1]


def layer(block_in, out_grad, small, freqs, w_up, w_qkv, w_down, w_out, S, TP, DP):
    T, D = block_in.shape
    rows, FS = w_up.shape[0], w_down.shape[0]
    NT, ND = 2 ** len(TP), 2 ** len(DP)
    FD, AD = FS // NT, w_out.shape[0] // NT
    heads = AD // HD
    scale = HD ** (-0.5)
    part = rows // ND
    third = w_qkv.shape[1] // 3
    tile = NT * T
    per = third * 3 // S // 128
    rest = D // S // 128
    base_out = 3 * third // 128
    base_up = base_out + D // 128
    base_norm = base_up + FS * S // 128
    count = base_norm + 4 * D // 128
    widths = [D, D, AD, FD, 3 * AD, FD, D, D]

    def kernel(
        small_ref, grad_ref, in_ref, up_ref, qkv_ref, down_ref, out_ref, freqs_ref,
        first_hbm, second_hbm, attended_hbm, activated_hbm, mixed_hbm, hidden_hbm, branch_hbm, inner_hbm, grad_hbm,
        small_all, sums_ref, bias_sum_ref,
        first_v, second_v, attended_v, activated_v, mixed_v, hidden_v, branch_v, inner_v,
        grad_all, in_all, up_all, qkv_all, down_all, out_all,
        wide_small, norms_ref, bias_ref, bias_up_ref, sum_qkv_ref, sum_up_ref, sum_norm_ref, sum_grad_ref,
        small_send, small_recv, line_send, line_recv, tp_send, tp_recv, z_send, z_recv, dp_send, dp_recv, local, leave,
    ):
        s = lax.axis_index("shard")
        r = lax.axis_index("replica")
        t = sum(((r // bit) % 2 * 2**i for i, bit in enumerate(TP)), jnp.int32(0))
        d = sum(((r // bit) % 2 * 2**i for i, bit in enumerate(DP)), jnp.int32(0))
        place = s * NT + t

        def flipped(value, mask):
            return sum((bit * (1 - 2 * ((value // bit) % 2)) for bit in bits_of(mask)), value)

        def other(k, m):
            mask = sum(bit for i, bit in enumerate(TP) if m >> i & 1)
            return {"shard": lax.rem(s + k, S), "replica": flipped(r, mask)}

        def mate(m):
            return {"replica": flipped(r, sum(bit for i, bit in enumerate(DP) if m >> i & 1))}

        group = [(k, m) for k in range(S) for m in range(NT) if k or m]
        plane = range(1, ND)
        gathered = (grad_all, in_all)
        mine = (grad_ref, in_ref)

        def columns(ref, at, n):
            return ref.at[:, pl.ds(pl.multiple_of(at, n), n)]

        here = pl.ds(pl.multiple_of(s * rows, rows), rows)
        copies = [
            pltpu.make_async_copy(small_ref, small_all.at[t, s], local.at[0]),
            pltpu.make_async_copy(grad_ref, grad_all.at[t, s], local.at[1]),
            pltpu.make_async_copy(in_ref, in_all.at[t, s], local.at[2]),
            pltpu.make_async_copy(columns(up_ref, place * FD, FD), up_all.at[here, :], local.at[3]),
            pltpu.make_async_copy(down_ref.at[pl.ds(pl.multiple_of(t * FD, FD), FD), :], down_all, local.at[4]),
            pltpu.make_async_copy(out_ref.at[pl.ds(pl.multiple_of(t * AD, AD), AD), :], out_all, local.at[5]),
        ]
        for j in range(3):
            source = columns(qkv_ref, j * third + place * AD, AD)
            copies.append(
                pltpu.make_async_copy(source, qkv_all.at[here, j * AD : (j + 1) * AD], local.at[6 + j])
            )
        for copy in copies:
            copy.start()

        barrier = pltpu.get_barrier_semaphore()
        for k, m in group:
            pl.semaphore_signal(barrier, inc=1, device_id=other(k, m), device_id_type=MESH)
        for m in plane:
            pl.semaphore_signal(barrier, inc=1, device_id=mate(m), device_id_type=MESH)
        pl.semaphore_wait(barrier, len(group) + len(plane))

        def small_copy(k, m):
            return pltpu.make_async_remote_copy(
                src_ref=small_ref, dst_ref=small_all.at[t, s], send_sem=small_send.at[k, m],
                recv_sem=small_recv.at[k, m], device_id=other(k, m), device_id_type=MESH,
            )

        def line(i, j, way, source):
            return pltpu.make_async_remote_copy(
                src_ref=source, dst_ref=gathered[i].at[t, j], send_sem=line_send.at[i, j, way],
                recv_sem=line_recv.at[i, j], device_id={"shard": s + 2 * way - 1}, device_id_type=MESH,
            )

        def across(i, j, m, source):
            slot = gathered[i].at[t, j]
            return pltpu.make_async_remote_copy(
                src_ref=slot if source is None else source, dst_ref=slot, send_sem=tp_send.at[i, j, m],
                recv_sem=tp_recv.at[i, j, m], device_id=other(0, m), device_id_type=MESH,
            )

        def z_copies(w, k, sending):
            to = lax.rem(s + k, S)
            at = (s if sending else lax.rem(s + S - k, S)) * rows + d * part
            at = pl.ds(pl.multiple_of(at, part), part)
            source_rows = pl.ds(pl.multiple_of(d * part, part), part)
            out = []
            for j in range(1 if w == 0 else 3):
                if w == 0:
                    source = up_ref.at[source_rows, pl.ds(pl.multiple_of((to * NT + t) * FD, FD), FD)]
                    target = up_all.at[at, :]
                else:
                    col = pl.multiple_of(j * third + (to * NT + t) * AD, AD)
                    source = qkv_ref.at[source_rows, pl.ds(col, AD)]
                    target = qkv_all.at[at, j * AD : (j + 1) * AD]
                out.append(
                    pltpu.make_async_remote_copy(
                        src_ref=source, dst_ref=target, send_sem=z_send.at[k, w + j], recv_sem=z_recv.at[k, w + j],
                        device_id={"shard": to}, device_id_type=MESH,
                    )
                )
            return out

        def shared(w, k, m):
            at = pl.multiple_of(lax.rem(s + S - k, S) * rows + d * part, part)
            slot = (up_all, qkv_all)[w].at[pl.ds(at, part), :]
            return pltpu.make_async_remote_copy(
                src_ref=slot, dst_ref=slot, send_sem=dp_send.at[w, k, m], recv_sem=dp_recv.at[w, k, m],
                device_id=mate(m), device_id_type=MESH,
            )

        for k, m in group:
            small_copy(k, m).start()
        for w in range(2):
            for k in range(1, S):
                for copy in z_copies(w, k, True):
                    copy.start()
        for i in range(2):

            @pl.when(s + 1 < S)
            def _():
                line(i, s, 1, mine[i]).start()

            @pl.when(s > 0)
            def _():
                line(i, s, 0, mine[i]).start()

            for m in range(1, NT):
                across(i, s, m, mine[i]).start()

        for ref in (sum_qkv_ref, sum_up_ref, sum_norm_ref, sum_grad_ref):
            ref[...] = jnp.zeros_like(ref)
        for w in range(2):
            for k in range(1, S):
                for copy in z_copies(w, k, False):
                    copy.wait_recv()
                for m in plane:
                    shared(w, k, m).start()
        for k, m in group:
            small_copy(k, m).wait_recv()
        for copy in copies:
            copy.wait()

        wide_small[...] = small_all[0].astype(F32)
        for v in range(4):
            for j in range(S):
                for i in range(rest):
                    at = (j * rest + i) * 128
                    row = per + (2 + v) * rest + i
                    norms_ref[v : v + 1, at : at + 128] = wide_small[j, row : row + 1, :]
        for j in range(S):
            for i in range(rest):
                at = (j * rest + i) * 128
                row = per + i
                bias_sum_ref[0:1, at : at + 128] = (
                    wide_small[j, row : row + 1, :] + wide_small[j, row + rest : row + rest + 1, :]
                )
        for v in range(3):
            for i in range(AD // 128):
                flat = v * (third // 128) + place * (AD // 128) + i
                at = v * AD + i * 128
                bias_ref[0:1, at : at + 128] = wide_small[flat // per, pl.ds(flat % per, 1), :]
        for i in range(FD // 128):
            row = per + 6 * rest + t * (FD // 128) + i
            bias_up_ref[0:1, i * 128 : (i + 1) * 128] = wide_small[s, pl.ds(row, 1), :]

        def from_line(i, j, way):
            line(i, j, way, gathered[i].at[t, j]).wait_recv()

            @pl.when((s + 1 < S) if way else (s > 0))
            def _():
                line(i, j, way, gathered[i].at[t, j]).start()

            for m in range(1, NT):
                across(i, j, m, None).start()

        def advance(k):
            for i in range(2):

                @pl.when(s - k >= 0)
                def _():
                    from_line(i, s - k, 1)

                @pl.when(s + k < S)
                def _():
                    from_line(i, s + k, 0)

        least = jnp.where(s < S - 1 - s, s, S - 1 - s)

        def block_at(i):
            both = jnp.where(i % 2 == 1, s - (i + 1) // 2, s + i // 2)
            one = jnp.where(s < S - 1 - s, i, S - 1 - i)
            return jnp.where(i <= 2 * least, both, one)

        row = lax.broadcasted_iota(jnp.int32, (T, T), 0)
        col = lax.broadcasted_iota(jnp.int32, (T, T), 1)
        away = (row - col).astype(F32)
        lane = lax.broadcasted_iota(jnp.int32, (T, 128), 1)

        def turn(value, table, sign):
            straight, ahead, back = table
            low = value[:, :128]
            low = low * straight + sign * (
                pltpu.roll(low, 128 - ROT // 2, 1) * ahead + pltpu.roll(low, ROT // 2, 1) * back
            )
            return jnp.concatenate([low, value[:, 128:]], axis=1)

        leaving = (
            (first_v, first_hbm), (second_v, second_hbm), (attended_v, attended_hbm), (activated_v, activated_hbm),
            (mixed_v, mixed_hbm), (hidden_v, hidden_hbm), (branch_v, branch_hbm), (inner_v, inner_hbm),
            (grad_all, grad_hbm),
        )

        def depart(v, u, j):
            source, target = leaving[v]
            return pltpu.make_async_copy(source.at[u, j], target.at[u, j], leave.at[v, u, j])

        def compute(i, carry):
            j = block_at(i)

            @pl.when(i == 0)
            def _():
                advance(1)
                for k in range(1, S):
                    for m in plane:
                        shared(0, k, m).wait_recv()

            @pl.when(i == 1)
            def _():
                advance(2)

            @pl.when(i >= 3)
            def _():
                advance(i)

            for m in range(1, NT):
                for v in range(2):
                    across(v, j, m, None).wait_recv()

            def join(ref):
                return jnp.concatenate([ref[u, j] for u in range(NT)], axis=0)

            def put(v, value):
                for u in range(NT):
                    leaving[v][0][u, j] = value[u * T : (u + 1) * T]

            gain_1, shift_1, gain_2, shift_2 = [norms_ref[v : v + 1, :] for v in range(4)]
            wide = join(in_all).astype(F32)
            offsets = wide - jnp.mean(wide, axis=-1, keepdims=True)
            inverse = lax.rsqrt(jnp.mean(offsets * offsets, axis=-1, keepdims=True) + epsilon)
            normed = offsets * inverse
            first = (normed * gain_1 + shift_1).astype(BF16)
            second = (normed * gain_2 + shift_2).astype(BF16)
            put(0, first)
            put(1, second)
            grad = join(grad_all)
            sum_grad_ref[...] += jnp.sum(grad.astype(F32), axis=0, keepdims=True)

            pre = dot(second, up_all[...], 1, 0) + bias_up_ref[...]
            bell = 0.5 * (1.0 + lax.erf(pre * 0.7071067811865476))
            activated = (pre * bell).astype(BF16)
            put(3, activated)
            slope = bell + pre * jnp.exp(-0.5 * pre * pre) * 0.3989422804014327
            hidden_grad = dot(grad, down_all[...], 1, 1) * slope
            sum_up_ref[...] += jnp.sum(hidden_grad, axis=0, keepdims=True)
            hidden_low = hidden_grad.astype(BF16)
            put(5, hidden_low)

            @pl.when(i == 0)
            def _():
                for k in range(1, S):
                    for m in plane:
                        shared(1, k, m).wait_recv()

            mixed = dot(first, qkv_all[...], 1, 0) + bias_ref[...]
            attended_grad = dot(grad, out_all[...], 1, 1).astype(BF16)
            attended_parts, mixed_parts = [], []
            for u in range(NT):
                flat = small_all[u, j, -1:, :].astype(F32)
                position = jnp.sum(jnp.where(row == col, flat, 0.0), axis=1, keepdims=True)
                angle = position * freqs_ref[...]
                sine = jnp.sin(angle)
                table = (
                    jnp.cos(angle),
                    jnp.where(lane < ROT // 2, -sine, 0.0),
                    jnp.where((lane >= ROT // 2) & (lane < ROT), sine, 0.0),
                )
                allowed = (away >= 0) & (away <= position)
                at_rows = slice(u * T, (u + 1) * T)
                outs, q_grads, k_grads, v_grads = [], [], [], []
                for h in range(heads):
                    at = slice(h * HD, (h + 1) * HD)
                    ag = attended_grad[at_rows, at]
                    q = turn(mixed[at_rows, at], table, 1.0).astype(BF16)
                    k = turn(mixed[at_rows, AD + h * HD : AD + (h + 1) * HD], table, 1.0).astype(BF16)
                    v = mixed[at_rows, 2 * AD + h * HD : 2 * AD + (h + 1) * HD].astype(BF16)
                    scores = jnp.where(allowed, dot(q, k, 1, 1) * scale, -1e30)
                    peak = jnp.max(scores, axis=-1, keepdims=True)
                    logsum = peak + jnp.log(jnp.sum(jnp.exp(scores - peak), axis=-1, keepdims=True))
                    probs = jnp.exp(scores - logsum)
                    low = probs.astype(BF16)
                    outs.append(dot(low, v, 1, 0).astype(BF16))
                    dprobs = dot(ag, v, 1, 1)
                    total = jnp.sum(probs * dprobs, axis=-1, keepdims=True)
                    dscores = (probs * (dprobs - total) * scale).astype(BF16)
                    q_grads.append(turn(dot(dscores, k, 1, 0), table, -1.0))
                    k_grads.append(turn(dot(dscores, q, 0, 0), table, -1.0))
                    v_grads.append(dot(low, ag, 0, 0))
                attended_parts.append(jnp.concatenate(outs, axis=1))
                mixed_parts.append(jnp.concatenate(q_grads + k_grads + v_grads, axis=1))
            attended = jnp.concatenate(attended_parts, axis=0)
            put(2, attended)
            mixed_grad = jnp.concatenate(mixed_parts, axis=0)
            sum_qkv_ref[...] += jnp.sum(mixed_grad, axis=0, keepdims=True)
            mixed_low = mixed_grad.astype(BF16)
            put(4, mixed_low)

            branch = dot(attended, out_all[...], 1, 0) + dot(activated, down_all[...], 1, 0)
            put(6, branch.astype(BF16))
            first_grad = dot(mixed_low, qkv_all[...], 1, 1)
            second_grad = dot(hidden_low, up_all[...], 1, 1)
            sum_norm_ref[0:1, :] += jnp.sum(first_grad * normed, axis=0, keepdims=True)
            sum_norm_ref[1:2, :] += jnp.sum(first_grad, axis=0, keepdims=True)
            sum_norm_ref[2:3, :] += jnp.sum(second_grad * normed, axis=0, keepdims=True)
            sum_norm_ref[3:4, :] += jnp.sum(second_grad, axis=0, keepdims=True)
            put(7, (first_grad * gain_1 + second_grad * gain_2).astype(BF16))
            for v in range(len(leaving)):
                for u in range(NT):
                    depart(v, u, j).start()
            return carry

        lax.fori_loop(0, S, compute, 0)

        sums_ref[...] = jnp.zeros_like(sums_ref)
        n = AD // 128
        for v in range(3):
            for i in range(n):
                at = v * AD + i * 128
                sums_ref[pl.ds(v * (third // 128) + place * n + i, 1), :] = sum_qkv_ref[:, at : at + 128]
        for i in range(FD // 128):
            sums_ref[pl.ds(base_up + place * (FD // 128) + i, 1), :] = sum_up_ref[:, i * 128 : (i + 1) * 128]
        for i in range(D // 128):
            at = slice(i * 128, (i + 1) * 128)
            sums_ref[base_out + i : base_out + i + 1, :] = sum_grad_ref[:, at] * (1.0 / (S * NT))
            for v in range(4):
                at_row = base_norm + v * (D // 128) + i
                sums_ref[at_row : at_row + 1, :] = sum_norm_ref[v : v + 1, at]

        for i in range(2):
            for j in range(S):

                @pl.when((s + 1 < S) & (j <= s))
                def _():
                    line(i, j, 1, gathered[i].at[t, j]).wait_send()

                @pl.when((s > 0) & (j >= s))
                def _():
                    line(i, j, 0, gathered[i].at[t, j]).wait_send()

                for m in range(1, NT):
                    across(i, j, m, None).wait_send()
        for k, m in group:
            small_copy(k, m).wait_send()
        for w in range(2):
            for k in range(1, S):
                for copy in z_copies(w, k, True):
                    copy.wait_send()
                for m in plane:
                    shared(w, k, m).wait_send()
        for v in range(len(leaving)):
            for u in range(NT):
                for j in range(S):
                    depart(v, u, j).wait()

    any_spec = pl.BlockSpec(memory_space=pl.ANY)
    vmem_spec = pl.BlockSpec(memory_space=pltpu.VMEM)
    outs = [jax.ShapeDtypeStruct((NT, S, T, w), BF16) for w in widths + [D]]
    outs += [jax.ShapeDtypeStruct((NT, S) + small.shape, BF16), jax.ShapeDtypeStruct((count, 128), F32)]
    outs += [jax.ShapeDtypeStruct((1, D), F32)]
    flops = 2 * S * tile * D * (2 * 3 * AD + 2 * FD + 2 * FD + 2 * AD)
    return pl.pallas_call(
        kernel,
        out_shape=outs,
        in_specs=[any_spec] * 7 + [vmem_spec],
        out_specs=[any_spec] * 9 + [vmem_spec] * 3,
        scratch_shapes=[pltpu.VMEM((NT, S, T, w), BF16) for w in widths]
        + [
            pltpu.VMEM((NT, S, T, D), BF16),
            pltpu.VMEM((NT, S, T, D), BF16),
            pltpu.VMEM((D, FD), BF16),
            pltpu.VMEM((D, 3 * AD), BF16),
            pltpu.VMEM((FD, D), BF16),
            pltpu.VMEM((AD, D), BF16),
            pltpu.VMEM((S,) + small.shape, F32),
            pltpu.VMEM((4, D), F32),
            pltpu.VMEM((1, 3 * AD), F32),
            pltpu.VMEM((1, FD), F32),
            pltpu.VMEM((1, 3 * AD), F32),
            pltpu.VMEM((1, FD), F32),
            pltpu.VMEM((4, D), F32),
            pltpu.VMEM((1, D), F32),
            pltpu.SemaphoreType.DMA((S, NT)),
            pltpu.SemaphoreType.DMA((S, NT)),
            pltpu.SemaphoreType.DMA((2, S, 2)),
            pltpu.SemaphoreType.DMA((2, S)),
            pltpu.SemaphoreType.DMA((2, S, NT)),
            pltpu.SemaphoreType.DMA((2, S, NT)),
            pltpu.SemaphoreType.DMA((S, 4)),
            pltpu.SemaphoreType.DMA((S, 4)),
            pltpu.SemaphoreType.DMA((2, S, ND)),
            pltpu.SemaphoreType.DMA((2, S, ND)),
            pltpu.SemaphoreType.DMA((9,)),
            pltpu.SemaphoreType.DMA((9, NT, S)),
        ],
        compiler_params=pltpu.CompilerParams(
            collective_id=0, has_side_effects=True, vmem_limit_bytes=67043328
        ),
        cost_estimate=pl.CostEstimate(flops=flops, bytes_accessed=80 * 2**20, transcendentals=S * tile * FD * 2),
        name="layer",
    )(small, out_grad, block_in, w_up, w_qkv, w_down, w_out, freqs)


def grads(
    first, second, attended, activated, mixed, hidden, grad, branch, inner, sums, block_in, bias, S, R, TP, DP
):
    N, D = grad.shape
    T = block_in.shape[0]
    NT, ND, steps = 2 ** len(TP), 2 ** len(DP), len(DP)
    lefts = (second, first, activated, attended)
    rights = (hidden, mixed, grad, grad)
    pieces = []
    for left, right, lead, mid in zip(lefts, rights, (S, S, 1, 1), (NT, NT, 1, 1)):
        pieces.append((lead, mid, left.shape[1] // (lead * ND * mid * 2), right.shape[1]))
    ways = []
    for way in (DP, DP[::-1]):
        ways.append([(bit, 1 << DP.index(bit)) for bit in way])

    def masks(bits):
        out = [0]
        for _, bit in bits:
            out += [v | bit for v in out]
        return sorted(out)

    slots = []
    for way in ways:
        table = {}
        for j in range(steps):
            for u in masks(way[j + 1 :]):
                table[j, u] = len(table)
        slots.append(table)

    def kernel(
        second_hbm, first_hbm, activated_hbm, attended_hbm, hidden_hbm, mixed_hbm, grad_hbm, branch_hbm, inner_hbm, sums_hbm,
        block_hbm, bias_ref,
        whole_up, whole_out, own_down_0, own_down_1, own_qkv_0, own_qkv_1, block_out, inner_own, inner_rest, sums_out,
        own_up, own_out, block_v, near, near_came, far_came, held, held_came,
        second_v, first_v, activated_v, attended_v, hidden_v, mixed_v, grad_v,
        part_up, part_qkv, part_down, part_out, came_up, came_qkv, came_down, came_out, all_up, all_qkv,
        load, dp_send, dp_recv, z_send, z_recv, near_send, near_recv, far_send, far_recv, held_send, held_recv,
        plane_send, plane_recv,
    ):
        s = lax.axis_index("shard")
        r = lax.axis_index("replica")
        t = sum(((r // bit) % 2 * 2**i for i, bit in enumerate(TP)), jnp.int32(0))
        d = sum(((r // bit) % 2 * 2**i for i, bit in enumerate(DP)), jnp.int32(0))

        def flipped(value, mask):
            return sum((bit * (1 - 2 * ((value // bit) % 2)) for bit in bits_of(mask)), value)

        def other(k, m):
            mask = sum(bit for i, bit in enumerate(TP) if m >> i & 1)
            return {"shard": lax.rem(s + k, S), "replica": flipped(r, mask)}

        loads = []
        order = ((hidden_hbm, hidden_v), (second_hbm, second_v), (mixed_hbm, mixed_v), (first_hbm, first_v),
                 (grad_hbm, grad_v), (activated_hbm, activated_v), (attended_hbm, attended_v))
        parts_hbm = (branch_hbm, inner_hbm)
        for i, (source, target) in enumerate(order):
            loads.append(pltpu.make_async_copy(source, target, load.at[i]))
        token_loads = [
            pltpu.make_async_copy(parts_hbm[i].at[t], near.at[i], load.at[7 + i]) for i in range(2)
        ]
        held_load = pltpu.make_async_copy(sums_hbm, held.at[0], load.at[9])
        own_load = pltpu.make_async_copy(block_hbm, block_v, load.at[16])
        for copy in (loads[6], loads[4], *loads[:2], held_load, *token_loads, *loads[2:4], loads[5], own_load):
            copy.start()

        group = [(k, m) for k in range(S) for m in range(NT) if k or m]
        barrier = pltpu.get_barrier_semaphore()
        for k, m in group:
            pl.semaphore_signal(barrier, inc=1, device_id=other(k, m), device_id_type=MESH)
        for bit in DP:
            pl.semaphore_signal(barrier, inc=1, device_id={"replica": flipped(r, bit)}, device_id_type=MESH)
        pl.semaphore_wait(barrier, len(group) + steps)

        left_refs = (second_v, first_v, activated_v, attended_v)
        right_refs = (hidden_v, mixed_v, grad_v, grad_v)
        part = (part_up, part_qkv, part_down, part_out)
        came = (came_up, came_qkv, came_down, came_out)
        own = (own_up, (own_qkv_0, own_qkv_1), (own_down_0, own_down_1), own_out)

        def product(i):
            lead, mid, n, _ = pieces[i]
            if lead > 1:
                width = ND * mid * 2 * n

                def body(l, carry):
                    cols = pl.ds(pl.multiple_of(l * width, width), width)
                    value = dot(left_refs[i][:, cols], right_refs[i][...], 0, 0).astype(BF16)
                    for q in range(ND):
                        for c in range(mid):
                            for h in range(2):
                                at = ((q * mid + c) * 2 + h) * n
                                part[i][h, q, l, c] = value[at : at + n]
                    return carry

                lax.fori_loop(0, lead, body, 0)
            else:
                total = ND * 2 * n
                chunk = min(total, 512)
                per = chunk // (2 * n)

                def body(l, carry):
                    cols = pl.ds(pl.multiple_of(l * chunk, chunk), chunk)
                    value = dot(left_refs[i][:, cols], right_refs[i][...], 0, 0).astype(BF16)
                    for q in range(per):
                        for h in range(2):
                            at = (q * 2 + h) * n
                            part[i][h, l * per + q, 0, 0] = value[at : at + n]
                    return carry

                lax.fori_loop(0, total // chunk, body, 0)

        def halving(i, h, j, u):
            bit, dbit = ways[h][j]
            slot = slots[h][j, u]
            return pltpu.make_async_remote_copy(
                src_ref=part[i].at[h, flipped(d, dbit | u)], dst_ref=came[i].at[h, slot],
                send_sem=dp_send.at[i, h, slot], recv_sem=dp_recv.at[i, h, slot],
                device_id={"replica": flipped(r, bit)}, device_id_type=MESH,
            )

        def summed(i, h, mask, count, write):
            lead, mid, _, _ = pieces[i]
            at = flipped(d, mask)
            for j in range(count):
                halving(i, h, j, mask).wait_recv()

            def body(l, carry):
                for c in range(mid):
                    value = part[i][h, at, l, c].astype(F32)
                    for j in range(count):
                        value = value + came[i][h, slots[h][j, mask], l, c].astype(F32)
                    write(l, c, value.astype(BF16))
                return carry

            lax.fori_loop(0, lead, body, 0)

        def step(i, j):
            for h in range(2):
                for u in masks(ways[h][j + 1 :]):
                    mask = ways[h][j][1] | u
                    at = flipped(d, mask)
                    if j:

                        def write(l, c, value, h=h, at=at):
                            part[i][h, at, l, c] = value

                        summed(i, h, mask, j, write)
                    halving(i, h, j, u).start()

        everyone = (all_up, all_qkv)

        def to_shard(i, h, k, m):
            there = lax.rem(s + k, S)
            return pltpu.make_async_remote_copy(
                src_ref=part[i].at[h, d, there, flipped(t, m)], dst_ref=everyone[i].at[s, t, h],
                send_sem=z_send.at[i, h, k, m], recv_sem=z_recv.at[i, h, k, m],
                device_id=other(k, m), device_id_type=MESH,
            )

        def last(i):
            for h in range(2):
                if i < 2:

                    def write(l, c, value, h=h):
                        part[i][h, d, l, c] = value

                else:

                    def write(l, c, value, h=h):
                        if i == 2:
                            own[i][h][...] = value
                        else:
                            own[i][h] = value

                summed(i, h, 0, steps, write)
            if i < 2:
                for k, m in group:
                    for h in range(2):
                        to_shard(i, h, k, m).start()
                for h in range(2):
                    everyone[i][s, t, h] = part[i][h, d, s, t]

        def collect(i):
            width = pieces[i][3]
            runs = 1 if i == 0 else 3
            n = width // runs
            for k, m in group:
                for h in range(2):
                    to_shard(i, h, k, m).wait_recv()
            for h in range(2):
                for j in range(S):
                    for u in range(NT):
                        block = everyone[i][j, u, h]
                        for v in range(runs):
                            at = (v * S * NT + j * NT + u) * n
                            target = own[i][h] if i == 1 else own[i].at[h]
                            target[:, at : at + n] = block[:, v * n : (v + 1) * n]

        def near_copy(i, m):
            return pltpu.make_async_remote_copy(
                src_ref=parts_hbm[i].at[flipped(t, m)], dst_ref=near_came.at[i, m - 1],
                send_sem=near_send.at[i, m], recv_sem=near_recv.at[i, m], device_id=other(0, m), device_id_type=MESH,
            )

        def far_copy(k):
            there = lax.rem(s + k, S)
            return pltpu.make_async_remote_copy(
                src_ref=near.at[0, there] if NT > 1 else branch_hbm.at[t, there], dst_ref=far_came.at[k - 1],
                send_sem=far_send.at[k], recv_sem=far_recv.at[k], device_id=other(k, 0), device_id_type=MESH,
            )

        def near_sum(i, j):
            value = near[i, j].astype(F32)
            for m in range(1, NT):
                value = value + near_came[i, m - 1, j].astype(F32)
            return value

        def near_wait(i):
            token_loads[i].wait()
            for m in range(1, NT):
                near_copy(i, m).wait_recv()

        def branch_near():
            near_wait(0)

            def body(k, carry):
                j = lax.rem(s + k, S)
                near[0, j] = near_sum(0, j).astype(BF16)
                return carry

            if NT > 1:
                lax.fori_loop(1, S, body, 0)
            for k in range(1, S):
                far_copy(k).start()

        def branch_far():
            value = near_sum(0, s)
            for k in range(1, S):
                far_copy(k).wait_recv()
                value = value + far_came[k - 1].astype(F32)
            own_load.wait()
            block_out[...] = (block_v[...].astype(F32) + value + bias_ref[...]).astype(BF16)

        def inner_near():
            near_wait(1)
            inner_own[...] = near_sum(1, s)
            for k in range(1, S):
                inner_rest[k - 1] = near_sum(1, lax.rem(s + k, S)).astype(BF16)

        bits = [(0, bit) for bit in bits_of(R - 1)] + [(1, bit) for bit in bits_of(S - 1)]

        def double(i):
            axis, bit = bits[i]
            to = {"replica": flipped(r, bit)} if axis == 0 else {"shard": flipped(s, bit)}
            return pltpu.make_async_remote_copy(
                src_ref=held.at[i], dst_ref=held_came.at[i], send_sem=held_send.at[i], recv_sem=held_recv.at[i],
                device_id=to, device_id_type=MESH,
            )

        def doubled(i):
            double(i).wait_recv()
            value = held[i] + held_came[i]
            if i + 1 < len(bits):
                held[i + 1] = value
                double(i + 1).start()
            else:
                sums_out[...] = value

        wholes = {0: whole_up, 3: whole_out}
        order_of = {0: 0, 3: 1}

        def slot_of(i, h, dd, tt):
            n = pieces[i][2]
            if i == 0:
                at = (dd * NT + tt) * 2 * n + h * n
            else:
                at = tt * (ND * 2 * n) + dd * 2 * n + h * n
            return wholes[i].at[pl.ds(pl.multiple_of(at, n), n), :]

        def gather(i, h, m, b):
            dmask = sum(ways[h][v][1] for v in range(steps) if m >> v & 1)
            tmask = m >> steps
            slot = slot_of(i, h, flipped(d, dmask), flipped(t, tmask))
            bit = ways[h][b][0] if b < steps else TP[b - steps]
            return pltpu.make_async_remote_copy(
                src_ref=own[i].at[h] if m == 0 else slot, dst_ref=slot,
                send_sem=plane_send.at[order_of[i], h, m | 1 << b], recv_sem=plane_recv.at[order_of[i], h, m | 1 << b],
                device_id={"replica": flipped(r, bit)}, device_id_type=MESH,
            )

        positions = steps + len(TP)

        def keep_own(i, h):
            return pltpu.make_async_copy(own[i].at[h], slot_of(i, h, d, t), load.at[10 + order_of[i] * 2 + h])

        def share_own(i):
            for h in range(2):
                for b in range(positions):
                    gather(i, h, 0, b).start()
                keep_own(i, h).start()

        def share_on(i, m):
            top = m.bit_length() - 1
            for h in range(2):
                gather(i, h, m ^ 1 << top, top).wait_recv()
                for b in range(top + 1, positions):
                    gather(i, h, m, b).start()

        for i in range(2):
            for m in range(1, NT):
                near_copy(i, m).start()
        held_load.wait()
        double(0).start()
        loads[4].wait()
        loads[6].wait()
        product(3)
        step(3, 0)
        loads[0].wait()
        loads[1].wait()
        product(0)
        step(0, 0)
        branch_near()
        doubled(0)
        loads[2].wait()
        loads[3].wait()
        product(1)
        step(1, 0)
        for j in range(1, steps):
            step(0, j)
        doubled(1)
        loads[5].wait()
        product(2)
        step(2, 0)
        for j in range(1, steps):
            step(1, j)
        last(0)
        for i in range(2, len(bits)):
            doubled(i)
        for j in range(1, steps):
            step(2, j)
        last(1)
        for j in range(1, steps):
            step(3, j)
        collect(0)
        share_own(0)
        last(2)
        last(3)
        share_own(3)
        for m in range(1, 1 << steps):
            for i in (0, 3):
                share_on(i, m)
            if m == 1:
                collect(1)
                branch_far()
                inner_near()
        for m in range(1 << steps, 1 << positions):
            for i in (0, 3):
                share_on(i, m)

        for i in (3, 0):
            for h in range(2):
                keep_own(i, h).wait()
                for m in range(1 << positions):
                    for b in range(m.bit_length(), positions):
                        gather(i, h, m, b).wait_send()
        for i in range(2):
            for m in range(1, NT):
                near_copy(i, m).wait_send()
        for k in range(1, S):
            far_copy(k).wait_send()
        for i in range(len(bits)):
            double(i).wait_send()
        for i in range(4):
            for h in range(2):
                for j, u in slots[h]:
                    halving(i, h, j, u).wait_send()
        for i in range(2):
            for h in range(2):
                for k, m in group:
                    to_shard(i, h, k, m).wait_send()

    def scratch(value):
        return pltpu.VMEM(value.shape, BF16)

    any_spec = pl.BlockSpec(memory_space=pl.ANY)
    vmem_spec = pl.BlockSpec(memory_space=pltpu.VMEM)
    operands = (second, first, activated, attended, hidden, mixed, grad)
    owns = [(2, n, width * S * NT if lead > 1 else width) for lead, _, n, width in pieces]
    wholes = [(2 * n * ND * NT, width) for _, n, width in owns]
    outs = [jax.ShapeDtypeStruct(wholes[i], BF16) for i in (0, 3)]
    outs += [jax.ShapeDtypeStruct(owns[i][1:], BF16) for i in (2, 2, 1, 1)] + [jax.ShapeDtypeStruct((T, D), BF16)]
    outs += [jax.ShapeDtypeStruct((T, D), F32), jax.ShapeDtypeStruct((S - 1, T, D), BF16)]
    outs += [jax.ShapeDtypeStruct(sums.shape, F32)]
    sent = sum(2 * (ND - 1) * a * b * n * w * 2 for a, b, n, w in pieces)
    count = len(bits_of(R - 1)) + len(bits_of(S - 1))
    return pl.pallas_call(
        kernel,
        out_shape=outs,
        in_specs=[any_spec] * 11 + [vmem_spec],
        out_specs=[any_spec] * 2 + [vmem_spec] * 8,
        scratch_shapes=[pltpu.VMEM(owns[i], BF16) for i in (0, 3)]
        + [
            pltpu.VMEM((T, D), BF16),
            pltpu.VMEM((2, S, T, D), BF16),
            pltpu.VMEM((2, NT - 1, S, T, D) if NT > 1 else (1, 1, 1, 16, 128), BF16),
            pltpu.VMEM((S - 1, T, D), BF16),
            pltpu.VMEM((count,) + sums.shape, F32),
            pltpu.VMEM((count,) + sums.shape, F32),
        ]
        + [scratch(v) for v in operands]
        + [pltpu.VMEM((2, ND) + piece, BF16) for piece in pieces]
        + [pltpu.VMEM((2, ND - 1) + piece, BF16) for piece in pieces]
        + [pltpu.VMEM((S, NT, 2) + piece[2:], BF16) for piece in pieces[:2]]
        + [
            pltpu.SemaphoreType.DMA((18,)),
            pltpu.SemaphoreType.DMA((4, 2, ND - 1)),
            pltpu.SemaphoreType.DMA((4, 2, ND - 1)),
            pltpu.SemaphoreType.DMA((2, 2, S, NT)),
            pltpu.SemaphoreType.DMA((2, 2, S, NT)),
            pltpu.SemaphoreType.DMA((2, NT)),
            pltpu.SemaphoreType.DMA((2, NT)),
            pltpu.SemaphoreType.DMA((S,)),
            pltpu.SemaphoreType.DMA((S,)),
            pltpu.SemaphoreType.DMA((count,)),
            pltpu.SemaphoreType.DMA((count,)),
            pltpu.SemaphoreType.DMA((2, 2, ND * NT)),
            pltpu.SemaphoreType.DMA((2, 2, ND * NT)),
        ],
        compiler_params=pltpu.CompilerParams(
            collective_id=1, has_side_effects=True, vmem_limit_bytes=67043328
        ),
        cost_estimate=pl.CostEstimate(
            flops=2 * N * sum(v.shape[1] * w.shape[1] for v, w in zip(lefts, rights)),
            bytes_accessed=sent * 8, transcendentals=0,
        ),
        name="grads",
    )(*operands, branch, inner, sums, block_in, bias)


def solution(mesh):
    S = mesh.shape["shard"]
    R = mesh.shape["replica"]
    TP = [1] if R > 1 and H % (2 * S) == 0 else []
    DP = [bit for bit in bits_of(R - 1) if bit not in TP]
    NT = 2 ** len(TP)

    def flip(value, bit):
        return lax.ppermute(value, "replica", [(i, i ^ bit) for i in range(R)])

    def body(
        block_in, positions, out_grad, w_qkv, b_qkv, w_out, b_out, w_up, b_up, w_down, b_down,
        first_gain, first_shift, second_gain, second_shift,
    ):
        T, D = block_in.shape
        FS = w_down.shape[0]
        FD = FS // NT
        s = lax.axis_index("shard")
        r = lax.axis_index("replica")
        mine = {bit: (r // bit) % 2 for bit in bits_of(R - 1)}
        t = sum((mine[bit] * 2**i for i, bit in enumerate(TP)), jnp.int32(0))

        vectors = [
            b_qkv, b_out, b_down, first_gain, first_shift, second_gain, second_shift, b_up, positions.astype(BF16)
        ]
        ends = [sum(v.shape[0] for v in vectors[: i + 1]) for i in range(len(vectors))]
        small = sum(lax.pad(v, jnp.zeros((), BF16), [(end - v.shape[0], ends[-1] - end, 0)]) for v, end in zip(vectors, ends))
        small = small.reshape(-1, 128)
        (
            first_low, second_low, attended, activated, mixed_low, hidden_low, branch_part, inner_part, grad_all,
            _, sums, bias,
        ) = layer(block_in, out_grad, small, rotary_freqs(), w_up, w_qkv, w_down, w_out, S, TP, DP)
        first_low, second_low, attended, activated, mixed_low, hidden_low, grad_all = [
            v.reshape(NT * S * T, -1)
            for v in (first_low, second_low, attended, activated, mixed_low, hidden_low, grad_all)
        ]
        d = sum((mine[bit] * 2**i for i, bit in enumerate(DP)), jnp.int32(0))

        whole_up, whole_out, *owned_rows, block_out, inner_own, inner_rest, sums = grads(
            first_low, second_low, attended, activated, mixed_low, hidden_low, grad_all, branch_part, inner_part,
            sums, block_in, bias, S, R, TP, DP,
        )

        sums = sums.reshape(-1)
        width = w_out.shape[0] * S
        lengths = [width] * 3 + [D, FS * S] + [D] * 4
        at = [sum(lengths[:i]) for i in range(len(lengths))]

        def owned(start, length):
            return lax.dynamic_slice_in_dim(sums, start + s * (length // S), length // S, 0)

        grad_b_qkv = owned(at[0], 3 * width)
        grad_b_out = owned(at[3], D)
        grad_b_up = owned(at[4], FS * S)
        smalls = [owned(at[5 + i], D) for i in range(4)]
        whole_out, grad_b_qkv, grad_b_out, grad_b_up, smalls = lax.optimization_barrier(
            (whole_out, grad_b_qkv, grad_b_out, grad_b_up, smalls)
        )

        ways = [DP, DP[::-1]]

        def indices(m):
            dmask = sum(2**i for i, bit in enumerate(DP) if m & bit)
            tmask = sum(2**i for i, bit in enumerate(TP) if m & bit)
            return d ^ dmask, t ^ tmask

        def down_row(half, m, n):
            dd, tt = indices(m)
            return tt * FD + (dd * 2 + half) * n

        def qkv_row(half, m, n):
            dd, tt = indices(m)
            return ((dd * NT + tt) * 2 + half) * n

        def placed(result, pieces, row):
            for bit in TP:
                pieces = pieces + [(half, m | bit, flip(value, bit)) for half, m, value in pieces]
            at = jnp.stack([row(half, m, value.shape[0]) for half, m, value in pieces])
            return place([value for _, _, value in pieces], at, result)

        got = [[{0: owned_rows[2 * i + half]} for half in range(2)] for i in range(2)]

        def fetched(i, half, masks):
            for m in masks:
                bit = [b for b in ways[half] if m & b][-1]
                got[i][half][m] = flip(got[i][half][m ^ bit], bit)

        several = [m for m in all_masks(DP) if m and m not in DP]
        for masks in (DP, several):
            for i in range(2):
                for half in range(2):
                    fetched(i, half, masks)

        def pieces_of(i, masks):
            return [(half, m, got[i][half][m]) for half in range(2) for m in masks]

        scaled = []
        for k in range(1, S):
            scaled.append(lax.ppermute(inner_rest[k - 1], "shard", [(i, (i + k) % S) for i in range(S)]))
        in_grad = input_grad(block_in, out_grad, inner_own, scaled)
        grad_w_up = widen(whole_up)
        grad_w_out = widen(whole_out)
        grad_w_down = placed(unwritten(w_down.shape, F32), pieces_of(0, [0] + DP), down_row)
        grad_w_qkv = placed(unwritten(w_qkv.shape, F32), pieces_of(1, [0] + DP), qkv_row)
        if several:
            grad_w_down = placed(grad_w_down, pieces_of(0, several), down_row)
            grad_w_qkv = placed(grad_w_qkv, pieces_of(1, several), qkv_row)

        return (
            block_out, in_grad, grad_w_qkv, grad_b_qkv, grad_w_out, grad_b_out, grad_w_up, grad_b_up,
            grad_w_down, grad_b_out, *smalls,
        )

    rows2, row1, par2, par1 = P(("shard", "replica"), None), P(("shard", "replica")), P("shard", None), P("shard")
    return jax.shard_map(
        body,
        mesh=mesh,
        in_specs=(
            rows2, row1, rows2, par2, par1, par2, par1, par2, par1, par2, par1, par1, par1, par1, par1,
        ),
        out_specs=(
            rows2, rows2, par2, par1, par2, par1, par2, par1, par2, par1, par1, par1, par1, par1,
        ),
        check_vma=False,
    )
```

```python
import jax
import jax.numpy as jnp
import numpy as np
from jax import lax
from jax.experimental import pallas as pl
from jax.experimental.pallas import tpu as pltpu
from jax.sharding import PartitionSpec as P

H = 8
HD = 256
ROT = 64

epsilon = 1e-05


F32 = jnp.float32
BF16 = jnp.bfloat16
MESH = pl.DeviceIdType.MESH


def rotary_freqs():
    freqs = 10000.0 ** (-(np.arange(ROT // 2) * (2.0 / ROT)))
    return np.concatenate([freqs, freqs, np.zeros(128 - ROT)]).astype(np.float32).reshape(1, 128)


def all_masks(bits):
    out = [0]
    for bit in bits:
        out += [v | bit for v in out]
    return sorted(out, key=lambda v: (v.bit_count(), v))


def dot(left, right, left_dim, right_dim):
    return lax.dot_general(
        left, right, (((left_dim,), (right_dim,)), ((), ())), preferred_element_type=F32
    )


def widen(value):
    rows, width = value.shape
    n = min(rows // 2, max(8, 2**20 // width))

    def kernel(in_ref, out_ref):
        out_ref[...] = in_ref[...].astype(F32)

    spec = pl.BlockSpec((n, width), lambda i: (i, 0))
    return pl.pallas_call(
        kernel,
        grid=(rows // n,),
        in_specs=[spec],
        out_specs=spec,
        out_shape=jax.ShapeDtypeStruct(value.shape, F32),
        cost_estimate=pl.CostEstimate(flops=0, bytes_accessed=6 * rows * width, transcendentals=0),
        name="widen",
    )(value)


def place(pieces, rows, result):
    n, width = pieces[0].shape
    count = len(pieces)

    def kernel(rows_ref, *refs):
        sources, target = refs[:count], refs[count + 1]
        wide, go = refs[count + 2 :]
        copies = []
        for i in range(count):
            wide[i] = sources[i][...].astype(F32)
            at = pl.multiple_of(rows_ref[i], n)
            copies.append(pltpu.make_async_copy(wide.at[i], target.at[pl.ds(at, n), :], go.at[i]))
            copies[-1].start()
        for copy in copies:
            copy.wait()

    any_spec = pl.BlockSpec(memory_space=pl.ANY)
    return pl.pallas_call(
        kernel,
        in_specs=[pl.BlockSpec(memory_space=pltpu.SMEM)] + [pl.BlockSpec(memory_space=pltpu.VMEM)] * count + [any_spec],
        out_specs=any_spec,
        out_shape=jax.ShapeDtypeStruct(result.shape, F32),
        scratch_shapes=[pltpu.VMEM((count, n, width), F32), pltpu.SemaphoreType.DMA((count,))],
        input_output_aliases={count + 1: 0},
        cost_estimate=pl.CostEstimate(flops=0, bytes_accessed=6 * count * n * width, transcendentals=0),
        name="place",
    )(rows, *pieces, result)


def finish(block_in, out_grad, branch, bias, own, others, sums, s, lengths, S):
    count = len(others)
    order = [0, 1, 1] + list(range(2, len(lengths)))

    def kernel(s_ref, block_ref, out_ref, branch_ref, bias_ref, own_ref, sums_ref, *refs):
        block_out, in_grad, *smalls = refs[count:]
        wide = block_ref[...].astype(F32)
        block_out[...] = (wide + branch_ref[...] + bias_ref[...]).astype(BF16)
        offsets = wide - jnp.mean(wide, axis=-1, keepdims=True)
        inverse = lax.rsqrt(jnp.mean(offsets * offsets, axis=-1, keepdims=True) + epsilon)
        normed = offsets * inverse
        scaled = own_ref[...]
        for ref in refs[:count]:
            scaled = scaled + ref[...].astype(F32)
        term = inverse * (
            scaled
            - jnp.mean(scaled, axis=-1, keepdims=True)
            - normed * jnp.mean(scaled * normed, axis=-1, keepdims=True)
        )
        in_grad[...] = (out_ref[...].astype(F32) + term).astype(BF16)
        for ref, i in zip(smalls, order):
            n = lengths[i] // S
            ref[...] = sums_ref[pl.ds(sum(lengths[:i]) + s_ref[0] * n, n), :]

    outs = [jax.ShapeDtypeStruct(block_in.shape, BF16)] * 2
    outs += [jax.ShapeDtypeStruct((lengths[i] // S, 128), F32) for i in order]
    vmem_spec = pl.BlockSpec(memory_space=pltpu.VMEM)
    return pl.pallas_call(
        kernel,
        in_specs=[pl.BlockSpec(memory_space=pltpu.SMEM)] + [vmem_spec] * (6 + count),
        out_specs=[vmem_spec] * len(outs),
        out_shape=outs,
        cost_estimate=pl.CostEstimate(flops=0, bytes_accessed=8 * 2**20, transcendentals=0),
        name="finish",
    )(s.reshape(1), block_in, out_grad, branch, bias, own, sums, *others)


def unwritten(shape, dtype):
    return pl.pallas_call(
        lambda out_ref: None,
        out_shape=jax.ShapeDtypeStruct(shape, dtype),
        out_specs=pl.BlockSpec(memory_space=pl.ANY),
    )()


def bits_of(mask):
    return [1 << i for i in range(mask.bit_length()) if mask >> i & 1]


def layer(block_in, out_grad, small, freqs, w_up, w_qkv, w_down, w_out, S, TP, DP):
    T, D = block_in.shape
    rows, FS = w_up.shape[0], w_down.shape[0]
    NT, ND = 2 ** len(TP), 2 ** len(DP)
    FD, AD = FS // NT, w_out.shape[0] // NT
    heads = AD // HD
    scale = HD ** (-0.5)
    part = rows // ND
    third = w_qkv.shape[1] // 3
    tile = NT * T
    per = third * 3 // S // 128
    rest = D // S // 128
    base_out = 3 * third // 128
    base_up = base_out + D // 128
    base_norm = base_up + FS * S // 128
    count = base_norm + 4 * D // 128
    widths = [D, D, AD, FD, 3 * AD, FD, D, D]

    def kernel(
        small_ref, grad_ref, in_ref, up_ref, qkv_ref, down_ref, out_ref, freqs_ref,
        first_hbm, second_hbm, attended_hbm, activated_hbm, mixed_hbm, hidden_hbm, branch_hbm, inner_hbm, grad_hbm,
        small_all, sums_ref, bias_sum_ref,
        first_v, second_v, attended_v, activated_v, mixed_v, hidden_v, branch_v, inner_v,
        grad_all, in_all, up_all, qkv_all, down_all, out_all,
        wide_small, norms_ref, bias_ref, bias_up_ref, sum_qkv_ref, sum_up_ref, sum_norm_ref, sum_grad_ref,
        small_send, small_recv, line_send, line_recv, tp_send, tp_recv, z_send, z_recv, dp_send, dp_recv, local, leave,
    ):
        s = lax.axis_index("shard")
        r = lax.axis_index("replica")
        t = sum(((r // bit) % 2 * 2**i for i, bit in enumerate(TP)), jnp.int32(0))
        d = sum(((r // bit) % 2 * 2**i for i, bit in enumerate(DP)), jnp.int32(0))
        place = s * NT + t

        def flipped(value, mask):
            return sum((bit * (1 - 2 * ((value // bit) % 2)) for bit in bits_of(mask)), value)

        def other(k, m):
            mask = sum(bit for i, bit in enumerate(TP) if m >> i & 1)
            return {"shard": lax.rem(s + k, S), "replica": flipped(r, mask)}

        def mate(m):
            return {"replica": flipped(r, sum(bit for i, bit in enumerate(DP) if m >> i & 1))}

        group = [(k, m) for k in range(S) for m in range(NT) if k or m]
        plane = range(1, ND)
        gathered = (grad_all, in_all)
        mine = (grad_ref, in_ref)

        def columns(ref, at, n):
            return ref.at[:, pl.ds(pl.multiple_of(at, n), n)]

        here = pl.ds(pl.multiple_of(s * rows, rows), rows)
        copies = [
            pltpu.make_async_copy(small_ref, small_all.at[t, s], local.at[0]),
            pltpu.make_async_copy(grad_ref, grad_all.at[t, s], local.at[1]),
            pltpu.make_async_copy(in_ref, in_all.at[t, s], local.at[2]),
            pltpu.make_async_copy(columns(up_ref, place * FD, FD), up_all.at[here, :], local.at[3]),
            pltpu.make_async_copy(down_ref.at[pl.ds(pl.multiple_of(t * FD, FD), FD), :], down_all, local.at[4]),
            pltpu.make_async_copy(out_ref.at[pl.ds(pl.multiple_of(t * AD, AD), AD), :], out_all, local.at[5]),
        ]
        for j in range(3):
            source = columns(qkv_ref, j * third + place * AD, AD)
            copies.append(
                pltpu.make_async_copy(source, qkv_all.at[here, j * AD : (j + 1) * AD], local.at[6 + j])
            )
        for copy in copies:
            copy.start()

        barrier = pltpu.get_barrier_semaphore()
        for k, m in group:
            pl.semaphore_signal(barrier, inc=1, device_id=other(k, m), device_id_type=MESH)
        for m in plane:
            pl.semaphore_signal(barrier, inc=1, device_id=mate(m), device_id_type=MESH)
        pl.semaphore_wait(barrier, len(group) + len(plane))

        def small_copy(k, m):
            return pltpu.make_async_remote_copy(
                src_ref=small_ref, dst_ref=small_all.at[t, s], send_sem=small_send.at[k, m],
                recv_sem=small_recv.at[k, m], device_id=other(k, m), device_id_type=MESH,
            )

        def line(i, j, way, source):
            return pltpu.make_async_remote_copy(
                src_ref=source, dst_ref=gathered[i].at[t, j], send_sem=line_send.at[i, j, way],
                recv_sem=line_recv.at[i, j], device_id={"shard": s + 2 * way - 1}, device_id_type=MESH,
            )

        def across(i, j, m, source):
            slot = gathered[i].at[t, j]
            return pltpu.make_async_remote_copy(
                src_ref=slot if source is None else source, dst_ref=slot, send_sem=tp_send.at[i, j, m],
                recv_sem=tp_recv.at[i, j, m], device_id=other(0, m), device_id_type=MESH,
            )

        def z_copies(w, k, sending):
            to = lax.rem(s + k, S)
            at = (s if sending else lax.rem(s + S - k, S)) * rows + d * part
            at = pl.ds(pl.multiple_of(at, part), part)
            source_rows = pl.ds(pl.multiple_of(d * part, part), part)
            out = []
            for j in range(1 if w == 0 else 3):
                if w == 0:
                    source = up_ref.at[source_rows, pl.ds(pl.multiple_of((to * NT + t) * FD, FD), FD)]
                    target = up_all.at[at, :]
                else:
                    col = pl.multiple_of(j * third + (to * NT + t) * AD, AD)
                    source = qkv_ref.at[source_rows, pl.ds(col, AD)]
                    target = qkv_all.at[at, j * AD : (j + 1) * AD]
                out.append(
                    pltpu.make_async_remote_copy(
                        src_ref=source, dst_ref=target, send_sem=z_send.at[k, w + j], recv_sem=z_recv.at[k, w + j],
                        device_id={"shard": to}, device_id_type=MESH,
                    )
                )
            return out

        def shared(w, k, m):
            at = pl.multiple_of(lax.rem(s + S - k, S) * rows + d * part, part)
            slot = (up_all, qkv_all)[w].at[pl.ds(at, part), :]
            return pltpu.make_async_remote_copy(
                src_ref=slot, dst_ref=slot, send_sem=dp_send.at[w, k, m], recv_sem=dp_recv.at[w, k, m],
                device_id=mate(m), device_id_type=MESH,
            )

        for k, m in group:
            small_copy(k, m).start()
        for w in range(2):
            for k in range(1, S):
                for copy in z_copies(w, k, True):
                    copy.start()
        for i in range(2):

            @pl.when(s + 1 < S)
            def _():
                line(i, s, 1, mine[i]).start()

            @pl.when(s > 0)
            def _():
                line(i, s, 0, mine[i]).start()

            for m in range(1, NT):
                across(i, s, m, mine[i]).start()

        for ref in (sum_qkv_ref, sum_up_ref, sum_norm_ref, sum_grad_ref):
            ref[...] = jnp.zeros_like(ref)
        for w in range(2):
            for k in range(1, S):
                for copy in z_copies(w, k, False):
                    copy.wait_recv()
                for m in plane:
                    shared(w, k, m).start()
        for k, m in group:
            small_copy(k, m).wait_recv()
        for copy in copies:
            copy.wait()

        wide_small[...] = small_all[0].astype(F32)
        for v in range(4):
            for j in range(S):
                for i in range(rest):
                    at = (j * rest + i) * 128
                    row = per + (2 + v) * rest + i
                    norms_ref[v : v + 1, at : at + 128] = wide_small[j, row : row + 1, :]
        for j in range(S):
            for i in range(rest):
                at = (j * rest + i) * 128
                row = per + i
                bias_sum_ref[0:1, at : at + 128] = (
                    wide_small[j, row : row + 1, :] + wide_small[j, row + rest : row + rest + 1, :]
                )
        for v in range(3):
            for i in range(AD // 128):
                flat = v * (third // 128) + place * (AD // 128) + i
                at = v * AD + i * 128
                bias_ref[0:1, at : at + 128] = wide_small[flat // per, pl.ds(flat % per, 1), :]
        for i in range(FD // 128):
            row = per + 6 * rest + t * (FD // 128) + i
            bias_up_ref[0:1, i * 128 : (i + 1) * 128] = wide_small[s, pl.ds(row, 1), :]

        def from_line(i, j, way):
            line(i, j, way, gathered[i].at[t, j]).wait_recv()

            @pl.when((s + 1 < S) if way else (s > 0))
            def _():
                line(i, j, way, gathered[i].at[t, j]).start()

            for m in range(1, NT):
                across(i, j, m, None).start()

        def advance(k):
            for i in range(2):

                @pl.when(s - k >= 0)
                def _():
                    from_line(i, s - k, 1)

                @pl.when(s + k < S)
                def _():
                    from_line(i, s + k, 0)

        least = jnp.where(s < S - 1 - s, s, S - 1 - s)

        def block_at(i):
            both = jnp.where(i % 2 == 1, s - (i + 1) // 2, s + i // 2)
            one = jnp.where(s < S - 1 - s, i, S - 1 - i)
            return jnp.where(i <= 2 * least, both, one)

        row = lax.broadcasted_iota(jnp.int32, (T, T), 0)
        col = lax.broadcasted_iota(jnp.int32, (T, T), 1)
        away = (row - col).astype(F32)
        lane = lax.broadcasted_iota(jnp.int32, (T, 128), 1)

        def turn(value, table, sign):
            straight, ahead, back = table
            low = value[:, :128]
            low = low * straight + sign * (
                pltpu.roll(low, 128 - ROT // 2, 1) * ahead + pltpu.roll(low, ROT // 2, 1) * back
            )
            return jnp.concatenate([low, value[:, 128:]], axis=1)

        leaving = (
            (first_v, first_hbm), (second_v, second_hbm), (attended_v, attended_hbm), (activated_v, activated_hbm),
            (mixed_v, mixed_hbm), (hidden_v, hidden_hbm), (branch_v, branch_hbm), (inner_v, inner_hbm),
            (grad_all, grad_hbm),
        )

        def depart(v, u, j):
            source, target = leaving[v]
            return pltpu.make_async_copy(source.at[u, j], target.at[u, j], leave.at[v, u, j])

        def compute(i, carry):
            j = block_at(i)

            @pl.when(i == 0)
            def _():
                advance(1)
                for k in range(1, S):
                    for m in plane:
                        shared(0, k, m).wait_recv()

            @pl.when(i == 1)
            def _():
                advance(2)

            @pl.when(i >= 3)
            def _():
                advance(i)

            for m in range(1, NT):
                for v in range(2):
                    across(v, j, m, None).wait_recv()

            def join(ref):
                return jnp.concatenate([ref[u, j] for u in range(NT)], axis=0)

            def put(v, value):
                for u in range(NT):
                    leaving[v][0][u, j] = value[u * T : (u + 1) * T]

            gain_1, shift_1, gain_2, shift_2 = [norms_ref[v : v + 1, :] for v in range(4)]
            wide = join(in_all).astype(F32)
            offsets = wide - jnp.mean(wide, axis=-1, keepdims=True)
            inverse = lax.rsqrt(jnp.mean(offsets * offsets, axis=-1, keepdims=True) + epsilon)
            normed = offsets * inverse
            first = (normed * gain_1 + shift_1).astype(BF16)
            second = (normed * gain_2 + shift_2).astype(BF16)
            put(0, first)
            put(1, second)
            grad = join(grad_all)
            sum_grad_ref[...] += jnp.sum(grad.astype(F32), axis=0, keepdims=True)

            pre = dot(second, up_all[...], 1, 0) + bias_up_ref[...]
            bell = 0.5 * (1.0 + lax.erf(pre * 0.7071067811865476))
            activated = (pre * bell).astype(BF16)
            put(3, activated)
            slope = bell + pre * jnp.exp(-0.5 * pre * pre) * 0.3989422804014327
            hidden_grad = dot(grad, down_all[...], 1, 1) * slope
            sum_up_ref[...] += jnp.sum(hidden_grad, axis=0, keepdims=True)
            hidden_low = hidden_grad.astype(BF16)
            put(5, hidden_low)

            @pl.when(i == 0)
            def _():
                for k in range(1, S):
                    for m in plane:
                        shared(1, k, m).wait_recv()

            mixed = dot(first, qkv_all[...], 1, 0) + bias_ref[...]
            attended_grad = dot(grad, out_all[...], 1, 1).astype(BF16)
            attended_parts, mixed_parts = [], []
            for u in range(NT):
                flat = small_all[u, j, -1:, :].astype(F32)
                position = jnp.sum(jnp.where(row == col, flat, 0.0), axis=1, keepdims=True)
                angle = position * freqs_ref[...]
                sine = jnp.sin(angle)
                table = (
                    jnp.cos(angle),
                    jnp.where(lane < ROT // 2, -sine, 0.0),
                    jnp.where((lane >= ROT // 2) & (lane < ROT), sine, 0.0),
                )
                allowed = (away >= 0) & (away <= position)
                at_rows = slice(u * T, (u + 1) * T)
                outs, q_grads, k_grads, v_grads = [], [], [], []
                for h in range(heads):
                    at = slice(h * HD, (h + 1) * HD)
                    ag = attended_grad[at_rows, at]
                    q = turn(mixed[at_rows, at], table, 1.0).astype(BF16)
                    k = turn(mixed[at_rows, AD + h * HD : AD + (h + 1) * HD], table, 1.0).astype(BF16)
                    v = mixed[at_rows, 2 * AD + h * HD : 2 * AD + (h + 1) * HD].astype(BF16)
                    scores = jnp.where(allowed, dot(q, k, 1, 1) * scale, -1e30)
                    peak = jnp.max(scores, axis=-1, keepdims=True)
                    logsum = peak + jnp.log(jnp.sum(jnp.exp(scores - peak), axis=-1, keepdims=True))
                    probs = jnp.exp(scores - logsum)
                    low = probs.astype(BF16)
                    outs.append(dot(low, v, 1, 0).astype(BF16))
                    dprobs = dot(ag, v, 1, 1)
                    total = jnp.sum(probs * dprobs, axis=-1, keepdims=True)
                    dscores = (probs * (dprobs - total) * scale).astype(BF16)
                    q_grads.append(turn(dot(dscores, k, 1, 0), table, -1.0))
                    k_grads.append(turn(dot(dscores, q, 0, 0), table, -1.0))
                    v_grads.append(dot(low, ag, 0, 0))
                attended_parts.append(jnp.concatenate(outs, axis=1))
                mixed_parts.append(jnp.concatenate(q_grads + k_grads + v_grads, axis=1))
            attended = jnp.concatenate(attended_parts, axis=0)
            put(2, attended)
            mixed_grad = jnp.concatenate(mixed_parts, axis=0)
            sum_qkv_ref[...] += jnp.sum(mixed_grad, axis=0, keepdims=True)
            mixed_low = mixed_grad.astype(BF16)
            put(4, mixed_low)

            branch = dot(attended, out_all[...], 1, 0) + dot(activated, down_all[...], 1, 0)
            put(6, branch.astype(BF16))
            first_grad = dot(mixed_low, qkv_all[...], 1, 1)
            second_grad = dot(hidden_low, up_all[...], 1, 1)
            sum_norm_ref[0:1, :] += jnp.sum(first_grad * normed, axis=0, keepdims=True)
            sum_norm_ref[1:2, :] += jnp.sum(first_grad, axis=0, keepdims=True)
            sum_norm_ref[2:3, :] += jnp.sum(second_grad * normed, axis=0, keepdims=True)
            sum_norm_ref[3:4, :] += jnp.sum(second_grad, axis=0, keepdims=True)
            put(7, (first_grad * gain_1 + second_grad * gain_2).astype(BF16))
            for v in range(len(leaving)):
                for u in range(NT):
                    depart(v, u, j).start()
            return carry

        lax.fori_loop(0, S, compute, 0)

        sums_ref[...] = jnp.zeros_like(sums_ref)
        n = AD // 128
        for v in range(3):
            for i in range(n):
                at = v * AD + i * 128
                sums_ref[pl.ds(v * (third // 128) + place * n + i, 1), :] = sum_qkv_ref[:, at : at + 128]
        for i in range(FD // 128):
            sums_ref[pl.ds(base_up + place * (FD // 128) + i, 1), :] = sum_up_ref[:, i * 128 : (i + 1) * 128]
        for i in range(D // 128):
            at = slice(i * 128, (i + 1) * 128)
            sums_ref[base_out + i : base_out + i + 1, :] = sum_grad_ref[:, at] * (1.0 / (S * NT))
            for v in range(4):
                at_row = base_norm + v * (D // 128) + i
                sums_ref[at_row : at_row + 1, :] = sum_norm_ref[v : v + 1, at]

        for i in range(2):
            for j in range(S):

                @pl.when((s + 1 < S) & (j <= s))
                def _():
                    line(i, j, 1, gathered[i].at[t, j]).wait_send()

                @pl.when((s > 0) & (j >= s))
                def _():
                    line(i, j, 0, gathered[i].at[t, j]).wait_send()

                for m in range(1, NT):
                    across(i, j, m, None).wait_send()
        for k, m in group:
            small_copy(k, m).wait_send()
        for w in range(2):
            for k in range(1, S):
                for copy in z_copies(w, k, True):
                    copy.wait_send()
                for m in plane:
                    shared(w, k, m).wait_send()
        for v in range(len(leaving)):
            for u in range(NT):
                for j in range(S):
                    depart(v, u, j).wait()

    any_spec = pl.BlockSpec(memory_space=pl.ANY)
    vmem_spec = pl.BlockSpec(memory_space=pltpu.VMEM)
    outs = [jax.ShapeDtypeStruct((NT, S, T, w), BF16) for w in widths + [D]]
    outs += [jax.ShapeDtypeStruct((NT, S) + small.shape, BF16), jax.ShapeDtypeStruct((count, 128), F32)]
    outs += [jax.ShapeDtypeStruct((1, D), F32)]
    flops = 2 * S * tile * D * (2 * 3 * AD + 2 * FD + 2 * FD + 2 * AD)
    return pl.pallas_call(
        kernel,
        out_shape=outs,
        in_specs=[any_spec] * 7 + [vmem_spec],
        out_specs=[any_spec] * 9 + [vmem_spec] * 3,
        scratch_shapes=[pltpu.VMEM((NT, S, T, w), BF16) for w in widths]
        + [
            pltpu.VMEM((NT, S, T, D), BF16),
            pltpu.VMEM((NT, S, T, D), BF16),
            pltpu.VMEM((D, FD), BF16),
            pltpu.VMEM((D, 3 * AD), BF16),
            pltpu.VMEM((FD, D), BF16),
            pltpu.VMEM((AD, D), BF16),
            pltpu.VMEM((S,) + small.shape, F32),
            pltpu.VMEM((4, D), F32),
            pltpu.VMEM((1, 3 * AD), F32),
            pltpu.VMEM((1, FD), F32),
            pltpu.VMEM((1, 3 * AD), F32),
            pltpu.VMEM((1, FD), F32),
            pltpu.VMEM((4, D), F32),
            pltpu.VMEM((1, D), F32),
            pltpu.SemaphoreType.DMA((S, NT)),
            pltpu.SemaphoreType.DMA((S, NT)),
            pltpu.SemaphoreType.DMA((2, S, 2)),
            pltpu.SemaphoreType.DMA((2, S)),
            pltpu.SemaphoreType.DMA((2, S, NT)),
            pltpu.SemaphoreType.DMA((2, S, NT)),
            pltpu.SemaphoreType.DMA((S, 4)),
            pltpu.SemaphoreType.DMA((S, 4)),
            pltpu.SemaphoreType.DMA((2, S, ND)),
            pltpu.SemaphoreType.DMA((2, S, ND)),
            pltpu.SemaphoreType.DMA((9,)),
            pltpu.SemaphoreType.DMA((9, NT, S)),
        ],
        compiler_params=pltpu.CompilerParams(
            collective_id=0, has_side_effects=True, vmem_limit_bytes=67043328
        ),
        cost_estimate=pl.CostEstimate(flops=flops, bytes_accessed=80 * 2**20, transcendentals=S * tile * FD * 2),
        name="layer",
    )(small, out_grad, block_in, w_up, w_qkv, w_down, w_out, freqs)


def grads(
    first, second, attended, activated, mixed, hidden, grad, branch, inner, sums, S, R, T, TP, DP
):
    N, D = grad.shape
    NT, ND, steps = 2 ** len(TP), 2 ** len(DP), len(DP)
    lefts = (second, first, activated, attended)
    rights = (hidden, mixed, grad, grad)
    pieces = []
    for left, right, lead, mid in zip(lefts, rights, (S, S, 1, 1), (NT, NT, 1, 1)):
        pieces.append((lead, mid, left.shape[1] // (lead * ND * mid * 2), right.shape[1]))
    ways = []
    for way in (DP, DP[::-1]):
        ways.append([(bit, 1 << DP.index(bit)) for bit in way])

    def masks(bits):
        out = [0]
        for _, bit in bits:
            out += [v | bit for v in out]
        return sorted(out)

    slots = []
    for way in ways:
        table = {}
        for j in range(steps):
            for u in masks(way[j + 1 :]):
                table[j, u] = len(table)
        slots.append(table)

    def kernel(
        second_hbm, first_hbm, activated_hbm, attended_hbm, hidden_hbm, mixed_hbm, grad_hbm, branch_hbm, inner_hbm, sums_hbm,
        whole_up, whole_out, own_down_0, own_down_1, own_qkv_0, own_qkv_1, branch_own, inner_own, *more,
    ):
        inner_rest, sums_out = more[: S - 1], more[S - 1]
        mates = [more[S + 4 * m : S + 4 * m + 4] for m in range(NT - 1)]
        (
            own_up, own_out, near, near_came, far_came, held, held_came,
            second_v, first_v, activated_v, attended_v, hidden_v, mixed_v, grad_v,
            part_up, part_qkv, part_down, part_out, came_up, came_qkv, came_down, came_out, all_up, all_qkv,
            load, dp_send, dp_recv, z_send, z_recv, near_send, near_recv, far_send, far_recv, held_send, held_recv,
            plane_send, plane_recv, mate_send, mate_recv,
        ) = more[S + 4 * (NT - 1) :]
        s = lax.axis_index("shard")
        r = lax.axis_index("replica")
        t = sum(((r // bit) % 2 * 2**i for i, bit in enumerate(TP)), jnp.int32(0))
        d = sum(((r // bit) % 2 * 2**i for i, bit in enumerate(DP)), jnp.int32(0))

        def flipped(value, mask):
            return sum((bit * (1 - 2 * ((value // bit) % 2)) for bit in bits_of(mask)), value)

        def other(k, m):
            mask = sum(bit for i, bit in enumerate(TP) if m >> i & 1)
            return {"shard": lax.rem(s + k, S), "replica": flipped(r, mask)}

        loads = []
        order = ((hidden_hbm, hidden_v), (second_hbm, second_v), (mixed_hbm, mixed_v), (first_hbm, first_v),
                 (grad_hbm, grad_v), (activated_hbm, activated_v), (attended_hbm, attended_v))
        parts_hbm = (branch_hbm, inner_hbm)
        for i, (source, target) in enumerate(order):
            loads.append(pltpu.make_async_copy(source, target, load.at[i]))
        token_loads = [
            pltpu.make_async_copy(parts_hbm[i].at[t], near.at[i], load.at[7 + i]) for i in range(2)
        ]
        held_load = pltpu.make_async_copy(sums_hbm, held.at[0], load.at[9])
        for copy in (loads[6], loads[4], *loads[:2], held_load, *token_loads, *loads[2:4], loads[5]):
            copy.start()

        group = [(k, m) for k in range(S) for m in range(NT) if k or m]
        barrier = pltpu.get_barrier_semaphore()
        for k, m in group:
            pl.semaphore_signal(barrier, inc=1, device_id=other(k, m), device_id_type=MESH)
        for bit in DP:
            pl.semaphore_signal(barrier, inc=1, device_id={"replica": flipped(r, bit)}, device_id_type=MESH)
        pl.semaphore_wait(barrier, len(group) + steps)

        left_refs = (second_v, first_v, activated_v, attended_v)
        right_refs = (hidden_v, mixed_v, grad_v, grad_v)
        part = (part_up, part_qkv, part_down, part_out)
        came = (came_up, came_qkv, came_down, came_out)
        own = (own_up, (own_qkv_0, own_qkv_1), (own_down_0, own_down_1), own_out)

        def product(i):
            lead, mid, n, _ = pieces[i]
            if lead > 1:
                width = ND * mid * 2 * n

                def body(l, carry):
                    cols = pl.ds(pl.multiple_of(l * width, width), width)
                    value = dot(left_refs[i][:, cols], right_refs[i][...], 0, 0).astype(BF16)
                    for q in range(ND):
                        for c in range(mid):
                            for h in range(2):
                                at = ((q * mid + c) * 2 + h) * n
                                part[i][h, q, l, c] = value[at : at + n]
                    return carry

                lax.fori_loop(0, lead, body, 0)
            else:
                total = ND * 2 * n
                chunk = min(total, 512)
                per = chunk // (2 * n)

                def body(l, carry):
                    cols = pl.ds(pl.multiple_of(l * chunk, chunk), chunk)
                    value = dot(left_refs[i][:, cols], right_refs[i][...], 0, 0).astype(BF16)
                    for q in range(per):
                        for h in range(2):
                            at = (q * 2 + h) * n
                            part[i][h, l * per + q, 0, 0] = value[at : at + n]
                    return carry

                lax.fori_loop(0, total // chunk, body, 0)

        def halving(i, h, j, u):
            bit, dbit = ways[h][j]
            slot = slots[h][j, u]
            return pltpu.make_async_remote_copy(
                src_ref=part[i].at[h, flipped(d, dbit | u)], dst_ref=came[i].at[h, slot],
                send_sem=dp_send.at[i, h, slot], recv_sem=dp_recv.at[i, h, slot],
                device_id={"replica": flipped(r, bit)}, device_id_type=MESH,
            )

        def summed(i, h, mask, count, write):
            lead, mid, _, _ = pieces[i]
            at = flipped(d, mask)
            for j in range(count):
                halving(i, h, j, mask).wait_recv()

            def body(l, carry):
                for c in range(mid):
                    value = part[i][h, at, l, c].astype(F32)
                    for j in range(count):
                        value = value + came[i][h, slots[h][j, mask], l, c].astype(F32)
                    write(l, c, value.astype(BF16))
                return carry

            lax.fori_loop(0, lead, body, 0)

        def step(i, j):
            for h in range(2):
                for u in masks(ways[h][j + 1 :]):
                    mask = ways[h][j][1] | u
                    at = flipped(d, mask)
                    if j:

                        def write(l, c, value, h=h, at=at):
                            part[i][h, at, l, c] = value

                        summed(i, h, mask, j, write)
                    halving(i, h, j, u).start()

        everyone = (all_up, all_qkv)

        def to_shard(i, h, k, m):
            there = lax.rem(s + k, S)
            return pltpu.make_async_remote_copy(
                src_ref=part[i].at[h, d, there, flipped(t, m)], dst_ref=everyone[i].at[s, t, h],
                send_sem=z_send.at[i, h, k, m], recv_sem=z_recv.at[i, h, k, m],
                device_id=other(k, m), device_id_type=MESH,
            )

        def last(i):
            for h in range(2):
                if i < 2:

                    def write(l, c, value, h=h):
                        part[i][h, d, l, c] = value

                else:

                    def write(l, c, value, h=h):
                        if i == 2:
                            own[i][h][...] = value
                        else:
                            own[i][h] = value

                summed(i, h, 0, steps, write)
            if i < 2:
                for k, m in group:
                    for h in range(2):
                        to_shard(i, h, k, m).start()
                for h in range(2):
                    everyone[i][s, t, h] = part[i][h, d, s, t]

        def collect(i):
            width = pieces[i][3]
            runs = 1 if i == 0 else 3
            n = width // runs
            for k, m in group:
                for h in range(2):
                    to_shard(i, h, k, m).wait_recv()
            for h in range(2):
                for j in range(S):
                    for u in range(NT):
                        block = everyone[i][j, u, h]
                        for v in range(runs):
                            at = (v * S * NT + j * NT + u) * n
                            target = own[i][h] if i == 1 else own[i].at[h]
                            target[:, at : at + n] = block[:, v * n : (v + 1) * n]

        def near_copy(i, m):
            return pltpu.make_async_remote_copy(
                src_ref=parts_hbm[i].at[flipped(t, m)], dst_ref=near_came.at[i, m - 1],
                send_sem=near_send.at[i, m], recv_sem=near_recv.at[i, m], device_id=other(0, m), device_id_type=MESH,
            )

        def far_copy(k):
            there = lax.rem(s + k, S)
            return pltpu.make_async_remote_copy(
                src_ref=near.at[0, there] if NT > 1 else branch_hbm.at[t, there], dst_ref=far_came.at[k - 1],
                send_sem=far_send.at[k], recv_sem=far_recv.at[k], device_id=other(k, 0), device_id_type=MESH,
            )

        def near_sum(i, j):
            value = near[i, j].astype(F32)
            for m in range(1, NT):
                value = value + near_came[i, m - 1, j].astype(F32)
            return value

        def near_wait(i):
            token_loads[i].wait()
            for m in range(1, NT):
                near_copy(i, m).wait_recv()

        def branch_near():
            near_wait(0)

            def body(k, carry):
                j = lax.rem(s + k, S)
                near[0, j] = near_sum(0, j).astype(BF16)
                return carry

            if NT > 1:
                lax.fori_loop(1, S, body, 0)
            for k in range(1, S):
                far_copy(k).start()

        def branch_far():
            value = near_sum(0, s)
            for k in range(1, S):
                far_copy(k).wait_recv()
                value = value + far_came[k - 1].astype(F32)
            branch_own[...] = value

        def inner_near():
            near_wait(1)
            inner_own[...] = near_sum(1, s)
            for k in range(1, S):
                inner_rest[k - 1][...] = near_sum(1, lax.rem(s + k, S)).astype(BF16)

        bits = [(0, bit) for bit in bits_of(R - 1)] + [(1, bit) for bit in bits_of(S - 1)]

        def double(i):
            axis, bit = bits[i]
            to = {"replica": flipped(r, bit)} if axis == 0 else {"shard": flipped(s, bit)}
            return pltpu.make_async_remote_copy(
                src_ref=held.at[i], dst_ref=held_came.at[i], send_sem=held_send.at[i], recv_sem=held_recv.at[i],
                device_id=to, device_id_type=MESH,
            )

        def doubled(i):
            double(i).wait_recv()
            value = held[i] + held_came[i]
            if i + 1 < len(bits):
                held[i + 1] = value
                double(i + 1).start()
            else:
                sums_out[...] = value

        wholes = {0: whole_up, 3: whole_out}
        order_of = {0: 0, 3: 1}

        def slot_of(i, h, dd, tt):
            n = pieces[i][2]
            if i == 0:
                at = (dd * NT + tt) * 2 * n + h * n
            else:
                at = tt * (ND * 2 * n) + dd * 2 * n + h * n
            return wholes[i].at[pl.ds(pl.multiple_of(at, n), n), :]

        def gather(i, h, m, b):
            dmask = sum(ways[h][v][1] for v in range(steps) if m >> v & 1)
            tmask = m >> steps
            slot = slot_of(i, h, flipped(d, dmask), flipped(t, tmask))
            bit = ways[h][b][0] if b < steps else TP[b - steps]
            return pltpu.make_async_remote_copy(
                src_ref=own[i].at[h] if m == 0 else slot, dst_ref=slot,
                send_sem=plane_send.at[order_of[i], h, m | 1 << b], recv_sem=plane_recv.at[order_of[i], h, m | 1 << b],
                device_id={"replica": flipped(r, bit)}, device_id_type=MESH,
            )

        positions = steps + len(TP)

        def keep_own(i, h):
            return pltpu.make_async_copy(own[i].at[h], slot_of(i, h, d, t), load.at[10 + order_of[i] * 2 + h])

        def share_own(i):
            for h in range(2):
                for b in range(positions):
                    gather(i, h, 0, b).start()
                keep_own(i, h).start()

        def share_on(i, m):
            top = m.bit_length() - 1
            for h in range(2):
                gather(i, h, m ^ 1 << top, top).wait_recv()
                for b in range(top + 1, positions):
                    gather(i, h, m, b).start()

        def to_mate(i, h, m):
            at = (2 - i) * 2 + h
            return pltpu.make_async_remote_copy(
                src_ref=own[i][h], dst_ref=mates[m - 1][at], send_sem=mate_send.at[at, m], recv_sem=mate_recv.at[at, m],
                device_id=other(0, m), device_id_type=MESH,
            )

        def to_mates(i):
            for h in range(2):
                for m in range(1, NT):
                    to_mate(i, h, m).start()

        for i in range(2):
            for m in range(1, NT):
                near_copy(i, m).start()
        held_load.wait()
        double(0).start()
        loads[4].wait()
        loads[6].wait()
        product(3)
        step(3, 0)
        loads[0].wait()
        loads[1].wait()
        product(0)
        step(0, 0)
        branch_near()
        doubled(0)
        loads[2].wait()
        loads[3].wait()
        product(1)
        step(1, 0)
        for j in range(1, steps):
            step(0, j)
        doubled(1)
        loads[5].wait()
        product(2)
        step(2, 0)
        for j in range(1, steps):
            step(1, j)
        last(0)
        for i in range(2, len(bits)):
            doubled(i)
        for j in range(1, steps):
            step(2, j)
        last(1)
        for j in range(1, steps):
            step(3, j)
        collect(0)
        share_own(0)
        last(2)
        to_mates(2)
        last(3)
        share_own(3)
        for m in range(1, 1 << steps):
            for i in (0, 3):
                share_on(i, m)
            if m == 1:
                collect(1)
                to_mates(1)
                branch_far()
                inner_near()
        for m in range(1 << steps, 1 << positions):
            for i in (0, 3):
                share_on(i, m)

        for i in (1, 2):
            for h in range(2):
                for m in range(1, NT):
                    to_mate(i, h, m).wait()
        for i in (3, 0):
            for h in range(2):
                keep_own(i, h).wait()
                for m in range(1 << positions):
                    for b in range(m.bit_length(), positions):
                        gather(i, h, m, b).wait_send()
        for i in range(2):
            for m in range(1, NT):
                near_copy(i, m).wait_send()
        for k in range(1, S):
            far_copy(k).wait_send()
        for i in range(len(bits)):
            double(i).wait_send()
        for i in range(4):
            for h in range(2):
                for j, u in slots[h]:
                    halving(i, h, j, u).wait_send()
        for i in range(2):
            for h in range(2):
                for k, m in group:
                    to_shard(i, h, k, m).wait_send()

    def scratch(value):
        return pltpu.VMEM(value.shape, BF16)

    any_spec = pl.BlockSpec(memory_space=pl.ANY)
    vmem_spec = pl.BlockSpec(memory_space=pltpu.VMEM)
    operands = (second, first, activated, attended, hidden, mixed, grad)
    owns = [(2, n, width * S * NT if lead > 1 else width) for lead, _, n, width in pieces]
    wholes = [(2 * n * ND * NT, width) for _, n, width in owns]
    outs = [jax.ShapeDtypeStruct(wholes[i], BF16) for i in (0, 3)]
    owned = [jax.ShapeDtypeStruct(owns[i][1:], BF16) for i in (2, 2, 1, 1)]
    outs += owned + [jax.ShapeDtypeStruct((T, D), F32)] * 2 + [jax.ShapeDtypeStruct((T, D), BF16)] * (S - 1)
    outs += [jax.ShapeDtypeStruct(sums.shape, F32)] + owned * (NT - 1)
    sent = sum(2 * (ND - 1) * a * b * n * w * 2 for a, b, n, w in pieces)
    count = len(bits_of(R - 1)) + len(bits_of(S - 1))
    return pl.pallas_call(
        kernel,
        out_shape=outs,
        in_specs=[any_spec] * 10,
        out_specs=[any_spec] * 2 + [vmem_spec] * (7 + S - 1 + 4 * (NT - 1)),
        scratch_shapes=[pltpu.VMEM(owns[i], BF16) for i in (0, 3)]
        + [
            pltpu.VMEM((2, S, T, D), BF16),
            pltpu.VMEM((2, NT - 1, S, T, D) if NT > 1 else (1, 1, 1, 16, 128), BF16),
            pltpu.VMEM((S - 1, T, D), BF16),
            pltpu.VMEM((count,) + sums.shape, F32),
            pltpu.VMEM((count,) + sums.shape, F32),
        ]
        + [scratch(v) for v in operands]
        + [pltpu.VMEM((2, ND) + piece, BF16) for piece in pieces]
        + [pltpu.VMEM((2, ND - 1) + piece, BF16) for piece in pieces]
        + [pltpu.VMEM((S, NT, 2) + piece[2:], BF16) for piece in pieces[:2]]
        + [
            pltpu.SemaphoreType.DMA((18,)),
            pltpu.SemaphoreType.DMA((4, 2, ND - 1)),
            pltpu.SemaphoreType.DMA((4, 2, ND - 1)),
            pltpu.SemaphoreType.DMA((2, 2, S, NT)),
            pltpu.SemaphoreType.DMA((2, 2, S, NT)),
            pltpu.SemaphoreType.DMA((2, NT)),
            pltpu.SemaphoreType.DMA((2, NT)),
            pltpu.SemaphoreType.DMA((S,)),
            pltpu.SemaphoreType.DMA((S,)),
            pltpu.SemaphoreType.DMA((count,)),
            pltpu.SemaphoreType.DMA((count,)),
            pltpu.SemaphoreType.DMA((2, 2, ND * NT)),
            pltpu.SemaphoreType.DMA((2, 2, ND * NT)),
            pltpu.SemaphoreType.DMA((4, NT)),
            pltpu.SemaphoreType.DMA((4, NT)),
        ],
        compiler_params=pltpu.CompilerParams(
            collective_id=1, has_side_effects=True, vmem_limit_bytes=67043328
        ),
        cost_estimate=pl.CostEstimate(
            flops=2 * N * sum(v.shape[1] * w.shape[1] for v, w in zip(lefts, rights)),
            bytes_accessed=sent * 8, transcendentals=0,
        ),
        name="grads",
    )(*operands, branch, inner, sums)


def solution(mesh):
    S = mesh.shape["shard"]
    R = mesh.shape["replica"]
    TP = [1] if R > 1 and H % (2 * S) == 0 else []
    DP = [bit for bit in bits_of(R - 1) if bit not in TP]
    NT = 2 ** len(TP)

    def flip(value, bit):
        return lax.ppermute(value, "replica", [(i, i ^ bit) for i in range(R)])

    def body(
        block_in, positions, out_grad, w_qkv, b_qkv, w_out, b_out, w_up, b_up, w_down, b_down,
        first_gain, first_shift, second_gain, second_shift,
    ):
        T, _ = block_in.shape
        FS = w_down.shape[0]
        FD = FS // NT
        s = lax.axis_index("shard")
        r = lax.axis_index("replica")
        mine = {bit: (r // bit) % 2 for bit in bits_of(R - 1)}
        t = sum((mine[bit] * 2**i for i, bit in enumerate(TP)), jnp.int32(0))

        vectors = [
            b_qkv, b_out, b_down, first_gain, first_shift, second_gain, second_shift, b_up, positions.astype(BF16)
        ]
        ends = [sum(v.shape[0] for v in vectors[: i + 1]) for i in range(len(vectors))]
        small = sum(lax.pad(v, jnp.zeros((), BF16), [(end - v.shape[0], ends[-1] - end, 0)]) for v, end in zip(vectors, ends))
        small = small.reshape(-1, 128)
        (
            first_low, second_low, attended, activated, mixed_low, hidden_low, branch_part, inner_part, grad_all,
            _, sums, bias,
        ) = layer(block_in, out_grad, small, rotary_freqs(), w_up, w_qkv, w_down, w_out, S, TP, DP)
        first_low, second_low, attended, activated, mixed_low, hidden_low, grad_all = [
            v.reshape(NT * S * T, -1)
            for v in (first_low, second_low, attended, activated, mixed_low, hidden_low, grad_all)
        ]
        d = sum((mine[bit] * 2**i for i, bit in enumerate(DP)), jnp.int32(0))

        whole_up, whole_out, *more = grads(
            first_low, second_low, attended, activated, mixed_low, hidden_low, grad_all, branch_part, inner_part,
            sums, S, R, T, TP, DP,
        )
        owned_rows, (branch_own, inner_own), inner_rest, sums = more[:4], more[4:6], more[6 : 5 + S], more[5 + S]
        mates = [more[6 + S + 4 * m : 10 + S + 4 * m] for m in range(NT - 1)]

        ways = [DP, DP[::-1]]

        def indices(m):
            dmask = sum(2**i for i, bit in enumerate(DP) if m & bit)
            tmask = sum(2**i for i, bit in enumerate(TP) if m & bit)
            return d ^ dmask, t ^ tmask

        def down_row(half, m, n):
            dd, tt = indices(m)
            return tt * FD + (dd * 2 + half) * n

        def qkv_row(half, m, n):
            dd, tt = indices(m)
            return ((dd * NT + tt) * 2 + half) * n

        def placed(result, which, pieces, row):
            for bit in TP:
                pieces = pieces + [
                    (half, m | bit, mates[0][2 * which + half] if m == 0 else flip(value, bit))
                    for half, m, value in pieces
                ]
            at = jnp.stack([row(half, m, value.shape[0]) for half, m, value in pieces])
            return place([value for _, _, value in pieces], at, result)

        got = [[{0: owned_rows[2 * i + half]} for half in range(2)] for i in range(2)]

        def fetched(i, half, masks):
            for m in masks:
                bit = [b for b in ways[half] if m & b][-1]
                got[i][half][m] = flip(got[i][half][m ^ bit], bit)

        several = [m for m in all_masks(DP) if m and m not in DP]
        for masks in (DP, several):
            for i in range(2):
                for half in range(2):
                    fetched(i, half, masks)

        def pieces_of(i, masks):
            return [(half, m, got[i][half][m]) for half in range(2) for m in masks]

        scaled = []
        for k in range(1, S):
            scaled.append(lax.ppermute(inner_rest[k - 1], "shard", [(i, (i + k) % S) for i in range(S)]))
        block_out, in_grad, *smalls = finish(
            block_in, out_grad, branch_own, bias, inner_own, scaled, sums, s,
            [v.shape[0] * S // 128 for v in (b_qkv, b_out, b_up) + (first_gain,) * 4], S,
        )
        grad_w_up = widen(whole_up)
        grad_w_out = widen(whole_out)
        grad_w_down = placed(unwritten(w_down.shape, F32), 0, pieces_of(0, [0] + DP), down_row)
        grad_w_qkv = placed(unwritten(w_qkv.shape, F32), 1, pieces_of(1, [0] + DP), qkv_row)
        if several:
            grad_w_down = placed(grad_w_down, 0, pieces_of(0, several), down_row)
            grad_w_qkv = placed(grad_w_qkv, 1, pieces_of(1, several), qkv_row)

        grad_b_qkv, grad_b_out, grad_b_down, grad_b_up, *norm_grads = [v.reshape(-1) for v in smalls]
        return (
            block_out, in_grad, grad_w_qkv, grad_b_qkv, grad_w_out, grad_b_out, grad_w_up, grad_b_up,
            grad_w_down, grad_b_down, *norm_grads,
        )

    rows2, row1, par2, par1 = P(("shard", "replica"), None), P(("shard", "replica")), P("shard", None), P("shard")
    return jax.shard_map(
        body,
        mesh=mesh,
        in_specs=(
            rows2, row1, rows2, par2, par1, par2, par1, par2, par1, par2, par1, par1, par1, par1, par1,
        ),
        out_specs=(
            rows2, rows2, par2, par1, par2, par1, par2, par1, par2, par1, par1, par1, par1, par1,
        ),
        check_vma=False,
    )
```

```python
import jax
import jax.numpy as jnp
import numpy as np
from jax import lax
from jax.experimental import pallas as pl
from jax.experimental.pallas import tpu as pltpu
from jax.sharding import PartitionSpec as P

H = 8
HD = 256
ROT = 64

epsilon = 1e-05


F32 = jnp.float32
BF16 = jnp.bfloat16
MESH = pl.DeviceIdType.MESH


def rotary_freqs():
    freqs = 10000.0 ** (-(np.arange(ROT // 2) * (2.0 / ROT)))
    return np.concatenate([freqs, freqs, np.zeros(128 - ROT)]).astype(np.float32).reshape(1, 128)


def all_masks(bits):
    out = [0]
    for bit in bits:
        out += [v | bit for v in out]
    return sorted(out, key=lambda v: (v.bit_count(), v))


def dot(left, right, left_dim, right_dim):
    return lax.dot_general(
        left, right, (((left_dim,), (right_dim,)), ((), ())), preferred_element_type=F32
    )


def widen(value):
    rows, width = value.shape
    n = min(rows // 2, max(8, 2**20 // width))

    def kernel(in_ref, out_ref):
        out_ref[...] = in_ref[...].astype(F32)

    spec = pl.BlockSpec((n, width), lambda i: (i, 0))
    return pl.pallas_call(
        kernel,
        grid=(rows // n,),
        in_specs=[spec],
        out_specs=spec,
        out_shape=jax.ShapeDtypeStruct(value.shape, F32),
        cost_estimate=pl.CostEstimate(flops=0, bytes_accessed=6 * rows * width, transcendentals=0),
        name="widen",
    )(value)


def place(pieces, rows, result):
    n, width = pieces[0].shape
    count = len(pieces)

    def kernel(rows_ref, *refs):
        sources, target = refs[:count], refs[count + 1]
        wide, go = refs[count + 2 :]
        copies = []
        for i in range(count):
            wide[i] = sources[i][...].astype(F32)
            at = pl.multiple_of(rows_ref[i], n)
            copies.append(pltpu.make_async_copy(wide.at[i], target.at[pl.ds(at, n), :], go.at[i]))
            copies[-1].start()
        for copy in copies:
            copy.wait()

    any_spec = pl.BlockSpec(memory_space=pl.ANY)
    return pl.pallas_call(
        kernel,
        in_specs=[pl.BlockSpec(memory_space=pltpu.SMEM)] + [pl.BlockSpec(memory_space=pltpu.VMEM)] * count + [any_spec],
        out_specs=any_spec,
        out_shape=jax.ShapeDtypeStruct(result.shape, F32),
        scratch_shapes=[pltpu.VMEM((count, n, width), F32), pltpu.SemaphoreType.DMA((count,))],
        input_output_aliases={count + 1: 0},
        cost_estimate=pl.CostEstimate(flops=0, bytes_accessed=6 * count * n * width, transcendentals=0),
        name="place",
    )(rows, *pieces, result)


def finish(block_in, out_grad, branch, bias, own, others, sums, s, lengths, S):
    count = len(others)
    order = [0, 1, 1] + list(range(2, len(lengths)))

    def kernel(s_ref, block_ref, out_ref, branch_ref, bias_ref, own_ref, sums_ref, *refs):
        block_out, in_grad, *smalls = refs[count:]
        wide = block_ref[...].astype(F32)
        block_out[...] = (wide + branch_ref[...] + bias_ref[...]).astype(BF16)
        offsets = wide - jnp.mean(wide, axis=-1, keepdims=True)
        inverse = lax.rsqrt(jnp.mean(offsets * offsets, axis=-1, keepdims=True) + epsilon)
        normed = offsets * inverse
        scaled = own_ref[...]
        for ref in refs[:count]:
            scaled = scaled + ref[...].astype(F32)
        term = inverse * (
            scaled
            - jnp.mean(scaled, axis=-1, keepdims=True)
            - normed * jnp.mean(scaled * normed, axis=-1, keepdims=True)
        )
        in_grad[...] = (out_ref[...].astype(F32) + term).astype(BF16)
        for ref, i in zip(smalls, order):
            n = lengths[i] // S
            ref[...] = sums_ref[pl.ds(sum(lengths[:i]) + s_ref[0] * n, n), :]

    outs = [jax.ShapeDtypeStruct(block_in.shape, BF16)] * 2
    outs += [jax.ShapeDtypeStruct((lengths[i] // S, 128), F32) for i in order]
    vmem_spec = pl.BlockSpec(memory_space=pltpu.VMEM)
    return pl.pallas_call(
        kernel,
        in_specs=[pl.BlockSpec(memory_space=pltpu.SMEM)] + [vmem_spec] * (6 + count),
        out_specs=[vmem_spec] * len(outs),
        out_shape=outs,
        cost_estimate=pl.CostEstimate(flops=0, bytes_accessed=8 * 2**20, transcendentals=0),
        name="finish",
    )(s.reshape(1), block_in, out_grad, branch, bias, own, sums, *others)


def unwritten(shape, dtype):
    return pl.pallas_call(
        lambda out_ref: None,
        out_shape=jax.ShapeDtypeStruct(shape, dtype),
        out_specs=pl.BlockSpec(memory_space=pl.ANY),
    )()


def bits_of(mask):
    return [1 << i for i in range(mask.bit_length()) if mask >> i & 1]


def layer(block_in, out_grad, small, freqs, w_up, w_qkv, w_down, w_out, S, TP, DP):
    T, D = block_in.shape
    rows, FS = w_up.shape[0], w_down.shape[0]
    NT, ND = 2 ** len(TP), 2 ** len(DP)
    FD, AD = FS // NT, w_out.shape[0] // NT
    heads = AD // HD
    scale = HD ** (-0.5)
    part = rows // ND
    third = w_qkv.shape[1] // 3
    tile = NT * T
    per = third * 3 // S // 128
    rest = D // S // 128
    base_out = 3 * third // 128
    base_up = base_out + D // 128
    base_norm = base_up + FS * S // 128
    count = base_norm + 4 * D // 128
    widths = [D, D, AD, FD, 3 * AD, FD, D, D]

    def kernel(
        small_ref, grad_ref, in_ref, up_ref, qkv_ref, down_ref, out_ref, freqs_ref,
        first_hbm, second_hbm, attended_hbm, activated_hbm, mixed_hbm, hidden_hbm, branch_hbm, inner_hbm, grad_hbm,
        small_all, sums_ref, bias_sum_ref,
        first_v, second_v, attended_v, activated_v, mixed_v, hidden_v, branch_v, inner_v,
        grad_all, in_all, up_all, qkv_all, down_all, out_all,
        wide_small, norms_ref, bias_ref, bias_up_ref, sum_qkv_ref, sum_up_ref, sum_norm_ref, sum_grad_ref,
        small_send, small_recv, line_send, line_recv, tp_send, tp_recv, z_send, z_recv, dp_send, dp_recv, local, leave,
    ):
        s = lax.axis_index("shard")
        r = lax.axis_index("replica")
        t = sum(((r // bit) % 2 * 2**i for i, bit in enumerate(TP)), jnp.int32(0))
        d = sum(((r // bit) % 2 * 2**i for i, bit in enumerate(DP)), jnp.int32(0))
        place = s * NT + t

        def flipped(value, mask):
            return sum((bit * (1 - 2 * ((value // bit) % 2)) for bit in bits_of(mask)), value)

        def other(k, m):
            mask = sum(bit for i, bit in enumerate(TP) if m >> i & 1)
            return {"shard": lax.rem(s + k, S), "replica": flipped(r, mask)}

        def mate(m):
            return {"replica": flipped(r, sum(bit for i, bit in enumerate(DP) if m >> i & 1))}

        group = [(k, m) for k in range(S) for m in range(NT) if k or m]
        plane = range(1, ND)
        gathered = (grad_all, in_all)
        mine = (grad_ref, in_ref)

        def columns(ref, at, n):
            return ref.at[:, pl.ds(pl.multiple_of(at, n), n)]

        here = pl.ds(pl.multiple_of(s * rows, rows), rows)
        copies = [
            pltpu.make_async_copy(small_ref, small_all.at[t, s], local.at[0]),
            pltpu.make_async_copy(grad_ref, grad_all.at[t, s], local.at[1]),
            pltpu.make_async_copy(in_ref, in_all.at[t, s], local.at[2]),
            pltpu.make_async_copy(columns(up_ref, place * FD, FD), up_all.at[here, :], local.at[3]),
            pltpu.make_async_copy(down_ref.at[pl.ds(pl.multiple_of(t * FD, FD), FD), :], down_all, local.at[4]),
            pltpu.make_async_copy(out_ref.at[pl.ds(pl.multiple_of(t * AD, AD), AD), :], out_all, local.at[5]),
        ]
        for j in range(3):
            source = columns(qkv_ref, j * third + place * AD, AD)
            copies.append(
                pltpu.make_async_copy(source, qkv_all.at[here, j * AD : (j + 1) * AD], local.at[6 + j])
            )
        for copy in copies:
            copy.start()

        barrier = pltpu.get_barrier_semaphore()
        for k, m in group:
            pl.semaphore_signal(barrier, inc=1, device_id=other(k, m), device_id_type=MESH)
        for m in plane:
            pl.semaphore_signal(barrier, inc=1, device_id=mate(m), device_id_type=MESH)
        pl.semaphore_wait(barrier, len(group) + len(plane))

        def small_copy(k, m):
            return pltpu.make_async_remote_copy(
                src_ref=small_ref, dst_ref=small_all.at[t, s], send_sem=small_send.at[k, m],
                recv_sem=small_recv.at[k, m], device_id=other(k, m), device_id_type=MESH,
            )

        def line(i, j, way, source):
            return pltpu.make_async_remote_copy(
                src_ref=source, dst_ref=gathered[i].at[t, j], send_sem=line_send.at[i, j, way],
                recv_sem=line_recv.at[i, j], device_id={"shard": s + 2 * way - 1}, device_id_type=MESH,
            )

        def across(i, j, m, source):
            slot = gathered[i].at[t, j]
            return pltpu.make_async_remote_copy(
                src_ref=slot if source is None else source, dst_ref=slot, send_sem=tp_send.at[i, j, m],
                recv_sem=tp_recv.at[i, j, m], device_id=other(0, m), device_id_type=MESH,
            )

        def z_copies(w, k, sending):
            to = lax.rem(s + k, S)
            at = (s if sending else lax.rem(s + S - k, S)) * rows + d * part
            at = pl.ds(pl.multiple_of(at, part), part)
            source_rows = pl.ds(pl.multiple_of(d * part, part), part)
            out = []
            for j in range(1 if w == 0 else 3):
                if w == 0:
                    source = up_ref.at[source_rows, pl.ds(pl.multiple_of((to * NT + t) * FD, FD), FD)]
                    target = up_all.at[at, :]
                else:
                    col = pl.multiple_of(j * third + (to * NT + t) * AD, AD)
                    source = qkv_ref.at[source_rows, pl.ds(col, AD)]
                    target = qkv_all.at[at, j * AD : (j + 1) * AD]
                out.append(
                    pltpu.make_async_remote_copy(
                        src_ref=source, dst_ref=target, send_sem=z_send.at[k, w + j], recv_sem=z_recv.at[k, w + j],
                        device_id={"shard": to}, device_id_type=MESH,
                    )
                )
            return out

        def shared(w, k, m):
            at = pl.multiple_of(lax.rem(s + S - k, S) * rows + d * part, part)
            slot = (up_all, qkv_all)[w].at[pl.ds(at, part), :]
            return pltpu.make_async_remote_copy(
                src_ref=slot, dst_ref=slot, send_sem=dp_send.at[w, k, m], recv_sem=dp_recv.at[w, k, m],
                device_id=mate(m), device_id_type=MESH,
            )

        for k, m in group:
            small_copy(k, m).start()
        for w in range(2):
            for k in range(1, S):
                for copy in z_copies(w, k, True):
                    copy.start()
        for i in range(2):

            @pl.when(s + 1 < S)
            def _():
                line(i, s, 1, mine[i]).start()

            @pl.when(s > 0)
            def _():
                line(i, s, 0, mine[i]).start()

            for m in range(1, NT):
                across(i, s, m, mine[i]).start()

        for ref in (sum_qkv_ref, sum_up_ref, sum_norm_ref, sum_grad_ref):
            ref[...] = jnp.zeros_like(ref)
        for w in range(2):
            for k in range(1, S):
                for copy in z_copies(w, k, False):
                    copy.wait_recv()
                for m in plane:
                    shared(w, k, m).start()
        for k, m in group:
            small_copy(k, m).wait_recv()
        for copy in copies:
            copy.wait()

        wide_small[...] = small_all[0].astype(F32)
        for v in range(4):
            for j in range(S):
                for i in range(rest):
                    at = (j * rest + i) * 128
                    row = per + (2 + v) * rest + i
                    norms_ref[v : v + 1, at : at + 128] = wide_small[j, row : row + 1, :]
        for j in range(S):
            for i in range(rest):
                at = (j * rest + i) * 128
                row = per + i
                bias_sum_ref[0:1, at : at + 128] = (
                    wide_small[j, row : row + 1, :] + wide_small[j, row + rest : row + rest + 1, :]
                )
        for v in range(3):
            for i in range(AD // 128):
                flat = v * (third // 128) + place * (AD // 128) + i
                at = v * AD + i * 128
                bias_ref[0:1, at : at + 128] = wide_small[flat // per, pl.ds(flat % per, 1), :]
        for i in range(FD // 128):
            row = per + 6 * rest + t * (FD // 128) + i
            bias_up_ref[0:1, i * 128 : (i + 1) * 128] = wide_small[s, pl.ds(row, 1), :]

        def from_line(i, j, way):
            line(i, j, way, gathered[i].at[t, j]).wait_recv()

            @pl.when((s + 1 < S) if way else (s > 0))
            def _():
                line(i, j, way, gathered[i].at[t, j]).start()

            for m in range(1, NT):
                across(i, j, m, None).start()

        def advance(k):
            for i in range(2):

                @pl.when(s - k >= 0)
                def _():
                    from_line(i, s - k, 1)

                @pl.when(s + k < S)
                def _():
                    from_line(i, s + k, 0)

        least = jnp.where(s < S - 1 - s, s, S - 1 - s)

        def block_at(i):
            both = jnp.where(i % 2 == 1, s - (i + 1) // 2, s + i // 2)
            one = jnp.where(s < S - 1 - s, i, S - 1 - i)
            return jnp.where(i <= 2 * least, both, one)

        row = lax.broadcasted_iota(jnp.int32, (T, T), 0)
        col = lax.broadcasted_iota(jnp.int32, (T, T), 1)
        away = (row - col).astype(F32)
        lane = lax.broadcasted_iota(jnp.int32, (T, 128), 1)

        def turn(value, table, sign):
            straight, ahead, back = table
            low = value[:, :128]
            low = low * straight + sign * (
                pltpu.roll(low, 128 - ROT // 2, 1) * ahead + pltpu.roll(low, ROT // 2, 1) * back
            )
            return jnp.concatenate([low, value[:, 128:]], axis=1)

        leaving = (
            (first_v, first_hbm), (second_v, second_hbm), (attended_v, attended_hbm), (activated_v, activated_hbm),
            (mixed_v, mixed_hbm), (hidden_v, hidden_hbm), (branch_v, branch_hbm), (inner_v, inner_hbm),
            (grad_all, grad_hbm),
        )

        def depart(v, u, j):
            source, target = leaving[v]
            return pltpu.make_async_copy(source.at[u, j], target.at[u, j], leave.at[v, u, j])

        def compute(i, carry):
            j = block_at(i)

            @pl.when(i == 0)
            def _():
                advance(1)
                for k in range(1, S):
                    for m in plane:
                        shared(0, k, m).wait_recv()

            @pl.when(i == 1)
            def _():
                advance(2)

            @pl.when(i >= 3)
            def _():
                advance(i)

            for m in range(1, NT):
                for v in range(2):
                    across(v, j, m, None).wait_recv()

            def join(ref):
                return jnp.concatenate([ref[u, j] for u in range(NT)], axis=0)

            def put(v, value):
                for u in range(NT):
                    leaving[v][0][u, j] = value[u * T : (u + 1) * T]

            def leave_now(*arrays):
                for v in arrays:
                    for u in range(NT):
                        depart(v, u, j).start()

            gain_1, shift_1, gain_2, shift_2 = [norms_ref[v : v + 1, :] for v in range(4)]
            wide = join(in_all).astype(F32)
            offsets = wide - jnp.mean(wide, axis=-1, keepdims=True)
            inverse = lax.rsqrt(jnp.mean(offsets * offsets, axis=-1, keepdims=True) + epsilon)
            normed = offsets * inverse
            first = (normed * gain_1 + shift_1).astype(BF16)
            second = (normed * gain_2 + shift_2).astype(BF16)
            put(0, first)
            put(1, second)
            leave_now(8)
            grad = join(grad_all)
            sum_grad_ref[...] += jnp.sum(grad.astype(F32), axis=0, keepdims=True)

            pre = dot(second, up_all[...], 1, 0) + bias_up_ref[...]
            bell = 0.5 * (1.0 + lax.erf(pre * 0.7071067811865476))
            activated = (pre * bell).astype(BF16)
            put(3, activated)
            slope = bell + pre * jnp.exp(-0.5 * pre * pre) * 0.3989422804014327
            hidden_grad = dot(grad, down_all[...], 1, 1) * slope
            sum_up_ref[...] += jnp.sum(hidden_grad, axis=0, keepdims=True)
            hidden_low = hidden_grad.astype(BF16)
            put(5, hidden_low)
            leave_now(0, 1, 3)

            @pl.when(i == 0)
            def _():
                for k in range(1, S):
                    for m in plane:
                        shared(1, k, m).wait_recv()

            mixed = dot(first, qkv_all[...], 1, 0) + bias_ref[...]
            attended_grad = dot(grad, out_all[...], 1, 1).astype(BF16)
            attended_parts, mixed_parts = [], []
            for u in range(NT):
                flat = small_all[u, j, -1:, :].astype(F32)
                position = jnp.sum(jnp.where(row == col, flat, 0.0), axis=1, keepdims=True)
                angle = position * freqs_ref[...]
                sine = jnp.sin(angle)
                table = (
                    jnp.cos(angle),
                    jnp.where(lane < ROT // 2, -sine, 0.0),
                    jnp.where((lane >= ROT // 2) & (lane < ROT), sine, 0.0),
                )
                allowed = (away >= 0) & (away <= position)
                at_rows = slice(u * T, (u + 1) * T)
                outs, q_grads, k_grads, v_grads = [], [], [], []
                for h in range(heads):
                    at = slice(h * HD, (h + 1) * HD)
                    ag = attended_grad[at_rows, at]
                    q = turn(mixed[at_rows, at], table, 1.0).astype(BF16)
                    k = turn(mixed[at_rows, AD + h * HD : AD + (h + 1) * HD], table, 1.0).astype(BF16)
                    v = mixed[at_rows, 2 * AD + h * HD : 2 * AD + (h + 1) * HD].astype(BF16)
                    scores = jnp.where(allowed, dot(q, k, 1, 1) * scale, -1e30)
                    peak = jnp.max(scores, axis=-1, keepdims=True)
                    logsum = peak + jnp.log(jnp.sum(jnp.exp(scores - peak), axis=-1, keepdims=True))
                    probs = jnp.exp(scores - logsum)
                    low = probs.astype(BF16)
                    outs.append(dot(low, v, 1, 0).astype(BF16))
                    dprobs = dot(ag, v, 1, 1)
                    total = jnp.sum(probs * dprobs, axis=-1, keepdims=True)
                    dscores = (probs * (dprobs - total) * scale).astype(BF16)
                    q_grads.append(turn(dot(dscores, k, 1, 0), table, -1.0))
                    k_grads.append(turn(dot(dscores, q, 0, 0), table, -1.0))
                    v_grads.append(dot(low, ag, 0, 0))
                attended_parts.append(jnp.concatenate(outs, axis=1))
                mixed_parts.append(jnp.concatenate(q_grads + k_grads + v_grads, axis=1))
            attended = jnp.concatenate(attended_parts, axis=0)
            put(2, attended)
            mixed_grad = jnp.concatenate(mixed_parts, axis=0)
            sum_qkv_ref[...] += jnp.sum(mixed_grad, axis=0, keepdims=True)
            mixed_low = mixed_grad.astype(BF16)
            put(4, mixed_low)

            branch = dot(attended, out_all[...], 1, 0) + dot(activated, down_all[...], 1, 0)
            put(6, branch.astype(BF16))
            leave_now(2, 4, 5)
            first_grad = dot(mixed_low, qkv_all[...], 1, 1)
            second_grad = dot(hidden_low, up_all[...], 1, 1)
            sum_norm_ref[0:1, :] += jnp.sum(first_grad * normed, axis=0, keepdims=True)
            sum_norm_ref[1:2, :] += jnp.sum(first_grad, axis=0, keepdims=True)
            sum_norm_ref[2:3, :] += jnp.sum(second_grad * normed, axis=0, keepdims=True)
            sum_norm_ref[3:4, :] += jnp.sum(second_grad, axis=0, keepdims=True)
            put(7, (first_grad * gain_1 + second_grad * gain_2).astype(BF16))
            leave_now(6, 7)
            return carry

        lax.fori_loop(0, S, compute, 0)

        sums_ref[...] = jnp.zeros_like(sums_ref)
        n = AD // 128
        for v in range(3):
            for i in range(n):
                at = v * AD + i * 128
                sums_ref[pl.ds(v * (third // 128) + place * n + i, 1), :] = sum_qkv_ref[:, at : at + 128]
        for i in range(FD // 128):
            sums_ref[pl.ds(base_up + place * (FD // 128) + i, 1), :] = sum_up_ref[:, i * 128 : (i + 1) * 128]
        for i in range(D // 128):
            at = slice(i * 128, (i + 1) * 128)
            sums_ref[base_out + i : base_out + i + 1, :] = sum_grad_ref[:, at] * (1.0 / (S * NT))
            for v in range(4):
                at_row = base_norm + v * (D // 128) + i
                sums_ref[at_row : at_row + 1, :] = sum_norm_ref[v : v + 1, at]

        for i in range(2):
            for j in range(S):

                @pl.when((s + 1 < S) & (j <= s))
                def _():
                    line(i, j, 1, gathered[i].at[t, j]).wait_send()

                @pl.when((s > 0) & (j >= s))
                def _():
                    line(i, j, 0, gathered[i].at[t, j]).wait_send()

                for m in range(1, NT):
                    across(i, j, m, None).wait_send()
        for k, m in group:
            small_copy(k, m).wait_send()
        for w in range(2):
            for k in range(1, S):
                for copy in z_copies(w, k, True):
                    copy.wait_send()
                for m in plane:
                    shared(w, k, m).wait_send()
        for v in range(len(leaving)):
            for u in range(NT):
                for j in range(S):
                    depart(v, u, j).wait()

    any_spec = pl.BlockSpec(memory_space=pl.ANY)
    vmem_spec = pl.BlockSpec(memory_space=pltpu.VMEM)
    outs = [jax.ShapeDtypeStruct((NT, S, T, w), BF16) for w in widths + [D]]
    outs += [jax.ShapeDtypeStruct((NT, S) + small.shape, BF16), jax.ShapeDtypeStruct((count, 128), F32)]
    outs += [jax.ShapeDtypeStruct((1, D), F32)]
    flops = 2 * S * tile * D * (2 * 3 * AD + 2 * FD + 2 * FD + 2 * AD)
    return pl.pallas_call(
        kernel,
        out_shape=outs,
        in_specs=[any_spec] * 7 + [vmem_spec],
        out_specs=[any_spec] * 9 + [vmem_spec] * 3,
        scratch_shapes=[pltpu.VMEM((NT, S, T, w), BF16) for w in widths]
        + [
            pltpu.VMEM((NT, S, T, D), BF16),
            pltpu.VMEM((NT, S, T, D), BF16),
            pltpu.VMEM((D, FD), BF16),
            pltpu.VMEM((D, 3 * AD), BF16),
            pltpu.VMEM((FD, D), BF16),
            pltpu.VMEM((AD, D), BF16),
            pltpu.VMEM((S,) + small.shape, F32),
            pltpu.VMEM((4, D), F32),
            pltpu.VMEM((1, 3 * AD), F32),
            pltpu.VMEM((1, FD), F32),
            pltpu.VMEM((1, 3 * AD), F32),
            pltpu.VMEM((1, FD), F32),
            pltpu.VMEM((4, D), F32),
            pltpu.VMEM((1, D), F32),
            pltpu.SemaphoreType.DMA((S, NT)),
            pltpu.SemaphoreType.DMA((S, NT)),
            pltpu.SemaphoreType.DMA((2, S, 2)),
            pltpu.SemaphoreType.DMA((2, S)),
            pltpu.SemaphoreType.DMA((2, S, NT)),
            pltpu.SemaphoreType.DMA((2, S, NT)),
            pltpu.SemaphoreType.DMA((S, 4)),
            pltpu.SemaphoreType.DMA((S, 4)),
            pltpu.SemaphoreType.DMA((2, S, ND)),
            pltpu.SemaphoreType.DMA((2, S, ND)),
            pltpu.SemaphoreType.DMA((9,)),
            pltpu.SemaphoreType.DMA((9, NT, S)),
        ],
        compiler_params=pltpu.CompilerParams(
            collective_id=0, has_side_effects=True, vmem_limit_bytes=67043328
        ),
        cost_estimate=pl.CostEstimate(flops=flops, bytes_accessed=80 * 2**20, transcendentals=S * tile * FD * 2),
        name="layer",
    )(small, out_grad, block_in, w_up, w_qkv, w_down, w_out, freqs)


def grads(
    first, second, attended, activated, mixed, hidden, grad, branch, inner, sums, S, R, T, TP, DP
):
    N, D = grad.shape
    NT, ND, steps = 2 ** len(TP), 2 ** len(DP), len(DP)
    lefts = (second, first, activated, attended)
    rights = (hidden, mixed, grad, grad)
    pieces = []
    for left, right, lead, mid in zip(lefts, rights, (S, S, 1, 1), (NT, NT, 1, 1)):
        pieces.append((lead, mid, left.shape[1] // (lead * ND * mid * 2), right.shape[1]))
    ways = []
    for way in (DP, DP[::-1]):
        ways.append([(bit, 1 << DP.index(bit)) for bit in way])

    def masks(bits):
        out = [0]
        for _, bit in bits:
            out += [v | bit for v in out]
        return sorted(out)

    slots = []
    for way in ways:
        table = {}
        for j in range(steps):
            for u in masks(way[j + 1 :]):
                table[j, u] = len(table)
        slots.append(table)

    def kernel(
        second_hbm, first_hbm, activated_hbm, attended_hbm, hidden_hbm, mixed_hbm, grad_hbm, branch_hbm, inner_hbm, sums_hbm,
        whole_up, whole_out, own_down_0, own_down_1, own_qkv_0, own_qkv_1, branch_own, inner_own, *more,
    ):
        inner_rest, sums_out = more[: S - 1], more[S - 1]
        mates = [more[S + 4 * m : S + 4 * m + 4] for m in range(NT - 1)]
        (
            own_up, own_out, near, near_came, far_came, held, held_came,
            second_v, first_v, activated_v, attended_v, hidden_v, mixed_v, grad_v,
            part_up, part_qkv, part_down, part_out, came_up, came_qkv, came_down, came_out, all_up, all_qkv,
            load, dp_send, dp_recv, z_send, z_recv, near_send, near_recv, far_send, far_recv, held_send, held_recv,
            plane_send, plane_recv, mate_send, mate_recv,
        ) = more[S + 4 * (NT - 1) :]
        s = lax.axis_index("shard")
        r = lax.axis_index("replica")
        t = sum(((r // bit) % 2 * 2**i for i, bit in enumerate(TP)), jnp.int32(0))
        d = sum(((r // bit) % 2 * 2**i for i, bit in enumerate(DP)), jnp.int32(0))

        def flipped(value, mask):
            return sum((bit * (1 - 2 * ((value // bit) % 2)) for bit in bits_of(mask)), value)

        def other(k, m):
            mask = sum(bit for i, bit in enumerate(TP) if m >> i & 1)
            return {"shard": lax.rem(s + k, S), "replica": flipped(r, mask)}

        loads = []
        order = ((hidden_hbm, hidden_v), (second_hbm, second_v), (mixed_hbm, mixed_v), (first_hbm, first_v),
                 (grad_hbm, grad_v), (activated_hbm, activated_v), (attended_hbm, attended_v))
        parts_hbm = (branch_hbm, inner_hbm)
        for i, (source, target) in enumerate(order):
            loads.append(pltpu.make_async_copy(source, target, load.at[i]))
        token_loads = [
            pltpu.make_async_copy(parts_hbm[i].at[t], near.at[i], load.at[7 + i]) for i in range(2)
        ]
        held_load = pltpu.make_async_copy(sums_hbm, held.at[0], load.at[9])
        for copy in (loads[6], loads[4], *loads[:2], held_load, *token_loads, *loads[2:4], loads[5]):
            copy.start()

        group = [(k, m) for k in range(S) for m in range(NT) if k or m]
        barrier = pltpu.get_barrier_semaphore()
        for k, m in group:
            pl.semaphore_signal(barrier, inc=1, device_id=other(k, m), device_id_type=MESH)
        for bit in DP:
            pl.semaphore_signal(barrier, inc=1, device_id={"replica": flipped(r, bit)}, device_id_type=MESH)
        pl.semaphore_wait(barrier, len(group) + steps)

        left_refs = (second_v, first_v, activated_v, attended_v)
        right_refs = (hidden_v, mixed_v, grad_v, grad_v)
        part = (part_up, part_qkv, part_down, part_out)
        came = (came_up, came_qkv, came_down, came_out)
        own = (own_up, (own_qkv_0, own_qkv_1), (own_down_0, own_down_1), own_out)

        def product(i):
            lead, mid, n, _ = pieces[i]
            if lead > 1:
                width = ND * mid * 2 * n

                def body(l, carry):
                    cols = pl.ds(pl.multiple_of(l * width, width), width)
                    value = dot(left_refs[i][:, cols], right_refs[i][...], 0, 0).astype(BF16)
                    for q in range(ND):
                        for c in range(mid):
                            for h in range(2):
                                at = ((q * mid + c) * 2 + h) * n
                                part[i][h, q, l, c] = value[at : at + n]
                    return carry

                lax.fori_loop(0, lead, body, 0)
            else:
                total = ND * 2 * n
                chunk = min(total, 512)
                per = chunk // (2 * n)

                def body(l, carry):
                    cols = pl.ds(pl.multiple_of(l * chunk, chunk), chunk)
                    value = dot(left_refs[i][:, cols], right_refs[i][...], 0, 0).astype(BF16)
                    for q in range(per):
                        for h in range(2):
                            at = (q * 2 + h) * n
                            part[i][h, l * per + q, 0, 0] = value[at : at + n]
                    return carry

                lax.fori_loop(0, total // chunk, body, 0)

        def halving(i, h, j, u):
            bit, dbit = ways[h][j]
            slot = slots[h][j, u]
            return pltpu.make_async_remote_copy(
                src_ref=part[i].at[h, flipped(d, dbit | u)], dst_ref=came[i].at[h, slot],
                send_sem=dp_send.at[i, h, slot], recv_sem=dp_recv.at[i, h, slot],
                device_id={"replica": flipped(r, bit)}, device_id_type=MESH,
            )

        def summed(i, h, mask, count, write):
            lead, mid, _, _ = pieces[i]
            at = flipped(d, mask)
            for j in range(count):
                halving(i, h, j, mask).wait_recv()

            def body(l, carry):
                for c in range(mid):
                    value = part[i][h, at, l, c].astype(F32)
                    for j in range(count):
                        value = value + came[i][h, slots[h][j, mask], l, c].astype(F32)
                    write(l, c, value.astype(BF16))
                return carry

            lax.fori_loop(0, lead, body, 0)

        def step(i, j):
            for h in range(2):
                for u in masks(ways[h][j + 1 :]):
                    mask = ways[h][j][1] | u
                    at = flipped(d, mask)
                    if j:

                        def write(l, c, value, h=h, at=at):
                            part[i][h, at, l, c] = value

                        summed(i, h, mask, j, write)
                    halving(i, h, j, u).start()

        everyone = (all_up, all_qkv)

        def to_shard(i, h, k, m):
            there = lax.rem(s + k, S)
            return pltpu.make_async_remote_copy(
                src_ref=part[i].at[h, d, there, flipped(t, m)], dst_ref=everyone[i].at[s, t, h],
                send_sem=z_send.at[i, h, k, m], recv_sem=z_recv.at[i, h, k, m],
                device_id=other(k, m), device_id_type=MESH,
            )

        def last(i):
            for h in range(2):
                if i < 2:

                    def write(l, c, value, h=h):
                        part[i][h, d, l, c] = value

                else:

                    def write(l, c, value, h=h):
                        if i == 2:
                            own[i][h][...] = value
                        else:
                            own[i][h] = value

                summed(i, h, 0, steps, write)
            if i < 2:
                for k, m in group:
                    for h in range(2):
                        to_shard(i, h, k, m).start()
                for h in range(2):
                    everyone[i][s, t, h] = part[i][h, d, s, t]

        def collect(i):
            width = pieces[i][3]
            runs = 1 if i == 0 else 3
            n = width // runs
            for k, m in group:
                for h in range(2):
                    to_shard(i, h, k, m).wait_recv()
            for h in range(2):
                for j in range(S):
                    for u in range(NT):
                        block = everyone[i][j, u, h]
                        for v in range(runs):
                            at = (v * S * NT + j * NT + u) * n
                            target = own[i][h] if i == 1 else own[i].at[h]
                            target[:, at : at + n] = block[:, v * n : (v + 1) * n]

        def near_copy(i, m):
            return pltpu.make_async_remote_copy(
                src_ref=parts_hbm[i].at[flipped(t, m)], dst_ref=near_came.at[i, m - 1],
                send_sem=near_send.at[i, m], recv_sem=near_recv.at[i, m], device_id=other(0, m), device_id_type=MESH,
            )

        def far_copy(k):
            there = lax.rem(s + k, S)
            return pltpu.make_async_remote_copy(
                src_ref=near.at[0, there] if NT > 1 else branch_hbm.at[t, there], dst_ref=far_came.at[k - 1],
                send_sem=far_send.at[k], recv_sem=far_recv.at[k], device_id=other(k, 0), device_id_type=MESH,
            )

        def near_sum(i, j):
            value = near[i, j].astype(F32)
            for m in range(1, NT):
                value = value + near_came[i, m - 1, j].astype(F32)
            return value

        def near_wait(i):
            token_loads[i].wait()
            for m in range(1, NT):
                near_copy(i, m).wait_recv()

        def branch_near():
            near_wait(0)

            def body(k, carry):
                j = lax.rem(s + k, S)
                near[0, j] = near_sum(0, j).astype(BF16)
                return carry

            if NT > 1:
                lax.fori_loop(1, S, body, 0)
            for k in range(1, S):
                far_copy(k).start()

        def branch_far():
            value = near_sum(0, s)
            for k in range(1, S):
                far_copy(k).wait_recv()
                value = value + far_came[k - 1].astype(F32)
            branch_own[...] = value

        def inner_near():
            near_wait(1)
            inner_own[...] = near_sum(1, s)
            for k in range(1, S):
                inner_rest[k - 1][...] = near_sum(1, lax.rem(s + k, S)).astype(BF16)

        bits = [(0, bit) for bit in bits_of(R - 1)] + [(1, bit) for bit in bits_of(S - 1)]

        def double(i):
            axis, bit = bits[i]
            to = {"replica": flipped(r, bit)} if axis == 0 else {"shard": flipped(s, bit)}
            return pltpu.make_async_remote_copy(
                src_ref=held.at[i], dst_ref=held_came.at[i], send_sem=held_send.at[i], recv_sem=held_recv.at[i],
                device_id=to, device_id_type=MESH,
            )

        def doubled(i):
            double(i).wait_recv()
            value = held[i] + held_came[i]
            if i + 1 < len(bits):
                held[i + 1] = value
                double(i + 1).start()
            else:
                sums_out[...] = value

        wholes = {0: whole_up, 3: whole_out}
        order_of = {0: 0, 3: 1}

        def slot_of(i, h, dd, tt):
            n = pieces[i][2]
            if i == 0:
                at = (dd * NT + tt) * 2 * n + h * n
            else:
                at = tt * (ND * 2 * n) + dd * 2 * n + h * n
            return wholes[i].at[pl.ds(pl.multiple_of(at, n), n), :]

        def gather(i, h, m, b):
            dmask = sum(ways[h][v][1] for v in range(steps) if m >> v & 1)
            tmask = m >> steps
            slot = slot_of(i, h, flipped(d, dmask), flipped(t, tmask))
            bit = ways[h][b][0] if b < steps else TP[b - steps]
            return pltpu.make_async_remote_copy(
                src_ref=own[i].at[h] if m == 0 else slot, dst_ref=slot,
                send_sem=plane_send.at[order_of[i], h, m | 1 << b], recv_sem=plane_recv.at[order_of[i], h, m | 1 << b],
                device_id={"replica": flipped(r, bit)}, device_id_type=MESH,
            )

        positions = steps + len(TP)

        def keep_own(i, h):
            return pltpu.make_async_copy(own[i].at[h], slot_of(i, h, d, t), load.at[10 + order_of[i] * 2 + h])

        def share_own(i):
            for h in range(2):
                for b in range(positions):
                    gather(i, h, 0, b).start()
                keep_own(i, h).start()

        def share_on(i, m):
            top = m.bit_length() - 1
            for h in range(2):
                gather(i, h, m ^ 1 << top, top).wait_recv()
                for b in range(top + 1, positions):
                    gather(i, h, m, b).start()

        def to_mate(i, h, m):
            at = (2 - i) * 2 + h
            return pltpu.make_async_remote_copy(
                src_ref=own[i][h], dst_ref=mates[m - 1][at], send_sem=mate_send.at[at, m], recv_sem=mate_recv.at[at, m],
                device_id=other(0, m), device_id_type=MESH,
            )

        def to_mates(i):
            for h in range(2):
                for m in range(1, NT):
                    to_mate(i, h, m).start()

        for i in range(2):
            for m in range(1, NT):
                near_copy(i, m).start()
        held_load.wait()
        double(0).start()
        loads[4].wait()
        loads[6].wait()
        product(3)
        step(3, 0)
        loads[0].wait()
        loads[1].wait()
        product(0)
        step(0, 0)
        branch_near()
        doubled(0)
        loads[2].wait()
        loads[3].wait()
        product(1)
        step(1, 0)
        for j in range(1, steps):
            step(0, j)
        doubled(1)
        loads[5].wait()
        product(2)
        step(2, 0)
        for j in range(1, steps):
            step(1, j)
        last(0)
        for i in range(2, len(bits)):
            doubled(i)
        for j in range(1, steps):
            step(2, j)
        last(1)
        for j in range(1, steps):
            step(3, j)
        collect(0)
        share_own(0)
        last(2)
        to_mates(2)
        last(3)
        share_own(3)
        for m in range(1, 1 << steps):
            for i in (0, 3):
                share_on(i, m)
            if m == 1:
                collect(1)
                to_mates(1)
                branch_far()
                inner_near()
        for m in range(1 << steps, 1 << positions):
            for i in (0, 3):
                share_on(i, m)

        for i in (1, 2):
            for h in range(2):
                for m in range(1, NT):
                    to_mate(i, h, m).wait()
        for i in (3, 0):
            for h in range(2):
                keep_own(i, h).wait()
                for m in range(1 << positions):
                    for b in range(m.bit_length(), positions):
                        gather(i, h, m, b).wait_send()
        for i in range(2):
            for m in range(1, NT):
                near_copy(i, m).wait_send()
        for k in range(1, S):
            far_copy(k).wait_send()
        for i in range(len(bits)):
            double(i).wait_send()
        for i in range(4):
            for h in range(2):
                for j, u in slots[h]:
                    halving(i, h, j, u).wait_send()
        for i in range(2):
            for h in range(2):
                for k, m in group:
                    to_shard(i, h, k, m).wait_send()

    def scratch(value):
        return pltpu.VMEM(value.shape, BF16)

    any_spec = pl.BlockSpec(memory_space=pl.ANY)
    vmem_spec = pl.BlockSpec(memory_space=pltpu.VMEM)
    operands = (second, first, activated, attended, hidden, mixed, grad)
    owns = [(2, n, width * S * NT if lead > 1 else width) for lead, _, n, width in pieces]
    wholes = [(2 * n * ND * NT, width) for _, n, width in owns]
    outs = [jax.ShapeDtypeStruct(wholes[i], BF16) for i in (0, 3)]
    owned = [jax.ShapeDtypeStruct(owns[i][1:], BF16) for i in (2, 2, 1, 1)]
    outs += owned + [jax.ShapeDtypeStruct((T, D), F32)] * 2 + [jax.ShapeDtypeStruct((T, D), BF16)] * (S - 1)
    outs += [jax.ShapeDtypeStruct(sums.shape, F32)] + owned * (NT - 1)
    sent = sum(2 * (ND - 1) * a * b * n * w * 2 for a, b, n, w in pieces)
    count = len(bits_of(R - 1)) + len(bits_of(S - 1))
    return pl.pallas_call(
        kernel,
        out_shape=outs,
        in_specs=[any_spec] * 10,
        out_specs=[any_spec] * 2 + [vmem_spec] * (7 + S - 1 + 4 * (NT - 1)),
        scratch_shapes=[pltpu.VMEM(owns[i], BF16) for i in (0, 3)]
        + [
            pltpu.VMEM((2, S, T, D), BF16),
            pltpu.VMEM((2, NT - 1, S, T, D) if NT > 1 else (1, 1, 1, 16, 128), BF16),
            pltpu.VMEM((S - 1, T, D), BF16),
            pltpu.VMEM((count,) + sums.shape, F32),
            pltpu.VMEM((count,) + sums.shape, F32),
        ]
        + [scratch(v) for v in operands]
        + [pltpu.VMEM((2, ND) + piece, BF16) for piece in pieces]
        + [pltpu.VMEM((2, ND - 1) + piece, BF16) for piece in pieces]
        + [pltpu.VMEM((S, NT, 2) + piece[2:], BF16) for piece in pieces[:2]]
        + [
            pltpu.SemaphoreType.DMA((18,)),
            pltpu.SemaphoreType.DMA((4, 2, ND - 1)),
            pltpu.SemaphoreType.DMA((4, 2, ND - 1)),
            pltpu.SemaphoreType.DMA((2, 2, S, NT)),
            pltpu.SemaphoreType.DMA((2, 2, S, NT)),
            pltpu.SemaphoreType.DMA((2, NT)),
            pltpu.SemaphoreType.DMA((2, NT)),
            pltpu.SemaphoreType.DMA((S,)),
            pltpu.SemaphoreType.DMA((S,)),
            pltpu.SemaphoreType.DMA((count,)),
            pltpu.SemaphoreType.DMA((count,)),
            pltpu.SemaphoreType.DMA((2, 2, ND * NT)),
            pltpu.SemaphoreType.DMA((2, 2, ND * NT)),
            pltpu.SemaphoreType.DMA((4, NT)),
            pltpu.SemaphoreType.DMA((4, NT)),
        ],
        compiler_params=pltpu.CompilerParams(
            collective_id=1, has_side_effects=True, vmem_limit_bytes=67043328
        ),
        cost_estimate=pl.CostEstimate(
            flops=2 * N * sum(v.shape[1] * w.shape[1] for v, w in zip(lefts, rights)),
            bytes_accessed=sent * 8, transcendentals=0,
        ),
        name="grads",
    )(*operands, branch, inner, sums)


def solution(mesh):
    S = mesh.shape["shard"]
    R = mesh.shape["replica"]
    TP = [1] if R > 1 and H % (2 * S) == 0 else []
    DP = [bit for bit in bits_of(R - 1) if bit not in TP]
    NT = 2 ** len(TP)

    def flip(value, bit):
        return lax.ppermute(value, "replica", [(i, i ^ bit) for i in range(R)])

    def body(
        block_in, positions, out_grad, w_qkv, b_qkv, w_out, b_out, w_up, b_up, w_down, b_down,
        first_gain, first_shift, second_gain, second_shift,
    ):
        T, _ = block_in.shape
        FS = w_down.shape[0]
        FD = FS // NT
        s = lax.axis_index("shard")
        r = lax.axis_index("replica")
        mine = {bit: (r // bit) % 2 for bit in bits_of(R - 1)}
        t = sum((mine[bit] * 2**i for i, bit in enumerate(TP)), jnp.int32(0))

        vectors = [
            b_qkv, b_out, b_down, first_gain, first_shift, second_gain, second_shift, b_up, positions.astype(BF16)
        ]
        ends = [sum(v.shape[0] for v in vectors[: i + 1]) for i in range(len(vectors))]
        small = sum(lax.pad(v, jnp.zeros((), BF16), [(end - v.shape[0], ends[-1] - end, 0)]) for v, end in zip(vectors, ends))
        small = small.reshape(-1, 128)
        (
            first_low, second_low, attended, activated, mixed_low, hidden_low, branch_part, inner_part, grad_all,
            _, sums, bias,
        ) = layer(block_in, out_grad, small, rotary_freqs(), w_up, w_qkv, w_down, w_out, S, TP, DP)
        first_low, second_low, attended, activated, mixed_low, hidden_low, grad_all = [
            v.reshape(NT * S * T, -1)
            for v in (first_low, second_low, attended, activated, mixed_low, hidden_low, grad_all)
        ]
        d = sum((mine[bit] * 2**i for i, bit in enumerate(DP)), jnp.int32(0))

        whole_up, whole_out, *more = grads(
            first_low, second_low, attended, activated, mixed_low, hidden_low, grad_all, branch_part, inner_part,
            sums, S, R, T, TP, DP,
        )
        owned_rows, (branch_own, inner_own), inner_rest, sums = more[:4], more[4:6], more[6 : 5 + S], more[5 + S]
        mates = [more[6 + S + 4 * m : 10 + S + 4 * m] for m in range(NT - 1)]

        ways = [DP, DP[::-1]]

        def indices(m):
            dmask = sum(2**i for i, bit in enumerate(DP) if m & bit)
            tmask = sum(2**i for i, bit in enumerate(TP) if m & bit)
            return d ^ dmask, t ^ tmask

        def down_row(half, m, n):
            dd, tt = indices(m)
            return tt * FD + (dd * 2 + half) * n

        def qkv_row(half, m, n):
            dd, tt = indices(m)
            return ((dd * NT + tt) * 2 + half) * n

        def placed(result, which, pieces, row):
            for bit in TP:
                pieces = pieces + [
                    (half, m | bit, mates[0][2 * which + half] if m == 0 else flip(value, bit))
                    for half, m, value in pieces
                ]
            at = jnp.stack([row(half, m, value.shape[0]) for half, m, value in pieces])
            return place([value for _, _, value in pieces], at, result)

        got = [[{0: owned_rows[2 * i + half]} for half in range(2)] for i in range(2)]

        def fetched(i, half, masks):
            for m in masks:
                bit = [b for b in ways[half] if m & b][-1]
                got[i][half][m] = flip(got[i][half][m ^ bit], bit)

        several = [m for m in all_masks(DP) if m and m not in DP]
        for masks in (DP, several):
            for i in range(2):
                for half in range(2):
                    fetched(i, half, masks)

        def pieces_of(i, masks):
            return [(half, m, got[i][half][m]) for half in range(2) for m in masks]

        scaled = []
        for k in range(1, S):
            scaled.append(lax.ppermute(inner_rest[k - 1], "shard", [(i, (i + k) % S) for i in range(S)]))
        grad_w_up = widen(whole_up)
        grad_w_out = widen(whole_out)
        grad_w_down = placed(unwritten(w_down.shape, F32), 0, pieces_of(0, [0]), down_row)
        grad_w_qkv = placed(unwritten(w_qkv.shape, F32), 1, pieces_of(1, [0]), qkv_row)
        grad_w_down = placed(grad_w_down, 0, pieces_of(0, DP), down_row)
        grad_w_qkv = placed(grad_w_qkv, 1, pieces_of(1, DP), qkv_row)
        bias, grad_w_qkv = lax.optimization_barrier((bias, grad_w_qkv))
        block_out, in_grad, *smalls = finish(
            block_in, out_grad, branch_own, bias, inner_own, scaled, sums, s,
            [v.shape[0] * S // 128 for v in (b_qkv, b_out, b_up) + (first_gain,) * 4], S,
        )
        if several:
            grad_w_down = placed(grad_w_down, 0, pieces_of(0, several), down_row)
            grad_w_qkv = placed(grad_w_qkv, 1, pieces_of(1, several), qkv_row)

        grad_b_qkv, grad_b_out, grad_b_down, grad_b_up, *norm_grads = [v.reshape(-1) for v in smalls]
        return (
            block_out, in_grad, grad_w_qkv, grad_b_qkv, grad_w_out, grad_b_out, grad_w_up, grad_b_up,
            grad_w_down, grad_b_down, *norm_grads,
        )

    rows2, row1, par2, par1 = P(("shard", "replica"), None), P(("shard", "replica")), P("shard", None), P("shard")
    return jax.shard_map(
        body,
        mesh=mesh,
        in_specs=(
            rows2, row1, rows2, par2, par1, par2, par1, par2, par1, par2, par1, par1, par1, par1, par1,
        ),
        out_specs=(
            rows2, rows2, par2, par1, par2, par1, par2, par1, par2, par1, par1, par1, par1, par1,
        ),
        check_vma=False,
    )
```

```python
import jax
import jax.numpy as jnp
import numpy as np
from jax import lax
from jax.experimental import pallas as pl
from jax.experimental.pallas import tpu as pltpu
from jax.sharding import PartitionSpec as P

H = 8
HD = 256
ROT = 64

epsilon = 1e-05


F32 = jnp.float32
BF16 = jnp.bfloat16
MESH = pl.DeviceIdType.MESH


def rotary_freqs():
    freqs = 10000.0 ** (-(np.arange(ROT // 2) * (2.0 / ROT)))
    return np.concatenate([freqs, freqs, np.zeros(128 - ROT)]).astype(np.float32).reshape(1, 128)


def all_masks(bits):
    out = [0]
    for bit in bits:
        out += [v | bit for v in out]
    return sorted(out, key=lambda v: (v.bit_count(), v))


def dot(left, right, left_dim, right_dim):
    return lax.dot_general(
        left, right, (((left_dim,), (right_dim,)), ((), ())), preferred_element_type=F32
    )


def widen(value):
    rows, width = value.shape
    n = min(rows // 2, max(8, 2**20 // width))

    def kernel(in_ref, out_ref):
        out_ref[...] = in_ref[...].astype(F32)

    spec = pl.BlockSpec((n, width), lambda i: (i, 0))
    return pl.pallas_call(
        kernel,
        grid=(rows // n,),
        in_specs=[spec],
        out_specs=spec,
        out_shape=jax.ShapeDtypeStruct(value.shape, F32),
        cost_estimate=pl.CostEstimate(flops=0, bytes_accessed=6 * rows * width, transcendentals=0),
        name="widen",
    )(value)


def place(pieces, rows, first, result):
    n, width = pieces[0].shape
    count = len(pieces)

    def kernel(rows_ref, *refs):
        sources, target = refs[:count], refs[count + 1]
        wide, go = refs[count + 2 :]
        copies = []
        for i in range(count):
            wide[i] = sources[i][...].astype(F32)
            at = pl.multiple_of(rows_ref[first + i], n)
            copies.append(pltpu.make_async_copy(wide.at[i], target.at[pl.ds(at, n), :], go.at[i]))
            copies[-1].start()
        for copy in copies:
            copy.wait()

    any_spec = pl.BlockSpec(memory_space=pl.ANY)
    return pl.pallas_call(
        kernel,
        in_specs=[pl.BlockSpec(memory_space=pltpu.SMEM)] + [pl.BlockSpec(memory_space=pltpu.VMEM)] * count + [any_spec],
        out_specs=any_spec,
        out_shape=jax.ShapeDtypeStruct(result.shape, F32),
        scratch_shapes=[pltpu.VMEM((count, n, width), F32), pltpu.SemaphoreType.DMA((count,))],
        input_output_aliases={count + 1: 0},
        cost_estimate=pl.CostEstimate(flops=0, bytes_accessed=6 * count * n * width, transcendentals=0),
        name="place",
    )(rows, *pieces, result)


def finish(block_in, out_grad, branch, bias, own, others, sums, s, lengths, S):
    count = len(others)
    order = [0, 1, 1] + list(range(2, len(lengths)))

    def kernel(s_ref, block_ref, out_ref, branch_ref, bias_ref, own_ref, sums_ref, *refs):
        block_out, in_grad, *smalls = refs[count:]
        wide = block_ref[...].astype(F32)
        block_out[...] = (wide + branch_ref[...] + bias_ref[...]).astype(BF16)
        offsets = wide - jnp.mean(wide, axis=-1, keepdims=True)
        inverse = lax.rsqrt(jnp.mean(offsets * offsets, axis=-1, keepdims=True) + epsilon)
        normed = offsets * inverse
        scaled = own_ref[...]
        for ref in refs[:count]:
            scaled = scaled + ref[...].astype(F32)
        term = inverse * (
            scaled
            - jnp.mean(scaled, axis=-1, keepdims=True)
            - normed * jnp.mean(scaled * normed, axis=-1, keepdims=True)
        )
        in_grad[...] = (out_ref[...].astype(F32) + term).astype(BF16)
        for ref, i in zip(smalls, order):
            n = lengths[i] // S
            ref[...] = sums_ref[pl.ds(sum(lengths[:i]) + s_ref[0] * n, n), :]

    outs = [jax.ShapeDtypeStruct(block_in.shape, BF16)] * 2
    outs += [jax.ShapeDtypeStruct((lengths[i] // S, 128), F32) for i in order]
    vmem_spec = pl.BlockSpec(memory_space=pltpu.VMEM)
    return pl.pallas_call(
        kernel,
        in_specs=[pl.BlockSpec(memory_space=pltpu.SMEM)] + [vmem_spec] * (6 + count),
        out_specs=[vmem_spec] * len(outs),
        out_shape=outs,
        cost_estimate=pl.CostEstimate(flops=0, bytes_accessed=8 * 2**20, transcendentals=0),
        name="finish",
    )(s.reshape(1), block_in, out_grad, branch, bias, own, sums, *others)


def unwritten(shape, dtype):
    return pl.pallas_call(
        lambda out_ref: None,
        out_shape=jax.ShapeDtypeStruct(shape, dtype),
        out_specs=pl.BlockSpec(memory_space=pl.ANY),
    )()


def bits_of(mask):
    return [1 << i for i in range(mask.bit_length()) if mask >> i & 1]


def layer(block_in, out_grad, small, freqs, w_up, w_qkv, w_down, w_out, S, TP, DP):
    T, D = block_in.shape
    rows, FS = w_up.shape[0], w_down.shape[0]
    NT, ND = 2 ** len(TP), 2 ** len(DP)
    FD, AD = FS // NT, w_out.shape[0] // NT
    heads = AD // HD
    scale = HD ** (-0.5)
    part = rows // ND
    third = w_qkv.shape[1] // 3
    tile = NT * T
    per = third * 3 // S // 128
    rest = D // S // 128
    base_out = 3 * third // 128
    base_up = base_out + D // 128
    base_norm = base_up + FS * S // 128
    count = base_norm + 4 * D // 128
    widths = [D, D, AD, FD, 3 * AD, FD, D, D]

    def kernel(
        small_ref, grad_ref, in_ref, up_ref, qkv_ref, down_ref, out_ref, freqs_ref,
        first_hbm, second_hbm, attended_hbm, activated_hbm, mixed_hbm, hidden_hbm, branch_hbm, inner_hbm, grad_hbm,
        small_all, sums_ref, bias_sum_ref,
        first_v, second_v, attended_v, activated_v, mixed_v, hidden_v, branch_v, inner_v,
        grad_all, in_all, up_all, qkv_all, down_all, out_all,
        wide_small, norms_ref, bias_ref, bias_up_ref, sum_qkv_ref, sum_up_ref, sum_norm_ref, sum_grad_ref,
        small_send, small_recv, line_send, line_recv, tp_send, tp_recv, z_send, z_recv, dp_send, dp_recv, local, leave,
    ):
        s = lax.axis_index("shard")
        r = lax.axis_index("replica")
        t = sum(((r // bit) % 2 * 2**i for i, bit in enumerate(TP)), jnp.int32(0))
        d = sum(((r // bit) % 2 * 2**i for i, bit in enumerate(DP)), jnp.int32(0))
        place = s * NT + t

        def flipped(value, mask):
            return sum((bit * (1 - 2 * ((value // bit) % 2)) for bit in bits_of(mask)), value)

        def other(k, m):
            mask = sum(bit for i, bit in enumerate(TP) if m >> i & 1)
            return {"shard": lax.rem(s + k, S), "replica": flipped(r, mask)}

        def mate(m):
            return {"replica": flipped(r, sum(bit for i, bit in enumerate(DP) if m >> i & 1))}

        group = [(k, m) for k in range(S) for m in range(NT) if k or m]
        plane = range(1, ND)
        gathered = (grad_all, in_all)
        mine = (grad_ref, in_ref)

        def columns(ref, at, n):
            return ref.at[:, pl.ds(pl.multiple_of(at, n), n)]

        here = pl.ds(pl.multiple_of(s * rows, rows), rows)
        copies = [
            pltpu.make_async_copy(small_ref, small_all.at[t, s], local.at[0]),
            pltpu.make_async_copy(grad_ref, grad_all.at[t, s], local.at[1]),
            pltpu.make_async_copy(in_ref, in_all.at[t, s], local.at[2]),
            pltpu.make_async_copy(columns(up_ref, place * FD, FD), up_all.at[here, :], local.at[3]),
            pltpu.make_async_copy(down_ref.at[pl.ds(pl.multiple_of(t * FD, FD), FD), :], down_all, local.at[4]),
            pltpu.make_async_copy(out_ref.at[pl.ds(pl.multiple_of(t * AD, AD), AD), :], out_all, local.at[5]),
        ]
        for j in range(3):
            source = columns(qkv_ref, j * third + place * AD, AD)
            copies.append(
                pltpu.make_async_copy(source, qkv_all.at[here, j * AD : (j + 1) * AD], local.at[6 + j])
            )
        for copy in copies:
            copy.start()

        barrier = pltpu.get_barrier_semaphore()
        for k, m in group:
            pl.semaphore_signal(barrier, inc=1, device_id=other(k, m), device_id_type=MESH)
        for m in plane:
            pl.semaphore_signal(barrier, inc=1, device_id=mate(m), device_id_type=MESH)
        pl.semaphore_wait(barrier, len(group) + len(plane))

        def small_copy(k, m):
            return pltpu.make_async_remote_copy(
                src_ref=small_ref, dst_ref=small_all.at[t, s], send_sem=small_send.at[k, m],
                recv_sem=small_recv.at[k, m], device_id=other(k, m), device_id_type=MESH,
            )

        def line(i, j, way, source):
            return pltpu.make_async_remote_copy(
                src_ref=source, dst_ref=gathered[i].at[t, j], send_sem=line_send.at[i, j, way],
                recv_sem=line_recv.at[i, j], device_id={"shard": s + 2 * way - 1}, device_id_type=MESH,
            )

        def across(i, j, m, source):
            slot = gathered[i].at[t, j]
            return pltpu.make_async_remote_copy(
                src_ref=slot if source is None else source, dst_ref=slot, send_sem=tp_send.at[i, j, m],
                recv_sem=tp_recv.at[i, j, m], device_id=other(0, m), device_id_type=MESH,
            )

        def z_copies(w, k, sending):
            to = lax.rem(s + k, S)
            at = (s if sending else lax.rem(s + S - k, S)) * rows + d * part
            at = pl.ds(pl.multiple_of(at, part), part)
            source_rows = pl.ds(pl.multiple_of(d * part, part), part)
            out = []
            for j in range(1 if w == 0 else 3):
                if w == 0:
                    source = up_ref.at[source_rows, pl.ds(pl.multiple_of((to * NT + t) * FD, FD), FD)]
                    target = up_all.at[at, :]
                else:
                    col = pl.multiple_of(j * third + (to * NT + t) * AD, AD)
                    source = qkv_ref.at[source_rows, pl.ds(col, AD)]
                    target = qkv_all.at[at, j * AD : (j + 1) * AD]
                out.append(
                    pltpu.make_async_remote_copy(
                        src_ref=source, dst_ref=target, send_sem=z_send.at[k, w + j], recv_sem=z_recv.at[k, w + j],
                        device_id={"shard": to}, device_id_type=MESH,
                    )
                )
            return out

        def shared(w, k, m):
            at = pl.multiple_of(lax.rem(s + S - k, S) * rows + d * part, part)
            slot = (up_all, qkv_all)[w].at[pl.ds(at, part), :]
            return pltpu.make_async_remote_copy(
                src_ref=slot, dst_ref=slot, send_sem=dp_send.at[w, k, m], recv_sem=dp_recv.at[w, k, m],
                device_id=mate(m), device_id_type=MESH,
            )

        for k, m in group:
            small_copy(k, m).start()
        for w in range(2):
            for k in range(1, S):
                for copy in z_copies(w, k, True):
                    copy.start()
        for i in range(2):

            @pl.when(s + 1 < S)
            def _():
                line(i, s, 1, mine[i]).start()

            @pl.when(s > 0)
            def _():
                line(i, s, 0, mine[i]).start()

            for m in range(1, NT):
                across(i, s, m, mine[i]).start()

        for ref in (sum_qkv_ref, sum_up_ref, sum_norm_ref, sum_grad_ref):
            ref[...] = jnp.zeros_like(ref)
        for w in range(2):
            for k in range(1, S):
                for copy in z_copies(w, k, False):
                    copy.wait_recv()
                for m in plane:
                    shared(w, k, m).start()
        for k, m in group:
            small_copy(k, m).wait_recv()
        for copy in copies:
            copy.wait()

        wide_small[...] = small_all[0].astype(F32)
        for v in range(4):
            for j in range(S):
                for i in range(rest):
                    at = (j * rest + i) * 128
                    row = per + (2 + v) * rest + i
                    norms_ref[v : v + 1, at : at + 128] = wide_small[j, row : row + 1, :]
        for j in range(S):
            for i in range(rest):
                at = (j * rest + i) * 128
                row = per + i
                bias_sum_ref[0:1, at : at + 128] = (
                    wide_small[j, row : row + 1, :] + wide_small[j, row + rest : row + rest + 1, :]
                )
        for v in range(3):
            for i in range(AD // 128):
                flat = v * (third // 128) + place * (AD // 128) + i
                at = v * AD + i * 128
                bias_ref[0:1, at : at + 128] = wide_small[flat // per, pl.ds(flat % per, 1), :]
        for i in range(FD // 128):
            row = per + 6 * rest + t * (FD // 128) + i
            bias_up_ref[0:1, i * 128 : (i + 1) * 128] = wide_small[s, pl.ds(row, 1), :]

        def from_line(i, j, way):
            line(i, j, way, gathered[i].at[t, j]).wait_recv()

            @pl.when((s + 1 < S) if way else (s > 0))
            def _():
                line(i, j, way, gathered[i].at[t, j]).start()

            for m in range(1, NT):
                across(i, j, m, None).start()

        def advance(k):
            for i in range(2):

                @pl.when(s - k >= 0)
                def _():
                    from_line(i, s - k, 1)

                @pl.when(s + k < S)
                def _():
                    from_line(i, s + k, 0)

        least = jnp.where(s < S - 1 - s, s, S - 1 - s)

        def block_at(i):
            both = jnp.where(i % 2 == 1, s - (i + 1) // 2, s + i // 2)
            one = jnp.where(s < S - 1 - s, i, S - 1 - i)
            return jnp.where(i <= 2 * least, both, one)

        row = lax.broadcasted_iota(jnp.int32, (T, T), 0)
        col = lax.broadcasted_iota(jnp.int32, (T, T), 1)
        away = (row - col).astype(F32)
        lane = lax.broadcasted_iota(jnp.int32, (T, 128), 1)

        def turn(value, table, sign):
            straight, ahead, back = table
            low = value[:, :128]
            low = low * straight + sign * (
                pltpu.roll(low, 128 - ROT // 2, 1) * ahead + pltpu.roll(low, ROT // 2, 1) * back
            )
            return jnp.concatenate([low, value[:, 128:]], axis=1)

        leaving = (
            (first_v, first_hbm), (second_v, second_hbm), (attended_v, attended_hbm), (activated_v, activated_hbm),
            (mixed_v, mixed_hbm), (hidden_v, hidden_hbm), (branch_v, branch_hbm), (inner_v, inner_hbm),
            (grad_all, grad_hbm),
        )

        def depart(v, u, j):
            source, target = leaving[v]
            return pltpu.make_async_copy(source.at[u, j], target.at[u, j], leave.at[v, u, j])

        def compute(i, carry):
            j = block_at(i)

            @pl.when(i == 0)
            def _():
                advance(1)
                for k in range(1, S):
                    for m in plane:
                        shared(0, k, m).wait_recv()

            @pl.when(i == 1)
            def _():
                advance(2)

            @pl.when(i >= 3)
            def _():
                advance(i)

            for m in range(1, NT):
                for v in range(2):
                    across(v, j, m, None).wait_recv()

            def join(ref):
                return jnp.concatenate([ref[u, j] for u in range(NT)], axis=0)

            def put(v, value):
                for u in range(NT):
                    leaving[v][0][u, j] = value[u * T : (u + 1) * T]

            def leave_now(*arrays):
                for v in arrays:
                    for u in range(NT):
                        depart(v, u, j).start()

            gain_1, shift_1, gain_2, shift_2 = [norms_ref[v : v + 1, :] for v in range(4)]
            wide = join(in_all).astype(F32)
            offsets = wide - jnp.mean(wide, axis=-1, keepdims=True)
            inverse = lax.rsqrt(jnp.mean(offsets * offsets, axis=-1, keepdims=True) + epsilon)
            normed = offsets * inverse
            first = (normed * gain_1 + shift_1).astype(BF16)
            second = (normed * gain_2 + shift_2).astype(BF16)
            put(0, first)
            put(1, second)
            leave_now(8)
            grad = join(grad_all)
            sum_grad_ref[...] += jnp.sum(grad.astype(F32), axis=0, keepdims=True)

            pre = dot(second, up_all[...], 1, 0) + bias_up_ref[...]
            bell = 0.5 * (1.0 + lax.erf(pre * 0.7071067811865476))
            activated = (pre * bell).astype(BF16)
            put(3, activated)
            slope = bell + pre * jnp.exp(-0.5 * pre * pre) * 0.3989422804014327
            hidden_grad = dot(grad, down_all[...], 1, 1) * slope
            sum_up_ref[...] += jnp.sum(hidden_grad, axis=0, keepdims=True)
            hidden_low = hidden_grad.astype(BF16)
            put(5, hidden_low)
            leave_now(0, 1, 3)

            @pl.when(i == 0)
            def _():
                for k in range(1, S):
                    for m in plane:
                        shared(1, k, m).wait_recv()

            mixed = dot(first, qkv_all[...], 1, 0) + bias_ref[...]
            attended_grad = dot(grad, out_all[...], 1, 1).astype(BF16)
            attended_parts, mixed_parts = [], []
            for u in range(NT):
                flat = small_all[u, j, -1:, :].astype(F32)
                position = jnp.sum(jnp.where(row == col, flat, 0.0), axis=1, keepdims=True)
                angle = position * freqs_ref[...]
                sine = jnp.sin(angle)
                table = (
                    jnp.cos(angle),
                    jnp.where(lane < ROT // 2, -sine, 0.0),
                    jnp.where((lane >= ROT // 2) & (lane < ROT), sine, 0.0),
                )
                allowed = (away >= 0) & (away <= position)
                at_rows = slice(u * T, (u + 1) * T)
                outs, q_grads, k_grads, v_grads = [], [], [], []
                for h in range(heads):
                    at = slice(h * HD, (h + 1) * HD)
                    ag = attended_grad[at_rows, at]
                    q = turn(mixed[at_rows, at], table, 1.0).astype(BF16)
                    k = turn(mixed[at_rows, AD + h * HD : AD + (h + 1) * HD], table, 1.0).astype(BF16)
                    v = mixed[at_rows, 2 * AD + h * HD : 2 * AD + (h + 1) * HD].astype(BF16)
                    scores = jnp.where(allowed, dot(q, k, 1, 1) * scale, -1e30)
                    peak = jnp.max(scores, axis=-1, keepdims=True)
                    logsum = peak + jnp.log(jnp.sum(jnp.exp(scores - peak), axis=-1, keepdims=True))
                    probs = jnp.exp(scores - logsum)
                    low = probs.astype(BF16)
                    outs.append(dot(low, v, 1, 0).astype(BF16))
                    dprobs = dot(ag, v, 1, 1)
                    total = jnp.sum(probs * dprobs, axis=-1, keepdims=True)
                    dscores = (probs * (dprobs - total) * scale).astype(BF16)
                    q_grads.append(turn(dot(dscores, k, 1, 0), table, -1.0))
                    k_grads.append(turn(dot(dscores, q, 0, 0), table, -1.0))
                    v_grads.append(dot(low, ag, 0, 0))
                attended_parts.append(jnp.concatenate(outs, axis=1))
                mixed_parts.append(jnp.concatenate(q_grads + k_grads + v_grads, axis=1))
            attended = jnp.concatenate(attended_parts, axis=0)
            put(2, attended)
            mixed_grad = jnp.concatenate(mixed_parts, axis=0)
            sum_qkv_ref[...] += jnp.sum(mixed_grad, axis=0, keepdims=True)
            mixed_low = mixed_grad.astype(BF16)
            put(4, mixed_low)

            branch = dot(attended, out_all[...], 1, 0) + dot(activated, down_all[...], 1, 0)
            put(6, branch.astype(BF16))
            leave_now(2, 4, 5)
            first_grad = dot(mixed_low, qkv_all[...], 1, 1)
            second_grad = dot(hidden_low, up_all[...], 1, 1)
            sum_norm_ref[0:1, :] += jnp.sum(first_grad * normed, axis=0, keepdims=True)
            sum_norm_ref[1:2, :] += jnp.sum(first_grad, axis=0, keepdims=True)
            sum_norm_ref[2:3, :] += jnp.sum(second_grad * normed, axis=0, keepdims=True)
            sum_norm_ref[3:4, :] += jnp.sum(second_grad, axis=0, keepdims=True)
            put(7, (first_grad * gain_1 + second_grad * gain_2).astype(BF16))
            leave_now(6, 7)
            return carry

        lax.fori_loop(0, S, compute, 0)

        sums_ref[...] = jnp.zeros_like(sums_ref)
        n = AD // 128
        for v in range(3):
            for i in range(n):
                at = v * AD + i * 128
                sums_ref[pl.ds(v * (third // 128) + place * n + i, 1), :] = sum_qkv_ref[:, at : at + 128]
        for i in range(FD // 128):
            sums_ref[pl.ds(base_up + place * (FD // 128) + i, 1), :] = sum_up_ref[:, i * 128 : (i + 1) * 128]
        for i in range(D // 128):
            at = slice(i * 128, (i + 1) * 128)
            sums_ref[base_out + i : base_out + i + 1, :] = sum_grad_ref[:, at] * (1.0 / (S * NT))
            for v in range(4):
                at_row = base_norm + v * (D // 128) + i
                sums_ref[at_row : at_row + 1, :] = sum_norm_ref[v : v + 1, at]

        for i in range(2):
            for j in range(S):

                @pl.when((s + 1 < S) & (j <= s))
                def _():
                    line(i, j, 1, gathered[i].at[t, j]).wait_send()

                @pl.when((s > 0) & (j >= s))
                def _():
                    line(i, j, 0, gathered[i].at[t, j]).wait_send()

                for m in range(1, NT):
                    across(i, j, m, None).wait_send()
        for k, m in group:
            small_copy(k, m).wait_send()
        for w in range(2):
            for k in range(1, S):
                for copy in z_copies(w, k, True):
                    copy.wait_send()
                for m in plane:
                    shared(w, k, m).wait_send()
        for v in range(len(leaving)):
            for u in range(NT):
                for j in range(S):
                    depart(v, u, j).wait()

    any_spec = pl.BlockSpec(memory_space=pl.ANY)
    vmem_spec = pl.BlockSpec(memory_space=pltpu.VMEM)
    outs = [jax.ShapeDtypeStruct((NT, S, T, w), BF16) for w in widths + [D]]
    outs += [jax.ShapeDtypeStruct((NT, S) + small.shape, BF16), jax.ShapeDtypeStruct((count, 128), F32)]
    outs += [jax.ShapeDtypeStruct((1, D), F32)]
    flops = 2 * S * tile * D * (2 * 3 * AD + 2 * FD + 2 * FD + 2 * AD)
    return pl.pallas_call(
        kernel,
        out_shape=outs,
        in_specs=[any_spec] * 7 + [vmem_spec],
        out_specs=[any_spec] * 9 + [vmem_spec] * 3,
        scratch_shapes=[pltpu.VMEM((NT, S, T, w), BF16) for w in widths]
        + [
            pltpu.VMEM((NT, S, T, D), BF16),
            pltpu.VMEM((NT, S, T, D), BF16),
            pltpu.VMEM((D, FD), BF16),
            pltpu.VMEM((D, 3 * AD), BF16),
            pltpu.VMEM((FD, D), BF16),
            pltpu.VMEM((AD, D), BF16),
            pltpu.VMEM((S,) + small.shape, F32),
            pltpu.VMEM((4, D), F32),
            pltpu.VMEM((1, 3 * AD), F32),
            pltpu.VMEM((1, FD), F32),
            pltpu.VMEM((1, 3 * AD), F32),
            pltpu.VMEM((1, FD), F32),
            pltpu.VMEM((4, D), F32),
            pltpu.VMEM((1, D), F32),
            pltpu.SemaphoreType.DMA((S, NT)),
            pltpu.SemaphoreType.DMA((S, NT)),
            pltpu.SemaphoreType.DMA((2, S, 2)),
            pltpu.SemaphoreType.DMA((2, S)),
            pltpu.SemaphoreType.DMA((2, S, NT)),
            pltpu.SemaphoreType.DMA((2, S, NT)),
            pltpu.SemaphoreType.DMA((S, 4)),
            pltpu.SemaphoreType.DMA((S, 4)),
            pltpu.SemaphoreType.DMA((2, S, ND)),
            pltpu.SemaphoreType.DMA((2, S, ND)),
            pltpu.SemaphoreType.DMA((9,)),
            pltpu.SemaphoreType.DMA((9, NT, S)),
        ],
        compiler_params=pltpu.CompilerParams(
            collective_id=0, has_side_effects=True, vmem_limit_bytes=67043328
        ),
        cost_estimate=pl.CostEstimate(flops=flops, bytes_accessed=80 * 2**20, transcendentals=S * tile * FD * 2),
        name="layer",
    )(small, out_grad, block_in, w_up, w_qkv, w_down, w_out, freqs)


def grads(
    first, second, attended, activated, mixed, hidden, grad, branch, inner, sums, S, R, T, TP, DP
):
    N, D = grad.shape
    NT, ND, steps = 2 ** len(TP), 2 ** len(DP), len(DP)
    lefts = (second, first, activated, attended)
    rights = (hidden, mixed, grad, grad)
    pieces = []
    for left, right, lead, mid in zip(lefts, rights, (S, S, 1, 1), (NT, NT, 1, 1)):
        pieces.append((lead, mid, left.shape[1] // (lead * ND * mid * 2), right.shape[1]))
    ways = []
    for way in (DP, DP[::-1]):
        ways.append([(bit, 1 << DP.index(bit)) for bit in way])

    def masks(bits):
        out = [0]
        for _, bit in bits:
            out += [v | bit for v in out]
        return sorted(out)

    slots = []
    for way in ways:
        table = {}
        for j in range(steps):
            for u in masks(way[j + 1 :]):
                table[j, u] = len(table)
        slots.append(table)

    def kernel(
        second_hbm, first_hbm, activated_hbm, attended_hbm, hidden_hbm, mixed_hbm, grad_hbm, branch_hbm, inner_hbm, sums_hbm,
        whole_up, whole_out, own_down_0, own_down_1, own_qkv_0, own_qkv_1, branch_own, inner_own, *more,
    ):
        inner_rest, sums_out = more[: S - 1], more[S - 1]
        mates = [more[S + 4 * m : S + 4 * m + 4] for m in range(NT - 1)]
        (
            own_up, own_out, near, near_came, far_came, held, held_came,
            second_v, first_v, activated_v, attended_v, hidden_v, mixed_v, grad_v,
            part_up, part_qkv, part_down, part_out, came_up, came_qkv, came_down, came_out, all_up, all_qkv,
            load, dp_send, dp_recv, z_send, z_recv, near_send, near_recv, far_send, far_recv, held_send, held_recv,
            plane_send, plane_recv, mate_send, mate_recv,
        ) = more[S + 4 * (NT - 1) :]
        s = lax.axis_index("shard")
        r = lax.axis_index("replica")
        t = sum(((r // bit) % 2 * 2**i for i, bit in enumerate(TP)), jnp.int32(0))
        d = sum(((r // bit) % 2 * 2**i for i, bit in enumerate(DP)), jnp.int32(0))

        def flipped(value, mask):
            return sum((bit * (1 - 2 * ((value // bit) % 2)) for bit in bits_of(mask)), value)

        def other(k, m):
            mask = sum(bit for i, bit in enumerate(TP) if m >> i & 1)
            return {"shard": lax.rem(s + k, S), "replica": flipped(r, mask)}

        loads = []
        order = ((hidden_hbm, hidden_v), (second_hbm, second_v), (mixed_hbm, mixed_v), (first_hbm, first_v),
                 (grad_hbm, grad_v), (activated_hbm, activated_v), (attended_hbm, attended_v))
        parts_hbm = (branch_hbm, inner_hbm)
        for i, (source, target) in enumerate(order):
            loads.append(pltpu.make_async_copy(source, target, load.at[i]))
        token_loads = [
            pltpu.make_async_copy(parts_hbm[i].at[t], near.at[i], load.at[7 + i]) for i in range(2)
        ]
        held_load = pltpu.make_async_copy(sums_hbm, held.at[0], load.at[9])
        for copy in (loads[6], loads[4], *loads[:2], held_load, *token_loads, *loads[2:4], loads[5]):
            copy.start()

        group = [(k, m) for k in range(S) for m in range(NT) if k or m]
        barrier = pltpu.get_barrier_semaphore()
        for k, m in group:
            pl.semaphore_signal(barrier, inc=1, device_id=other(k, m), device_id_type=MESH)
        for bit in DP:
            pl.semaphore_signal(barrier, inc=1, device_id={"replica": flipped(r, bit)}, device_id_type=MESH)
        pl.semaphore_wait(barrier, len(group) + steps)

        left_refs = (second_v, first_v, activated_v, attended_v)
        right_refs = (hidden_v, mixed_v, grad_v, grad_v)
        part = (part_up, part_qkv, part_down, part_out)
        came = (came_up, came_qkv, came_down, came_out)
        own = (own_up, (own_qkv_0, own_qkv_1), (own_down_0, own_down_1), own_out)

        def product(i):
            lead, mid, n, _ = pieces[i]
            if lead > 1:
                width = ND * mid * 2 * n

                def body(l, carry):
                    cols = pl.ds(pl.multiple_of(l * width, width), width)
                    value = dot(left_refs[i][:, cols], right_refs[i][...], 0, 0).astype(BF16)
                    for q in range(ND):
                        for c in range(mid):
                            for h in range(2):
                                at = ((q * mid + c) * 2 + h) * n
                                part[i][h, q, l, c] = value[at : at + n]
                    return carry

                lax.fori_loop(0, lead, body, 0)
            else:
                total = ND * 2 * n
                chunk = min(total, 512)
                per = chunk // (2 * n)

                def body(l, carry):
                    cols = pl.ds(pl.multiple_of(l * chunk, chunk), chunk)
                    value = dot(left_refs[i][:, cols], right_refs[i][...], 0, 0).astype(BF16)
                    for q in range(per):
                        for h in range(2):
                            at = (q * 2 + h) * n
                            part[i][h, l * per + q, 0, 0] = value[at : at + n]
                    return carry

                lax.fori_loop(0, total // chunk, body, 0)

        def halving(i, h, j, u):
            bit, dbit = ways[h][j]
            slot = slots[h][j, u]
            return pltpu.make_async_remote_copy(
                src_ref=part[i].at[h, flipped(d, dbit | u)], dst_ref=came[i].at[h, slot],
                send_sem=dp_send.at[i, h, slot], recv_sem=dp_recv.at[i, h, slot],
                device_id={"replica": flipped(r, bit)}, device_id_type=MESH,
            )

        def summed(i, h, mask, count, write):
            lead, mid, _, _ = pieces[i]
            at = flipped(d, mask)
            for j in range(count):
                halving(i, h, j, mask).wait_recv()

            def body(l, carry):
                for c in range(mid):
                    value = part[i][h, at, l, c].astype(F32)
                    for j in range(count):
                        value = value + came[i][h, slots[h][j, mask], l, c].astype(F32)
                    write(l, c, value.astype(BF16))
                return carry

            lax.fori_loop(0, lead, body, 0)

        def step(i, j):
            for h in range(2):
                for u in masks(ways[h][j + 1 :]):
                    mask = ways[h][j][1] | u
                    at = flipped(d, mask)
                    if j:

                        def write(l, c, value, h=h, at=at):
                            part[i][h, at, l, c] = value

                        summed(i, h, mask, j, write)
                    halving(i, h, j, u).start()

        everyone = (all_up, all_qkv)

        def to_shard(i, h, k, m):
            there = lax.rem(s + k, S)
            return pltpu.make_async_remote_copy(
                src_ref=part[i].at[h, d, there, flipped(t, m)], dst_ref=everyone[i].at[s, t, h],
                send_sem=z_send.at[i, h, k, m], recv_sem=z_recv.at[i, h, k, m],
                device_id=other(k, m), device_id_type=MESH,
            )

        def last(i):
            for h in range(2):
                if i < 2:

                    def write(l, c, value, h=h):
                        part[i][h, d, l, c] = value

                else:

                    def write(l, c, value, h=h):
                        if i == 2:
                            own[i][h][...] = value
                        else:
                            own[i][h] = value

                summed(i, h, 0, steps, write)
            if i < 2:
                for k, m in group:
                    for h in range(2):
                        to_shard(i, h, k, m).start()
                for h in range(2):
                    everyone[i][s, t, h] = part[i][h, d, s, t]

        def collect(i):
            width = pieces[i][3]
            runs = 1 if i == 0 else 3
            n = width // runs
            for k, m in group:
                for h in range(2):
                    to_shard(i, h, k, m).wait_recv()
            for h in range(2):
                for j in range(S):
                    for u in range(NT):
                        block = everyone[i][j, u, h]
                        for v in range(runs):
                            at = (v * S * NT + j * NT + u) * n
                            target = own[i][h] if i == 1 else own[i].at[h]
                            target[:, at : at + n] = block[:, v * n : (v + 1) * n]

        def near_copy(i, m):
            return pltpu.make_async_remote_copy(
                src_ref=parts_hbm[i].at[flipped(t, m)], dst_ref=near_came.at[i, m - 1],
                send_sem=near_send.at[i, m], recv_sem=near_recv.at[i, m], device_id=other(0, m), device_id_type=MESH,
            )

        def far_copy(k):
            there = lax.rem(s + k, S)
            return pltpu.make_async_remote_copy(
                src_ref=near.at[0, there] if NT > 1 else branch_hbm.at[t, there], dst_ref=far_came.at[k - 1],
                send_sem=far_send.at[k], recv_sem=far_recv.at[k], device_id=other(k, 0), device_id_type=MESH,
            )

        def near_sum(i, j):
            value = near[i, j].astype(F32)
            for m in range(1, NT):
                value = value + near_came[i, m - 1, j].astype(F32)
            return value

        def near_wait(i):
            token_loads[i].wait()
            for m in range(1, NT):
                near_copy(i, m).wait_recv()

        def branch_near():
            near_wait(0)

            def body(k, carry):
                j = lax.rem(s + k, S)
                near[0, j] = near_sum(0, j).astype(BF16)
                return carry

            if NT > 1:
                lax.fori_loop(1, S, body, 0)
            for k in range(1, S):
                far_copy(k).start()

        def branch_far():
            value = near_sum(0, s)
            for k in range(1, S):
                far_copy(k).wait_recv()
                value = value + far_came[k - 1].astype(F32)
            branch_own[...] = value

        def inner_near():
            near_wait(1)
            inner_own[...] = near_sum(1, s)
            for k in range(1, S):
                inner_rest[k - 1][...] = near_sum(1, lax.rem(s + k, S)).astype(BF16)

        bits = [(0, bit) for bit in bits_of(R - 1)] + [(1, bit) for bit in bits_of(S - 1)]

        def double(i):
            axis, bit = bits[i]
            to = {"replica": flipped(r, bit)} if axis == 0 else {"shard": flipped(s, bit)}
            return pltpu.make_async_remote_copy(
                src_ref=held.at[i], dst_ref=held_came.at[i], send_sem=held_send.at[i], recv_sem=held_recv.at[i],
                device_id=to, device_id_type=MESH,
            )

        def doubled(i):
            double(i).wait_recv()
            value = held[i] + held_came[i]
            if i + 1 < len(bits):
                held[i + 1] = value
                double(i + 1).start()
            else:
                sums_out[...] = value

        wholes = {0: whole_up, 3: whole_out}
        order_of = {0: 0, 3: 1}

        def slot_of(i, h, dd, tt):
            n = pieces[i][2]
            if i == 0:
                at = (dd * NT + tt) * 2 * n + h * n
            else:
                at = tt * (ND * 2 * n) + dd * 2 * n + h * n
            return wholes[i].at[pl.ds(pl.multiple_of(at, n), n), :]

        def gather(i, h, m, b):
            dmask = sum(ways[h][v][1] for v in range(steps) if m >> v & 1)
            tmask = m >> steps
            slot = slot_of(i, h, flipped(d, dmask), flipped(t, tmask))
            bit = ways[h][b][0] if b < steps else TP[b - steps]
            return pltpu.make_async_remote_copy(
                src_ref=own[i].at[h] if m == 0 else slot, dst_ref=slot,
                send_sem=plane_send.at[order_of[i], h, m | 1 << b], recv_sem=plane_recv.at[order_of[i], h, m | 1 << b],
                device_id={"replica": flipped(r, bit)}, device_id_type=MESH,
            )

        positions = steps + len(TP)

        def keep_own(i, h):
            return pltpu.make_async_copy(own[i].at[h], slot_of(i, h, d, t), load.at[10 + order_of[i] * 2 + h])

        def share_own(i):
            for h in range(2):
                for b in range(positions):
                    gather(i, h, 0, b).start()
                keep_own(i, h).start()

        def share_on(i, m):
            top = m.bit_length() - 1
            for h in range(2):
                gather(i, h, m ^ 1 << top, top).wait_recv()
                for b in range(top + 1, positions):
                    gather(i, h, m, b).start()

        def to_mate(i, h, m):
            at = (2 - i) * 2 + h
            return pltpu.make_async_remote_copy(
                src_ref=own[i][h], dst_ref=mates[m - 1][at], send_sem=mate_send.at[at, m], recv_sem=mate_recv.at[at, m],
                device_id=other(0, m), device_id_type=MESH,
            )

        def to_mates(i):
            for h in range(2):
                for m in range(1, NT):
                    to_mate(i, h, m).start()

        for i in range(2):
            for m in range(1, NT):
                near_copy(i, m).start()
        held_load.wait()
        double(0).start()
        loads[4].wait()
        loads[6].wait()
        product(3)
        step(3, 0)
        loads[0].wait()
        loads[1].wait()
        product(0)
        step(0, 0)
        branch_near()
        doubled(0)
        loads[2].wait()
        loads[3].wait()
        product(1)
        step(1, 0)
        for j in range(1, steps):
            step(0, j)
        doubled(1)
        loads[5].wait()
        product(2)
        step(2, 0)
        for j in range(1, steps):
            step(1, j)
        last(0)
        for i in range(2, len(bits)):
            doubled(i)
        for j in range(1, steps):
            step(2, j)
        last(1)
        for j in range(1, steps):
            step(3, j)
        collect(0)
        share_own(0)
        last(2)
        to_mates(2)
        last(3)
        share_own(3)
        for m in range(1, 1 << steps):
            for i in (0, 3):
                share_on(i, m)
            if m == 1:
                collect(1)
                to_mates(1)
                branch_far()
                inner_near()
        for m in range(1 << steps, 1 << positions):
            for i in (0, 3):
                share_on(i, m)

        for i in (1, 2):
            for h in range(2):
                for m in range(1, NT):
                    to_mate(i, h, m).wait()
        for i in (3, 0):
            for h in range(2):
                keep_own(i, h).wait()
                for m in range(1 << positions):
                    for b in range(m.bit_length(), positions):
                        gather(i, h, m, b).wait_send()
        for i in range(2):
            for m in range(1, NT):
                near_copy(i, m).wait_send()
        for k in range(1, S):
            far_copy(k).wait_send()
        for i in range(len(bits)):
            double(i).wait_send()
        for i in range(4):
            for h in range(2):
                for j, u in slots[h]:
                    halving(i, h, j, u).wait_send()
        for i in range(2):
            for h in range(2):
                for k, m in group:
                    to_shard(i, h, k, m).wait_send()

    def scratch(value):
        return pltpu.VMEM(value.shape, BF16)

    any_spec = pl.BlockSpec(memory_space=pl.ANY)
    vmem_spec = pl.BlockSpec(memory_space=pltpu.VMEM)
    operands = (second, first, activated, attended, hidden, mixed, grad)
    owns = [(2, n, width * S * NT if lead > 1 else width) for lead, _, n, width in pieces]
    wholes = [(2 * n * ND * NT, width) for _, n, width in owns]
    outs = [jax.ShapeDtypeStruct(wholes[i], BF16) for i in (0, 3)]
    owned = [jax.ShapeDtypeStruct(owns[i][1:], BF16) for i in (2, 2, 1, 1)]
    outs += owned + [jax.ShapeDtypeStruct((T, D), F32)] * 2 + [jax.ShapeDtypeStruct((T, D), BF16)] * (S - 1)
    outs += [jax.ShapeDtypeStruct(sums.shape, F32)] + owned * (NT - 1)
    sent = sum(2 * (ND - 1) * a * b * n * w * 2 for a, b, n, w in pieces)
    count = len(bits_of(R - 1)) + len(bits_of(S - 1))
    return pl.pallas_call(
        kernel,
        out_shape=outs,
        in_specs=[any_spec] * 10,
        out_specs=[any_spec] * 2 + [vmem_spec] * (7 + S - 1 + 4 * (NT - 1)),
        scratch_shapes=[pltpu.VMEM(owns[i], BF16) for i in (0, 3)]
        + [
            pltpu.VMEM((2, S, T, D), BF16),
            pltpu.VMEM((2, NT - 1, S, T, D) if NT > 1 else (1, 1, 1, 16, 128), BF16),
            pltpu.VMEM((S - 1, T, D), BF16),
            pltpu.VMEM((count,) + sums.shape, F32),
            pltpu.VMEM((count,) + sums.shape, F32),
        ]
        + [scratch(v) for v in operands]
        + [pltpu.VMEM((2, ND) + piece, BF16) for piece in pieces]
        + [pltpu.VMEM((2, ND - 1) + piece, BF16) for piece in pieces]
        + [pltpu.VMEM((S, NT, 2) + piece[2:], BF16) for piece in pieces[:2]]
        + [
            pltpu.SemaphoreType.DMA((18,)),
            pltpu.SemaphoreType.DMA((4, 2, ND - 1)),
            pltpu.SemaphoreType.DMA((4, 2, ND - 1)),
            pltpu.SemaphoreType.DMA((2, 2, S, NT)),
            pltpu.SemaphoreType.DMA((2, 2, S, NT)),
            pltpu.SemaphoreType.DMA((2, NT)),
            pltpu.SemaphoreType.DMA((2, NT)),
            pltpu.SemaphoreType.DMA((S,)),
            pltpu.SemaphoreType.DMA((S,)),
            pltpu.SemaphoreType.DMA((count,)),
            pltpu.SemaphoreType.DMA((count,)),
            pltpu.SemaphoreType.DMA((2, 2, ND * NT)),
            pltpu.SemaphoreType.DMA((2, 2, ND * NT)),
            pltpu.SemaphoreType.DMA((4, NT)),
            pltpu.SemaphoreType.DMA((4, NT)),
        ],
        compiler_params=pltpu.CompilerParams(
            collective_id=1, has_side_effects=True, vmem_limit_bytes=67043328
        ),
        cost_estimate=pl.CostEstimate(
            flops=2 * N * sum(v.shape[1] * w.shape[1] for v, w in zip(lefts, rights)),
            bytes_accessed=sent * 8, transcendentals=0,
        ),
        name="grads",
    )(*operands, branch, inner, sums)


def solution(mesh):
    S = mesh.shape["shard"]
    R = mesh.shape["replica"]
    TP = [1] if R > 1 and H % (2 * S) == 0 else []
    DP = [bit for bit in bits_of(R - 1) if bit not in TP]
    NT = 2 ** len(TP)

    def flip(value, bit):
        return lax.ppermute(value, "replica", [(i, i ^ bit) for i in range(R)])

    def body(
        block_in, positions, out_grad, w_qkv, b_qkv, w_out, b_out, w_up, b_up, w_down, b_down,
        first_gain, first_shift, second_gain, second_shift,
    ):
        T, _ = block_in.shape
        FS = w_down.shape[0]
        FD = FS // NT
        s = lax.axis_index("shard")
        r = lax.axis_index("replica")
        mine = {bit: (r // bit) % 2 for bit in bits_of(R - 1)}
        t = sum((mine[bit] * 2**i for i, bit in enumerate(TP)), jnp.int32(0))

        vectors = [
            b_qkv, b_out, b_down, first_gain, first_shift, second_gain, second_shift, b_up, positions.astype(BF16)
        ]
        ends = [sum(v.shape[0] for v in vectors[: i + 1]) for i in range(len(vectors))]
        small = sum(lax.pad(v, jnp.zeros((), BF16), [(end - v.shape[0], ends[-1] - end, 0)]) for v, end in zip(vectors, ends))
        small = small.reshape(-1, 128)
        (
            first_low, second_low, attended, activated, mixed_low, hidden_low, branch_part, inner_part, grad_all,
            _, sums, bias,
        ) = layer(block_in, out_grad, small, rotary_freqs(), w_up, w_qkv, w_down, w_out, S, TP, DP)
        first_low, second_low, attended, activated, mixed_low, hidden_low, grad_all = [
            v.reshape(NT * S * T, -1)
            for v in (first_low, second_low, attended, activated, mixed_low, hidden_low, grad_all)
        ]
        d = sum((mine[bit] * 2**i for i, bit in enumerate(DP)), jnp.int32(0))

        whole_up, whole_out, *more = grads(
            first_low, second_low, attended, activated, mixed_low, hidden_low, grad_all, branch_part, inner_part,
            sums, S, R, T, TP, DP,
        )
        owned_rows, (branch_own, inner_own), inner_rest, sums = more[:4], more[4:6], more[6 : 5 + S], more[5 + S]
        mates = [more[6 + S + 4 * m : 10 + S + 4 * m] for m in range(NT - 1)]

        ways = [DP, DP[::-1]]

        def indices(m):
            dmask = sum(2**i for i, bit in enumerate(DP) if m & bit)
            tmask = sum(2**i for i, bit in enumerate(TP) if m & bit)
            return d ^ dmask, t ^ tmask

        def down_row(half, m, n):
            dd, tt = indices(m)
            return tt * FD + (dd * 2 + half) * n

        def qkv_row(half, m, n):
            dd, tt = indices(m)
            return ((dd * NT + tt) * 2 + half) * n

        several = [m for m in all_masks(DP) if m and m not in DP]
        keys = [
            (which, half, m | u)
            for which in range(2)
            for masks in ([0], DP, several)
            for u in all_masks(TP)
            for half in range(2)
            for m in masks
        ]
        row_table = jnp.stack(
            [(down_row, qkv_row)[w](half, m, owned_rows[2 * w].shape[0]) for w, half, m in keys]
        )

        def placed(result, which, pieces):
            first = keys.index((which,) + pieces[0][:2])
            for bit in TP:
                pieces = pieces + [
                    (half, m | bit, mates[0][2 * which + half] if m == 0 else flip(value, bit))
                    for half, m, value in pieces
                ]
            assert keys[first : first + len(pieces)] == [(which, half, m) for half, m, _ in pieces]
            return place([value for _, _, value in pieces], row_table, first, result)

        got = [[{0: owned_rows[2 * i + half]} for half in range(2)] for i in range(2)]

        def fetched(i, half, masks):
            for m in masks:
                bit = [b for b in ways[half] if m & b][-1]
                got[i][half][m] = flip(got[i][half][m ^ bit], bit)

        for masks in (DP, several):
            for i in range(2):
                for half in range(2):
                    fetched(i, half, masks)

        def pieces_of(i, masks):
            return [(half, m, got[i][half][m]) for half in range(2) for m in masks]

        scaled = []
        for k in range(1, S):
            scaled.append(lax.ppermute(inner_rest[k - 1], "shard", [(i, (i + k) % S) for i in range(S)]))
        grad_w_up = widen(whole_up)
        grad_w_out = widen(whole_out)
        grad_w_down = placed(unwritten(w_down.shape, F32), 0, pieces_of(0, [0]))
        grad_w_qkv = placed(unwritten(w_qkv.shape, F32), 1, pieces_of(1, [0]))
        grad_w_down = placed(grad_w_down, 0, pieces_of(0, DP))
        grad_w_qkv = placed(grad_w_qkv, 1, pieces_of(1, DP))
        bias, grad_w_qkv = lax.optimization_barrier((bias, grad_w_qkv))
        block_out, in_grad, *smalls = finish(
            block_in, out_grad, branch_own, bias, inner_own, scaled, sums, s,
            [v.shape[0] * S // 128 for v in (b_qkv, b_out, b_up) + (first_gain,) * 4], S,
        )
        if several:
            grad_w_down = placed(grad_w_down, 0, pieces_of(0, several))
            grad_w_qkv = placed(grad_w_qkv, 1, pieces_of(1, several))

        grad_b_qkv, grad_b_out, grad_b_down, grad_b_up, *norm_grads = [v.reshape(-1) for v in smalls]
        return (
            block_out, in_grad, grad_w_qkv, grad_b_qkv, grad_w_out, grad_b_out, grad_w_up, grad_b_up,
            grad_w_down, grad_b_down, *norm_grads,
        )

    rows2, row1, par2, par1 = P(("shard", "replica"), None), P(("shard", "replica")), P("shard", None), P("shard")
    return jax.shard_map(
        body,
        mesh=mesh,
        in_specs=(
            rows2, row1, rows2, par2, par1, par2, par1, par2, par1, par2, par1, par1, par1, par1, par1,
        ),
        out_specs=(
            rows2, rows2, par2, par1, par2, par1, par2, par1, par2, par1, par1, par1, par1, par1,
        ),
        check_vma=False,
    )
```
